128 devices in a mesh: sp: 4 (over x), dp: 32 (over z, y, core).
Axes of the slice: x: 4, y: 4, z: 4, core: 2. Of those that a mesh axis runs over, the one named last changes fastest.
Arguments:
- hidden_in: bfloat16 [65536, 768], P(('dp', 'sp'))
- cu_seqlens: int32 [32, 9], P('dp')
- pos_ids: int32 [65536], P(('dp', 'sp'))
- w_qkv: bfloat16 [2, 768, 2304], replicated
- w_attn_out: bfloat16 [2, 768, 768], replicated
- w_mlp_in: bfloat16 [2, 768, 6144], replicated
- w_mlp_out: bfloat16 [2, 3072, 768], replicated
- ln_attn: float32 [2, 768], replicated
- ln_mlp: float32 [2, 768], replicated
- d_out: bfloat16 [65536, 768], P(('dp', 'sp'))
Outputs:
- output 1: bfloat16 [65536, 768], P(('dp', 'sp'))
- output 2: bfloat16 [65536, 768], P(('dp', 'sp'))
- output 3: float32 [2, 768, 2304], replicated
- output 4: float32 [2, 768, 768], replicated
- output 5: float32 [2, 768, 6144], replicated
- output 6: float32 [2, 3072, 768], replicated
- output 7: float32 [2, 768], replicated
- output 8: float32 [2, 768], replicated
All inputs are finite; a program needn't handle non-finite values.
Results may differ from the reference program's by a relative error of at most 0.02.
Values are sent between devices in bfloat16 or wider.
A program may use at most 1 GiB of HBM per device.

```python
import jax
import jax.numpy as jnp
from jax import lax

SEQ_SHARDS = 4
DATA_GROUPS = 32
TOK_DEV = 512
D_MODEL = 768
N_HEADS = 12
HEAD_DIM = 64
FF_DIM = 3072
N_DOCS = 8
WINDOW_HALF = 64
THETA_GLOBAL = 160000
THETA_LOCAL = 10000
GROUP_TOKENS = SEQ_SHARDS * TOK_DEV
ALL_TOKENS = DATA_GROUPS * GROUP_TOKENS
QUERY_BLOCK = WINDOW_HALF
LN_EPS = 1e-5


def draw_bounds(cut_key):
    cut_points = jax.random.permutation(cut_key, GROUP_TOKENS - 1)[: N_DOCS - 1] + 1
    inner_cuts = jnp.sort(cut_points).astype(jnp.int32)
    return jnp.concatenate([jnp.zeros((1,), jnp.int32), inner_cuts, jnp.full((1,), GROUP_TOKENS, jnp.int32)])


def doc_index(bounds):
    token_idx = jnp.arange(GROUP_TOKENS)
    return jnp.sum((bounds[None, 1:N_DOCS] <= token_idx[:, None]).astype(jnp.int32), axis=1)


def positions_of(bounds):
    token_idx = jnp.arange(GROUP_TOKENS)
    return (token_idx - bounds[doc_index(bounds)]).astype(jnp.int32)


def setup_inputs(seed: int = 0) -> dict:
    key_list = jax.random.split(jax.random.key(seed), 10)
    bounds = jax.vmap(draw_bounds)(jax.random.split(key_list[0], DATA_GROUPS))
    pos_ids = jax.vmap(positions_of)(bounds).reshape(ALL_TOKENS)

    def weight(key_idx, shape, fan_in):
        return (jax.random.normal(key_list[key_idx], shape, jnp.float32) * fan_in ** -0.5).astype(jnp.bfloat16)

    return {
        'hidden_in': jax.random.normal(key_list[1], (ALL_TOKENS, D_MODEL), jnp.float32).astype(jnp.bfloat16),
        'cu_seqlens': bounds,
        'pos_ids': pos_ids,
        'w_qkv': weight(2, (2, D_MODEL, 3 * D_MODEL), D_MODEL),
        'w_attn_out': weight(3, (2, D_MODEL, D_MODEL), D_MODEL),
        'w_mlp_in': weight(4, (2, D_MODEL, 2 * FF_DIM), D_MODEL),
        'w_mlp_out': weight(5, (2, FF_DIM, D_MODEL), FF_DIM),
        'ln_attn': 1.0 + 0.25 * jax.random.normal(key_list[6], (2, D_MODEL), jnp.float32),
        'ln_mlp': 1.0 + 0.25 * jax.random.normal(key_list[7], (2, D_MODEL), jnp.float32),
        'd_out': jax.random.normal(key_list[8], (ALL_TOKENS, D_MODEL), jnp.float32).astype(jnp.bfloat16),
    }


def layer_norm(in_rows, gain_row):
    rows32 = in_rows.astype(jnp.float32)
    centered = rows32 - jnp.mean(rows32, axis=-1, keepdims=True)
    var_row = jnp.mean(centered * centered, axis=-1, keepdims=True)
    return (centered * lax.rsqrt(var_row + LN_EPS) * gain_row).astype(jnp.bfloat16)


def rope(head_rows, pos_grp, rope_base):
    half_dim = HEAD_DIM // 2
    inv_freq = rope_base ** (jnp.arange(half_dim).astype(jnp.float32) * (-2.0 / HEAD_DIM))
    angles = pos_grp.astype(jnp.float32)[:, None] * inv_freq[None, :]
    cos_tab = jnp.concatenate([jnp.cos(angles), jnp.cos(angles)], axis=-1)[:, None, :]
    sin_tab = jnp.concatenate([jnp.sin(angles), jnp.sin(angles)], axis=-1)[:, None, :]
    rows32 = head_rows.astype(jnp.float32)
    rotated = jnp.concatenate([-rows32[..., half_dim:], rows32[..., :half_dim]], axis=-1)
    return (rows32 * cos_tab + rotated * sin_tab).astype(jnp.bfloat16)


def attention(query_rows, key_rows, val_rows, doc_ids, windowed):
    n_tok = query_rows.shape[0]
    key_f = key_rows.astype(jnp.float32)
    val_f = val_rows.astype(jnp.float32)
    token_idx = jnp.arange(n_tok)

    def one_block(blk_start):
        q_blk = lax.dynamic_slice_in_dim(query_rows, blk_start, QUERY_BLOCK, 0).astype(jnp.float32)
        doc_blk = lax.dynamic_slice_in_dim(doc_ids, blk_start, QUERY_BLOCK, 0)
        scores = jnp.einsum('qhd,khd->hqk', q_blk, key_f) * (HEAD_DIM ** -0.5)
        allowed = doc_blk[:, None] == doc_ids[None, :]
        if windowed:
            q_idx = blk_start + jnp.arange(QUERY_BLOCK)
            allowed = allowed & (jnp.abs(q_idx[:, None] - token_idx[None, :]) <= WINDOW_HALF)
        scores = jnp.where(allowed[None], scores, -1e30)
        prob_bf = jax.nn.softmax(scores, axis=-1).astype(jnp.bfloat16)
        return jnp.einsum('hqk,khd->qhd', prob_bf.astype(jnp.float32), val_f).astype(jnp.bfloat16)

    starts = jnp.arange(n_tok // QUERY_BLOCK) * QUERY_BLOCK
    return lax.map(jax.checkpoint(one_block), starts).reshape(query_rows.shape)


def layer(x_rows, pos_grp, doc_ids, params, rope_base, windowed):
    w_qkv, w_proj, w_up, w_down, g_attn, g_mlp = params
    n_tok = x_rows.shape[0]
    h_attn = layer_norm(x_rows, g_attn)
    qkv_rows = jnp.dot(h_attn.astype(jnp.float32), w_qkv, preferred_element_type=jnp.float32).astype(jnp.bfloat16)
    qkv_rows = qkv_rows.reshape(n_tok, 3, N_HEADS, HEAD_DIM)
    query_rows = rope(qkv_rows[:, 0], pos_grp, rope_base)
    key_rows = rope(qkv_rows[:, 1], pos_grp, rope_base)
    att_rows = attention(query_rows, key_rows, qkv_rows[:, 2], doc_ids, windowed).reshape(n_tok, D_MODEL)
    x_mid = (x_rows.astype(jnp.float32) + jnp.dot(att_rows.astype(jnp.float32), w_proj, preferred_element_type=jnp.float32)).astype(jnp.bfloat16)
    h_mlp = layer_norm(x_mid, g_mlp)
    up_rows = jnp.dot(h_mlp.astype(jnp.float32), w_up, preferred_element_type=jnp.float32).astype(jnp.bfloat16)
    gate_in = up_rows.astype(jnp.float32)
    act_rows = (jax.nn.gelu(gate_in[:, :FF_DIM], approximate=False) * gate_in[:, FF_DIM:]).astype(jnp.bfloat16)
    return (x_mid.astype(jnp.float32) + jnp.dot(act_rows.astype(jnp.float32), w_down, preferred_element_type=jnp.float32)).astype(jnp.bfloat16)


def two_layers(x_rows, pos_grp, doc_ids, all_params):
    first_params = tuple(stack_w[0] for stack_w in all_params)
    second_params = tuple(stack_w[1] for stack_w in all_params)
    hidden = layer(x_rows, pos_grp, doc_ids, first_params, THETA_GLOBAL, False)
    return layer(hidden, pos_grp, doc_ids, second_params, THETA_LOCAL, True)


def reference(hidden_in, cu_seqlens, pos_ids, w_qkv, w_attn_out, w_mlp_in, w_mlp_out, ln_attn, ln_mlp, d_out):
    all_params = (w_qkv.astype(jnp.float32), w_attn_out.astype(jnp.float32), w_mlp_in.astype(jnp.float32), w_mlp_out.astype(jnp.float32), ln_attn, ln_mlp)
    x_groups = hidden_in.reshape(DATA_GROUPS, GROUP_TOKENS, D_MODEL)
    dy_groups = d_out.reshape(DATA_GROUPS, GROUP_TOKENS, D_MODEL)
    pos_groups = pos_ids.reshape(DATA_GROUPS, GROUP_TOKENS)

    def group_step(grad_sum, group_in):
        x_grp, dy_grp, pos_grp, cu_row = group_in
        doc_ids = doc_index(cu_row)

        def forward(x_rows, layer_params):
            return two_layers(x_rows, pos_grp, doc_ids, layer_params)

        y_grp, vjp_pull = jax.vjp(forward, x_grp, all_params)
        dx_grp, d_params = vjp_pull(dy_grp)
        grad_sum = jax.tree.map(jnp.add, grad_sum, d_params)
        return grad_sum, (y_grp, dx_grp)

    zero_grads = jax.tree.map(jnp.zeros_like, all_params)
    grads, (y_groups, dx_groups) = lax.scan(group_step, zero_grads, (x_groups, dy_groups, pos_groups, cu_seqlens))
    return (y_groups.reshape(ALL_TOKENS, D_MODEL), dx_groups.reshape(ALL_TOKENS, D_MODEL)) + tuple(grads)
```

```python
import functools
import math
import jax
import jax.numpy as jnp
from jax import lax
from jax.experimental import pallas as pl
from jax.experimental.pallas import tpu as pltpu
from jax.sharding import PartitionSpec as P

ZERO, ONE, TWO, THREE, FOUR = range(5)
SIX, TWELVE = 6, 12
HEAD = 64
HALF = 32
NHEAD = 12
DM = 768
FF = 3072
TOK = 512
GRP = 2048
WIN = 64
LANE = 128
EPS = 1e-5
NEG = -1e30
SCALE = 0.125
BASES = (160000.0, 10000.0)
F32 = jnp.float32
BF = jnp.bfloat16
QT = 256
FT = 512
NFT = FF // FT
QTILES = GRP // QT
MIB = 1024 * 1024
ALLTOK = (TOK, DM)
ANY = pl.BlockSpec(memory_space=pl.ANY)
DMA = pltpu.SemaphoreType.DMA
MESH = pl.DeviceIdType.MESH


def dot(a, b, ca, cb):
    return lax.dot_general(a, b, (((ca,), (cb,)), ((), ())), preferred_element_type=F32)


def mm(a, b):
    return dot(a, b, ONE, ZERO)


def mm_nt(a, b):
    return dot(a, b, ONE, ONE)


def mm_tn(a, b):
    return dot(a, b, ZERO, ZERO)


def call(body, grid, in_specs, out_specs, out_shape, scratch=(), prefetch=ZERO, flops=ZERO, nbytes=ZERO, name=None,
         cid=None, alias=None):
    extra = {} if cid is None else dict(collective_id=cid, has_side_effects=True)
    return pl.pallas_call(
        body,
        grid_spec=pltpu.PrefetchScalarGridSpec(
            num_scalar_prefetch=prefetch, grid=grid, in_specs=in_specs, out_specs=out_specs, scratch_shapes=scratch),
        out_shape=out_shape,
        input_output_aliases=alias or {},
        compiler_params=pltpu.CompilerParams(vmem_limit_bytes=60 * MIB, **extra),
        cost_estimate=pl.CostEstimate(flops=int(flops), bytes_accessed=int(nbytes), transcendentals=ZERO),
        name=name,
    )


def sds(shape, dtype):
    return jax.ShapeDtypeStruct(shape, dtype)


def spec(shape, *idx):
    idx = idx or (ZERO,) * len(shape)
    return pl.BlockSpec(shape, lambda *g: tuple(i(*g) if callable(i) else i for i in idx))


def step_of(s, *_):
    return s


def core_and_partner():
    dp = lax.axis_index('dp')
    core = lax.rem(dp, TWO)
    return core, {'dp': dp + ONE - TWO * core}


def meet_partner(partner):
    bar = pltpu.get_barrier_semaphore()
    pl.semaphore_signal(bar, inc=ONE, device_id=partner, device_id_type=MESH)
    pl.semaphore_wait(bar, ONE)


def to_partner(partner, src, dst, ssem, rsem):
    return pltpu.make_async_remote_copy(src_ref=src, dst_ref=dst, send_sem=ssem, recv_sem=rsem,
                                        device_id=partner, device_id_type=MESH)


def norm_parts(x_bf):
    rows = x_bf.astype(F32)
    cen = rows - jnp.mean(rows, axis=ONE, keepdims=True)
    var = jnp.mean(cen * cen, axis=ONE, keepdims=True)
    return cen, lax.rsqrt(var + EPS)


def norm_rows(x_bf, gain):
    cen, inv = norm_parts(x_bf)
    return (cen * inv * gain).astype(BF)


def norm_rows_grad(x_bf, gain, d_bf):
    cen, inv = norm_parts(x_bf)
    hat = cen * inv
    d_out = d_bf.astype(F32)
    g_gain = jnp.sum(d_out * hat, axis=ZERO, keepdims=True)
    d_hat = d_out * gain
    d_x = inv * (d_hat - jnp.mean(d_hat, axis=ONE, keepdims=True) - hat * jnp.mean(d_hat * hat, axis=ONE, keepdims=True))
    return d_x.astype(BF), g_gain


def add_bf(a, b):
    return (a.astype(F32) + b.astype(F32)).astype(BF)


PARTS = 9
ROPED = 6


def part_of(s, *_):
    return s // THREE


def slot_of(s, *_):
    return s % THREE


def head_rows(ref, head):
    return ref.at[head, ZERO, ZERO] if ref.shape[ZERO] == FOUR else ref.at[ZERO, ZERO, head]


def heads_spec(dest_major):
    if dest_major:
        return spec((FOUR, ONE, ONE, HEAD, TOK), ZERO, part_of, slot_of, ZERO, ZERO)
    return spec((ONE, ONE, FOUR, HEAD, TOK), part_of, slot_of, ZERO, ZERO, ZERO)


def weight_cols(layer, width, first=ZERO):
    return spec((None, DM, width), layer, ZERO, lambda s: first + s)


def qkv_fwd_body(x_ref, g_ref, w_ref, cos_ref, sin_ref, h_ref, out_ref, hr_ref, ssem, rsem):
    step = pl.program_id(ZERO)
    core, partner = core_and_partner()
    swap = to_partner(partner, h_ref, hr_ref, ssem, rsem)

    @pl.when(step == ZERO)
    def _():
        h_ref[...] = norm_rows(x_ref[...], g_ref[...])
        meet_partner(partner)
        swap.start()

    t_rows = mm(h_ref[...], w_ref[...]).astype(BF).astype(F32).T

    @pl.when(step < ROPED)
    def _():
        cos, sin = cos_ref[...], sin_ref[...]
        for head in range(FOUR):
            at = HEAD * head
            a, b = t_rows[at:at + HALF], t_rows[at + HALF:at + HEAD]
            out = head_rows(out_ref, head)
            out[:HALF] = (a * cos - b * sin).astype(BF)
            out[HALF:] = (b * cos + a * sin).astype(BF)

    @pl.when(step >= ROPED)
    def _():
        for head in range(FOUR):
            head_rows(out_ref, head)[...] = t_rows[HEAD * head:HEAD * head + HEAD].astype(BF)

    @pl.when(step == PARTS - ONE)
    def _():
        swap.wait()


def qkv_fwd(x, gain, w_qkv, layer, cos_t, sin_t, dest_major, cid):
    oshape = (FOUR, THREE, THREE, HEAD, TOK) if dest_major else (THREE, THREE, FOUR, HEAD, TOK)
    table = spec((HALF, TOK))
    return call(
        qkv_fwd_body, (PARTS,),
        [spec(ALLTOK), spec((ONE, DM)), weight_cols(layer, QT), table, table],
        [spec(ALLTOK), heads_spec(dest_major), ANY],
        [sds(ALLTOK, BF), sds(oshape, BF), sds(ALLTOK, BF)],
        scratch=[DMA, DMA],
        flops=TWO * TOK * DM * THREE * DM, nbytes=8 * MIB, name="qkv_fwd", cid=cid,
    )(x, gain, w_qkv, cos_t, sin_t)


def tile_src(i, *_):
    return i // TWO


def tile_side(i, *_):
    return i % TWO


Q_SPEC = spec((ONE, ONE, THREE, HEAD, QT), tile_src, ZERO, ZERO, ZERO, tile_side)
O_SPEC = spec((ONE, THREE, HEAD, QT), tile_src, ZERO, ZERO, tile_side)
ROW_SPEC = spec((ONE, QT), ZERO, step_of)
STAT_SPEC = spec((8, QT), ZERO, step_of)
GROUP_QKV = (FOUR, THREE, THREE, HEAD, TOK)


def kv_spec(part):
    return spec((FOUR, ONE, THREE, HEAD, TOK), ZERO, part, ZERO, ZERO, ZERO)


def key_tile(kt):
    return kt // TWO, pl.ds(pl.multiple_of((kt % TWO) * QT, QT), QT)


def attn0_fwd_body(lo_s, hi_s, q_ref, k_ref, v_ref, st_ref, en_ref, o_ref, lse_ref, m_s, l_s, acc_s):
    tile = pl.program_id(ZERO)
    m_s[...] = jnp.full(m_s.shape, NEG, F32)
    l_s[...] = jnp.zeros(l_s.shape, F32)
    acc_s[...] = jnp.zeros(acc_s.shape, F32)
    st, en = st_ref[...], en_ref[...]
    io = lax.broadcasted_iota(jnp.int32, (QT, QT), ZERO)
    q_t = [q_ref[ZERO, ZERO, h] * SCALE for h in range(THREE)]

    def body(kt, carry):
        base = kt * QT
        src, cols = key_tile(kt)
        ok = (io >= st - base) & (io < en - base)
        for h in range(THREE):
            row = slice(h, h + ONE)
            k_t = k_ref[src, ZERO, h, :, cols]
            v_t = v_ref[src, ZERO, h, :, cols]
            s = jnp.where(ok, mm_tn(k_t, q_t[h]), NEG)
            m_old = m_s[row]
            m_new = jnp.maximum(m_old, jnp.max(s, axis=ZERO, keepdims=True))
            p = jnp.exp(s - m_new)
            alpha = jnp.exp(m_old - m_new)
            l_s[row] = l_s[row] * alpha + jnp.sum(p, axis=ZERO, keepdims=True)
            acc_s[h] = acc_s[h] * alpha + mm(v_t, p.astype(BF))
            m_s[row] = m_new
        return carry

    lax.fori_loop(lo_s[tile], hi_s[tile], body, ZERO)
    for h in range(THREE):
        row = slice(h, h + ONE)
        o_ref[ZERO, h] = (acc_s[h] / l_s[row]).astype(BF)
        lse_ref[row] = m_s[row] + jnp.log(l_s[row])


def attn0_fwd(lo, hi, qkv, st, en):
    stat = pltpu.VMEM((8, QT), F32)
    return call(
        attn0_fwd_body, (QTILES,),
        [Q_SPEC, kv_spec(ONE), kv_spec(TWO), ROW_SPEC, ROW_SPEC],
        [O_SPEC, STAT_SPEC],
        [sds((FOUR, THREE, HEAD, TOK), BF), sds((8, GRP), F32)],
        scratch=[stat, stat, pltpu.VMEM((THREE, HEAD, QT), F32)],
        prefetch=TWO, flops=TWELVE * GRP * GRP * HEAD, nbytes=6 * MIB, name="attn0_fwd",
    )(lo, hi, qkv, qkv, qkv, st, en)


def attn0_bwd_body(lo_s, hi_s, q_ref, k_ref, v_ref, o_ref, do_ref, lse_ref, st_ref, en_ref, out_ref, dk_s, dv_s, dq_s):
    tile = pl.program_id(ZERO)

    @pl.when(tile == ZERO)
    def _():
        dk_s[...] = jnp.zeros(dk_s.shape, F32)
        dv_s[...] = jnp.zeros(dv_s.shape, F32)

    dq_s[...] = jnp.zeros(dq_s.shape, F32)
    st, en = st_ref[...], en_ref[...]
    io = lax.broadcasted_iota(jnp.int32, (QT, QT), ZERO)
    heads = range(THREE)
    q_t = [q_ref[ZERO, ZERO, h] * SCALE for h in heads]
    do_t = [do_ref[ZERO, h] for h in heads]
    delta = [jnp.sum(do_t[h].astype(F32) * o_ref[ZERO, h].astype(F32), axis=ZERO, keepdims=True) for h in heads]
    lse = [lse_ref[h:h + ONE] for h in heads]

    def body(kt, carry):
        base = kt * QT
        src, cols = key_tile(kt)
        ok = (io >= st - base) & (io < en - base)
        for h in heads:
            k_t = k_ref[src, ZERO, h, :, cols]
            v_t = v_ref[src, ZERO, h, :, cols]
            p = jnp.exp(jnp.where(ok, mm_tn(k_t, q_t[h]) - lse[h], NEG))
            ds = (p * (mm_tn(v_t, do_t[h]) - delta[h])).astype(BF)
            at = (src, h, slice(None), cols)
            dv_s[at] += mm_nt(do_t[h], p.astype(BF))
            dk_s[at] += mm_nt(q_t[h], ds)
            dq_s[h] += mm(k_t, ds)
        return carry

    lax.fori_loop(lo_s[tile], hi_s[tile], body, ZERO)
    src, cols = key_tile(tile)
    for h in heads:
        out_ref[src, ZERO, h, :, cols] = (dq_s[h] * SCALE).astype(BF)

    @pl.when(tile == QTILES - ONE)
    def _():
        for src in range(FOUR):
            for h in heads:
                out_ref[src, ONE, h] = dk_s[src, h].astype(BF)
                out_ref[src, TWO, h] = dv_s[src, h].astype(BF)


def attn0_bwd(lo, hi, qkv, o_t, do_t, lse, st, en):
    acc = pltpu.VMEM((FOUR, THREE, HEAD, TOK), F32)
    return call(
        attn0_bwd_body, (QTILES,),
        [Q_SPEC, kv_spec(ONE), kv_spec(TWO), O_SPEC, O_SPEC, STAT_SPEC, ROW_SPEC, ROW_SPEC],
        spec(GROUP_QKV), sds(GROUP_QKV, BF),
        scratch=[acc, acc, pltpu.VMEM((THREE, HEAD, QT), F32)],
        prefetch=TWO, flops=30 * GRP * GRP * HEAD, nbytes=TWELVE * MIB, name="attn0_bwd",
    )(lo, hi, qkv, qkv, qkv, o_t, do_t, lse, st, en)


NBLK = TOK // LANE
EXT = TOK + TWO * LANE


def own_head(part):
    return spec((ONE, HEAD, TOK), lambda n: NHEAD * part + n, ZERO, ZERO)


def halo_head(part):
    return spec((ONE, HEAD, LANE), lambda n: NHEAD * part + n, ZERO, ZERO)


def joined(left, mid, right):
    return jnp.concatenate([left[ZERO], mid[ZERO], right[ZERO]], axis=ONE)


def blocks(first, last):
    return slice(LANE * first, LANE * last)


def in_bounds(lo_ref, hi_ref, blk, first, last):
    io = lax.broadcasted_iota(jnp.int32, (LANE * (last - first), LANE), ZERO) + LANE * first
    cols = blocks(blk, blk + ONE)
    return (io >= lo_ref[:, cols]) & (io < hi_ref[:, cols])


def attn1_fwd_body(q_ref, k_ref, v_ref, kl_ref, vl_ref, kr_ref, vr_ref, lo_ref, hi_ref, o_ref, lse_ref):
    q_t = q_ref[ZERO] * SCALE
    k_t = joined(kl_ref, k_ref, kr_ref)
    v_t = joined(vl_ref, v_ref, vr_ref)
    for i in range(NBLK):
        cols, wide = blocks(i, i + ONE), blocks(i, i + THREE)
        s = jnp.where(in_bounds(lo_ref, hi_ref, i + ONE, i, i + THREE), mm_tn(k_t[:, wide], q_t[:, cols]), NEG)
        m = jnp.max(s, axis=ZERO, keepdims=True)
        e = jnp.exp(s - m)
        l = jnp.sum(e, axis=ZERO, keepdims=True)
        o_ref[ZERO, :, cols] = mm(v_t[:, wide], (e / l).astype(BF)).astype(BF)
        lse_ref[ZERO, :, cols] = m + jnp.log(l)


def attn1_fwd(qkv, left, right, lo, hi):
    bound = spec((ONE, EXT))
    return call(
        attn1_fwd_body, (NHEAD,),
        [own_head(ZERO), own_head(ONE), own_head(TWO), halo_head(ZERO), halo_head(ONE), halo_head(ZERO), halo_head(ONE),
         bound, bound],
        [own_head(ZERO), spec((ONE, ONE, TOK), step_of, ZERO, ZERO)],
        [sds((NHEAD, HEAD, TOK), BF), sds((NHEAD, ONE, TOK), F32)],
        flops=NHEAD * FOUR * TOK * EXT * HALF, nbytes=FOUR * MIB, name="attn1_fwd",
    )(qkv, qkv, qkv, left, left, right, right, lo, hi)


def attn1_bwd_body(q_ref, k_ref, v_ref, do_ref, kl_ref, vl_ref, kr_ref, vr_ref, ql_ref, dl_ref, qr_ref, dr_ref,
                   lse_ref, del_ref, lo_ref, hi_ref, out_ref):
    q_t = joined(ql_ref, q_ref, qr_ref) * SCALE
    do_t = joined(dl_ref, do_ref, dr_ref)
    k_t = joined(kl_ref, k_ref, kr_ref)
    v_t = joined(vl_ref, v_ref, vr_ref)
    last_own = NBLK + ONE
    dk = [jnp.zeros((HEAD, LANE), F32) for _ in range(last_own)]
    dv = [jnp.zeros((HEAD, LANE), F32) for _ in range(last_own)]
    for e in range(NBLK + TWO):
        mine = ONE <= e <= NBLK
        first = e - ONE if mine else max(e - ONE, ONE)
        last = e + TWO if mine else min(e + TWO, last_own)
        cols, wide = blocks(e, e + ONE), blocks(first, last)
        ok = in_bounds(lo_ref, hi_ref, e, first, last)
        p = jnp.exp(jnp.where(ok, mm_tn(k_t[:, wide], q_t[:, cols]) - lse_ref[ZERO, :, cols], NEG))
        ds = jnp.where(ok, p * (mm_tn(v_t[:, wide], do_t[:, cols]) - del_ref[ZERO, :, cols]), F32(ZERO)).astype(BF)
        p_bf = p.astype(BF)
        if mine:
            out_ref[ZERO, ZERO, :, blocks(e - ONE, e)] = (mm(k_t[:, wide], ds) * SCALE).astype(BF)
        for kb in range(max(first, ONE), min(last, last_own)):
            rows = blocks(kb - first, kb - first + ONE)
            dv[kb] += mm_nt(do_t[:, cols], p_bf[rows])
            dk[kb] += mm_nt(q_t[:, cols], ds[rows])
    for kb in range(ONE, last_own):
        out_ref[ONE, ZERO, :, blocks(kb - ONE, kb)] = dk[kb].astype(BF)
        out_ref[TWO, ZERO, :, blocks(kb - ONE, kb)] = dv[kb].astype(BF)


def attn1_bwd(qkv, do_t, left, right, dleft, dright, lse_x, del_x, lo, hi):
    stat = spec((ONE, ONE, EXT), step_of, ZERO, ZERO)
    bound = spec((ONE, EXT))
    pair = [halo_head(ZERO), halo_head(ONE)]
    return call(
        attn1_bwd_body, (NHEAD,),
        [own_head(ZERO), own_head(ONE), own_head(TWO), own_head(ZERO)] + pair * FOUR + [stat, stat, bound, bound],
        spec((THREE, ONE, HEAD, TOK), ZERO, step_of, ZERO, ZERO),
        sds((THREE, NHEAD, HEAD, TOK), BF),
        flops=NHEAD * 10 * TOK * EXT * HALF, nbytes=8 * MIB, name="attn1_bwd",
    )(qkv, qkv, qkv, do_t, left, left, right, right, dleft, dleft, dright, dright, lse_x, del_x, lo, hi)


RB = 256
ROWBLK = [slice(r, r + RB) for r in range(ZERO, TOK, RB)]
HALFT = NFT // TWO
SQRT_HALF = math.sqrt(SCALE * FOUR)
PDF_SCALE = SQRT_HALF / math.sqrt(math.pi)
UBLK = (TWO, TOK, FT)
U_SPEC = spec(UBLK, ZERO, ZERO, step_of)


def normal_cdf(a):
    return SQRT_HALF * SQRT_HALF * (ONE + lax.erf(a * SQRT_HALF))


def att_block(ref, n):
    return ref.at[n % FOUR, n // FOUR] if ref.shape[ZERO] == FOUR else ref.at[n]


def half_rows(ref, which):
    n = ref.shape[ZERO] // TWO
    return ref.at[pl.ds(pl.multiple_of(which * n, n), n)]


def mlp_fwd_body(x_ref, o_ref, wp_ref, g_ref, wa_ref, wb_ref, wo_ref, x1_ref, h_ref, u_ref, m_ref, y_ref, of_ref,
                 mr_ref, hr_ref, or_ref, acc, m_s, ssem, rsem):
    step = pl.program_id(ZERO)
    core, partner = core_and_partner()
    other = ONE - core

    def send(n, src, dst):
        return to_partner(partner, src, dst, ssem.at[n], rsem.at[n])

    small = [send(HALFT, h_ref, hr_ref), send(HALFT + ONE, half_rows(of_ref, other), or_ref)]

    @pl.when(step == ZERO)
    def _():
        for n in range(NHEAD):
            of_ref[HEAD * n:HEAD * n + HEAD, :] = att_block(o_ref, n)[...]
        x1 = (x_ref[...].astype(F32) + mm_tn(of_ref[...], wp_ref[...])).astype(BF)
        x1_ref[...] = x1
        h_ref[...] = norm_rows(x1, g_ref[...])
        acc[...] = x1.astype(F32)
        meet_partner(partner)
        for cp in small:
            cp.start()

    slot = lax.rem(step, HALFT)
    for rows in ROWBLK:
        ua = mm(h_ref[rows], wa_ref[...]).astype(BF)
        ub = mm(h_ref[rows], wb_ref[...]).astype(BF)
        u_ref[ZERO, rows] = ua
        u_ref[ONE, rows] = ub
        a = ua.astype(F32)
        m = ((a * normal_cdf(a)) * ub.astype(F32)).astype(BF)
        m_ref[rows] = m
        acc[rows] += mm(m, wo_ref[...])

    @pl.when(step // HALFT == other)
    def _():
        m_s[slot] = m_ref[...]
        send(slot, m_s.at[slot], mr_ref.at[slot]).start()

    @pl.when(step == NFT - ONE)
    def _():
        y_ref[...] = acc[...].astype(BF)
        for n in range(HALFT):
            send(n, m_s.at[n], mr_ref.at[n]).wait()
        for cp in small:
            cp.wait()


def proj_spec(layer):
    return spec((None, DM, DM), layer, ZERO, ZERO)


def out_weight(layer):
    return spec((None, FT, DM), layer, step_of, ZERO)


def mlp_fwd(x, o_t, w_proj, gain, w_in, w_out, layer, cid):
    half_m = (HALFT, TOK, FT)
    toks = sds(ALLTOK, BF)
    return call(
        mlp_fwd_body, (NFT,),
        [spec(ALLTOK), spec(o_t.shape), proj_spec(layer), spec((ONE, DM)),
         weight_cols(layer, FT), weight_cols(layer, FT, NFT), out_weight(layer)],
        [spec(ALLTOK), spec(ALLTOK), U_SPEC, spec((TOK, FT), ZERO, step_of), spec(ALLTOK), spec((DM, TOK)), ANY, ANY, ANY],
        [toks, toks, sds((TWO, TOK, FF), BF), sds((TOK, FF), BF), toks, sds((DM, TOK), BF),
         sds(half_m, BF), toks, sds((DM // TWO, TOK), BF)],
        scratch=[pltpu.VMEM(ALLTOK, F32), pltpu.VMEM(half_m, BF), DMA((HALFT + TWO,)), DMA((HALFT + TWO,))],
        flops=TWO * TOK * DM * (DM + THREE * FF), nbytes=26 * MIB, name="mlp_fwd", cid=cid,
    )(x, o_t, w_proj, gain, w_in, w_in, w_out)


STATS = 16


def mlp_bwd_body(dy_ref, x1_ref, g_ref, wa_ref, wb_ref, wo_ref, u_ref, wp_ref, of_ref,
                 du_ref, dmid_ref, gg_ref, dot_ref, del_ref, dur_ref, dyr_ref, dmr_ref, acc, du_s, ssem, rsem):
    step = pl.program_id(ZERO)
    core, partner = core_and_partner()

    def send(n, src, dst):
        return to_partner(partner, src, dst, ssem.at[n], rsem.at[n])

    def send_du(n):
        return send(n, du_s.at[n], dur_ref.at[:, pl.ds(pl.multiple_of(n * FT, FT), FT)])

    send_dy = send(NFT, dy_ref, dyr_ref)
    send_dmid = send(NFT + ONE, dmid_ref, dmr_ref)

    @pl.when(step == ZERO)
    def _():
        acc[...] = jnp.zeros(acc.shape, F32)
        meet_partner(partner)
        send_dy.start()

    for rows in ROWBLK:
        dm = mm_nt(dy_ref[rows], wo_ref[...]).astype(BF).astype(F32)
        a = u_ref[ZERO, rows].astype(F32)
        b = u_ref[ONE, rows].astype(F32)
        cdf = normal_cdf(a)
        pdf = jnp.exp(a * a * (SCALE * FOUR - ONE)) * PDF_SCALE
        db = (dm * (a * cdf)).astype(BF)
        da = (dm * b * (cdf + a * pdf)).astype(BF)
        du_ref[ZERO, rows] = da
        du_ref[ONE, rows] = db
        acc[rows] += mm_nt(da, wa_ref[...]) + mm_nt(db, wb_ref[...])

    du_s[step] = du_ref[ONE - core]
    send_du(step).start()

    @pl.when(step == NFT - ONE)
    def _():
        d_ln, gg = norm_rows_grad(x1_ref[...], g_ref[...], acc[...].astype(BF))
        gg_ref[...] = gg
        d_mid = add_bf(dy_ref[...], d_ln)
        dmid_ref[...] = d_mid
        send_dmid.start()
        d_att = mm_nt(wp_ref[...], d_mid).astype(BF)
        for n in range(NHEAD):
            rows = slice(HEAD * n, HEAD * n + HEAD)
            blk = d_att[rows]
            att_block(dot_ref, n)[...] = blk
            del_ref[n:n + ONE, :] = jnp.sum(blk.astype(F32) * of_ref[rows].astype(F32), axis=ZERO, keepdims=True)
        del_ref[NHEAD:, :] = jnp.zeros((STATS - NHEAD, TOK), F32)
        for n in range(NFT):
            send_du(n).wait()
        send_dy.wait()
        send_dmid.wait()


def mlp_bwd(dy, x1, gain, w_in, w_out, u, w_proj, o_flat, layer, oshape, cid):
    du_half = (NFT, TOK, FT)
    toks = sds(ALLTOK, BF)
    return call(
        mlp_bwd_body, (NFT,),
        [spec(ALLTOK), spec(ALLTOK), spec((ONE, DM)), weight_cols(layer, FT), weight_cols(layer, FT, NFT),
         out_weight(layer), U_SPEC, proj_spec(layer), spec((DM, TOK))],
        [U_SPEC, spec(ALLTOK), spec((ONE, DM)), spec(oshape), spec((STATS, TOK)), ANY, ANY, ANY],
        [sds((TWO, TOK, FF), BF), toks, sds((ONE, DM), F32), sds(oshape, BF), sds((STATS, TOK), F32),
         sds((TOK, FF), BF), toks, toks],
        scratch=[pltpu.VMEM(ALLTOK, F32), pltpu.VMEM(du_half, BF), DMA((NFT + TWO,)), DMA((NFT + TWO,))],
        flops=TWO * TOK * DM * (DM + THREE * FF), nbytes=30 * MIB, name="mlp_bwd", cid=cid,
    )(dy, x1, gain, w_in, w_in, w_out, u, w_proj, o_flat)


def qkv_bwd_body(d_ref, cos_ref, sin_ref, w_ref, x_ref, g_ref, dmid_ref, dt_ref, dx_ref, gg_ref, dtr_ref,
                 acc, dt_s, ssem, rsem):
    step = pl.program_id(ZERO)
    core, partner = core_and_partner()

    def send(n):
        return to_partner(partner, dt_s.at[n, ONE - core], dtr_ref.at[pl.ds(pl.multiple_of(n * LANE, LANE), LANE)],
                          ssem.at[n], rsem.at[n])

    @pl.when(step == ZERO)
    def _():
        acc[...] = jnp.zeros(acc.shape, F32)
        meet_partner(partner)

    def put(head, row, val):
        at = row + HEAD * (head % TWO)
        dt_s[step, head // TWO, at:at + val.shape[ZERO]] = val

    @pl.when(step < ROPED)
    def _():
        cos, sin = cos_ref[...], sin_ref[...]
        for head in range(FOUR):
            d_head = head_rows(d_ref, head)[...].astype(F32)
            da, db = d_head[:HALF], d_head[HALF:]
            put(head, ZERO, (da * cos + db * sin).astype(BF))
            put(head, HALF, (db * cos - da * sin).astype(BF))

    @pl.when(step >= ROPED)
    def _():
        for head in range(FOUR):
            put(head, ZERO, head_rows(d_ref, head)[...])

    send(step).start()
    dt = dt_s[step]
    dt_ref[...] = dt
    acc[...] += mm(w_ref[...], dt.reshape(QT, TOK))

    @pl.when(step == PARTS - ONE)
    def _():
        d_ln, gg = norm_rows_grad(x_ref[...], g_ref[...], acc[...].T.astype(BF))
        gg_ref[...] = gg
        dx_ref[...] = add_bf(dmid_ref[...], d_ln)
        for n in range(PARTS):
            send(n).wait()


def qkv_bwd(d_qkv, cos_t, sin_t, w_qkv, x, gain, d_mid, layer, dest_major, cid):
    table = spec((HALF, TOK))
    feats = PARTS * LANE
    return call(
        qkv_bwd_body, (PARTS,),
        [heads_spec(dest_major), table, table, weight_cols(layer, QT), spec(ALLTOK), spec((ONE, DM)), spec(ALLTOK)],
        [spec((TWO, LANE, TOK), ZERO, step_of, ZERO), spec(ALLTOK), spec((ONE, DM)), ANY],
        [sds((TWO, feats, TOK), BF), sds(ALLTOK, BF), sds((ONE, DM), F32), sds((feats, TOK), BF)],
        scratch=[pltpu.VMEM((DM, TOK), F32), pltpu.VMEM((PARTS, TWO, LANE, TOK), BF), DMA((PARTS,)), DMA((PARTS,))],
        flops=TWO * TOK * DM * THREE * DM, nbytes=10 * MIB, name="qkv_bwd", cid=cid,
    )(d_qkv, cos_t, sin_t, w_qkv, x, gain, d_mid)


DOWN = FF // TWO
UP = FF
PROJ = DM // TWO
QKV = PARTS * LANE
LAYER_ROWS = DOWN + UP + PROJ + QKV
ALLROWS = TWO * LAYER_ROWS
NDOWN = DOWN // RB
NK = DM // RB


def up_step(s):
    return jnp.maximum(s - NDOWN, ZERO)


def down_step(s):
    return jnp.minimum(s, NDOWN - ONE)


def grad_mlp_body(core_s, g_ref, ma, mb, dya, dyb, ha, hb, dua, dub, out_ref):
    step = pl.program_id(ZERO)

    @pl.when(step < NDOWN)
    def _():
        out_ref[...] = mm_tn(ma[...], dya[...]) + mm_tn(mb[...], dyb[...])

    @pl.when(step >= NDOWN)
    def _():
        out_ref[...] = mm_tn(ha[...], dua[...]) + mm_tn(hb[...], dub[...])


def grad_call(body, core, grads, steps, in_specs, args, rows, first):
    shared = [] if grads is None else [grads]
    return call(
        body, (steps,), [ANY] * len(shared) + in_specs,
        spec((rows, DM), lambda s, c: first + s, ZERO), sds((ALLROWS, DM), F32),
        prefetch=ONE, flops=FOUR * steps * rows * TOK * DM, nbytes=20 * MIB, name=body.__name__,
        alias={ONE: ZERO} if shared else None,
    )(core, *shared, *args)


def grad_mlp_body(core_s, *refs):
    ma, mb, dya, dyb, ha, hb, dua, dub, out_ref = refs[-PARTS:]
    step = pl.program_id(ZERO)

    @pl.when(step < NDOWN)
    def _():
        out_ref[...] = mm_tn(ma[...], dya[...]) + mm_tn(mb[...], dyb[...])

    @pl.when(step >= NDOWN)
    def _():
        out_ref[...] = mm_tn(ha[...], dua[...]) + mm_tn(hb[...], dub[...])


def grad_mlp(core, grads, m, m_r, dy, dy_r, h, h_r, du, du_r, first_row):
    per_ft = FT // RB
    toks = spec(ALLTOK)
    hcol = spec((TOK, RB), ZERO, lambda s, c: up_step(s) % NK)
    col = lambda s, *_: up_step(s) // NK
    return grad_call(
        grad_mlp_body, core, grads, NDOWN + UP // RB,
        [spec((TOK, RB), ZERO, lambda s, c: NDOWN * c[ZERO] + down_step(s)),
         spec((None, TOK, RB), lambda s, c: down_step(s) // per_ft, ZERO, lambda s, c: down_step(s) % per_ft),
         toks, toks, hcol, hcol,
         spec((None, TOK, DM), lambda s, c: c[ZERO], ZERO, col), spec(ALLTOK, ZERO, col)],
        (m, m_r, dy, dy_r, h, h_r, du, du_r), RB, first_row // RB)


def grad_att_body(core_s, *refs):
    oa, ob, dma, dmb, ta, tb, ha, hb, out_ref = refs[-PARTS:]
    step = pl.program_id(ZERO)

    @pl.when(step == ZERO)
    def _():
        out_ref[...] = mm(oa[...], dma[...]) + mm(ob[...], dmb[...])

    @pl.when(step > ZERO)
    def _():
        out_ref[...] = mm(ta[...], ha[...]) + mm(tb[...], hb[...])


def grad_att(core, grads, of, of_r, dmid, dmid_r, dt, dt_r, h, h_r, first_row):
    toks = spec(ALLTOK)
    blk = (PROJ, TOK)
    qkv_step = lambda s, *_: jnp.maximum(s - ONE, ZERO)
    return grad_call(
        grad_att_body, core, grads, ONE + QKV // PROJ,
        [spec(blk, lambda s, c: c[ZERO], ZERO), spec(blk), toks, toks,
         spec((None,) + blk, lambda s, c: c[ZERO], qkv_step, ZERO), spec(blk, qkv_step, ZERO), toks, toks],
        (of, of_r, dmid, dmid_r, dt, dt_r, h, h_r), PROJ, (first_row + DOWN + UP) // PROJ)


NB, NS, CH, SB, LF = 4, 6, 128, 32, 8
RS = PARTS
LAST = RS + RS


def ring_body(g_ref, ln_ref, f_ref, lnout_ref, bufa, bufb, bufc, gath, stage, lnbuf,
              ssem, rsem, psem, qsem, csem, stsem, lns, lnr):
    core, partner = core_and_partner()
    dp = lax.axis_index('dp')
    pos = (lax.axis_index('sp'), lax.rem(dp // TWO, FOUR), dp // 8)
    streams = [(c, sg) for c in range(THREE) for sg in (ONE, -ONE)]
    bufs, sizes = (bufa, bufb, bufc), (CH, SB, LF)
    peers = range(ONE, FOUR)

    def mod4(v):
        return lax.rem(v + 8, FOUR)

    def at(axis, val):
        if axis == ZERO:
            return {'sp': val}
        yz = (val, pos[TWO]) if axis == ONE else (pos[ONE], val)
        return {'dp': yz[ONE] * 8 + yz[ZERO] * TWO + core}

    def shifted(axis, d):
        return at(axis, mod4(pos[axis] + d))

    def axis_of(s, ph):
        return (streams[s][ZERO] + ph) % THREE

    def idx(s, ph, t):
        return mod4(pos[axis_of(s, ph)] - streams[s][ONE] * t)

    def own(s, ph):
        return idx(s, ph, -ONE)

    def base(b, s):
        return (b * NS + s) * (FOUR * CH)

    bar = pltpu.get_barrier_semaphore()
    for ax in range(THREE):
        for d in peers:
            pl.semaphore_signal(bar, inc=ONE, device_id=shifted(ax, d), device_id_type=MESH)
    pl.semaphore_signal(bar, inc=ONE, device_id=partner, device_id_type=MESH)
    pl.semaphore_wait(bar, 10)

    def rows(ref, start, n):
        return ref.at[pl.ds(pl.multiple_of(start, LF), n)]

    def frows(start, n):
        return f_ref.at[core, pl.ds(pl.multiple_of(start, LF), n)]

    def same_bytes(b, k):
        if k < RS:
            return bufs[k // THREE].at[b, k % THREE]
        n = sizes[TWO - (k - RS) // THREE]
        return gath.at[b] if n == CH else gath.at[b, :, pl.ds(ZERO, n)]

    def wait_for(ref, sem):
        pltpu.make_async_copy(ref, ref, sem).wait()

    def send(b, s, k):
        ph = k // THREE if k < RS else TWO - (k - RS) // THREE
        t = k % THREE
        n = sizes[ph]
        if k < RS:
            dst = bufs[ph].at[b, t, s]
            if t:
                src = bufs[ph].at[b, t - ONE, s]
            elif ph:
                src = rows(bufs[ph - ONE].at[b, TWO, s], idx(s, ph, ZERO) * n, n)
            else:
                src = rows(g_ref, base(b, s) + idx(s, ZERO, ZERO) * n, n)
        elif ph:
            off = own(s, ONE) * SB if ph == TWO else ZERO
            src = dst = rows(gath.at[b, s], off + idx(s, ph, t - ONE) * n, n)
        else:
            dst = frows(base(b, s) + idx(s, ZERO, t - ONE) * n, n)
            src = dst if t else gath.at[b, s]
        pltpu.make_async_remote_copy(src_ref=src, dst_ref=dst, send_sem=ssem.at[b, k], recv_sem=rsem.at[b, k],
                                     device_id=shifted(axis_of(s, ph), streams[s][ONE]), device_id_type=MESH).start()

    def stage_load(n):
        t, b, slot = n // NB, lax.rem(n, NB), lax.rem(n, TWO)
        for s in range(NS):
            pltpu.make_async_copy(rows(g_ref, base(b, s) + idx(s, ZERO, t + ONE) * CH, CH), stage.at[slot, s],
                                  stsem.at[slot]).start()

    def ln_copy(ph, d):
        return pltpu.make_async_remote_copy(
            src_ref=lnbuf.at[ph, THREE] if ph else ln_ref, dst_ref=lnbuf.at[ph, d - ONE], send_sem=lns.at[ph, d - ONE],
            recv_sem=lnr.at[ph, d - ONE], device_id=shifted(ph, d) if ph < THREE else partner, device_id_type=MESH)

    def ln_sum(ph):
        vals = [lnbuf[ph, THREE] if ph else ln_ref[...]] + [lnbuf[ph, d - ONE] for d in peers]
        total = jnp.zeros_like(vals[ZERO])
        for p in range(FOUR):
            term = vals[ZERO]
            for d in peers:
                term = jnp.where(mod4(pos[ph] - d) == p, vals[d], term)
            total = total + term
        return total

    def batches(fn, start=ZERO):
        def body(b, c):
            fn(b)
            return c
        lax.fori_loop(start, NB, body, ZERO)

    def first(b):
        for s in range(NS):
            send(b, s, ZERO)

    first(ZERO)
    stage_load(jnp.int32(ZERO))
    for d in peers:
        ln_copy(ZERO, d).start()
    batches(first, ONE)

    for k in range(RS):
        ph, t = k // THREE, k % THREE
        buf, size = bufs[ph], sizes[ph]

        def step(b, k=k, ph=ph, t=t, buf=buf, size=size):
            n = k * NB + b
            slot = lax.rem(n, TWO)
            if not ph:
                @pl.when(n < THREE * NB - ONE)
                def _():
                    stage_load(n + ONE)
                wait_for(stage.at[slot], stsem.at[slot])
            wait_for(same_bytes(b, k), rsem.at[b, k])
            for s in range(NS):
                if ph:
                    off = pl.multiple_of(idx(s, ph, t + ONE) * size, LF)
                    buf[b, t, s] += bufs[ph - ONE][b, TWO, s, pl.ds(off, size)]
                else:
                    @pl.loop(ZERO, CH, step=SB)
                    def _(r):
                        at_r = pl.ds(pl.multiple_of(r, SB), SB)
                        buf[b, t, s, at_r] += stage[slot, s, at_r]
                if k == RS - ONE:
                    off = pl.multiple_of(own(s, ONE) * SB + own(s, TWO) * LF, LF)
                    gath[b, s, pl.ds(off, LF)] = bufc[b, TWO, s]
                send(b, s, k + ONE)

        batches(step)
        if k < SIX and k % TWO == ZERO:
            lp = k // TWO
            for d in peers:
                ln_copy(lp, d).wait()
            lnbuf[lp + ONE, THREE] = ln_sum(lp)
            for d in peers if lp < TWO else (ONE,):
                ln_copy(lp + ONE, d).start()

    def hand_over(b, s, j, src, start):
        pltpu.make_async_remote_copy(src_ref=src, dst_ref=frows(start, CH), send_sem=psem.at[b, j], recv_sem=qsem.at[b, j],
                                     device_id=partner, device_id_type=MESH).start()

    for k in range(RS, LAST):
        def step(b, k=k):
            wait_for(same_bytes(b, k), rsem.at[b, k])
            piece = k - (LAST - FOUR)
            for s in range(NS):
                if k < LAST - ONE:
                    send(b, s, k + ONE)
                if piece >= ZERO:
                    start = base(b, s) + idx(s, ZERO, piece - ONE) * CH
                    if piece:
                        hand_over(b, s, piece, frows(start, CH), start)
                    else:
                        pltpu.make_async_copy(gath.at[b, s], frows(start, CH), csem.at[b]).start()
                        hand_over(b, s, piece, gath.at[b, s], start)
        batches(step)

    ln_copy(THREE, ONE).wait()
    lnout_ref[...] = lnbuf[THREE, THREE] + lnbuf[THREE, ZERO]

    def finish(b):
        for k in range(LAST):
            wait_for(same_bytes(b, k), ssem.at[b, k])
        for j in range(FOUR):
            wait_for(gath.at[b], psem.at[b, j])
            wait_for(gath.at[b], qsem.at[b, j])
        wait_for(gath.at[b], csem.at[b])
    batches(finish)


def ring_all_reduce(g, ln, cid):
    vmem = pl.BlockSpec(memory_space=pltpu.VMEM)
    return pl.pallas_call(
        ring_body,
        in_specs=[ANY, vmem],
        out_specs=[ANY, vmem],
        out_shape=[sds((TWO, ALLROWS, DM), F32), sds(ln.shape, F32)],
        scratch_shapes=[
            pltpu.VMEM((NB, THREE, NS, CH, DM), F32), pltpu.VMEM((NB, THREE, NS, SB, DM), F32),
            pltpu.VMEM((NB, THREE, NS, LF, DM), F32), pltpu.VMEM((NB, NS, CH, DM), F32), pltpu.VMEM((TWO, NS, CH, DM), F32),
            pltpu.VMEM((FOUR, FOUR) + ln.shape, F32),
            DMA((NB, LAST)), DMA((NB, LAST)), DMA((NB, FOUR)), DMA((NB, FOUR)), DMA((NB,)), DMA((TWO,)),
            DMA((FOUR, THREE)), DMA((FOUR, THREE)),
        ],
        compiler_params=pltpu.CompilerParams(collective_id=cid, has_side_effects=True, vmem_limit_bytes=63 * MIB),
        name="ring_all_reduce",
    )(g, ln)


def copy_body(in_ref, out_ref):
    out_ref[...] = in_ref[...]


def turn_body(a_ref, b_ref, out_ref):
    out_ref[ZERO, :, :LANE] = a_ref[ZERO].T
    out_ref[ZERO, :, LANE:] = b_ref[ZERO].T


def unpack(f):
    def blk(rows, row0):
        return (ONE, rows, DM), (lambda l, *_: (ONE - l) * (LAYER_ROWS // rows) + row0 // rows)

    whole, at_layer = blk(DM, ZERO)
    core_of = lambda l, c, *_: c
    layer_of = lambda l, *_: l
    nbytes = 100 * MIB
    g_out = call(copy_body, (TWO, TWO, TWO),
                 [spec(whole, core_of, lambda l, c, i: at_layer(l) + i, ZERO)],
                 spec(whole, layer_of, lambda l, c, i: TWO * c + i, ZERO), sds((TWO, FF, DM), F32), nbytes=nbytes)(f)
    g_in = call(copy_body, (TWO, TWO, FOUR),
                [spec(whole, core_of, lambda l, c, j: at_layer(l) + TWO + j, ZERO)],
                spec(whole, layer_of, ZERO, lambda l, c, j: FOUR * c + j), sds((TWO, DM, TWO * FF), F32), nbytes=nbytes)(f)
    half, at_proj = blk(PROJ, DOWN + UP)
    g_proj = call(copy_body, (TWO, TWO), [spec(half, core_of, at_proj, ZERO)], spec(half, layer_of, core_of, ZERO),
                  sds((TWO, DM, DM), F32), nbytes=nbytes)(f)
    lane, at_qkv = blk(LANE, DOWN + UP + PROJ)
    row = lambda l, s: at_qkv(l) + s
    g_qkv = call(turn_body, (TWO, PARTS), [spec(lane, ZERO, row, ZERO), spec(lane, ONE, row, ZERO)],
                 spec((ONE, DM, QT), layer_of, ZERO, lambda l, s: s), sds((TWO, DM, THREE * DM), F32), nbytes=nbytes)(f, f)
    return g_qkv, g_proj, g_in, g_out


def rope_tables(pos, base):
    inv_freq = base ** (jnp.arange(HALF).astype(F32) * (-TWO / HEAD))
    angles = inv_freq[:, None] * pos.astype(F32)[None, :]
    return jnp.cos(angles), jnp.sin(angles)


def solution(mesh):
    token_spec = P(('dp', 'sp'), None)
    n_sp = mesh.shape['sp']
    to_right = [(i, i + ONE) for i in range(n_sp - ONE)]
    to_left = [(i + ONE, i) for i in range(n_sp - ONE)]
    cids = list(range(PARTS))

    def halo_swap(arr):
        from_left = lax.ppermute(arr[..., TOK - LANE:], 'sp', to_right)
        from_right = lax.ppermute(arr[..., :LANE], 'sp', to_left)
        return from_left, from_right

    def exchange(arr):
        return lax.all_to_all(arr, 'sp', ZERO, ZERO, tiled=True)

    def device_step(x_loc, cu_loc, pos_loc, w_qkv, w_proj, w_in, w_out, ln_attn, ln_mlp, d_out):
        sp = lax.axis_index('sp')
        core = (lax.axis_index('dp') % TWO).reshape(ONE)
        cu = cu_loc[ZERO][:, None]

        def bounds_of(tok):
            start = jnp.max(jnp.where(cu <= tok, cu, ZERO), axis=ZERO)
            return start, jnp.min(jnp.where(cu > tok, cu, GRP), axis=ZERO)

        start, stop = bounds_of(jnp.arange(GRP)[None, :])
        tiles = start[::QT] // QT, (stop[QT - ONE::QT] + QT - ONE) // QT
        rows = start[None, :], stop[None, :]
        shift = sp * TOK - LANE
        tok_x = jnp.arange(EXT) + shift
        start_x, stop_x = bounds_of(tok_x[None, :])
        inside = (tok_x >= ZERO) & (tok_x < GRP)
        near = (jnp.where(inside, jnp.maximum(start_x, tok_x - WIN) - shift, ZERO)[None, :],
                jnp.where(inside, jnp.minimum(stop_x, tok_x + WIN + ONE) - shift, ZERO)[None, :])
        tab0, tab1 = [rope_tables(pos_loc, base) for base in BASES]
        la0, la1, lm0, lm1 = ln_attn[:ONE], ln_attn[ONE:], ln_mlp[:ONE], ln_mlp[ONE:]
        per_head = (NHEAD, HEAD, TOK)

        h0, qkv0, h0r = qkv_fwd(x_loc, la0, w_qkv, ZERO, *tab0, True, cids[ONE])
        qkv0 = exchange(qkv0)
        oh0, lse0 = attn0_fwd(*tiles, qkv0, *rows)
        x01, h02, u0, m0, x1, of0, m0r, h02r, of0r = mlp_fwd(x_loc, exchange(oh0), w_proj, lm0, w_in, w_out, ZERO, cids[TWO])
        h1, qkv1, h1r = qkv_fwd(x1, la1, w_qkv, ONE, *tab1, False, cids[THREE])
        qkv1 = qkv1.reshape((THREE * NHEAD, HEAD, TOK))
        kv_halo = halo_swap(qkv1[NHEAD:])
        o1, lse1 = attn1_fwd(qkv1, *kv_halo, *near)
        x11, h12, u1, m1, y, of1, m1r, h12r, of1r = mlp_fwd(x1, o1, w_proj, lm1, w_in, w_out, ONE, cids[FOUR])
        du1, dmid1, ggm1, do1, del1, du1r, dy1r, dmid1r = mlp_bwd(
            d_out, x11, lm1, w_in, w_out, u1, w_proj, of1, ONE, per_head, cids[5])
        d_halo = halo_swap(jnp.concatenate([qkv1[:NHEAD], do1], axis=ZERO))
        stats = jnp.concatenate([lse1.reshape(NHEAD, TOK), del1[:NHEAD]], axis=ZERO)
        from_left, from_right = halo_swap(stats)
        lse_x, del_x = jnp.concatenate([from_left, stats, from_right], axis=ONE).reshape(TWO, NHEAD, ONE, EXT)
        dqkv1 = attn1_bwd(qkv1, do1, *kv_halo, *d_halo, lse_x, del_x, *near)
        dt1, dx1, gga1, dt1r = qkv_bwd(dqkv1.reshape(THREE, THREE, FOUR, HEAD, TOK), *tab1, w_qkv, x1, la1, dmid1,
                                       ONE, False, cids[SIX])
        grads = grad_mlp(core, None, m1, m1r, d_out, dy1r, h12, h12r, du1, du1r, ZERO)
        grads = grad_att(core, grads, of1, of1r, dmid1, dmid1r, dt1, dt1r, h1, h1r, ZERO)
        du0, dmid0, ggm0, do0, _, du0r, dy0r, dmid0r = mlp_bwd(
            dx1, x01, lm0, w_in, w_out, u0, w_proj, of0, ZERO, oh0.shape, cids[7])
        grads = grad_mlp(core, grads, m0, m0r, dx1, dy0r, h02, h02r, du0, du0r, LAYER_ROWS)
        dqkv0 = exchange(attn0_bwd(*tiles, qkv0, oh0, exchange(do0), lse0, *rows))
        dt0, dx0, gga0, dt0r = qkv_bwd(dqkv0, *tab0, w_qkv, x_loc, la0, dmid0, ZERO, True, cids[8])
        grads = grad_att(core, grads, of0, of0r, dmid0, dmid0r, dt0, dt0r, h0, h0r, LAYER_ROWS)

        gains = jnp.concatenate([gga0, gga1, ggm0, ggm1, jnp.zeros((FOUR, DM), F32)], axis=ZERO)
        summed, gains = ring_all_reduce(grads, gains, cids[ZERO])
        return (y, dx0) + unpack(summed) + (gains[:TWO], gains[TWO:FOUR])

    in_specs = (token_spec, P('dp', None), P(('dp', 'sp'))) + (P(),) * SIX + (token_spec,)
    out_specs = (token_spec, token_spec) + (P(),) * SIX
    return jax.shard_map(device_step, mesh=mesh, in_specs=in_specs, out_specs=out_specs, check_vma=False)
```

```python
import functools
import math
import jax
import jax.numpy as jnp
from jax import lax
from jax.experimental import pallas as pl
from jax.experimental.pallas import tpu as pltpu
from jax.sharding import PartitionSpec as P

ZERO, ONE, TWO, THREE, FOUR = range(5)
SIX, TWELVE = 6, 12
HEAD = 64
HALF = 32
NHEAD = 12
DM = 768
FF = 3072
TOK = 512
GRP = 2048
WIN = 64
LANE = 128
EPS = 1e-5
NEG = -1e30
SCALE = 0.125
BASES = (160000.0, 10000.0)
F32 = jnp.float32
BF = jnp.bfloat16
QT = 256
FT = 512
NFT = FF // FT
QTILES = GRP // QT
MIB = 1024 * 1024
ALLTOK = (TOK, DM)
PROJ = DM // 2
ANY = pl.BlockSpec(memory_space=pl.ANY)
DMA = pltpu.SemaphoreType.DMA
MESH = pl.DeviceIdType.MESH


def dot(a, b, ca, cb):
    return lax.dot_general(a, b, (((ca,), (cb,)), ((), ())), preferred_element_type=F32)


def mm(a, b):
    return dot(a, b, ONE, ZERO)


def mm_nt(a, b):
    return dot(a, b, ONE, ONE)


def mm_tn(a, b):
    return dot(a, b, ZERO, ZERO)


def call(body, grid, in_specs, out_specs, out_shape, scratch=(), prefetch=ZERO, flops=ZERO, nbytes=ZERO, name=None,
         cid=None, alias=None):
    extra = {} if cid is None else dict(collective_id=cid, has_side_effects=True)
    return pl.pallas_call(
        body,
        grid_spec=pltpu.PrefetchScalarGridSpec(
            num_scalar_prefetch=prefetch, grid=grid, in_specs=in_specs, out_specs=out_specs, scratch_shapes=scratch),
        out_shape=out_shape,
        input_output_aliases=alias or {},
        compiler_params=pltpu.CompilerParams(vmem_limit_bytes=60 * MIB, **extra),
        cost_estimate=pl.CostEstimate(flops=int(flops), bytes_accessed=int(nbytes), transcendentals=ZERO),
        name=name,
    )


def sds(shape, dtype):
    return jax.ShapeDtypeStruct(shape, dtype)


def spec(shape, *idx):
    idx = idx or (ZERO,) * len(shape)
    return pl.BlockSpec(shape, lambda *g: tuple(i(*g) if callable(i) else i for i in idx))


def step_of(s, *_):
    return s


def core_and_partner():
    dp = lax.axis_index('dp')
    core = lax.rem(dp, TWO)
    return core, {'dp': dp + ONE - TWO * core}


def meet_partner(partner):
    bar = pltpu.get_barrier_semaphore()
    pl.semaphore_signal(bar, inc=ONE, device_id=partner, device_id_type=MESH)
    pl.semaphore_wait(bar, ONE)


def to_partner(partner, src, dst, ssem, rsem):
    return pltpu.make_async_remote_copy(src_ref=src, dst_ref=dst, send_sem=ssem, recv_sem=rsem,
                                        device_id=partner, device_id_type=MESH)


def norm_parts(x_bf):
    rows = x_bf.astype(F32)
    cen = rows - jnp.mean(rows, axis=ONE, keepdims=True)
    var = jnp.mean(cen * cen, axis=ONE, keepdims=True)
    return cen, lax.rsqrt(var + EPS)


def norm_rows(x_bf, gain):
    cen, inv = norm_parts(x_bf)
    return (cen * inv * gain).astype(BF)


def norm_rows_grad(x_bf, gain, d_bf):
    cen, inv = norm_parts(x_bf)
    hat = cen * inv
    d_out = d_bf.astype(F32)
    g_gain = jnp.sum(d_out * hat, axis=ZERO, keepdims=True)
    d_hat = d_out * gain
    d_x = inv * (d_hat - jnp.mean(d_hat, axis=ONE, keepdims=True) - hat * jnp.mean(d_hat * hat, axis=ONE, keepdims=True))
    return d_x.astype(BF), g_gain


def add_bf(a, b):
    return (a.astype(F32) + b.astype(F32)).astype(BF)


RB = 256
CHUNKS = range(DM // RB)


def head_rows(ref, chunk, head):
    return ref.at[head, ZERO, chunk] if ref.shape[ZERO] == FOUR else ref.at[ZERO, chunk, head]


def heads_spec(dest_major):
    if dest_major:
        return spec((FOUR, ONE, THREE, HEAD, TOK), ZERO, step_of, ZERO, ZERO, ZERO)
    return spec((ONE, THREE, FOUR, HEAD, TOK), step_of, ZERO, ZERO, ZERO, ZERO)


def weight_cols(layer, width, first=ZERO):
    return spec((None, DM, width), layer, ZERO, lambda s: first + s)


def qkv_fwd_body(x_ref, g_ref, w_ref, cos_ref, sin_ref, h_ref, out_ref, hr_ref, ssem, rsem):
    step = pl.program_id(ZERO)
    core, partner = core_and_partner()
    swap = to_partner(partner, h_ref, hr_ref, ssem, rsem)

    @pl.when(step == ZERO)
    def _():
        h_ref[...] = norm_rows(x_ref[...], g_ref[...])
        meet_partner(partner)
        swap.start()

    def product(chunk):
        return mm(h_ref[...], w_ref[:, RB * chunk:RB * chunk + RB]).astype(BF).astype(F32).T

    @pl.when(step < TWO)
    def _():
        cos, sin = cos_ref[...], sin_ref[...]
        for chunk in CHUNKS:
            t_rows = product(chunk)
            for head in range(FOUR):
                at = HEAD * head
                a, b = t_rows[at:at + HALF], t_rows[at + HALF:at + HEAD]
                out = head_rows(out_ref, chunk, head)
                out[:HALF] = (a * cos - b * sin).astype(BF)
                out[HALF:] = (b * cos + a * sin).astype(BF)

    @pl.when(step == TWO)
    def _():
        for chunk in CHUNKS:
            t_rows = product(chunk).astype(BF)
            for head in range(FOUR):
                head_rows(out_ref, chunk, head)[...] = t_rows[HEAD * head:HEAD * head + HEAD]
        swap.wait()


def qkv_fwd(x, gain, w_qkv, layer, cos_t, sin_t, dest_major, cid):
    oshape = (FOUR, THREE, THREE, HEAD, TOK) if dest_major else (THREE, THREE, FOUR, HEAD, TOK)
    table = spec((HALF, TOK))
    return call(
        qkv_fwd_body, (THREE,),
        [spec(ALLTOK), spec((ONE, DM)), weight_cols(layer, DM), table, table],
        [spec(ALLTOK), heads_spec(dest_major), ANY],
        [sds(ALLTOK, BF), sds(oshape, BF), sds(ALLTOK, BF)],
        scratch=[DMA, DMA],
        flops=TWO * TOK * DM * THREE * DM, nbytes=8 * MIB, name="qkv_fwd", cid=cid,
    )(x, gain, w_qkv, cos_t, sin_t)


def tile_src(i, *_):
    return i // TWO


def tile_side(i, *_):
    return i % TWO


Q_SPEC = spec((ONE, ONE, THREE, HEAD, QT), tile_src, ZERO, ZERO, ZERO, tile_side)
O_SPEC = spec((ONE, THREE, HEAD, QT), tile_src, ZERO, ZERO, tile_side)
ROW_SPEC = spec((ONE, QT), ZERO, step_of)
STAT_SPEC = spec((8, QT), ZERO, step_of)
GROUP_QKV = (FOUR, THREE, THREE, HEAD, TOK)


def kv_spec(part):
    return spec((FOUR, ONE, THREE, HEAD, TOK), ZERO, part, ZERO, ZERO, ZERO)


def key_tile(kt):
    return kt // TWO, pl.ds(pl.multiple_of((kt % TWO) * QT, QT), QT)


def attn0_fwd_body(lo_s, hi_s, q_ref, k_ref, v_ref, st_ref, en_ref, o_ref, lse_ref, m_s, l_s, acc_s):
    tile = pl.program_id(ZERO)
    m_s[...] = jnp.full(m_s.shape, NEG, F32)
    l_s[...] = jnp.zeros(l_s.shape, F32)
    acc_s[...] = jnp.zeros(acc_s.shape, F32)
    st, en = st_ref[...], en_ref[...]
    io = lax.broadcasted_iota(jnp.int32, (QT, QT), ZERO)
    q_t = [q_ref[ZERO, ZERO, h] * SCALE for h in range(THREE)]

    def body(kt, carry):
        base = kt * QT
        src, cols = key_tile(kt)
        ok = (io >= st - base) & (io < en - base)
        for h in range(THREE):
            row = slice(h, h + ONE)
            k_t = k_ref[src, ZERO, h, :, cols]
            v_t = v_ref[src, ZERO, h, :, cols]
            s = jnp.where(ok, mm_tn(k_t, q_t[h]), NEG)
            m_old = m_s[row]
            m_new = jnp.maximum(m_old, jnp.max(s, axis=ZERO, keepdims=True))
            p = jnp.exp(s - m_new)
            alpha = jnp.exp(m_old - m_new)
            l_s[row] = l_s[row] * alpha + jnp.sum(p, axis=ZERO, keepdims=True)
            acc_s[h] = acc_s[h] * alpha + mm(v_t, p.astype(BF))
            m_s[row] = m_new
        return carry

    lax.fori_loop(lo_s[tile], hi_s[tile], body, ZERO)
    for h in range(THREE):
        row = slice(h, h + ONE)
        o_ref[ZERO, h] = (acc_s[h] / l_s[row]).astype(BF)
        lse_ref[row] = m_s[row] + jnp.log(l_s[row])


def attn0_fwd(lo, hi, qkv, st, en):
    stat = pltpu.VMEM((8, QT), F32)
    return call(
        attn0_fwd_body, (QTILES,),
        [Q_SPEC, kv_spec(ONE), kv_spec(TWO), ROW_SPEC, ROW_SPEC],
        [O_SPEC, STAT_SPEC],
        [sds((FOUR, THREE, HEAD, TOK), BF), sds((8, GRP), F32)],
        scratch=[stat, stat, pltpu.VMEM((THREE, HEAD, QT), F32)],
        prefetch=TWO, flops=TWELVE * GRP * GRP * HEAD, nbytes=6 * MIB, name="attn0_fwd",
    )(lo, hi, qkv, qkv, qkv, st, en)


def attn0_bwd_body(lo_s, hi_s, q_ref, k_ref, v_ref, o_ref, do_ref, lse_ref, st_ref, en_ref, out_ref, dk_s, dv_s, dq_s):
    tile = pl.program_id(ZERO)

    @pl.when(tile == ZERO)
    def _():
        dk_s[...] = jnp.zeros(dk_s.shape, F32)
        dv_s[...] = jnp.zeros(dv_s.shape, F32)

    dq_s[...] = jnp.zeros(dq_s.shape, F32)
    st, en = st_ref[...], en_ref[...]
    io = lax.broadcasted_iota(jnp.int32, (QT, QT), ZERO)
    heads = range(THREE)
    q_t = [q_ref[ZERO, ZERO, h] * SCALE for h in heads]
    do_t = [do_ref[ZERO, h] for h in heads]
    delta = [jnp.sum(do_t[h].astype(F32) * o_ref[ZERO, h].astype(F32), axis=ZERO, keepdims=True) for h in heads]
    lse = [lse_ref[h:h + ONE] for h in heads]

    def body(kt, carry):
        base = kt * QT
        src, cols = key_tile(kt)
        ok = (io >= st - base) & (io < en - base)
        for h in heads:
            k_t = k_ref[src, ZERO, h, :, cols]
            v_t = v_ref[src, ZERO, h, :, cols]
            p = jnp.exp(jnp.where(ok, mm_tn(k_t, q_t[h]) - lse[h], NEG))
            ds = (p * (mm_tn(v_t, do_t[h]) - delta[h])).astype(BF)
            at = (src, h, slice(None), cols)
            dv_s[at] += mm_nt(do_t[h], p.astype(BF))
            dk_s[at] += mm_nt(q_t[h], ds)
            dq_s[h] += mm(k_t, ds)
        return carry

    lax.fori_loop(lo_s[tile], hi_s[tile], body, ZERO)
    src, cols = key_tile(tile)
    for h in heads:
        out_ref[src, ZERO, h, :, cols] = (dq_s[h] * SCALE).astype(BF)

    @pl.when(tile == QTILES - ONE)
    def _():
        for src in range(FOUR):
            for h in heads:
                out_ref[src, ONE, h] = dk_s[src, h].astype(BF)
                out_ref[src, TWO, h] = dv_s[src, h].astype(BF)


def attn0_bwd(lo, hi, qkv, o_t, do_t, lse, st, en):
    acc = pltpu.VMEM((FOUR, THREE, HEAD, TOK), F32)
    return call(
        attn0_bwd_body, (QTILES,),
        [Q_SPEC, kv_spec(ONE), kv_spec(TWO), O_SPEC, O_SPEC, STAT_SPEC, ROW_SPEC, ROW_SPEC],
        spec(GROUP_QKV), sds(GROUP_QKV, BF),
        scratch=[acc, acc, pltpu.VMEM((THREE, HEAD, QT), F32)],
        prefetch=TWO, flops=30 * GRP * GRP * HEAD, nbytes=TWELVE * MIB, name="attn0_bwd",
    )(lo, hi, qkv, qkv, qkv, o_t, do_t, lse, st, en)


NBLK = TOK // LANE
EXT = TOK + TWO * LANE


HPS = 4
HSTEPS = NHEAD // HPS


def heads_of(width, part):
    return spec((HPS, HEAD, width), lambda n: HSTEPS * part + n, ZERO, ZERO)


def own_head(part):
    return heads_of(TOK, part)


def halo_head(part):
    return heads_of(LANE, part)


def joined(left, mid, right, h):
    return jnp.concatenate([left[h], mid[h], right[h]], axis=ONE)


def blocks(first, last):
    return slice(LANE * first, LANE * last)


def in_bounds(lo_ref, hi_ref, blk, first, last):
    io = lax.broadcasted_iota(jnp.int32, (LANE * (last - first), LANE), ZERO) + LANE * first
    cols = blocks(blk, blk + ONE)
    return (io >= lo_ref[:, cols]) & (io < hi_ref[:, cols])


def every_head(fn):
    def body(h, c):
        fn(h)
        return c
    lax.fori_loop(ZERO, HPS, body, ZERO)


def attn1_fwd_body(q_ref, k_ref, v_ref, kl_ref, vl_ref, kr_ref, vr_ref, lo_ref, hi_ref, o_ref, lse_ref):
    def head(h):
        q_t = q_ref[h] * SCALE
        k_rows = joined(kl_ref, k_ref, kr_ref, h).T
        v_t = joined(vl_ref, v_ref, vr_ref, h)
        for i in range(NBLK):
            cols, wide = blocks(i, i + ONE), blocks(i, i + THREE)
            s = jnp.where(in_bounds(lo_ref, hi_ref, i + ONE, i, i + THREE), mm(k_rows[wide], q_t[:, cols]), NEG)
            m = jnp.max(s, axis=ZERO, keepdims=True)
            e = jnp.exp(s - m)
            l = jnp.sum(e, axis=ZERO, keepdims=True)
            o_ref[h, :, cols] = mm(v_t[:, wide], (e * (ONE / l)).astype(BF)).astype(BF)
            lse_ref[h, :, cols] = m + jnp.log(l)
    every_head(head)


def attn1_fwd(qkv, left, right, lo, hi):
    bound = spec((ONE, EXT))
    return call(
        attn1_fwd_body, (HSTEPS,),
        [own_head(ZERO), own_head(ONE), own_head(TWO), halo_head(ZERO), halo_head(ONE), halo_head(ZERO), halo_head(ONE),
         bound, bound],
        [own_head(ZERO), spec((HPS, ONE, TOK), step_of, ZERO, ZERO)],
        [sds((NHEAD, HEAD, TOK), BF), sds((NHEAD, ONE, TOK), F32)],
        flops=NHEAD * FOUR * TOK * EXT * HALF, nbytes=FOUR * MIB, name="attn1_fwd",
    )(qkv, qkv, qkv, left, left, right, right, lo, hi)


def attn1_bwd_body(q_ref, k_ref, v_ref, do_ref, kl_ref, vl_ref, kr_ref, vr_ref, ql_ref, dl_ref, qr_ref, dr_ref,
                   lse_ref, del_ref, lo_ref, hi_ref, out_ref):
    last_own = NBLK + ONE

    def head(h):
        q_t = joined(ql_ref, q_ref, qr_ref, h) * SCALE
        do_t = joined(dl_ref, do_ref, dr_ref, h)
        k_t = joined(kl_ref, k_ref, kr_ref, h)
        k_rows, v_rows = k_t.T, joined(vl_ref, v_ref, vr_ref, h).T
        dk = [jnp.zeros((HEAD, LANE), F32) for _ in range(last_own)]
        dv = [jnp.zeros((HEAD, LANE), F32) for _ in range(last_own)]
        for e in range(NBLK + TWO):
            mine = ONE <= e <= NBLK
            first = e - ONE if mine else max(e - ONE, ONE)
            last = e + TWO if mine else min(e + TWO, last_own)
            cols, wide = blocks(e, e + ONE), blocks(first, last)
            ok = in_bounds(lo_ref, hi_ref, e, first, last)
            p = jnp.exp(jnp.where(ok, mm(k_rows[wide], q_t[:, cols]) - lse_ref[h, :, cols], NEG))
            ds = (p * (mm(v_rows[wide], do_t[:, cols]) - del_ref[h, :, cols])).astype(BF)
            p_bf = p.astype(BF)
            if mine:
                out_ref[ZERO, h, :, blocks(e - ONE, e)] = (mm(k_t[:, wide], ds) * SCALE).astype(BF)
            for kb in range(max(first, ONE), min(last, last_own)):
                rows = blocks(kb - first, kb - first + ONE)
                dv[kb] += mm_nt(do_t[:, cols], p_bf[rows])
                dk[kb] += mm_nt(q_t[:, cols], ds[rows])
        for kb in range(ONE, last_own):
            out_ref[ONE, h, :, blocks(kb - ONE, kb)] = dk[kb].astype(BF)
            out_ref[TWO, h, :, blocks(kb - ONE, kb)] = dv[kb].astype(BF)
    every_head(head)


def attn1_bwd(qkv, do_t, left, right, dleft, dright, lse_x, del_x, lo, hi):
    stat = spec((HPS, ONE, EXT), step_of, ZERO, ZERO)
    bound = spec((ONE, EXT))
    pair = [halo_head(ZERO), halo_head(ONE)]
    return call(
        attn1_bwd_body, (HSTEPS,),
        [own_head(ZERO), own_head(ONE), own_head(TWO), own_head(ZERO)] + pair * FOUR + [stat, stat, bound, bound],
        spec((THREE, HPS, HEAD, TOK), ZERO, step_of, ZERO, ZERO),
        sds((THREE, NHEAD, HEAD, TOK), BF),
        flops=NHEAD * 10 * TOK * EXT * HALF, nbytes=8 * MIB, name="attn1_bwd",
    )(qkv, qkv, qkv, do_t, left, left, right, right, dleft, dleft, dright, dright, lse_x, del_x, lo, hi)


ROWBLK = [slice(r, r + RB) for r in range(ZERO, TOK, RB)]
HALFT = NFT // TWO
SQRT_HALF = math.sqrt(SCALE * FOUR)
PDF_SCALE = SQRT_HALF / math.sqrt(math.pi)
STATS = 16


def normal_cdf(a):
    return SQRT_HALF * SQRT_HALF * (ONE + lax.erf(a * SQRT_HALF))


def att_block(ref, n):
    return ref.at[n % FOUR, n // FOUR] if ref.shape[ZERO] == FOUR else ref.at[n]


def half_rows(ref, which):
    n = ref.shape[ZERO] // TWO
    return ref.at[pl.ds(pl.multiple_of(which * n, n), n)]


def col_tile(ref, n):
    return ref.at[:, pl.ds(pl.multiple_of(n * FT, FT), FT)]


class Refs:
    def __init__(self, names, refs):
        self.__dict__.update(zip(names, refs))


class Swaps:
    def __init__(self, r):
        self.r, self.waits, self.n = r, [], ZERO
        self.core, self.partner = core_and_partner()
        self.other = ONE - self.core

    def remote(self, src, dst):
        cp = to_partner(self.partner, src, dst, self.r.ssem.at[self.n], self.r.rsem.at[self.n])
        return self.later(cp)

    def local(self, src, dst):
        return self.later(pltpu.make_async_copy(src, dst, self.r.lsem.at[self.n]))

    def later(self, cp):
        self.n += ONE
        self.waits.append(cp)
        return cp

    def wait(self):
        for cp in self.waits:
            cp.wait()


def mlp_body(*refs, names, fwd, bwd):
    r = Refs(names, refs)
    step = pl.program_id(ZERO)
    sw = Swaps(r)
    start, spread = [], []
    if fwd:
        start = [sw.remote(r.h, r.h_r), sw.remote(half_rows(r.of, sw.other), r.of_r),
                 sw.local(half_rows(r.of, sw.core), r.of_m)]
        m_out = [(sw.remote(r.m_s.at[HALFT * sw.other + n], col_tile(r.m_r, n)),
                  sw.local(r.m_s.at[HALFT * sw.core + n], col_tile(r.m_m, n))) for n in range(HALFT)]
    if bwd:
        start.append(sw.remote(r.dy, r.dy_r))
        dmid_out = sw.remote(r.dmid, r.dmid_r)
        du_out = [(sw.remote(r.du_s.at[n, sw.other], col_tile(r.du_r, n)),
                   sw.local(r.du_s.at[n, sw.core], col_tile(r.du_m, n))) for n in range(NFT)]

    @pl.when(step == ZERO)
    def _():
        if fwd:
            for n in range(NHEAD):
                r.of[HEAD * n:HEAD * n + HEAD, :] = att_block(r.o, n)[...]
            x1 = (r.x[...].astype(F32) + mm_tn(r.of[...], r.wp[...])).astype(BF)
            r.x1[...] = x1
            r.h[...] = norm_rows(x1, r.g[...])
            r.acc[...] = x1.astype(F32)
        if bwd:
            r.dacc[...] = jnp.zeros(r.dacc.shape, F32)
        meet_partner(sw.partner)
        for cp in start:
            cp.start()

    for rows in ROWBLK:
        if fwd:
            ua = mm(r.h[rows], r.wa[...]).astype(BF)
            ub = mm(r.h[rows], r.wb[...]).astype(BF)
            if not bwd:
                r.u[ZERO, rows] = ua
                r.u[ONE, rows] = ub
        else:
            ua, ub = r.u[ZERO, rows], r.u[ONE, rows]
        a, b = ua.astype(F32), ub.astype(F32)
        cdf = normal_cdf(a)
        gate = a * cdf
        if fwd:
            m = (gate * b).astype(BF)
            r.m_s[step, rows] = m
            r.acc[rows] += mm(m, r.wo[...])
        if bwd:
            dm = mm_nt(r.dy[rows], r.wo[...]).astype(BF).astype(F32)
            pdf = jnp.exp(a * a * (SCALE * FOUR - ONE)) * PDF_SCALE
            db = (dm * gate).astype(BF)
            da = (dm * b * (cdf + a * pdf)).astype(BF)
            r.du_s[step, ZERO, rows] = da
            r.du_s[step, ONE, rows] = db
            r.dacc[rows] += mm_nt(da, r.wa[...]) + mm_nt(db, r.wb[...])

    for n in range(NFT):
        @pl.when(step == n)
        def _(n=n):
            if fwd:
                there, here = m_out[n % HALFT]

                @pl.when(sw.core == n // HALFT)
                def _():
                    here.start()

                @pl.when(sw.other == n // HALFT)
                def _():
                    there.start()
            if bwd:
                for cp in du_out[n]:
                    cp.start()

    @pl.when(step == NFT - ONE)
    def _():
        if fwd:
            r.y[...] = r.acc[...].astype(BF)
        if bwd:
            d_ln, gg = norm_rows_grad(r.x1[...], r.g[...], r.dacc[...].astype(BF))
            r.gg[...] = gg
            d_mid = add_bf(r.dy[...], d_ln)
            r.dmid[...] = d_mid
            dmid_out.start()
            d_att = mm_nt(r.wp[...], d_mid).astype(BF)
            for n in range(NHEAD):
                rows = slice(HEAD * n, HEAD * n + HEAD)
                blk = d_att[rows]
                att_block(r.d_o, n)[...] = blk
                if fwd:
                    r.delta[n:n + ONE, :] = jnp.sum(blk.astype(F32) * r.of[rows].astype(F32), axis=ZERO, keepdims=True)
            if fwd:
                r.delta[NHEAD:, :] = jnp.zeros((STATS - NHEAD, TOK), F32)
        sw.wait()


def mlp_call(layer, cid, fwd, bwd, w_proj, gain, w_in, w_out, x=None, o_t=None, dy=None, x1=None, u=None, oshape=None):
    toks, tok_spec, vec = sds(ALLTOK, BF), spec(ALLTOK), spec((ONE, DM))
    u_spec = spec((TWO, TOK, FT), ZERO, ZERO, step_of)
    half_o = sds((DM // TWO, TOK), BF)
    half_m, half_u = sds((TOK, FF // TWO), BF), sds((TOK, FF), BF)
    ins = [('wp', w_proj, spec((None, DM, DM), layer, ZERO, ZERO)), ('g', gain, vec),
           ('wa', w_in, weight_cols(layer, FT)), ('wb', w_in, weight_cols(layer, FT, NFT)),
           ('wo', w_out, spec((None, FT, DM), layer, step_of, ZERO))]
    outs, scratch = [], []
    if fwd:
        ins += [('x', x, tok_spec), ('o', o_t, spec(o_t.shape))]
        outs += [('y', toks, tok_spec), ('h', toks, tok_spec), ('h_r', toks, ANY), ('of_m', half_o, ANY), ('of_r', half_o, ANY),
                 ('m_m', half_m, ANY), ('m_r', half_m, ANY)]
        scratch += [('acc', pltpu.VMEM(ALLTOK, F32)), ('of', pltpu.VMEM((DM, TOK), BF)), ('m_s', pltpu.VMEM((NFT, TOK, FT), BF))]
    if fwd and not bwd:
        outs += [('x1', toks, tok_spec), ('u', sds((TWO, TOK, FF), BF), u_spec)]
    if bwd:
        ins += [('dy', dy, tok_spec)]
        outs += [('dmid', toks, tok_spec), ('gg', sds((ONE, DM), F32), vec), ('d_o', sds(oshape, BF), spec(oshape)),
                 ('dy_r', toks, ANY), ('dmid_r', toks, ANY), ('du_m', half_u, ANY), ('du_r', half_u, ANY)]
        scratch += [('dacc', pltpu.VMEM(ALLTOK, F32)), ('du_s', pltpu.VMEM((NFT, TWO, TOK, FT), BF))]
    if fwd and bwd:
        outs += [('delta', sds((STATS, TOK), F32), spec((STATS, TOK)))]
        scratch += [('x1', pltpu.VMEM(ALLTOK, BF))]
    if not fwd:
        ins += [('x1', x1, tok_spec), ('u', u, u_spec)]
    sems = DMA((TWO * NFT + 8 + NFT,))
    scratch += [('ssem', sems), ('rsem', sems), ('lsem', sems)]
    names = [n for n, *_ in ins + outs + scratch]
    name = "mlp_" + "fwd" * fwd + "bwd" * bwd
    got = call(
        functools.partial(mlp_body, names=names, fwd=fwd, bwd=bwd), (NFT,),
        [sp for *_, sp in ins], [sp for *_, sp in outs], [sh for _, sh, _ in outs], scratch=[sh for _, sh in scratch],
        flops=TWO * TOK * DM * (DM + THREE * FF) * (fwd + bwd), nbytes=26 * MIB, name=name, cid=cid,
    )(*[arr for _, arr, _ in ins])
    return Refs([n for n, *_ in outs], got)


def qkv_bwd_body(d_ref, cos_ref, sin_ref, w_ref, x_ref, g_ref, dmid_ref, dx_ref, gg_ref, dtm_ref, dtr_ref,
                 acc, dt_s, dt_all, ssem, rsem, lsem):
    step = pl.program_id(ZERO)
    core, partner = core_and_partner()

    def dst(ref, n):
        rows = PROJ
        return ref.at[pl.ds(pl.multiple_of(n * rows, rows), rows)]

    def copies(n):
        return (to_partner(partner, dt_s.at[ONE - core, n], dst(dtr_ref, n), ssem.at[n], rsem.at[n]),
                pltpu.make_async_copy(dt_s.at[core, n], dst(dtm_ref, n), lsem.at[n]))

    @pl.when(step == ZERO)
    def _():
        acc[...] = jnp.zeros(acc.shape, F32)
        meet_partner(partner)

    def put(chunk, head, row, val):
        at = LANE * chunk + row + HEAD * (head % TWO)
        dt_s[head // TWO, step, at:at + val.shape[ZERO]] = val
        at = RB * chunk + row + HEAD * head
        dt_all[at:at + val.shape[ZERO]] = val

    @pl.when(step < TWO)
    def _():
        cos, sin = cos_ref[...], sin_ref[...]
        for chunk in CHUNKS:
            for head in range(FOUR):
                d_head = head_rows(d_ref, chunk, head)[...].astype(F32)
                da, db = d_head[:HALF], d_head[HALF:]
                put(chunk, head, ZERO, (da * cos + db * sin).astype(BF))
                put(chunk, head, HALF, (db * cos - da * sin).astype(BF))

    @pl.when(step == TWO)
    def _():
        for chunk in CHUNKS:
            for head in range(FOUR):
                put(chunk, head, ZERO, head_rows(d_ref, chunk, head)[...])

    for cp in copies(step):
        cp.start()
    acc[...] += mm(w_ref[...], dt_all[...])

    @pl.when(step == TWO)
    def _():
        d_ln, gg = norm_rows_grad(x_ref[...], g_ref[...], acc[...].T.astype(BF))
        gg_ref[...] = gg
        dx_ref[...] = add_bf(dmid_ref[...], d_ln)
        for n in range(THREE):
            for cp in copies(n):
                cp.wait()


def qkv_bwd(d_qkv, cos_t, sin_t, w_qkv, x, gain, d_mid, layer, dest_major, cid):
    table = spec((HALF, TOK))
    half = sds((THREE * PROJ, TOK), BF)
    return call(
        qkv_bwd_body, (THREE,),
        [heads_spec(dest_major), table, table, weight_cols(layer, DM), spec(ALLTOK), spec((ONE, DM)), spec(ALLTOK)],
        [spec(ALLTOK), spec((ONE, DM)), ANY, ANY],
        [sds(ALLTOK, BF), sds((ONE, DM), F32), half, half],
        scratch=[pltpu.VMEM((DM, TOK), F32), pltpu.VMEM((TWO, THREE, PROJ, TOK), BF), pltpu.VMEM((DM, TOK), BF),
                 DMA((THREE,)), DMA((THREE,)), DMA((THREE,))],
        flops=TWO * TOK * DM * THREE * DM, nbytes=10 * MIB, name="qkv_bwd", cid=cid,
    )(d_qkv, cos_t, sin_t, w_qkv, x, gain, d_mid)


DOWN = FF // TWO
UP = FF
QKV = THREE * PROJ
LAYER_ROWS = DOWN + UP + PROJ + QKV
ALLROWS = TWO * LAYER_ROWS
NDOWN = DOWN // DM
GRAD_REFS = 9


def grad_call(body, grads, steps, in_specs, args, rows, first, scratch=()):
    shared = [] if grads is None else [grads]
    return call(
        body, (steps,), [ANY] * len(shared) + in_specs,
        spec((rows, DM), lambda s: first + s, ZERO), sds((ALLROWS, DM), F32), scratch=scratch,
        flops=FOUR * steps * rows * TOK * DM, nbytes=20 * MIB, name=body.__name__,
        alias={ZERO: ZERO} if shared else None,
    )(*shared, *args)


def grad_mlp_body(*refs):
    ma, mb, dya, dyb, ha, hb, dua, dub, out_ref, h_t = refs[-GRAD_REFS - ONE:]
    step = pl.program_id(ZERO)

    @pl.when(step < NDOWN)
    def _():
        out_ref[...] = mm_tn(ma[...], dya[...]) + mm_tn(mb[...], dyb[...])

    @pl.when(step == NDOWN)
    def _():
        h_t[ZERO] = ha[...].T
        h_t[ONE] = hb[...].T

    @pl.when(step >= NDOWN)
    def _():
        out_ref[...] = mm(h_t[ZERO], dua[...]) + mm(h_t[ONE], dub[...])


def grad_mlp(grads, m, m_r, dy, dy_r, h, h_r, du, du_r, first_row):
    toks = spec(ALLTOK)
    m_col = spec(ALLTOK, ZERO, lambda s: jnp.minimum(s, NDOWN - ONE))
    du_col = spec(ALLTOK, ZERO, lambda s: jnp.maximum(s - NDOWN, ZERO))
    return grad_call(grad_mlp_body, grads, NDOWN + UP // DM, [m_col, m_col, toks, toks, toks, toks, du_col, du_col],
                     (m, m_r, dy, dy_r, h, h_r, du, du_r), DM, first_row // DM, scratch=[pltpu.VMEM((TWO, DM, TOK), BF)])


def grad_att_body(*refs):
    oa, ob, dma, dmb, ta, tb, ha, hb, out_ref = refs[-GRAD_REFS:]
    step = pl.program_id(ZERO)

    @pl.when(step == ZERO)
    def _():
        out_ref[...] = mm(oa[...], dma[...]) + mm(ob[...], dmb[...])

    @pl.when(step > ZERO)
    def _():
        out_ref[...] = mm(ta[...], ha[...]) + mm(tb[...], hb[...])


def grad_att(grads, of, of_r, dmid, dmid_r, dt, dt_r, h, h_r, first_row):
    toks = spec(ALLTOK)
    blk = (PROJ, TOK)
    dt_row = spec(blk, lambda s: jnp.maximum(s - ONE, ZERO), ZERO)
    return grad_call(grad_att_body, grads, ONE + QKV // PROJ, [spec(blk), spec(blk), toks, toks, dt_row, dt_row, toks, toks],
                     (of, of_r, dmid, dmid_r, dt, dt_r, h, h_r), PROJ, (first_row + DOWN + UP) // PROJ)


NB, NS, CH, SB, LF = 4, 6, 128, 32, 8
RS = 9
LAST = RS + RS


def ring_body(g_ref, ln_ref, f_ref, lnout_ref, bufa, bufb, bufc, gath, stage, lnbuf,
              ssem, rsem, psem, qsem, csem, stsem, lns, lnr):
    core, partner = core_and_partner()
    dp = lax.axis_index('dp')
    pos = (lax.axis_index('sp'), lax.rem(dp // TWO, FOUR), dp // 8)
    streams = [(c, sg) for c in range(THREE) for sg in (ONE, -ONE)]
    bufs, sizes = (bufa, bufb, bufc), (CH, SB, LF)
    peers = range(ONE, FOUR)

    def mod4(v):
        return lax.rem(v + 8, FOUR)

    def at(axis, val):
        if axis == ZERO:
            return {'sp': val}
        yz = (val, pos[TWO]) if axis == ONE else (pos[ONE], val)
        return {'dp': yz[ONE] * 8 + yz[ZERO] * TWO + core}

    def shifted(axis, d):
        return at(axis, mod4(pos[axis] + d))

    def axis_of(s, ph):
        return (streams[s][ZERO] + ph) % THREE

    def idx(s, ph, t):
        return mod4(pos[axis_of(s, ph)] - streams[s][ONE] * t)

    def own(s, ph):
        return idx(s, ph, -ONE)

    def base(b, s):
        return (b * NS + s) * (FOUR * CH)

    bar = pltpu.get_barrier_semaphore()
    for ax in range(THREE):
        for d in peers:
            pl.semaphore_signal(bar, inc=ONE, device_id=shifted(ax, d), device_id_type=MESH)
    pl.semaphore_signal(bar, inc=ONE, device_id=partner, device_id_type=MESH)
    pl.semaphore_wait(bar, 10)

    def rows(ref, start, n):
        return ref.at[pl.ds(pl.multiple_of(start, LF), n)]

    def frows(start, n):
        return f_ref.at[core, pl.ds(pl.multiple_of(start, LF), n)]

    def same_bytes(b, k):
        if k < RS:
            return bufs[k // THREE].at[b, k % THREE]
        n = sizes[TWO - (k - RS) // THREE]
        return gath.at[b] if n == CH else gath.at[b, :, pl.ds(ZERO, n)]

    def wait_for(ref, sem):
        pltpu.make_async_copy(ref, ref, sem).wait()

    def send(b, s, k):
        ph = k // THREE if k < RS else TWO - (k - RS) // THREE
        t = k % THREE
        n = sizes[ph]
        if k < RS:
            dst = bufs[ph].at[b, t, s]
            if t:
                src = bufs[ph].at[b, t - ONE, s]
            elif ph:
                src = rows(bufs[ph - ONE].at[b, TWO, s], idx(s, ph, ZERO) * n, n)
            else:
                src = rows(g_ref, base(b, s) + idx(s, ZERO, ZERO) * n, n)
        elif ph:
            off = own(s, ONE) * SB if ph == TWO else ZERO
            src = dst = rows(gath.at[b, s], off + idx(s, ph, t - ONE) * n, n)
        else:
            dst = frows(base(b, s) + idx(s, ZERO, t - ONE) * n, n)
            src = dst if t else gath.at[b, s]
        pltpu.make_async_remote_copy(src_ref=src, dst_ref=dst, send_sem=ssem.at[b, k], recv_sem=rsem.at[b, k],
                                     device_id=shifted(axis_of(s, ph), streams[s][ONE]), device_id_type=MESH).start()

    def stage_load(n):
        t, b, slot = n // NB, lax.rem(n, NB), lax.rem(n, TWO)
        for s in range(NS):
            pltpu.make_async_copy(rows(g_ref, base(b, s) + idx(s, ZERO, t + ONE) * CH, CH), stage.at[slot, s],
                                  stsem.at[slot]).start()

    def ln_copy(ph, d):
        return pltpu.make_async_remote_copy(
            src_ref=lnbuf.at[ph, THREE] if ph else ln_ref, dst_ref=lnbuf.at[ph, d - ONE], send_sem=lns.at[ph, d - ONE],
            recv_sem=lnr.at[ph, d - ONE], device_id=shifted(ph, d) if ph < THREE else partner, device_id_type=MESH)

    def ln_sum(ph):
        vals = [lnbuf[ph, THREE] if ph else ln_ref[...]] + [lnbuf[ph, d - ONE] for d in peers]
        total = jnp.zeros_like(vals[ZERO])
        for p in range(FOUR):
            term = vals[ZERO]
            for d in peers:
                term = jnp.where(mod4(pos[ph] - d) == p, vals[d], term)
            total = total + term
        return total

    def batches(fn, start=ZERO):
        def body(b, c):
            fn(b)
            return c
        lax.fori_loop(start, NB, body, ZERO)

    def first(b):
        for s in range(NS):
            send(b, s, ZERO)

    first(ZERO)
    stage_load(jnp.int32(ZERO))
    for d in peers:
        ln_copy(ZERO, d).start()
    batches(first, ONE)

    for k in range(RS):
        ph, t = k // THREE, k % THREE
        buf, size = bufs[ph], sizes[ph]

        def step(b, k=k, ph=ph, t=t, buf=buf, size=size):
            n = k * NB + b
            slot = lax.rem(n, TWO)
            if not ph:
                @pl.when(n < THREE * NB - ONE)
                def _():
                    stage_load(n + ONE)
                wait_for(stage.at[slot], stsem.at[slot])
            wait_for(same_bytes(b, k), rsem.at[b, k])
            for s in range(NS):
                if ph:
                    off = pl.multiple_of(idx(s, ph, t + ONE) * size, LF)
                    buf[b, t, s] += bufs[ph - ONE][b, TWO, s, pl.ds(off, size)]
                else:
                    @pl.loop(ZERO, CH, step=SB)
                    def _(r):
                        at_r = pl.ds(pl.multiple_of(r, SB), SB)
                        buf[b, t, s, at_r] += stage[slot, s, at_r]
                if k == RS - ONE:
                    off = pl.multiple_of(own(s, ONE) * SB + own(s, TWO) * LF, LF)
                    gath[b, s, pl.ds(off, LF)] = bufc[b, TWO, s]
                send(b, s, k + ONE)

        batches(step)
        if k < SIX and k % TWO == ZERO:
            lp = k // TWO
            for d in peers:
                ln_copy(lp, d).wait()
            lnbuf[lp + ONE, THREE] = ln_sum(lp)
            for d in peers if lp < TWO else (ONE,):
                ln_copy(lp + ONE, d).start()

    def hand_over(b, s, j, src, start):
        pltpu.make_async_remote_copy(src_ref=src, dst_ref=frows(start, CH), send_sem=psem.at[b, j], recv_sem=qsem.at[b, j],
                                     device_id=partner, device_id_type=MESH).start()

    for k in range(RS, LAST):
        def step(b, k=k):
            wait_for(same_bytes(b, k), rsem.at[b, k])
            piece = k - (LAST - FOUR)
            for s in range(NS):
                if k < LAST - ONE:
                    send(b, s, k + ONE)
                if piece >= ZERO:
                    start = base(b, s) + idx(s, ZERO, piece - ONE) * CH
                    if piece:
                        hand_over(b, s, piece, frows(start, CH), start)
                    else:
                        pltpu.make_async_copy(gath.at[b, s], frows(start, CH), csem.at[b]).start()
                        hand_over(b, s, piece, gath.at[b, s], start)
        batches(step)

    ln_copy(THREE, ONE).wait()
    lnout_ref[...] = lnbuf[THREE, THREE] + lnbuf[THREE, ZERO]

    def finish(b):
        for k in range(LAST):
            wait_for(same_bytes(b, k), ssem.at[b, k])
        for j in range(FOUR):
            wait_for(gath.at[b], psem.at[b, j])
            wait_for(gath.at[b], qsem.at[b, j])
        wait_for(gath.at[b], csem.at[b])
    batches(finish)


def ring_all_reduce(g, ln, cid):
    vmem = pl.BlockSpec(memory_space=pltpu.VMEM)
    return pl.pallas_call(
        ring_body,
        in_specs=[ANY, vmem],
        out_specs=[ANY, vmem],
        out_shape=[sds((TWO, ALLROWS, DM), F32), sds(ln.shape, F32)],
        scratch_shapes=[
            pltpu.VMEM((NB, THREE, NS, CH, DM), F32), pltpu.VMEM((NB, THREE, NS, SB, DM), F32),
            pltpu.VMEM((NB, THREE, NS, LF, DM), F32), pltpu.VMEM((NB, NS, CH, DM), F32), pltpu.VMEM((TWO, NS, CH, DM), F32),
            pltpu.VMEM((FOUR, FOUR) + ln.shape, F32),
            DMA((NB, LAST)), DMA((NB, LAST)), DMA((NB, FOUR)), DMA((NB, FOUR)), DMA((NB,)), DMA((TWO,)),
            DMA((FOUR, THREE)), DMA((FOUR, THREE)),
        ],
        compiler_params=pltpu.CompilerParams(collective_id=cid, has_side_effects=True, vmem_limit_bytes=63 * MIB),
        name="ring_all_reduce",
    )(g, ln)


def copy_body(in_ref, out_ref):
    out_ref[...] = in_ref[...]


def turn_body(a_ref, b_ref, out_ref):
    for n in CHUNKS:
        rows, col = slice(LANE * n, LANE * n + LANE), RB * n
        out_ref[ZERO, :, col:col + LANE] = a_ref[ZERO, rows].T
        out_ref[ZERO, :, col + LANE:col + RB] = b_ref[ZERO, rows].T


def unpack(f):
    def blk(rows, row0):
        return (ONE, rows, DM), (lambda l, *_: (ONE - l) * (LAYER_ROWS // rows) + row0 // rows)

    whole, at_layer = blk(DM, ZERO)
    core_of = lambda l, c, *_: c
    layer_of = lambda l, *_: l
    nbytes = 100 * MIB
    g_out = call(copy_body, (TWO, TWO, TWO),
                 [spec(whole, core_of, lambda l, c, i: at_layer(l) + i, ZERO)],
                 spec(whole, layer_of, lambda l, c, i: TWO * c + i, ZERO), sds((TWO, FF, DM), F32), nbytes=nbytes)(f)
    g_in = call(copy_body, (TWO, TWO, FOUR),
                [spec(whole, core_of, lambda l, c, j: at_layer(l) + TWO + j, ZERO)],
                spec(whole, layer_of, ZERO, lambda l, c, j: FOUR * c + j), sds((TWO, DM, TWO * FF), F32), nbytes=nbytes)(f)
    half, at_proj = blk(PROJ, DOWN + UP)
    g_proj = call(copy_body, (TWO, TWO), [spec(half, core_of, at_proj, ZERO)], spec(half, layer_of, core_of, ZERO),
                  sds((TWO, DM, DM), F32), nbytes=nbytes)(f)
    part, at_qkv = blk(PROJ, DOWN + UP + PROJ)
    row = lambda l, s: at_qkv(l) + s
    g_qkv = call(turn_body, (TWO, THREE), [spec(part, ZERO, row, ZERO), spec(part, ONE, row, ZERO)],
                 spec(whole, layer_of, ZERO, core_of), sds((TWO, DM, THREE * DM), F32), nbytes=nbytes)(f, f)
    return g_qkv, g_proj, g_in, g_out


def rope_tables(pos, base):
    inv_freq = base ** (jnp.arange(HALF).astype(F32) * (-TWO / HEAD))
    angles = inv_freq[:, None] * pos.astype(F32)[None, :]
    return jnp.cos(angles), jnp.sin(angles)


def solution(mesh):
    token_spec = P(('dp', 'sp'), None)
    n_sp = mesh.shape['sp']
    to_right = [(i, i + ONE) for i in range(n_sp - ONE)]
    to_left = [(i + ONE, i) for i in range(n_sp - ONE)]
    cids = list(range(RS))

    def halo_swap(arr):
        from_left = lax.ppermute(arr[..., TOK - LANE:], 'sp', to_right)
        from_right = lax.ppermute(arr[..., :LANE], 'sp', to_left)
        return from_left, from_right

    def exchange(arr):
        return lax.all_to_all(arr, 'sp', ZERO, ZERO, tiled=True)

    def device_step(x_loc, cu_loc, pos_loc, w_qkv, w_proj, w_in, w_out, ln_attn, ln_mlp, d_out):
        sp = lax.axis_index('sp')
        cu = cu_loc[ZERO][:, None]

        def bounds_of(tok):
            start = jnp.max(jnp.where(cu <= tok, cu, ZERO), axis=ZERO)
            return start, jnp.min(jnp.where(cu > tok, cu, GRP), axis=ZERO)

        start, stop = bounds_of(jnp.arange(GRP)[None, :])
        tiles = start[::QT] // QT, (stop[QT - ONE::QT] + QT - ONE) // QT
        rows = start[None, :], stop[None, :]
        shift = sp * TOK - LANE
        tok_x = jnp.arange(EXT) + shift
        start_x, stop_x = bounds_of(tok_x[None, :])
        inside = (tok_x >= ZERO) & (tok_x < GRP)
        near = (jnp.where(inside, jnp.maximum(start_x, tok_x - WIN) - shift, ZERO)[None, :],
                jnp.where(inside, jnp.minimum(stop_x, tok_x + WIN + ONE) - shift, ZERO)[None, :])
        tab0, tab1 = [rope_tables(pos_loc, base) for base in BASES]
        la0, la1, lm0, lm1 = ln_attn[:ONE], ln_attn[ONE:], ln_mlp[:ONE], ln_mlp[ONE:]

        w_mlp = (w_in, w_out)
        h0, qkv0, h0r = qkv_fwd(x_loc, la0, w_qkv, ZERO, *tab0, True, cids[ONE])
        qkv0 = exchange(qkv0)
        oh0, lse0 = attn0_fwd(*tiles, qkv0, *rows)
        f0 = mlp_call(ZERO, cids[TWO], True, False, w_proj, lm0, *w_mlp, x=x_loc, o_t=exchange(oh0))
        x1 = f0.y
        h1, qkv1, h1r = qkv_fwd(x1, la1, w_qkv, ONE, *tab1, False, cids[THREE])
        qkv1 = qkv1.reshape((THREE * NHEAD, HEAD, TOK))
        kv_halo = halo_swap(qkv1[NHEAD:])
        o1, lse1 = attn1_fwd(qkv1, *kv_halo, *near)
        f1 = mlp_call(ONE, cids[FOUR], True, True, w_proj, lm1, *w_mlp, x=x1, o_t=o1, dy=d_out, oshape=(NHEAD, HEAD, TOK))
        d_halo = halo_swap(jnp.concatenate([qkv1[:NHEAD], f1.d_o], axis=ZERO))
        stats = jnp.concatenate([lse1.reshape(NHEAD, TOK), f1.delta[:NHEAD]], axis=ZERO)
        from_left, from_right = halo_swap(stats)
        lse_x, del_x = jnp.concatenate([from_left, stats, from_right], axis=ONE).reshape(TWO, NHEAD, ONE, EXT)
        dqkv1 = attn1_bwd(qkv1, f1.d_o, *kv_halo, *d_halo, lse_x, del_x, *near)
        dx1, gga1, dt1, dt1r = qkv_bwd(dqkv1.reshape(THREE, THREE, FOUR, HEAD, TOK), *tab1, w_qkv, x1, la1, f1.dmid,
                                       ONE, False, cids[SIX])
        grads = grad_mlp(None, f1.m_m, f1.m_r, d_out, f1.dy_r, f1.h, f1.h_r, f1.du_m, f1.du_r, ZERO)
        grads = grad_att(grads, f1.of_m, f1.of_r, f1.dmid, f1.dmid_r, dt1, dt1r, h1, h1r, ZERO)
        b0 = mlp_call(ZERO, cids[5], False, True, w_proj, lm0, *w_mlp, dy=dx1, x1=f0.x1, u=f0.u, oshape=oh0.shape)
        grads = grad_mlp(grads, f0.m_m, f0.m_r, dx1, b0.dy_r, f0.h, f0.h_r, b0.du_m, b0.du_r, LAYER_ROWS)
        dqkv0 = exchange(attn0_bwd(*tiles, qkv0, oh0, exchange(b0.d_o), lse0, *rows))
        dx0, gga0, dt0, dt0r = qkv_bwd(dqkv0, *tab0, w_qkv, x_loc, la0, b0.dmid, ZERO, True, cids[7])
        grads = grad_att(grads, f0.of_m, f0.of_r, b0.dmid, b0.dmid_r, dt0, dt0r, h0, h0r, LAYER_ROWS)

        y, ggm0, ggm1 = f1.y, b0.gg, f1.gg
        gains = jnp.concatenate([gga0, gga1, ggm0, ggm1, jnp.zeros((FOUR, DM), F32)], axis=ZERO)
        summed, gains = ring_all_reduce(grads, gains, cids[ZERO])
        return (y, dx0) + unpack(summed) + (gains[:TWO], gains[TWO:FOUR])

    in_specs = (token_spec, P('dp', None), P(('dp', 'sp'))) + (P(),) * SIX + (token_spec,)
    out_specs = (token_spec, token_spec) + (P(),) * SIX
    return jax.shard_map(device_step, mesh=mesh, in_specs=in_specs, out_specs=out_specs, check_vma=False)
```

```python
import functools
import math
import jax
import jax.numpy as jnp
from jax import lax
from jax.experimental import pallas as pl
from jax.experimental.pallas import tpu as pltpu
from jax.sharding import Mesh, PartitionSpec as P

ZERO, ONE, TWO, THREE, FOUR = range(5)
SIX, TWELVE = 6, 12
HEAD = 64
HALF = 32
NHEAD = 12
DM = 768
FF = 3072
TOK = 512
GRP = 2048
WIN = 64
LANE = 128
EPS = 1e-5
NEG = -1e30
SCALE = 0.125
BASES = (160000.0, 10000.0)
F32 = jnp.float32
BF = jnp.bfloat16
QT = 256
FT = 512
NFT = FF // FT
QTILES = GRP // QT
MIB = 1024 * 1024
ALLTOK = (TOK, DM)
PROJ = DM // 2
ALLDM = (DM, DM)
ANY = pl.BlockSpec(memory_space=pl.ANY)
DMA = pltpu.SemaphoreType.DMA
MESH = pl.DeviceIdType.MESH


def dot(a, b, ca, cb):
    return lax.dot_general(a, b, (((ca,), (cb,)), ((), ())), preferred_element_type=F32)


def mm(a, b):
    return dot(a, b, ONE, ZERO)


def mm_nt(a, b):
    return dot(a, b, ONE, ONE)


def mm_tn(a, b):
    return dot(a, b, ZERO, ZERO)


def call(body, grid, in_specs, out_specs, out_shape, scratch=(), prefetch=ZERO, flops=ZERO, nbytes=ZERO, name=None,
         cid=None, alias=None):
    extra = {} if cid is None else dict(collective_id=cid, has_side_effects=True)
    return pl.pallas_call(
        body,
        grid_spec=pltpu.PrefetchScalarGridSpec(
            num_scalar_prefetch=prefetch, grid=grid, in_specs=in_specs, out_specs=out_specs, scratch_shapes=scratch),
        out_shape=out_shape,
        input_output_aliases=alias or {},
        compiler_params=pltpu.CompilerParams(vmem_limit_bytes=60 * MIB, **extra),
        cost_estimate=pl.CostEstimate(flops=int(flops), bytes_accessed=int(nbytes), transcendentals=ZERO),
        name=name,
    )


def sds(shape, dtype):
    return jax.ShapeDtypeStruct(shape, dtype)


def spec(shape, *idx):
    idx = idx or (ZERO,) * len(shape)
    return pl.BlockSpec(shape, lambda *g: tuple(i(*g) if callable(i) else i for i in idx))


def step_of(s, *_):
    return s


def core_and_partner():
    core = lax.axis_index('core')
    return core, {'core': ONE - core}


def meet_partner(partner):
    bar = pltpu.get_barrier_semaphore()
    pl.semaphore_signal(bar, inc=ONE, device_id=partner, device_id_type=MESH)
    pl.semaphore_wait(bar, ONE)


def to_partner(partner, src, dst, ssem, rsem):
    return pltpu.make_async_remote_copy(src_ref=src, dst_ref=dst, send_sem=ssem, recv_sem=rsem,
                                        device_id=partner, device_id_type=MESH)


def norm_parts(x_bf):
    rows = x_bf.astype(F32)
    cen = rows - jnp.mean(rows, axis=ONE, keepdims=True)
    var = jnp.mean(cen * cen, axis=ONE, keepdims=True)
    return cen, lax.rsqrt(var + EPS)


def norm_rows(x_bf, gain):
    cen, inv = norm_parts(x_bf)
    return (cen * inv * gain).astype(BF)


def norm_rows_grad(x_bf, gain, d_bf):
    cen, inv = norm_parts(x_bf)
    hat = cen * inv
    d_out = d_bf.astype(F32)
    g_gain = jnp.sum(d_out * hat, axis=ZERO, keepdims=True)
    d_hat = d_out * gain
    d_x = inv * (d_hat - jnp.mean(d_hat, axis=ONE, keepdims=True) - hat * jnp.mean(d_hat * hat, axis=ONE, keepdims=True))
    return d_x.astype(BF), g_gain


def add_bf(a, b):
    return (a.astype(F32) + b.astype(F32)).astype(BF)


RB = 256
CHUNKS = range(DM // RB)


def head_rows(ref, chunk, head):
    return ref.at[head, ZERO, chunk] if ref.shape[ZERO] == FOUR else ref.at[ZERO, chunk, head]


def heads_spec(dest_major):
    if dest_major:
        return spec((FOUR, ONE, THREE, HEAD, TOK), ZERO, step_of, ZERO, ZERO, ZERO)
    return spec((ONE, THREE, FOUR, HEAD, TOK), step_of, ZERO, ZERO, ZERO, ZERO)


def weight_cols(layer, width, first=ZERO):
    return spec((None, DM, width), layer, ZERO, lambda s: first + s)


def qkv_fwd_body(x_ref, g_ref, w_ref, cos_ref, sin_ref, h_ref, out_ref, hr_ref, ssem, rsem):
    step = pl.program_id(ZERO)
    core, partner = core_and_partner()
    swap = to_partner(partner, h_ref, hr_ref, ssem, rsem)

    @pl.when(step == ZERO)
    def _():
        h_ref[...] = norm_rows(x_ref[...], g_ref[...])
        meet_partner(partner)
        swap.start()

    def product(chunk):
        return mm(h_ref[...], w_ref[:, RB * chunk:RB * chunk + RB]).astype(BF).astype(F32).T

    @pl.when(step < TWO)
    def _():
        cos, sin = cos_ref[...], sin_ref[...]
        for chunk in CHUNKS:
            t_rows = product(chunk)
            for head in range(FOUR):
                at = HEAD * head
                a, b = t_rows[at:at + HALF], t_rows[at + HALF:at + HEAD]
                out = head_rows(out_ref, chunk, head)
                out[:HALF] = (a * cos - b * sin).astype(BF)
                out[HALF:] = (b * cos + a * sin).astype(BF)

    @pl.when(step == TWO)
    def _():
        for chunk in CHUNKS:
            t_rows = product(chunk).astype(BF)
            for head in range(FOUR):
                head_rows(out_ref, chunk, head)[...] = t_rows[HEAD * head:HEAD * head + HEAD]
        swap.wait()


def qkv_fwd(x, gain, w_qkv, layer, cos_t, sin_t, dest_major, cid):
    oshape = (FOUR, THREE, THREE, HEAD, TOK) if dest_major else (THREE, THREE, FOUR, HEAD, TOK)
    table = spec((HALF, TOK))
    return call(
        qkv_fwd_body, (THREE,),
        [spec(ALLTOK), spec((ONE, DM)), weight_cols(layer, DM), table, table],
        [spec(ALLTOK), heads_spec(dest_major), ANY],
        [sds(ALLTOK, BF), sds(oshape, BF), sds(ALLTOK, BF)],
        scratch=[DMA, DMA],
        flops=TWO * TOK * DM * THREE * DM, nbytes=8 * MIB, name="qkv_fwd", cid=cid,
    )(x, gain, w_qkv, cos_t, sin_t)


def tile_src(i, *_):
    return i // TWO


def tile_side(i, *_):
    return i % TWO


Q_SPEC = spec((ONE, ONE, THREE, HEAD, QT), tile_src, ZERO, ZERO, ZERO, tile_side)
O_SPEC = spec((ONE, THREE, HEAD, QT), tile_src, ZERO, ZERO, tile_side)
ROW_SPEC = spec((ONE, QT), ZERO, step_of)
STAT_SPEC = spec((8, QT), ZERO, step_of)
GROUP_QKV = (FOUR, THREE, THREE, HEAD, TOK)


def kv_spec(part):
    return spec((FOUR, ONE, THREE, HEAD, TOK), ZERO, part, ZERO, ZERO, ZERO)


def key_tile(kt):
    return kt // TWO, pl.ds(pl.multiple_of((kt % TWO) * QT, QT), QT)


def attn0_fwd_body(lo_s, hi_s, q_ref, k_ref, v_ref, st_ref, en_ref, o_ref, lse_ref, m_s, l_s, acc_s):
    tile = pl.program_id(ZERO)
    m_s[...] = jnp.full(m_s.shape, NEG, F32)
    l_s[...] = jnp.zeros(l_s.shape, F32)
    acc_s[...] = jnp.zeros(acc_s.shape, F32)
    st, en = st_ref[...], en_ref[...]
    io = lax.broadcasted_iota(jnp.int32, (QT, QT), ZERO)
    q_t = [q_ref[ZERO, ZERO, h] * SCALE for h in range(THREE)]

    def body(kt, carry):
        base = kt * QT
        src, cols = key_tile(kt)
        ok = (io >= st - base) & (io < en - base)
        for h in range(THREE):
            row = slice(h, h + ONE)
            k_t = k_ref[src, ZERO, h, :, cols]
            v_t = v_ref[src, ZERO, h, :, cols]
            s = jnp.where(ok, mm_tn(k_t, q_t[h]), NEG)
            m_old = m_s[row]
            m_new = jnp.maximum(m_old, jnp.max(s, axis=ZERO, keepdims=True))
            p = jnp.exp(s - m_new)
            alpha = jnp.exp(m_old - m_new)
            l_s[row] = l_s[row] * alpha + jnp.sum(p, axis=ZERO, keepdims=True)
            acc_s[h] = acc_s[h] * alpha + mm(v_t, p.astype(BF))
            m_s[row] = m_new
        return carry

    lax.fori_loop(lo_s[tile], hi_s[tile], body, ZERO)
    for h in range(THREE):
        row = slice(h, h + ONE)
        o_ref[ZERO, h] = (acc_s[h] / l_s[row]).astype(BF)
        lse_ref[row] = m_s[row] + jnp.log(l_s[row])


def attn0_fwd(lo, hi, qkv, st, en):
    stat = pltpu.VMEM((8, QT), F32)
    return call(
        attn0_fwd_body, (QTILES,),
        [Q_SPEC, kv_spec(ONE), kv_spec(TWO), ROW_SPEC, ROW_SPEC],
        [O_SPEC, STAT_SPEC],
        [sds((FOUR, THREE, HEAD, TOK), BF), sds((8, GRP), F32)],
        scratch=[stat, stat, pltpu.VMEM((THREE, HEAD, QT), F32)],
        prefetch=TWO, flops=TWELVE * GRP * GRP * HEAD, nbytes=6 * MIB, name="attn0_fwd",
    )(lo, hi, qkv, qkv, qkv, st, en)


def attn0_bwd_body(lo_s, hi_s, q_ref, k_ref, v_ref, o_ref, do_ref, lse_ref, st_ref, en_ref, out_ref, dk_s, dv_s, dq_s):
    tile = pl.program_id(ZERO)

    @pl.when(tile == ZERO)
    def _():
        dk_s[...] = jnp.zeros(dk_s.shape, F32)
        dv_s[...] = jnp.zeros(dv_s.shape, F32)

    dq_s[...] = jnp.zeros(dq_s.shape, F32)
    st, en = st_ref[...], en_ref[...]
    io = lax.broadcasted_iota(jnp.int32, (QT, QT), ZERO)
    heads = range(THREE)
    q_t = [q_ref[ZERO, ZERO, h] * SCALE for h in heads]
    do_t = [do_ref[ZERO, h] for h in heads]
    delta = [jnp.sum(do_t[h].astype(F32) * o_ref[ZERO, h].astype(F32), axis=ZERO, keepdims=True) for h in heads]
    lse = [lse_ref[h:h + ONE] for h in heads]

    def body(kt, carry):
        base = kt * QT
        src, cols = key_tile(kt)
        ok = (io >= st - base) & (io < en - base)
        for h in heads:
            k_t = k_ref[src, ZERO, h, :, cols]
            v_t = v_ref[src, ZERO, h, :, cols]
            p = jnp.exp(jnp.where(ok, mm_tn(k_t, q_t[h]) - lse[h], NEG))
            ds = (p * (mm_tn(v_t, do_t[h]) - delta[h])).astype(BF)
            at = (src, h, slice(None), cols)
            dv_s[at] += mm_nt(do_t[h], p.astype(BF))
            dk_s[at] += mm_nt(q_t[h], ds)
            dq_s[h] += mm(k_t, ds)
        return carry

    lax.fori_loop(lo_s[tile], hi_s[tile], body, ZERO)
    src, cols = key_tile(tile)
    for h in heads:
        out_ref[src, ZERO, h, :, cols] = (dq_s[h] * SCALE).astype(BF)

    @pl.when(tile == QTILES - ONE)
    def _():
        for src in range(FOUR):
            for h in heads:
                out_ref[src, ONE, h] = dk_s[src, h].astype(BF)
                out_ref[src, TWO, h] = dv_s[src, h].astype(BF)


def attn0_bwd(lo, hi, qkv, o_t, do_t, lse, st, en):
    acc = pltpu.VMEM((FOUR, THREE, HEAD, TOK), F32)
    return call(
        attn0_bwd_body, (QTILES,),
        [Q_SPEC, kv_spec(ONE), kv_spec(TWO), O_SPEC, O_SPEC, STAT_SPEC, ROW_SPEC, ROW_SPEC],
        spec(GROUP_QKV), sds(GROUP_QKV, BF),
        scratch=[acc, acc, pltpu.VMEM((THREE, HEAD, QT), F32)],
        prefetch=TWO, flops=30 * GRP * GRP * HEAD, nbytes=TWELVE * MIB, name="attn0_bwd",
    )(lo, hi, qkv, qkv, qkv, o_t, do_t, lse, st, en)


NBLK = TOK // LANE
EXT = TOK + TWO * LANE


HPS = 4
HSTEPS = NHEAD // HPS


def heads_of(width, part):
    return spec((HPS, HEAD, width), lambda n: HSTEPS * part + n, ZERO, ZERO)


def own_head(part):
    return heads_of(TOK, part)


def halo_head(part):
    return heads_of(LANE, part)


def joined(left, mid, right, h):
    return jnp.concatenate([left[h], mid[h], right[h]], axis=ONE)


def blocks(first, last):
    return slice(LANE * first, LANE * last)


def in_bounds(lo_ref, hi_ref, blk, first, last):
    io = lax.broadcasted_iota(jnp.int32, (LANE * (last - first), LANE), ZERO) + LANE * first
    cols = blocks(blk, blk + ONE)
    return (io >= lo_ref[:, cols]) & (io < hi_ref[:, cols])


def every_head(fn):
    def body(h, c):
        fn(h)
        return c
    lax.fori_loop(ZERO, HPS, body, ZERO)


def attn1_fwd_body(q_ref, k_ref, v_ref, kl_ref, vl_ref, kr_ref, vr_ref, lo_ref, hi_ref, o_ref, lse_ref):
    def head(h):
        q_t = q_ref[h] * SCALE
        k_rows = joined(kl_ref, k_ref, kr_ref, h).T
        v_t = joined(vl_ref, v_ref, vr_ref, h)
        for i in range(NBLK):
            cols, wide = blocks(i, i + ONE), blocks(i, i + THREE)
            s = jnp.where(in_bounds(lo_ref, hi_ref, i + ONE, i, i + THREE), mm(k_rows[wide], q_t[:, cols]), NEG)
            m = jnp.max(s, axis=ZERO, keepdims=True)
            e = jnp.exp(s - m)
            l = jnp.sum(e, axis=ZERO, keepdims=True)
            o_ref[h, :, cols] = mm(v_t[:, wide], (e * (ONE / l)).astype(BF)).astype(BF)
            lse_ref[h, :, cols] = m + jnp.log(l)
    every_head(head)


def attn1_fwd(qkv, left, right, lo, hi):
    bound = spec((ONE, EXT))
    return call(
        attn1_fwd_body, (HSTEPS,),
        [own_head(ZERO), own_head(ONE), own_head(TWO), halo_head(ZERO), halo_head(ONE), halo_head(ZERO), halo_head(ONE),
         bound, bound],
        [own_head(ZERO), spec((HPS, ONE, TOK), step_of, ZERO, ZERO)],
        [sds((NHEAD, HEAD, TOK), BF), sds((NHEAD, ONE, TOK), F32)],
        flops=NHEAD * FOUR * TOK * EXT * HALF, nbytes=FOUR * MIB, name="attn1_fwd",
    )(qkv, qkv, qkv, left, left, right, right, lo, hi)


def attn1_bwd_body(q_ref, k_ref, v_ref, do_ref, kl_ref, vl_ref, kr_ref, vr_ref, ql_ref, dl_ref, qr_ref, dr_ref,
                   lse_ref, del_ref, lo_ref, hi_ref, out_ref):
    last_own = NBLK + ONE

    def head(h):
        q_t = joined(ql_ref, q_ref, qr_ref, h) * SCALE
        do_t = joined(dl_ref, do_ref, dr_ref, h)
        k_t = joined(kl_ref, k_ref, kr_ref, h)
        k_rows, v_rows = k_t.T, joined(vl_ref, v_ref, vr_ref, h).T
        dk = [jnp.zeros((HEAD, LANE), F32) for _ in range(last_own)]
        dv = [jnp.zeros((HEAD, LANE), F32) for _ in range(last_own)]
        for e in range(NBLK + TWO):
            mine = ONE <= e <= NBLK
            first = e - ONE if mine else max(e - ONE, ONE)
            last = e + TWO if mine else min(e + TWO, last_own)
            cols, wide = blocks(e, e + ONE), blocks(first, last)
            ok = in_bounds(lo_ref, hi_ref, e, first, last)
            p = jnp.exp(jnp.where(ok, mm(k_rows[wide], q_t[:, cols]) - lse_ref[h, :, cols], NEG))
            ds = (p * (mm(v_rows[wide], do_t[:, cols]) - del_ref[h, :, cols])).astype(BF)
            p_bf = p.astype(BF)
            if mine:
                out_ref[ZERO, h, :, blocks(e - ONE, e)] = (mm(k_t[:, wide], ds) * SCALE).astype(BF)
            for kb in range(max(first, ONE), min(last, last_own)):
                rows = blocks(kb - first, kb - first + ONE)
                dv[kb] += mm_nt(do_t[:, cols], p_bf[rows])
                dk[kb] += mm_nt(q_t[:, cols], ds[rows])
        for kb in range(ONE, last_own):
            out_ref[ONE, h, :, blocks(kb - ONE, kb)] = dk[kb].astype(BF)
            out_ref[TWO, h, :, blocks(kb - ONE, kb)] = dv[kb].astype(BF)
    every_head(head)


def attn1_bwd(qkv, do_t, left, right, dleft, dright, lse_x, del_x, lo, hi):
    stat = spec((HPS, ONE, EXT), step_of, ZERO, ZERO)
    bound = spec((ONE, EXT))
    pair = [halo_head(ZERO), halo_head(ONE)]
    return call(
        attn1_bwd_body, (HSTEPS,),
        [own_head(ZERO), own_head(ONE), own_head(TWO), own_head(ZERO)] + pair * FOUR + [stat, stat, bound, bound],
        spec((THREE, HPS, HEAD, TOK), ZERO, step_of, ZERO, ZERO),
        sds((THREE, NHEAD, HEAD, TOK), BF),
        flops=NHEAD * 10 * TOK * EXT * HALF, nbytes=8 * MIB, name="attn1_bwd",
    )(qkv, qkv, qkv, do_t, left, left, right, right, dleft, dleft, dright, dright, lse_x, del_x, lo, hi)


ROWBLK = [slice(r, r + RB) for r in range(ZERO, TOK, RB)]
HALFT = NFT // TWO
SQRT_HALF = math.sqrt(SCALE * FOUR)
PDF_SCALE = SQRT_HALF / math.sqrt(math.pi)
STATS = 16


def normal_cdf(a):
    return SQRT_HALF * SQRT_HALF * (ONE + lax.erf(a * SQRT_HALF))


def att_block(ref, n):
    return ref.at[n % FOUR, n // FOUR] if ref.shape[ZERO] == FOUR else ref.at[n]


def half_rows(ref, which):
    n = ref.shape[ZERO] // TWO
    return ref.at[pl.ds(pl.multiple_of(which * n, n), n)]


def col_tile(ref, n):
    return ref.at[:, pl.ds(pl.multiple_of(n * FT, FT), FT)]


class Refs:
    def __init__(self, names, refs):
        self.__dict__.update(zip(names, refs))


class Swaps:
    def __init__(self, r):
        self.r, self.waits, self.n = r, [], ZERO
        self.core, self.partner = core_and_partner()
        self.other = ONE - self.core

    def remote(self, src, dst):
        cp = to_partner(self.partner, src, dst, self.r.ssem.at[self.n], self.r.rsem.at[self.n])
        return self.later(cp)

    def local(self, src, dst):
        return self.later(pltpu.make_async_copy(src, dst, self.r.lsem.at[self.n]))

    def later(self, cp):
        self.n += ONE
        self.waits.append(cp)
        return cp

    def wait(self):
        for cp in self.waits:
            cp.wait()


def mlp_body(*refs, names, fwd, bwd):
    r = Refs(names, refs)
    step = pl.program_id(ZERO)
    sw = Swaps(r)
    start, spread = [], []
    if fwd:
        start = [sw.remote(r.h, r.h_r), sw.remote(half_rows(r.of, sw.other), r.of_r),
                 sw.local(half_rows(r.of, sw.core), r.of_m)]
        m_out = [(sw.remote(r.m_s.at[HALFT * sw.other + n], col_tile(r.m_r, n)),
                  sw.local(r.m_s.at[HALFT * sw.core + n], col_tile(r.m_m, n))) for n in range(HALFT)]
    if bwd:
        start.append(sw.remote(r.dy, r.dy_r))
        dmid_out = sw.remote(r.dmid, r.dmid_r)
        du_out = [(sw.remote(r.du_s.at[n, sw.other], col_tile(r.du_r, n)),
                   sw.local(r.du_s.at[n, sw.core], col_tile(r.du_m, n))) for n in range(NFT)]

    @pl.when(step == ZERO)
    def _():
        if fwd:
            for n in range(NHEAD):
                r.of[HEAD * n:HEAD * n + HEAD, :] = att_block(r.o, n)[...]
            x1 = (r.x[...].astype(F32) + mm_tn(r.of[...], r.wp[...])).astype(BF)
            r.x1[...] = x1
            r.h[...] = norm_rows(x1, r.g[...])
            r.acc[...] = x1.astype(F32)
        if bwd:
            r.dacc[...] = jnp.zeros(r.dacc.shape, F32)
        meet_partner(sw.partner)
        for cp in start:
            cp.start()

    for rows in ROWBLK:
        if fwd:
            ua = mm(r.h[rows], r.wa[...]).astype(BF)
            ub = mm(r.h[rows], r.wb[...]).astype(BF)
            if not bwd:
                r.u[ZERO, rows] = ua
                r.u[ONE, rows] = ub
        else:
            ua, ub = r.u[ZERO, rows], r.u[ONE, rows]
        a, b = ua.astype(F32), ub.astype(F32)
        cdf = normal_cdf(a)
        gate = a * cdf
        if fwd:
            m = (gate * b).astype(BF)
            r.m_s[step, rows] = m
            r.acc[rows] += mm(m, r.wo[...])
        if bwd:
            dm = mm_nt(r.dy[rows], r.wo[...]).astype(BF).astype(F32)
            pdf = jnp.exp(a * a * (SCALE * FOUR - ONE)) * PDF_SCALE
            db = (dm * gate).astype(BF)
            da = (dm * b * (cdf + a * pdf)).astype(BF)
            r.du_s[step, ZERO, rows] = da
            r.du_s[step, ONE, rows] = db
            r.dacc[rows] += mm_nt(da, r.wa[...]) + mm_nt(db, r.wb[...])

    for n in range(NFT):
        @pl.when(step == n)
        def _(n=n):
            if fwd:
                there, here = m_out[n % HALFT]

                @pl.when(sw.core == n // HALFT)
                def _():
                    here.start()

                @pl.when(sw.other == n // HALFT)
                def _():
                    there.start()
            if bwd:
                for cp in du_out[n]:
                    cp.start()

    @pl.when(step == NFT - ONE)
    def _():
        if fwd:
            r.y[...] = r.acc[...].astype(BF)
        if bwd:
            d_ln, gg = norm_rows_grad(r.x1[...], r.g[...], r.dacc[...].astype(BF))
            r.gg[...] = gg
            d_mid = add_bf(r.dy[...], d_ln)
            r.dmid[...] = d_mid
            dmid_out.start()
            d_att = mm_nt(r.wp[...], d_mid).astype(BF)
            for n in range(NHEAD):
                rows = slice(HEAD * n, HEAD * n + HEAD)
                blk = d_att[rows]
                att_block(r.d_o, n)[...] = blk
                if fwd:
                    r.delta[n:n + ONE, :] = jnp.sum(blk.astype(F32) * r.of[rows].astype(F32), axis=ZERO, keepdims=True)
            if fwd:
                r.delta[NHEAD:, :] = jnp.zeros((STATS - NHEAD, TOK), F32)
        sw.wait()


def mlp_call(layer, cid, fwd, bwd, w_proj, gain, w_in, w_out, x=None, o_t=None, dy=None, x1=None, u=None, oshape=None):
    toks, tok_spec, vec = sds(ALLTOK, BF), spec(ALLTOK), spec((ONE, DM))
    u_spec = spec((TWO, TOK, FT), ZERO, ZERO, step_of)
    half_o = sds((DM // TWO, TOK), BF)
    half_m, half_u = sds((TOK, FF // TWO), BF), sds((TOK, FF), BF)
    ins = [('wp', w_proj, spec((None, DM, DM), layer, ZERO, ZERO)), ('g', gain, vec),
           ('wa', w_in, weight_cols(layer, FT)), ('wb', w_in, weight_cols(layer, FT, NFT)),
           ('wo', w_out, spec((None, FT, DM), layer, step_of, ZERO))]
    outs, scratch = [], []
    if fwd:
        ins += [('x', x, tok_spec), ('o', o_t, spec(o_t.shape))]
        outs += [('y', toks, tok_spec), ('h', toks, tok_spec), ('h_r', toks, ANY), ('of_m', half_o, ANY), ('of_r', half_o, ANY),
                 ('m_m', half_m, ANY), ('m_r', half_m, ANY)]
        scratch += [('acc', pltpu.VMEM(ALLTOK, F32)), ('of', pltpu.VMEM((DM, TOK), BF)), ('m_s', pltpu.VMEM((NFT, TOK, FT), BF))]
    if fwd and not bwd:
        outs += [('x1', toks, tok_spec), ('u', sds((TWO, TOK, FF), BF), u_spec)]
    if bwd:
        ins += [('dy', dy, tok_spec)]
        outs += [('dmid', toks, tok_spec), ('gg', sds((ONE, DM), F32), vec), ('d_o', sds(oshape, BF), spec(oshape)),
                 ('dy_r', toks, ANY), ('dmid_r', toks, ANY), ('du_m', half_u, ANY), ('du_r', half_u, ANY)]
        scratch += [('dacc', pltpu.VMEM(ALLTOK, F32)), ('du_s', pltpu.VMEM((NFT, TWO, TOK, FT), BF))]
    if fwd and bwd:
        outs += [('delta', sds((STATS, TOK), F32), spec((STATS, TOK)))]
        scratch += [('x1', pltpu.VMEM(ALLTOK, BF))]
    if not fwd:
        ins += [('x1', x1, tok_spec), ('u', u, u_spec)]
    sems = DMA((TWO * NFT + 8 + NFT,))
    scratch += [('ssem', sems), ('rsem', sems), ('lsem', sems)]
    names = [n for n, *_ in ins + outs + scratch]
    name = "mlp_" + "fwd" * fwd + "bwd" * bwd
    got = call(
        functools.partial(mlp_body, names=names, fwd=fwd, bwd=bwd), (NFT,),
        [sp for *_, sp in ins], [sp for *_, sp in outs], [sh for _, sh, _ in outs], scratch=[sh for _, sh in scratch],
        flops=TWO * TOK * DM * (DM + THREE * FF) * (fwd + bwd), nbytes=26 * MIB, name=name, cid=cid,
    )(*[arr for _, arr, _ in ins])
    return Refs([n for n, *_ in outs], got)


def qkv_bwd_body(d_ref, cos_ref, sin_ref, w_ref, x_ref, g_ref, dmid_ref, dx_ref, gg_ref, dtm_ref, dtr_ref,
                 acc, dt_s, dt_all, ssem, rsem, lsem):
    step = pl.program_id(ZERO)
    core, partner = core_and_partner()

    def dst(ref, n):
        rows = PROJ
        return ref.at[pl.ds(pl.multiple_of(n * rows, rows), rows)]

    def copies(n):
        return (to_partner(partner, dt_s.at[ONE - core, n], dst(dtr_ref, n), ssem.at[n], rsem.at[n]),
                pltpu.make_async_copy(dt_s.at[core, n], dst(dtm_ref, n), lsem.at[n]))

    @pl.when(step == ZERO)
    def _():
        acc[...] = jnp.zeros(acc.shape, F32)
        meet_partner(partner)

    def put(chunk, head, row, val):
        at = LANE * chunk + row + HEAD * (head % TWO)
        dt_s[head // TWO, step, at:at + val.shape[ZERO]] = val
        at = RB * chunk + row + HEAD * head
        dt_all[at:at + val.shape[ZERO]] = val

    @pl.when(step < TWO)
    def _():
        cos, sin = cos_ref[...], sin_ref[...]
        for chunk in CHUNKS:
            for head in range(FOUR):
                d_head = head_rows(d_ref, chunk, head)[...].astype(F32)
                da, db = d_head[:HALF], d_head[HALF:]
                put(chunk, head, ZERO, (da * cos + db * sin).astype(BF))
                put(chunk, head, HALF, (db * cos - da * sin).astype(BF))

    @pl.when(step == TWO)
    def _():
        for chunk in CHUNKS:
            for head in range(FOUR):
                put(chunk, head, ZERO, head_rows(d_ref, chunk, head)[...])

    for cp in copies(step):
        cp.start()
    acc[...] += mm(w_ref[...], dt_all[...])

    @pl.when(step == TWO)
    def _():
        d_ln, gg = norm_rows_grad(x_ref[...], g_ref[...], acc[...].T.astype(BF))
        gg_ref[...] = gg
        dx_ref[...] = add_bf(dmid_ref[...], d_ln)
        for n in range(THREE):
            for cp in copies(n):
                cp.wait()


def qkv_bwd(d_qkv, cos_t, sin_t, w_qkv, x, gain, d_mid, layer, dest_major, cid):
    table = spec((HALF, TOK))
    half = sds((THREE * PROJ, TOK), BF)
    return call(
        qkv_bwd_body, (THREE,),
        [heads_spec(dest_major), table, table, weight_cols(layer, DM), spec(ALLTOK), spec((ONE, DM)), spec(ALLTOK)],
        [spec(ALLTOK), spec((ONE, DM)), ANY, ANY],
        [sds(ALLTOK, BF), sds((ONE, DM), F32), half, half],
        scratch=[pltpu.VMEM((DM, TOK), F32), pltpu.VMEM((TWO, THREE, PROJ, TOK), BF), pltpu.VMEM((DM, TOK), BF),
                 DMA((THREE,)), DMA((THREE,)), DMA((THREE,))],
        flops=TWO * TOK * DM * THREE * DM, nbytes=10 * MIB, name="qkv_bwd", cid=cid,
    )(d_qkv, cos_t, sin_t, w_qkv, x, gain, d_mid)


DOWN = FF // TWO
UP = FF
QKV = THREE * PROJ
MLP_ROWS = DOWN + UP
ATT_ROWS = PROJ + QKV
RING_ROWS = TWO * ATT_ROWS + MLP_ROWS
NDOWN = DOWN // DM
GRAD_REFS = 9


def grad_call(body, grads, steps, in_specs, args, rows, first_row, total, scratch=()):
    shared = [] if grads is None else [grads]
    first = first_row // rows
    return call(
        body, (steps,), [ANY] * len(shared) + in_specs,
        spec((rows, DM), lambda s: first + s, ZERO), sds((total, DM), F32), scratch=scratch,
        flops=FOUR * steps * rows * TOK * DM, nbytes=20 * MIB, name=body.__name__,
        alias={ZERO: ZERO} if shared else None,
    )(*shared, *args)


def grad_mlp_body(*refs):
    ma, mb, dya, dyb, ha, hb, dua, dub, out_ref, h_t = refs[-GRAD_REFS - ONE:]
    step = pl.program_id(ZERO)

    @pl.when(step < NDOWN)
    def _():
        out_ref[...] = mm_tn(ma[...], dya[...]) + mm_tn(mb[...], dyb[...])

    @pl.when(step == NDOWN)
    def _():
        h_t[ZERO] = ha[...].T
        h_t[ONE] = hb[...].T

    @pl.when(step >= NDOWN)
    def _():
        out_ref[...] = mm(h_t[ZERO], dua[...]) + mm(h_t[ONE], dub[...])


def grad_mlp(grads, m, m_r, dy, dy_r, h, h_r, du, du_r, first_row, total):
    toks = spec(ALLTOK)
    m_col = spec(ALLTOK, ZERO, lambda s: jnp.minimum(s, NDOWN - ONE))
    du_col = spec(ALLTOK, ZERO, lambda s: jnp.maximum(s - NDOWN, ZERO))
    return grad_call(grad_mlp_body, grads, NDOWN + UP // DM, [m_col, m_col, toks, toks, toks, toks, du_col, du_col],
                     (m, m_r, dy, dy_r, h, h_r, du, du_r), DM, first_row, total, scratch=[pltpu.VMEM((TWO, DM, TOK), BF)])


def grad_att_body(*refs):
    oa, ob, dma, dmb, ta, tb, ha, hb, out_ref = refs[-GRAD_REFS:]
    step = pl.program_id(ZERO)

    @pl.when(step == ZERO)
    def _():
        out_ref[...] = mm(oa[...], dma[...]) + mm(ob[...], dmb[...])

    @pl.when(step > ZERO)
    def _():
        out_ref[...] = mm(ta[...], ha[...]) + mm(tb[...], hb[...])


def grad_att(grads, of, of_r, dmid, dmid_r, dt, dt_r, h, h_r, first_row):
    toks = spec(ALLTOK)
    blk = (PROJ, TOK)
    dt_row = spec(blk, lambda s: jnp.maximum(s - ONE, ZERO), ZERO)
    return grad_call(grad_att_body, grads, ONE + QKV // PROJ, [spec(blk), spec(blk), toks, toks, dt_row, dt_row, toks, toks],
                     (of, of_r, dmid, dmid_r, dt, dt_r, h, h_r), PROJ, first_row, RING_ROWS)


NB, NS = 5, 6
CH = RING_ROWS // (NB * FOUR)
SB, LF = CH // FOUR, CH // 16
RS = 9
LAST = RS + RS
ADD_ROWS = 96


def ring_body(g_ref, ln_ref, f_ref, lnout_ref, bufa, bufb, bufc, gath, stage, lnbuf,
              ssem, rsem, psem, qsem, csem, stsem, lns, lnr):
    core, partner = core_and_partner()
    zy = lax.axis_index('zy')
    pos = (lax.axis_index('sp'), lax.rem(zy, FOUR), zy // FOUR)
    streams = [(c, sg) for c in range(THREE) for sg in (ONE, -ONE)]
    bufs, sizes = (bufa, bufb, bufc), (CH, SB, LF)
    peers = range(ONE, FOUR)

    def mod4(v):
        return lax.rem(v + 8, FOUR)

    def at(axis, val):
        if axis == ZERO:
            return {'sp': val}
        yz = (val, pos[TWO]) if axis == ONE else (pos[ONE], val)
        return {'zy': yz[ONE] * FOUR + yz[ZERO]}

    def shifted(axis, d):
        return at(axis, mod4(pos[axis] + d))

    def axis_of(s, ph):
        return (streams[s][ZERO] + ph) % THREE

    def idx(s, ph, t):
        return mod4(pos[axis_of(s, ph)] - streams[s][ONE] * t)

    def own(s, ph):
        return idx(s, ph, -ONE)

    def base(b):
        return b * (FOUR * CH)

    bar = pltpu.get_barrier_semaphore()
    for ax in range(THREE):
        for d in peers:
            pl.semaphore_signal(bar, inc=ONE, device_id=shifted(ax, d), device_id_type=MESH)
    pl.semaphore_signal(bar, inc=ONE, device_id=partner, device_id_type=MESH)
    pl.semaphore_wait(bar, 10)

    def rows(ref, start, n):
        return ref.at[pl.ds(pl.multiple_of(start, LF), n)]

    def grows(s, start, n):
        return g_ref.at[pl.ds(pl.multiple_of(start, LF), n), LANE * s:LANE * s + LANE]

    def frows(s, start, n):
        return f_ref.at[core, pl.ds(pl.multiple_of(start, LF), n), LANE * s:LANE * s + LANE]

    def same_bytes(b, k):
        if k < RS:
            return bufs[k // THREE].at[b, k % THREE]
        n = sizes[TWO - (k - RS) // THREE]
        return gath.at[b] if n == CH else gath.at[b, :, pl.ds(ZERO, n)]

    def wait_for(ref, sem):
        pltpu.make_async_copy(ref, ref, sem).wait()

    def send(b, s, k):
        ph = k // THREE if k < RS else TWO - (k - RS) // THREE
        t = k % THREE
        n = sizes[ph]
        if k < RS:
            dst = bufs[ph].at[b, t, s]
            if t:
                src = bufs[ph].at[b, t - ONE, s]
            elif ph:
                src = rows(bufs[ph - ONE].at[b, TWO, s], idx(s, ph, ZERO) * n, n)
            else:
                src = grows(s, base(b) + idx(s, ZERO, ZERO) * n, n)
        elif ph:
            off = own(s, ONE) * SB if ph == TWO else ZERO
            src = dst = rows(gath.at[b, s], off + idx(s, ph, t - ONE) * n, n)
        else:
            dst = frows(s, base(b) + idx(s, ZERO, t - ONE) * n, n)
            src = dst if t else gath.at[b, s]
        pltpu.make_async_remote_copy(src_ref=src, dst_ref=dst, send_sem=ssem.at[b, k], recv_sem=rsem.at[b, k],
                                     device_id=shifted(axis_of(s, ph), streams[s][ONE]), device_id_type=MESH).start()

    def stage_load(n):
        t, b, slot = n // NB, lax.rem(n, NB), lax.rem(n, TWO)
        for s in range(NS):
            pltpu.make_async_copy(grows(s, base(b) + idx(s, ZERO, t + ONE) * CH, CH), stage.at[slot, s],
                                  stsem.at[slot]).start()

    def ln_copy(ph, d):
        return pltpu.make_async_remote_copy(
            src_ref=lnbuf.at[ph, THREE] if ph else ln_ref, dst_ref=lnbuf.at[ph, d - ONE], send_sem=lns.at[ph, d - ONE],
            recv_sem=lnr.at[ph, d - ONE], device_id=shifted(ph, d) if ph < THREE else partner, device_id_type=MESH)

    def ln_sum(ph):
        vals = [lnbuf[ph, THREE] if ph else ln_ref[...]] + [lnbuf[ph, d - ONE] for d in peers]
        total = jnp.zeros_like(vals[ZERO])
        for p in range(FOUR):
            term = vals[ZERO]
            for d in peers:
                term = jnp.where(mod4(pos[ph] - d) == p, vals[d], term)
            total = total + term
        return total

    def batches(fn, start=ZERO):
        def body(b, c):
            fn(b)
            return c
        lax.fori_loop(start, NB, body, ZERO)

    def first(b):
        for s in range(NS):
            send(b, s, ZERO)

    first(ZERO)
    stage_load(jnp.int32(ZERO))
    for d in peers:
        ln_copy(ZERO, d).start()
    batches(first, ONE)

    for k in range(RS):
        ph, t = k // THREE, k % THREE
        buf, size = bufs[ph], sizes[ph]

        def step(b, k=k, ph=ph, t=t, buf=buf, size=size):
            n = k * NB + b
            slot = lax.rem(n, TWO)
            if not ph:
                @pl.when(n < THREE * NB - ONE)
                def _():
                    stage_load(n + ONE)
                wait_for(stage.at[slot], stsem.at[slot])
            wait_for(same_bytes(b, k), rsem.at[b, k])
            for s in range(NS):
                if ph:
                    off = pl.multiple_of(idx(s, ph, t + ONE) * size, LF)
                    buf[b, t, s] += bufs[ph - ONE][b, TWO, s, pl.ds(off, size)]
                else:
                    @pl.loop(ZERO, CH, step=ADD_ROWS)
                    def _(r):
                        at_r = pl.ds(pl.multiple_of(r, ADD_ROWS), ADD_ROWS)
                        buf[b, t, s, at_r] += stage[slot, s, at_r]
                if k == RS - ONE:
                    off = pl.multiple_of(own(s, ONE) * SB + own(s, TWO) * LF, LF)
                    gath[b, s, pl.ds(off, LF)] = bufc[b, TWO, s]
                send(b, s, k + ONE)

        batches(step)
        if k < SIX and k % TWO == ZERO:
            lp = k // TWO
            for d in peers:
                ln_copy(lp, d).wait()
            lnbuf[lp + ONE, THREE] = ln_sum(lp)
            for d in peers if lp < TWO else (ONE,):
                ln_copy(lp + ONE, d).start()

    def hand_over(b, s, j, src, start):
        pltpu.make_async_remote_copy(src_ref=src, dst_ref=frows(s, start, CH), send_sem=psem.at[b, j], recv_sem=qsem.at[b, j],
                                     device_id=partner, device_id_type=MESH).start()

    for k in range(RS, LAST):
        def step(b, k=k):
            wait_for(same_bytes(b, k), rsem.at[b, k])
            piece = k - (LAST - FOUR)
            for s in range(NS):
                if k < LAST - ONE:
                    send(b, s, k + ONE)
                if piece >= ZERO:
                    start = base(b) + idx(s, ZERO, piece - ONE) * CH
                    if piece:
                        hand_over(b, s, piece, frows(s, start, CH), start)
                    else:
                        pltpu.make_async_copy(gath.at[b, s], frows(s, start, CH), csem.at[b]).start()
                        hand_over(b, s, piece, gath.at[b, s], start)
        batches(step)

    ln_copy(THREE, ONE).wait()
    lnout_ref[...] = lnbuf[THREE, THREE] + lnbuf[THREE, ZERO]

    def finish(b):
        for k in range(LAST):
            wait_for(same_bytes(b, k), ssem.at[b, k])
        for j in range(FOUR):
            wait_for(gath.at[b], psem.at[b, j])
            wait_for(gath.at[b], qsem.at[b, j])
        wait_for(gath.at[b], csem.at[b])
    batches(finish)


def ring_all_reduce(g, ln, cid):
    vmem = pl.BlockSpec(memory_space=pltpu.VMEM)
    return pl.pallas_call(
        ring_body,
        in_specs=[ANY, vmem],
        out_specs=[ANY, vmem],
        out_shape=[sds((TWO, RING_ROWS, DM), F32), sds(ln.shape, F32)],
        scratch_shapes=[
            pltpu.VMEM((NB, THREE, NS, CH, LANE), F32), pltpu.VMEM((NB, THREE, NS, SB, LANE), F32),
            pltpu.VMEM((NB, THREE, NS, LF, LANE), F32), pltpu.VMEM((NB, NS, CH, LANE), F32),
            pltpu.VMEM((TWO, NS, CH, LANE), F32),
            pltpu.VMEM((FOUR, FOUR) + ln.shape, F32),
            DMA((NB, LAST)), DMA((NB, LAST)), DMA((NB, FOUR)), DMA((NB, FOUR)), DMA((NB,)), DMA((TWO,)),
            DMA((FOUR, THREE)), DMA((FOUR, THREE)),
        ],
        compiler_params=pltpu.CompilerParams(collective_id=cid, has_side_effects=True, vmem_limit_bytes=60 * MIB),
        cost_estimate=pl.CostEstimate(flops=MIB * MIB // FOUR, bytes_accessed=200 * MIB, transcendentals=ZERO),
        name="ring_all_reduce",
    )(g, ln)


def copy_body(in_ref, out_ref):
    out_ref[...] = in_ref[...]


def turn_body(a_ref, b_ref, out_ref):
    for n in CHUNKS:
        rows, col = slice(LANE * n, LANE * n + LANE), RB * n
        out_ref[ZERO, :, col:col + LANE] = a_ref[ZERO, rows].T
        out_ref[ZERO, :, col + LANE:col + RB] = b_ref[ZERO, rows].T


WHOLE = (ONE, DM, DM)
BLOCK3 = (ONE, PROJ, DM)
OUT_SHAPE, IN_SHAPE = (TWO, FF, DM), (TWO, DM, TWO * FF)
UNPACK = dict(nbytes=100 * MIB)
C_OF = lambda l, c, *_: c


def unpack_ring(f):
    att = lambda l, *_: (ONE - l) * (ATT_ROWS + MLP_ROWS) // PROJ
    mlp0 = ATT_ROWS // DM
    g_out = call(copy_body, (TWO, NDOWN), [spec(WHOLE, step_of, lambda c, i: mlp0 + i, ZERO)],
                 spec(WHOLE, ZERO, lambda c, i: NDOWN * c + i, ZERO), sds(OUT_SHAPE, F32), **UNPACK)(f)
    g_in = call(copy_body, (TWO, FOUR), [spec(WHOLE, step_of, lambda c, j: mlp0 + NDOWN + j, ZERO)],
                spec(WHOLE, ZERO, ZERO, lambda c, j: FOUR * c + j), sds(IN_SHAPE, F32), **UNPACK)(f)
    g_proj = call(copy_body, (TWO, TWO), [spec(BLOCK3, C_OF, att, ZERO)], spec(BLOCK3, step_of, C_OF, ZERO),
                  sds((TWO, DM, DM), F32), **UNPACK)(f)
    row = lambda l, s: att(l) + ONE + s
    g_qkv = call(turn_body, (TWO, THREE), [spec(BLOCK3, ZERO, row, ZERO), spec(BLOCK3, ONE, row, ZERO)],
                 spec(WHOLE, step_of, ZERO, C_OF), sds((TWO, DM, THREE * DM), F32), **UNPACK)(f, f)
    return g_qkv, g_proj, g_in, g_out


def pick_body(core_s, own_ref, other_ref, _, out_ref):
    mine = pl.program_id(ZERO) == ZERO

    @pl.when(mine)
    def _():
        out_ref[ZERO] = own_ref[...]

    @pl.when(jnp.logical_not(mine))
    def _():
        out_ref[ZERO] = other_ref[...]


def unpack_mlp(core, own, other, g_in, g_out):
    def write(out, n, first, at):
        rows_a = lambda p, i, *_: first + jnp.where(p == ZERO, i, n - ONE)
        rows_b = lambda p, i, *_: first + jnp.where(p == ZERO, ZERO, i)
        side = lambda p, c: (p + c[ZERO]) % TWO
        return call(pick_body, (TWO, n), [spec(ALLDM, rows_a, ZERO), spec(ALLDM, rows_b, ZERO), ANY],
                    spec(WHOLE, *at(lambda p, i, c: n * side(p, c) + i)), sds(out.shape, F32),
                    prefetch=ONE, alias={THREE: ZERO}, **UNPACK)(core, own, other, out)
    g_out = write(g_out, NDOWN, ZERO, lambda blk: (ONE, blk, ZERO))
    g_in = write(g_in, FOUR, NDOWN, lambda blk: (ONE, ZERO, blk))
    return g_in, g_out


def rope_tables(pos, base):
    inv_freq = base ** (jnp.arange(HALF).astype(F32) * (-TWO / HEAD))
    angles = inv_freq[:, None] * pos.astype(F32)[None, :]
    return jnp.cos(angles), jnp.sin(angles)


def solution(mesh):
    n_sp = mesh.shape['sp']
    by_core = mesh.devices.reshape(n_sp, mesh.shape['dp'] // TWO, TWO)
    mesh = Mesh(by_core, ('sp', 'zy', 'core'))
    dp_axes = ('zy', 'core')
    row_axes = dp_axes + ('sp',)
    token_spec = P(row_axes, None)
    to_right = [(i, i + ONE) for i in range(n_sp - ONE)]
    to_left = [(i + ONE, i) for i in range(n_sp - ONE)]
    swap_cores = [(ZERO, ONE), (ONE, ZERO)]
    cids = list(range(RS))

    def halo_swap(arr):
        from_left = lax.ppermute(arr[..., TOK - LANE:], 'sp', to_right)
        from_right = lax.ppermute(arr[..., :LANE], 'sp', to_left)
        return from_left, from_right

    def exchange(arr):
        return lax.all_to_all(arr, 'sp', ZERO, ZERO, tiled=True)

    def device_step(x_loc, cu_loc, pos_loc, w_qkv, w_proj, w_in, w_out, ln_attn, ln_mlp, d_out):
        sp = lax.axis_index('sp')
        core = lax.axis_index('core').reshape(ONE)
        cu = cu_loc[ZERO][:, None]

        def bounds_of(tok):
            start = jnp.max(jnp.where(cu <= tok, cu, ZERO), axis=ZERO)
            return start, jnp.min(jnp.where(cu > tok, cu, GRP), axis=ZERO)

        start, stop = bounds_of(jnp.arange(GRP)[None, :])
        tiles = start[::QT] // QT, (stop[QT - ONE::QT] + QT - ONE) // QT
        rows = start[None, :], stop[None, :]
        shift = sp * TOK - LANE
        tok_x = jnp.arange(EXT) + shift
        start_x, stop_x = bounds_of(tok_x[None, :])
        inside = (tok_x >= ZERO) & (tok_x < GRP)
        near = (jnp.where(inside, jnp.maximum(start_x, tok_x - WIN) - shift, ZERO)[None, :],
                jnp.where(inside, jnp.minimum(stop_x, tok_x + WIN + ONE) - shift, ZERO)[None, :])
        tab0, tab1 = [rope_tables(pos_loc, base) for base in BASES]
        la0, la1, lm0, lm1 = ln_attn[:ONE], ln_attn[ONE:], ln_mlp[:ONE], ln_mlp[ONE:]

        w_mlp = (w_in, w_out)
        h0, qkv0, h0r = qkv_fwd(x_loc, la0, w_qkv, ZERO, *tab0, True, cids[ONE])
        qkv0 = exchange(qkv0)
        oh0, lse0 = attn0_fwd(*tiles, qkv0, *rows)
        f0 = mlp_call(ZERO, cids[TWO], True, False, w_proj, lm0, *w_mlp, x=x_loc, o_t=exchange(oh0))
        x1 = f0.y
        h1, qkv1, h1r = qkv_fwd(x1, la1, w_qkv, ONE, *tab1, False, cids[THREE])
        qkv1 = qkv1.reshape((THREE * NHEAD, HEAD, TOK))
        kv_halo = halo_swap(qkv1[NHEAD:])
        o1, lse1 = attn1_fwd(qkv1, *kv_halo, *near)
        f1 = mlp_call(ONE, cids[FOUR], True, True, w_proj, lm1, *w_mlp, x=x1, o_t=o1, dy=d_out, oshape=(NHEAD, HEAD, TOK))
        g_side = grad_mlp(None, f1.m_m, f1.m_r, d_out, f1.dy_r, f1.h, f1.h_r, f1.du_m, f1.du_r, ZERO, MLP_ROWS)
        d_o1, g_side = lax.optimization_barrier((f1.d_o, g_side))
        g_side = lax.psum(g_side, ('sp', 'zy'))
        d_halo = halo_swap(jnp.concatenate([qkv1[:NHEAD], d_o1], axis=ZERO))
        stats = jnp.concatenate([lse1.reshape(NHEAD, TOK), f1.delta[:NHEAD]], axis=ZERO)
        from_left, from_right = halo_swap(stats)
        lse_x, del_x = jnp.concatenate([from_left, stats, from_right], axis=ONE).reshape(TWO, NHEAD, ONE, EXT)
        dqkv1 = attn1_bwd(qkv1, d_o1, *kv_halo, *d_halo, lse_x, del_x, *near)
        dx1, gga1, dt1, dt1r = qkv_bwd(dqkv1.reshape(THREE, THREE, FOUR, HEAD, TOK), *tab1, w_qkv, x1, la1, f1.dmid,
                                       ONE, False, cids[SIX])
        b0 = mlp_call(ZERO, cids[5], False, True, w_proj, lm0, *w_mlp, dy=dx1, x1=f0.x1, u=f0.u, oshape=oh0.shape)
        dqkv0 = exchange(attn0_bwd(*tiles, qkv0, oh0, exchange(b0.d_o), lse0, *rows))
        grads = grad_att(None, f1.of_m, f1.of_r, f1.dmid, f1.dmid_r, dt1, dt1r, h1, h1r, ZERO)
        grads = grad_mlp(grads, f0.m_m, f0.m_r, dx1, b0.dy_r, f0.h, f0.h_r, b0.du_m, b0.du_r, ATT_ROWS, RING_ROWS)
        dx0, gga0, dt0, dt0r = qkv_bwd(dqkv0, *tab0, w_qkv, x_loc, la0, b0.dmid, ZERO, True, cids[7])
        grads = grad_att(grads, f0.of_m, f0.of_r, b0.dmid, b0.dmid_r, dt0, dt0r, h0, h0r, ATT_ROWS + MLP_ROWS)

        gains = jnp.concatenate([gga0, gga1, b0.gg, f1.gg, jnp.zeros((FOUR, DM), F32)], axis=ZERO)
        summed, gains = ring_all_reduce(grads, gains, cids[ZERO])
        summed, g_side = lax.optimization_barrier((summed, g_side))
        from_partner = lax.ppermute(g_side, 'core', swap_cores)
        g_qkv, g_proj, g_in, g_out = unpack_ring(summed)
        g_in, g_out = unpack_mlp(core, g_side, from_partner, g_in, g_out)
        return f1.y, dx0, g_qkv, g_proj, g_in, g_out, gains[:TWO], gains[TWO:FOUR]

    in_specs = (token_spec, P(dp_axes, None), P(row_axes)) + (P(),) * SIX + (token_spec,)
    out_specs = (token_spec, token_spec) + (P(),) * SIX
    return jax.shard_map(device_step, mesh=mesh, in_specs=in_specs, out_specs=out_specs, check_vma=False)
```

```python
import functools
import math
import jax
import jax.numpy as jnp
from jax import lax
from jax.experimental import pallas as pl
from jax.experimental.pallas import tpu as pltpu
from jax.sharding import Mesh, PartitionSpec as P

ZERO, ONE, TWO, THREE, FOUR = range(5)
SIX, TWELVE = 6, 12
HEAD = 64
HALF = 32
NHEAD = 12
DM = 768
FF = 3072
TOK = 512
GRP = 2048
WIN = 64
LANE = 128
EPS = 1e-5
NEG = -1e30
SCALE = 0.125
BASES = (160000.0, 10000.0)
F32 = jnp.float32
BF = jnp.bfloat16
QT = 256
FT = 512
NFT = FF // FT
QTILES = GRP // QT
MIB = 1024 * 1024
ALLTOK = (TOK, DM)
PROJ = DM // 2
ALLDM = (DM, DM)
ANY = pl.BlockSpec(memory_space=pl.ANY)
DMA = pltpu.SemaphoreType.DMA
MESH = pl.DeviceIdType.MESH


def dot(a, b, ca, cb):
    return lax.dot_general(a, b, (((ca,), (cb,)), ((), ())), preferred_element_type=F32)


def mm(a, b):
    return dot(a, b, ONE, ZERO)


def mm_nt(a, b):
    return dot(a, b, ONE, ONE)


def mm_tn(a, b):
    return dot(a, b, ZERO, ZERO)


def call(body, grid, in_specs, out_specs, out_shape, scratch=(), prefetch=ZERO, flops=ZERO, nbytes=ZERO, name=None,
         cid=None, alias=None):
    extra = {} if cid is None else dict(collective_id=cid, has_side_effects=True)
    return pl.pallas_call(
        body,
        grid_spec=pltpu.PrefetchScalarGridSpec(
            num_scalar_prefetch=prefetch, grid=grid, in_specs=in_specs, out_specs=out_specs, scratch_shapes=scratch),
        out_shape=out_shape,
        input_output_aliases=alias or {},
        compiler_params=pltpu.CompilerParams(vmem_limit_bytes=60 * MIB, **extra),
        cost_estimate=pl.CostEstimate(flops=int(flops), bytes_accessed=int(nbytes), transcendentals=ZERO),
        name=name,
    )


def sds(shape, dtype):
    return jax.ShapeDtypeStruct(shape, dtype)


def spec(shape, *idx):
    idx = idx or (ZERO,) * len(shape)
    return pl.BlockSpec(shape, lambda *g: tuple(i(*g) if callable(i) else i for i in idx))


def step_of(s, *_):
    return s


def core_and_partner():
    core = lax.axis_index('core')
    return core, {'core': ONE - core}


def meet_partner(partner):
    bar = pltpu.get_barrier_semaphore()
    pl.semaphore_signal(bar, inc=ONE, device_id=partner, device_id_type=MESH)
    pl.semaphore_wait(bar, ONE)


def to_partner(partner, src, dst, ssem, rsem):
    return pltpu.make_async_remote_copy(src_ref=src, dst_ref=dst, send_sem=ssem, recv_sem=rsem,
                                        device_id=partner, device_id_type=MESH)


def norm_parts(x_bf):
    rows = x_bf.astype(F32)
    cen = rows - jnp.mean(rows, axis=ONE, keepdims=True)
    var = jnp.mean(cen * cen, axis=ONE, keepdims=True)
    return cen, lax.rsqrt(var + EPS)


def norm_rows(x_bf, gain):
    cen, inv = norm_parts(x_bf)
    return (cen * inv * gain).astype(BF)


def norm_rows_grad(x_bf, gain, d_bf):
    cen, inv = norm_parts(x_bf)
    hat = cen * inv
    d_out = d_bf.astype(F32)
    g_gain = jnp.sum(d_out * hat, axis=ZERO, keepdims=True)
    d_hat = d_out * gain
    d_x = inv * (d_hat - jnp.mean(d_hat, axis=ONE, keepdims=True) - hat * jnp.mean(d_hat * hat, axis=ONE, keepdims=True))
    return d_x.astype(BF), g_gain


def add_bf(a, b):
    return (a.astype(F32) + b.astype(F32)).astype(BF)


RB = 256
CHUNKS = range(DM // RB)


def head_rows(ref, chunk, head):
    return ref.at[head, ZERO, chunk] if ref.shape[ZERO] == FOUR else ref.at[ZERO, chunk, head]


def heads_spec(dest_major):
    if dest_major:
        return spec((FOUR, ONE, THREE, HEAD, TOK), ZERO, step_of, ZERO, ZERO, ZERO)
    return spec((ONE, THREE, FOUR, HEAD, TOK), step_of, ZERO, ZERO, ZERO, ZERO)


def weight_cols(layer, width, first=ZERO):
    return spec((None, DM, width), layer, ZERO, lambda s: first + s)


def qkv_fwd_body(x_ref, g_ref, w_ref, cos_ref, sin_ref, h_ref, out_ref, hr_ref, ssem, rsem):
    step = pl.program_id(ZERO)
    core, partner = core_and_partner()
    swap = to_partner(partner, h_ref, hr_ref, ssem, rsem)

    @pl.when(step == ZERO)
    def _():
        h_ref[...] = norm_rows(x_ref[...], g_ref[...])
        meet_partner(partner)
        swap.start()

    def product(chunk):
        return mm(h_ref[...], w_ref[:, RB * chunk:RB * chunk + RB]).astype(BF).astype(F32).T

    @pl.when(step < TWO)
    def _():
        cos, sin = cos_ref[...], sin_ref[...]
        for chunk in CHUNKS:
            t_rows = product(chunk)
            for head in range(FOUR):
                at = HEAD * head
                a, b = t_rows[at:at + HALF], t_rows[at + HALF:at + HEAD]
                out = head_rows(out_ref, chunk, head)
                out[:HALF] = (a * cos - b * sin).astype(BF)
                out[HALF:] = (b * cos + a * sin).astype(BF)

    @pl.when(step == TWO)
    def _():
        for chunk in CHUNKS:
            t_rows = product(chunk).astype(BF)
            for head in range(FOUR):
                head_rows(out_ref, chunk, head)[...] = t_rows[HEAD * head:HEAD * head + HEAD]
        swap.wait()


def qkv_fwd(x, gain, w_qkv, layer, cos_t, sin_t, dest_major, cid):
    oshape = (FOUR, THREE, THREE, HEAD, TOK) if dest_major else (THREE, THREE, FOUR, HEAD, TOK)
    table = spec((HALF, TOK))
    return call(
        qkv_fwd_body, (THREE,),
        [spec(ALLTOK), spec((ONE, DM)), weight_cols(layer, DM), table, table],
        [spec(ALLTOK), heads_spec(dest_major), ANY],
        [sds(ALLTOK, BF), sds(oshape, BF), sds(ALLTOK, BF)],
        scratch=[DMA, DMA],
        flops=TWO * TOK * DM * THREE * DM, nbytes=8 * MIB, name="qkv_fwd", cid=cid,
    )(x, gain, w_qkv, cos_t, sin_t)


def tile_src(i, *_):
    return i // TWO


def tile_side(i, *_):
    return i % TWO


Q_SPEC = spec((ONE, ONE, THREE, HEAD, QT), tile_src, ZERO, ZERO, ZERO, tile_side)
O_SPEC = spec((ONE, THREE, HEAD, QT), tile_src, ZERO, ZERO, tile_side)
ROW_SPEC = spec((ONE, QT), ZERO, step_of)
STAT_SPEC = spec((8, QT), ZERO, step_of)
GROUP_QKV = (FOUR, THREE, THREE, HEAD, TOK)


def kv_spec(part):
    return spec((FOUR, ONE, THREE, HEAD, TOK), ZERO, part, ZERO, ZERO, ZERO)


def key_tile(kt):
    return kt // TWO, pl.ds(pl.multiple_of((kt % TWO) * QT, QT), QT)


def key_rows(dst, k_ref):
    for src in range(FOUR):
        for h in range(THREE):
            dst[h, TOK * src:TOK * src + TOK] = k_ref[src, ZERO, h].T


def row_tile(kt):
    return pl.ds(pl.multiple_of(kt * QT, QT), QT)


def attn0_fwd_body(lo_s, hi_s, q_ref, k_ref, v_ref, st_ref, en_ref, o_ref, lse_ref, m_s, l_s, acc_s, kr_s, s_s, p_s):
    tile = pl.program_id(ZERO)
    heads, pair = range(THREE), range(TWO)

    @pl.when(tile == ZERO)
    def _():
        key_rows(kr_s, k_ref)

    m_s[...] = jnp.full(m_s.shape, NEG, F32)
    l_s[...] = jnp.zeros(l_s.shape, F32)
    acc_s[...] = jnp.zeros(acc_s.shape, F32)
    st, en = st_ref[...], en_ref[...]
    io = lax.broadcasted_iota(jnp.int32, (QT, QT), ZERO)
    q_t = [q_ref[ZERO, ZERO, h] * SCALE for h in heads]
    first, n_tiles = lo_s[tile], hi_s[tile] - lo_s[tile]

    def body(g, carry):
        kts = [first + TWO * g + a for a in pair]
        safe = [jnp.minimum(kt, QTILES - ONE) for kt in kts]
        for h in heads:
            for a in pair:
                s_s[h, a] = mm(kr_s[h, row_tile(safe[a])], q_t[h])
        for h in heads:
            row = slice(h, h + ONE)
            s = [jnp.where((io >= st - kts[a] * QT) & (io < en - kts[a] * QT), s_s[h, a], NEG) for a in pair]
            m_old = m_s[row]
            m_new = m_old
            for a in pair:
                m_new = jnp.maximum(m_new, jnp.max(s[a], axis=ZERO, keepdims=True))
            alpha = jnp.exp(m_old - m_new)
            total = l_s[row] * alpha
            for a in pair:
                p = jnp.exp(s[a] - m_new)
                total += jnp.sum(p, axis=ZERO, keepdims=True)
                p_s[h, a] = p.astype(BF)
            l_s[row] = total
            m_s[row] = m_new
            acc_s[h] = acc_s[h] * alpha
        for h in heads:
            part = acc_s[h]
            for a in pair:
                src, cols = key_tile(safe[a])
                part += mm(v_ref[src, ZERO, h, :, cols], p_s[h, a])
            acc_s[h] = part
        return carry

    lax.fori_loop(ZERO, (n_tiles + ONE) // TWO, body, ZERO)
    for h in heads:
        row = slice(h, h + ONE)
        o_ref[ZERO, h] = (acc_s[h] / l_s[row]).astype(BF)
        lse_ref[row] = m_s[row] + jnp.log(l_s[row])


def attn0_fwd(lo, hi, qkv, st, en):
    stat = pltpu.VMEM((8, QT), F32)
    return call(
        attn0_fwd_body, (QTILES,),
        [Q_SPEC, kv_spec(ONE), kv_spec(TWO), ROW_SPEC, ROW_SPEC],
        [O_SPEC, STAT_SPEC],
        [sds((FOUR, THREE, HEAD, TOK), BF), sds((8, GRP), F32)],
        scratch=[stat, stat, pltpu.VMEM((THREE, HEAD, QT), F32), pltpu.VMEM((THREE, GRP, HEAD), BF),
                 pltpu.VMEM((THREE, TWO, QT, QT), F32), pltpu.VMEM((THREE, TWO, QT, QT), BF)],
        prefetch=TWO, flops=TWELVE * GRP * GRP * HEAD, nbytes=6 * MIB, name="attn0_fwd",
    )(lo, hi, qkv, qkv, qkv, st, en)


def attn0_bwd_body(lo_s, hi_s, q_ref, k_ref, v_ref, o_ref, do_ref, lse_ref, st_ref, en_ref, out_ref,
                   dk_s, dv_s, dq_s, kr_s, vr_s, s_s, d_s, p_s, t_s):
    tile = pl.program_id(ZERO)
    heads = range(THREE)

    @pl.when(tile == ZERO)
    def _():
        dk_s[...] = jnp.zeros(dk_s.shape, F32)
        dv_s[...] = jnp.zeros(dv_s.shape, F32)
        key_rows(kr_s, k_ref)
        key_rows(vr_s, v_ref)

    dq_s[...] = jnp.zeros(dq_s.shape, F32)
    st, en = st_ref[...], en_ref[...]
    io = lax.broadcasted_iota(jnp.int32, (QT, QT), ZERO)
    q_t = [q_ref[ZERO, ZERO, h] * SCALE for h in heads]
    do_t = [do_ref[ZERO, h] for h in heads]
    q_rows, do_rows = [q_t[h].T for h in heads], [do_t[h].T for h in heads]
    delta = [jnp.sum(do_t[h].astype(F32) * o_ref[ZERO, h].astype(F32), axis=ZERO, keepdims=True) for h in heads]
    lse = [lse_ref[h:h + ONE] for h in heads]

    def body(kt, carry):
        base = kt * QT
        src, cols = key_tile(kt)
        rows = row_tile(kt)
        ok = (io >= st - base) & (io < en - base)
        for h in heads:
            s_s[h] = mm(kr_s[h, rows], q_t[h])
            d_s[h] = mm(vr_s[h, rows], do_t[h])
        for h in heads:
            p = jnp.exp(jnp.where(ok, s_s[h] - lse[h], NEG))
            p_s[h] = p.astype(BF)
            t_s[h] = (p * (d_s[h] - delta[h])).astype(BF)
        for h in heads:
            dv_s[h, rows] += mm(p_s[h], do_rows[h])
            dk_s[h, rows] += mm(t_s[h], q_rows[h])
            dq_s[h] += mm(k_ref[src, ZERO, h, :, cols], t_s[h])
        return carry

    lax.fori_loop(lo_s[tile], hi_s[tile], body, ZERO)
    src, cols = key_tile(tile)
    for h in heads:
        out_ref[src, ZERO, h, :, cols] = (dq_s[h] * SCALE).astype(BF)

    @pl.when(tile == QTILES - ONE)
    def _():
        for src in range(FOUR):
            for h in heads:
                out_ref[src, ONE, h] = dk_s[h, TOK * src:TOK * src + TOK].T.astype(BF)
                out_ref[src, TWO, h] = dv_s[h, TOK * src:TOK * src + TOK].T.astype(BF)


def attn0_bwd(lo, hi, qkv, o_t, do_t, lse, st, en):
    acc, rows = pltpu.VMEM((THREE, GRP, HEAD), F32), pltpu.VMEM((THREE, GRP, HEAD), BF)
    sq32, sq16 = pltpu.VMEM((THREE, QT, QT), F32), pltpu.VMEM((THREE, QT, QT), BF)
    return call(
        attn0_bwd_body, (QTILES,),
        [Q_SPEC, kv_spec(ONE), kv_spec(TWO), O_SPEC, O_SPEC, STAT_SPEC, ROW_SPEC, ROW_SPEC],
        spec(GROUP_QKV), sds(GROUP_QKV, BF),
        scratch=[acc, acc, pltpu.VMEM((THREE, HEAD, QT), F32), rows, rows, sq32, sq32, sq16, sq16],
        prefetch=TWO, flops=30 * GRP * GRP * HEAD, nbytes=TWELVE * MIB, name="attn0_bwd",
    )(lo, hi, qkv, qkv, qkv, o_t, do_t, lse, st, en)


NBLK = TOK // LANE
EXT = TOK + TWO * LANE


HPS = 4
HSTEPS = NHEAD // HPS


def heads_of(width, part):
    return spec((HPS, HEAD, width), lambda n: HSTEPS * part + n, ZERO, ZERO)


def own_head(part):
    return heads_of(TOK, part)


def halo_head(part):
    return heads_of(LANE, part)


def joined(left, mid, right, h):
    return jnp.concatenate([left[h], mid[h], right[h]], axis=ONE)


def blocks(first, last):
    return slice(LANE * first, LANE * last)


REACH = LANE + TWO * WIN
AHEAD_FWD, AHEAD_BWD = 4, 2


def in_bounds(lo_ref, hi_ref, blk, first, n):
    io = lax.broadcasted_iota(jnp.int32, (n, LANE), ZERO) + first
    cols = blocks(blk, blk + ONE)
    return (io >= lo_ref[:, cols]) & (io < hi_ref[:, cols])


def every_head(fn, ahead):
    def body(g, c):
        fn([ahead * g + a for a in range(ahead)])
        return c
    lax.fori_loop(ZERO, HPS // ahead, body, ZERO)


def attn1_fwd_body(q_ref, k_ref, v_ref, kl_ref, vl_ref, kr_ref, vr_ref, lo_ref, hi_ref, o_ref, lse_ref, s_s, p_s):
    def some(heads):
        v_all = []
        for a, h in enumerate(heads):
            q_t = q_ref[h] * SCALE
            k_rows = joined(kl_ref, k_ref, kr_ref, h).T
            v_all.append(joined(vl_ref, v_ref, vr_ref, h)[:, WIN:EXT - WIN])
            for i in range(NBLK):
                at = LANE * i + WIN
                s_s[a, i] = mm(k_rows[at:at + REACH], q_t[:, blocks(i, i + ONE)])
        for a, h in enumerate(heads):
            for i in range(NBLK):
                s = jnp.where(in_bounds(lo_ref, hi_ref, i + ONE, LANE * i + WIN, REACH), s_s[a, i], NEG)
                m = jnp.max(s, axis=ZERO, keepdims=True)
                e = jnp.exp(s - m)
                l = jnp.sum(e, axis=ZERO, keepdims=True)
                p_s[a, i] = (e * (ONE / l)).astype(BF)
                lse_ref[h, :, blocks(i, i + ONE)] = m + jnp.log(l)
        for a, h in enumerate(heads):
            for i in range(NBLK):
                o_ref[h, :, blocks(i, i + ONE)] = mm(v_all[a][:, LANE * i:LANE * i + REACH], p_s[a, i]).astype(BF)
    every_head(some, AHEAD_FWD)


def attn1_fwd(qkv, left, right, lo, hi):
    bound = spec((ONE, EXT))
    return call(
        attn1_fwd_body, (HSTEPS,),
        [own_head(ZERO), own_head(ONE), own_head(TWO), halo_head(ZERO), halo_head(ONE), halo_head(ZERO), halo_head(ONE),
         bound, bound],
        [own_head(ZERO), spec((HPS, ONE, TOK), step_of, ZERO, ZERO)],
        [sds((NHEAD, HEAD, TOK), BF), sds((NHEAD, ONE, TOK), F32)],
        scratch=[pltpu.VMEM((AHEAD_FWD, NBLK, REACH, LANE), F32), pltpu.VMEM((AHEAD_FWD, NBLK, REACH, LANE), BF)],
        flops=NHEAD * FOUR * TOK * EXT * HALF, nbytes=FOUR * MIB, name="attn1_fwd",
    )(qkv, qkv, qkv, left, left, right, right, lo, hi)


def attn1_bwd_body(q_ref, k_ref, v_ref, do_ref, kl_ref, vl_ref, kr_ref, vr_ref, ql_ref, dl_ref, qr_ref, dr_ref,
                   lse_ref, del_ref, lo_ref, hi_ref, out_ref, s_s, d_s, p_s, t_s):
    def window(e):
        if e == ZERO:
            return LANE, WIN
        if e > NBLK:
            return TOK + WIN, WIN
        return LANE * e - WIN, REACH

    def some(heads):
        for a, h in enumerate(heads):
            q_t = joined(ql_ref, q_ref, qr_ref, h) * SCALE
            do_t = joined(dl_ref, do_ref, dr_ref, h)
            k_rows, v_rows = joined(kl_ref, k_ref, kr_ref, h).T, joined(vl_ref, v_ref, vr_ref, h).T
            for e in range(NBLK + TWO):
                first, n = window(e)
                cols = blocks(e, e + ONE)
                s_s[a, e, :n] = mm(k_rows[first:first + n], q_t[:, cols])
                d_s[a, e, :n] = mm(v_rows[first:first + n], do_t[:, cols])
        for a, h in enumerate(heads):
            for e in range(NBLK + TWO):
                first, n = window(e)
                cols = blocks(e, e + ONE)
                ok = in_bounds(lo_ref, hi_ref, e, first, n)
                p = jnp.exp(jnp.where(ok, s_s[a, e, :n] - lse_ref[h, :, cols], NEG))
                p_s[a, first:first + n, cols] = p.astype(BF)
                t_s[a, first:first + n, cols] = (p * (d_s[a, e, :n] - del_ref[h, :, cols])).astype(BF)
        for a, h in enumerate(heads):
            q_t = joined(ql_ref, q_ref, qr_ref, h) * SCALE
            do_t = joined(dl_ref, do_ref, dr_ref, h)
            k_t = joined(kl_ref, k_ref, kr_ref, h)
            for b in range(ONE, NBLK + ONE):
                cols, rows, wide = blocks(b, b + ONE), blocks(b, b + ONE), blocks(b - ONE, b + TWO)
                out = blocks(b - ONE, b)
                out_ref[ZERO, h, :, out] = (mm(k_t[:, wide], t_s[a, wide, cols]) * SCALE).astype(BF)
                out_ref[ONE, h, :, out] = mm_nt(q_t[:, wide], t_s[a, rows, wide]).astype(BF)
                out_ref[TWO, h, :, out] = mm_nt(do_t[:, wide], p_s[a, rows, wide]).astype(BF)

    @pl.when(pl.program_id(ZERO) == ZERO)
    def _():
        p_s[...] = jnp.zeros(p_s.shape, BF)
        t_s[...] = jnp.zeros(t_s.shape, BF)

    every_head(some, AHEAD_BWD)


def attn1_bwd(qkv, do_t, left, right, dleft, dright, lse_x, del_x, lo, hi):
    stat = spec((HPS, ONE, EXT), step_of, ZERO, ZERO)
    bound = spec((ONE, EXT))
    pair = [halo_head(ZERO), halo_head(ONE)]
    return call(
        attn1_bwd_body, (HSTEPS,),
        [own_head(ZERO), own_head(ONE), own_head(TWO), own_head(ZERO)] + pair * FOUR + [stat, stat, bound, bound],
        spec((THREE, HPS, HEAD, TOK), ZERO, step_of, ZERO, ZERO),
        sds((THREE, NHEAD, HEAD, TOK), BF),
        scratch=[pltpu.VMEM((AHEAD_BWD, NBLK + TWO, REACH, LANE), F32)] * TWO + [pltpu.VMEM((AHEAD_BWD, EXT, EXT), BF)] * TWO,
        flops=NHEAD * 10 * TOK * EXT * HALF, nbytes=8 * MIB, name="attn1_bwd",
    )(qkv, qkv, qkv, do_t, left, left, right, right, dleft, dleft, dright, dright, lse_x, del_x, lo, hi)


ROWBLK = [slice(r, r + RB) for r in range(ZERO, TOK, RB)]
HALFT = NFT // TWO
SQRT_HALF = math.sqrt(SCALE * FOUR)
PDF_SCALE = SQRT_HALF / math.sqrt(math.pi)
STATS = 16


def normal_cdf(a):
    return SQRT_HALF * SQRT_HALF * (ONE + lax.erf(a * SQRT_HALF))


def att_block(ref, n):
    return ref.at[n % FOUR, n // FOUR] if ref.shape[ZERO] == FOUR else ref.at[n]


def half_rows(ref, which):
    n = ref.shape[ZERO] // TWO
    return ref.at[pl.ds(pl.multiple_of(which * n, n), n)]


def col_tile(ref, n):
    return ref.at[:, pl.ds(pl.multiple_of(n * FT, FT), FT)]


class Refs:
    def __init__(self, names, refs):
        self.__dict__.update(zip(names, refs))


class Swaps:
    def __init__(self, r):
        self.r, self.waits, self.n = r, [], ZERO
        self.core, self.partner = core_and_partner()
        self.other = ONE - self.core

    def remote(self, src, dst):
        cp = to_partner(self.partner, src, dst, self.r.ssem.at[self.n], self.r.rsem.at[self.n])
        return self.later(cp)

    def local(self, src, dst):
        return self.later(pltpu.make_async_copy(src, dst, self.r.lsem.at[self.n]))

    def later(self, cp):
        self.n += ONE
        self.waits.append(cp)
        return cp

    def wait(self):
        for cp in self.waits:
            cp.wait()


def mlp_body(*refs, names, fwd, bwd):
    r = Refs(names, refs)
    step = pl.program_id(ZERO)
    sw = Swaps(r)
    start, spread = [], []
    if fwd:
        start = [sw.remote(r.h, r.h_r), sw.remote(half_rows(r.of, sw.other), r.of_r),
                 sw.local(half_rows(r.of, sw.core), r.of_m)]
        m_out = [(sw.remote(r.m_s.at[HALFT * sw.other + n], col_tile(r.m_r, n)),
                  sw.local(r.m_s.at[HALFT * sw.core + n], col_tile(r.m_m, n))) for n in range(HALFT)]
    if bwd:
        start.append(sw.remote(r.dy, r.dy_r))
        dmid_out = sw.remote(r.dmid, r.dmid_r)
        du_out = [(sw.remote(r.du_s.at[n, sw.other], col_tile(r.du_r, n)),
                   sw.local(r.du_s.at[n, sw.core], col_tile(r.du_m, n))) for n in range(NFT)]

    @pl.when(step == ZERO)
    def _():
        if fwd:
            for n in range(NHEAD):
                r.of[HEAD * n:HEAD * n + HEAD, :] = att_block(r.o, n)[...]
            x1 = (r.x[...].astype(F32) + mm_tn(r.of[...], r.wp[...])).astype(BF)
            r.x1[...] = x1
            r.h[...] = norm_rows(x1, r.g[...])
            r.acc[...] = x1.astype(F32)
        if bwd:
            r.dacc[...] = jnp.zeros(r.dacc.shape, F32)
        meet_partner(sw.partner)
        for cp in start:
            cp.start()

    for rows in ROWBLK:
        if fwd:
            ua = mm(r.h[rows], r.wa[...]).astype(BF)
            ub = mm(r.h[rows], r.wb[...]).astype(BF)
            if not bwd:
                r.u[ZERO, rows] = ua
                r.u[ONE, rows] = ub
        else:
            ua, ub = r.u[ZERO, rows], r.u[ONE, rows]
        a, b = ua.astype(F32), ub.astype(F32)
        cdf = normal_cdf(a)
        gate = a * cdf
        if fwd:
            m = (gate * b).astype(BF)
            r.m_s[step, rows] = m
            r.acc[rows] += mm(m, r.wo[...])
        if bwd:
            dm = mm_nt(r.dy[rows], r.wo[...]).astype(BF).astype(F32)
            pdf = jnp.exp(a * a * (SCALE * FOUR - ONE)) * PDF_SCALE
            db = (dm * gate).astype(BF)
            da = (dm * b * (cdf + a * pdf)).astype(BF)
            r.du_s[step, ZERO, rows] = da
            r.du_s[step, ONE, rows] = db
            r.dacc[rows] += mm_nt(da, r.wa[...]) + mm_nt(db, r.wb[...])

    for n in range(NFT):
        @pl.when(step == n)
        def _(n=n):
            if fwd:
                there, here = m_out[n % HALFT]

                @pl.when(sw.core == n // HALFT)
                def _():
                    here.start()

                @pl.when(sw.other == n // HALFT)
                def _():
                    there.start()
            if bwd:
                for cp in du_out[n]:
                    cp.start()

    @pl.when(step == NFT - ONE)
    def _():
        if fwd:
            r.y[...] = r.acc[...].astype(BF)
        if bwd:
            d_ln, gg = norm_rows_grad(r.x1[...], r.g[...], r.dacc[...].astype(BF))
            r.gg[...] = gg
            d_mid = add_bf(r.dy[...], d_ln)
            r.dmid[...] = d_mid
            dmid_out.start()
            d_att = mm_nt(r.wp[...], d_mid).astype(BF)
            for n in range(NHEAD):
                rows = slice(HEAD * n, HEAD * n + HEAD)
                blk = d_att[rows]
                att_block(r.d_o, n)[...] = blk
                if fwd:
                    r.delta[n:n + ONE, :] = jnp.sum(blk.astype(F32) * r.of[rows].astype(F32), axis=ZERO, keepdims=True)
            if fwd:
                r.delta[NHEAD:, :] = jnp.zeros((STATS - NHEAD, TOK), F32)
        sw.wait()


def mlp_call(layer, cid, fwd, bwd, w_proj, gain, w_in, w_out, x=None, o_t=None, dy=None, x1=None, u=None, oshape=None):
    toks, tok_spec, vec = sds(ALLTOK, BF), spec(ALLTOK), spec((ONE, DM))
    u_spec = spec((TWO, TOK, FT), ZERO, ZERO, step_of)
    half_o = sds((DM // TWO, TOK), BF)
    half_m, half_u = sds((TOK, FF // TWO), BF), sds((TOK, FF), BF)
    ins = [('wp', w_proj, spec((None, DM, DM), layer, ZERO, ZERO)), ('g', gain, vec),
           ('wa', w_in, weight_cols(layer, FT)), ('wb', w_in, weight_cols(layer, FT, NFT)),
           ('wo', w_out, spec((None, FT, DM), layer, step_of, ZERO))]
    outs, scratch = [], []
    if fwd:
        ins += [('x', x, tok_spec), ('o', o_t, spec(o_t.shape))]
        outs += [('y', toks, tok_spec), ('h', toks, tok_spec), ('h_r', toks, ANY), ('of_m', half_o, ANY), ('of_r', half_o, ANY),
                 ('m_m', half_m, ANY), ('m_r', half_m, ANY)]
        scratch += [('acc', pltpu.VMEM(ALLTOK, F32)), ('of', pltpu.VMEM((DM, TOK), BF)), ('m_s', pltpu.VMEM((NFT, TOK, FT), BF))]
    if fwd and not bwd:
        outs += [('x1', toks, tok_spec), ('u', sds((TWO, TOK, FF), BF), u_spec)]
    if bwd:
        ins += [('dy', dy, tok_spec)]
        outs += [('dmid', toks, tok_spec), ('gg', sds((ONE, DM), F32), vec), ('d_o', sds(oshape, BF), spec(oshape)),
                 ('dy_r', toks, ANY), ('dmid_r', toks, ANY), ('du_m', half_u, ANY), ('du_r', half_u, ANY)]
        scratch += [('dacc', pltpu.VMEM(ALLTOK, F32)), ('du_s', pltpu.VMEM((NFT, TWO, TOK, FT), BF))]
    if fwd and bwd:
        outs += [('delta', sds((STATS, TOK), F32), spec((STATS, TOK)))]
        scratch += [('x1', pltpu.VMEM(ALLTOK, BF))]
    if not fwd:
        ins += [('x1', x1, tok_spec), ('u', u, u_spec)]
    sems = DMA((TWO * NFT + 8 + NFT,))
    scratch += [('ssem', sems), ('rsem', sems), ('lsem', sems)]
    names = [n for n, *_ in ins + outs + scratch]
    name = "mlp_" + "fwd" * fwd + "bwd" * bwd
    got = call(
        functools.partial(mlp_body, names=names, fwd=fwd, bwd=bwd), (NFT,),
        [sp for *_, sp in ins], [sp for *_, sp in outs], [sh for _, sh, _ in outs], scratch=[sh for _, sh in scratch],
        flops=TWO * TOK * DM * (DM + THREE * FF) * (fwd + bwd), nbytes=26 * MIB, name=name, cid=cid,
    )(*[arr for _, arr, _ in ins])
    return Refs([n for n, *_ in outs], got)


def qkv_bwd_body(d_ref, cos_ref, sin_ref, w_ref, x_ref, g_ref, dmid_ref, dx_ref, gg_ref, dtm_ref, dtr_ref,
                 acc, dt_s, dt_all, ssem, rsem, lsem):
    step = pl.program_id(ZERO)
    core, partner = core_and_partner()

    def dst(ref, n):
        rows = PROJ
        return ref.at[pl.ds(pl.multiple_of(n * rows, rows), rows)]

    def copies(n):
        return (to_partner(partner, dt_s.at[ONE - core, n], dst(dtr_ref, n), ssem.at[n], rsem.at[n]),
                pltpu.make_async_copy(dt_s.at[core, n], dst(dtm_ref, n), lsem.at[n]))

    @pl.when(step == ZERO)
    def _():
        acc[...] = jnp.zeros(acc.shape, F32)
        meet_partner(partner)

    def put(chunk, head, row, val):
        at = LANE * chunk + row + HEAD * (head % TWO)
        dt_s[head // TWO, step, at:at + val.shape[ZERO]] = val
        at = RB * chunk + row + HEAD * head
        dt_all[at:at + val.shape[ZERO]] = val

    @pl.when(step < TWO)
    def _():
        cos, sin = cos_ref[...], sin_ref[...]
        for chunk in CHUNKS:
            for head in range(FOUR):
                d_head = head_rows(d_ref, chunk, head)[...].astype(F32)
                da, db = d_head[:HALF], d_head[HALF:]
                put(chunk, head, ZERO, (da * cos + db * sin).astype(BF))
                put(chunk, head, HALF, (db * cos - da * sin).astype(BF))

    @pl.when(step == TWO)
    def _():
        for chunk in CHUNKS:
            for head in range(FOUR):
                put(chunk, head, ZERO, head_rows(d_ref, chunk, head)[...])

    for cp in copies(step):
        cp.start()
    acc[...] += mm(w_ref[...], dt_all[...])

    @pl.when(step == TWO)
    def _():
        d_ln, gg = norm_rows_grad(x_ref[...], g_ref[...], acc[...].T.astype(BF))
        gg_ref[...] = gg
        dx_ref[...] = add_bf(dmid_ref[...], d_ln)
        for n in range(THREE):
            for cp in copies(n):
                cp.wait()


def qkv_bwd(d_qkv, cos_t, sin_t, w_qkv, x, gain, d_mid, layer, dest_major, cid):
    table = spec((HALF, TOK))
    half = sds((THREE * PROJ, TOK), BF)
    return call(
        qkv_bwd_body, (THREE,),
        [heads_spec(dest_major), table, table, weight_cols(layer, DM), spec(ALLTOK), spec((ONE, DM)), spec(ALLTOK)],
        [spec(ALLTOK), spec((ONE, DM)), ANY, ANY],
        [sds(ALLTOK, BF), sds((ONE, DM), F32), half, half],
        scratch=[pltpu.VMEM((DM, TOK), F32), pltpu.VMEM((TWO, THREE, PROJ, TOK), BF), pltpu.VMEM((DM, TOK), BF),
                 DMA((THREE,)), DMA((THREE,)), DMA((THREE,))],
        flops=TWO * TOK * DM * THREE * DM, nbytes=10 * MIB, name="qkv_bwd", cid=cid,
    )(d_qkv, cos_t, sin_t, w_qkv, x, gain, d_mid)


DOWN = FF // TWO
UP = FF
QKV = THREE * PROJ
MLP_ROWS = DOWN + UP
ATT_ROWS = PROJ + QKV
RING_ROWS = TWO * ATT_ROWS + MLP_ROWS
NDOWN = DOWN // DM
GRAD_REFS = 9


def grad_call(body, grads, steps, in_specs, args, rows, first_row, total, scratch=()):
    shared = [] if grads is None else [grads]
    first = first_row // rows
    return call(
        body, (steps,), [ANY] * len(shared) + in_specs,
        spec((rows, DM), lambda s: first + s, ZERO), sds((total, DM), F32), scratch=scratch,
        flops=FOUR * steps * rows * TOK * DM, nbytes=20 * MIB, name=body.__name__,
        alias={ZERO: ZERO} if shared else None,
    )(*shared, *args)


def grad_mlp_body(*refs):
    ma, mb, dya, dyb, ha, hb, dua, dub, out_ref, h_t = refs[-GRAD_REFS - ONE:]
    step = pl.program_id(ZERO)

    @pl.when(step < NDOWN)
    def _():
        out_ref[...] = mm_tn(ma[...], dya[...]) + mm_tn(mb[...], dyb[...])

    @pl.when(step == NDOWN)
    def _():
        h_t[ZERO] = ha[...].T
        h_t[ONE] = hb[...].T

    @pl.when(step >= NDOWN)
    def _():
        out_ref[...] = mm(h_t[ZERO], dua[...]) + mm(h_t[ONE], dub[...])


def grad_mlp(grads, m, m_r, dy, dy_r, h, h_r, du, du_r, first_row, total):
    toks = spec(ALLTOK)
    m_col = spec(ALLTOK, ZERO, lambda s: jnp.minimum(s, NDOWN - ONE))
    du_col = spec(ALLTOK, ZERO, lambda s: jnp.maximum(s - NDOWN, ZERO))
    return grad_call(grad_mlp_body, grads, NDOWN + UP // DM, [m_col, m_col, toks, toks, toks, toks, du_col, du_col],
                     (m, m_r, dy, dy_r, h, h_r, du, du_r), DM, first_row, total, scratch=[pltpu.VMEM((TWO, DM, TOK), BF)])


def grad_att_body(*refs):
    oa, ob, dma, dmb, ta, tb, ha, hb, out_ref = refs[-GRAD_REFS:]
    step = pl.program_id(ZERO)

    @pl.when(step == ZERO)
    def _():
        out_ref[...] = mm(oa[...], dma[...]) + mm(ob[...], dmb[...])

    @pl.when(step > ZERO)
    def _():
        out_ref[...] = mm(ta[...], ha[...]) + mm(tb[...], hb[...])


def grad_att(grads, of, of_r, dmid, dmid_r, dt, dt_r, h, h_r, first_row):
    toks = spec(ALLTOK)
    blk = (PROJ, TOK)
    dt_row = spec(blk, lambda s: jnp.maximum(s - ONE, ZERO), ZERO)
    return grad_call(grad_att_body, grads, ONE + QKV // PROJ, [spec(blk), spec(blk), toks, toks, dt_row, dt_row, toks, toks],
                     (of, of_r, dmid, dmid_r, dt, dt_r, h, h_r), PROJ, first_row, RING_ROWS)


NB, NS = 5, 6
CH = RING_ROWS // (NB * FOUR)
SB, LF = CH // FOUR, CH // 16
RS = 9
LAST = RS + RS
ADD_ROWS = 96


def ring_body(g_ref, ln_ref, f_ref, lnout_ref, bufa, bufb, bufc, gath, stage, lnbuf,
              ssem, rsem, psem, qsem, csem, stsem, lns, lnr):
    core, partner = core_and_partner()
    zy = lax.axis_index('zy')
    pos = (lax.axis_index('sp'), lax.rem(zy, FOUR), zy // FOUR)
    streams = [(c, sg) for c in range(THREE) for sg in (ONE, -ONE)]
    bufs, sizes = (bufa, bufb, bufc), (CH, SB, LF)
    peers = range(ONE, FOUR)

    def mod4(v):
        return lax.rem(v + 8, FOUR)

    def at(axis, val):
        if axis == ZERO:
            return {'sp': val}
        yz = (val, pos[TWO]) if axis == ONE else (pos[ONE], val)
        return {'zy': yz[ONE] * FOUR + yz[ZERO]}

    def shifted(axis, d):
        return at(axis, mod4(pos[axis] + d))

    def axis_of(s, ph):
        return (streams[s][ZERO] + ph) % THREE

    def idx(s, ph, t):
        return mod4(pos[axis_of(s, ph)] - streams[s][ONE] * t)

    def own(s, ph):
        return idx(s, ph, -ONE)

    def base(b):
        return b * (FOUR * CH)

    bar = pltpu.get_barrier_semaphore()
    for ax in range(THREE):
        for d in peers:
            pl.semaphore_signal(bar, inc=ONE, device_id=shifted(ax, d), device_id_type=MESH)
    pl.semaphore_signal(bar, inc=ONE, device_id=partner, device_id_type=MESH)
    pl.semaphore_wait(bar, 10)

    def rows(ref, start, n):
        return ref.at[pl.ds(pl.multiple_of(start, LF), n)]

    def grows(s, start, n):
        return g_ref.at[pl.ds(pl.multiple_of(start, LF), n), LANE * s:LANE * s + LANE]

    def frows(s, start, n):
        return f_ref.at[core, pl.ds(pl.multiple_of(start, LF), n), LANE * s:LANE * s + LANE]

    def same_bytes(b, k):
        if k < RS:
            return bufs[k // THREE].at[b, k % THREE]
        n = sizes[TWO - (k - RS) // THREE]
        return gath.at[b] if n == CH else gath.at[b, :, pl.ds(ZERO, n)]

    def wait_for(ref, sem):
        pltpu.make_async_copy(ref, ref, sem).wait()

    def send(b, s, k):
        ph = k // THREE if k < RS else TWO - (k - RS) // THREE
        t = k % THREE
        n = sizes[ph]
        if k < RS:
            dst = bufs[ph].at[b, t, s]
            if t:
                src = bufs[ph].at[b, t - ONE, s]
            elif ph:
                src = rows(bufs[ph - ONE].at[b, TWO, s], idx(s, ph, ZERO) * n, n)
            else:
                src = grows(s, base(b) + idx(s, ZERO, ZERO) * n, n)
        elif ph:
            off = own(s, ONE) * SB if ph == TWO else ZERO
            src = dst = rows(gath.at[b, s], off + idx(s, ph, t - ONE) * n, n)
        else:
            dst = frows(s, base(b) + idx(s, ZERO, t - ONE) * n, n)
            src = dst if t else gath.at[b, s]
        pltpu.make_async_remote_copy(src_ref=src, dst_ref=dst, send_sem=ssem.at[b, k], recv_sem=rsem.at[b, k],
                                     device_id=shifted(axis_of(s, ph), streams[s][ONE]), device_id_type=MESH).start()

    def stage_load(n):
        t, b, slot = n // NB, lax.rem(n, NB), lax.rem(n, TWO)
        for s in range(NS):
            pltpu.make_async_copy(grows(s, base(b) + idx(s, ZERO, t + ONE) * CH, CH), stage.at[slot, s],
                                  stsem.at[slot]).start()

    def ln_copy(ph, d):
        return pltpu.make_async_remote_copy(
            src_ref=lnbuf.at[ph, THREE] if ph else ln_ref, dst_ref=lnbuf.at[ph, d - ONE], send_sem=lns.at[ph, d - ONE],
            recv_sem=lnr.at[ph, d - ONE], device_id=shifted(ph, d) if ph < THREE else partner, device_id_type=MESH)

    def ln_sum(ph):
        vals = [lnbuf[ph, THREE] if ph else ln_ref[...]] + [lnbuf[ph, d - ONE] for d in peers]
        total = jnp.zeros_like(vals[ZERO])
        for p in range(FOUR):
            term = vals[ZERO]
            for d in peers:
                term = jnp.where(mod4(pos[ph] - d) == p, vals[d], term)
            total = total + term
        return total

    def batches(fn, start=ZERO):
        def body(b, c):
            fn(b)
            return c
        lax.fori_loop(start, NB, body, ZERO)

    def first(b):
        for s in range(NS):
            send(b, s, ZERO)

    first(ZERO)
    stage_load(jnp.int32(ZERO))
    for d in peers:
        ln_copy(ZERO, d).start()
    batches(first, ONE)

    for k in range(RS):
        ph, t = k // THREE, k % THREE
        buf, size = bufs[ph], sizes[ph]

        def step(b, k=k, ph=ph, t=t, buf=buf, size=size):
            n = k * NB + b
            slot = lax.rem(n, TWO)
            if not ph:
                @pl.when(n < THREE * NB - ONE)
                def _():
                    stage_load(n + ONE)
                wait_for(stage.at[slot], stsem.at[slot])
            wait_for(same_bytes(b, k), rsem.at[b, k])
            for s in range(NS):
                if ph:
                    off = pl.multiple_of(idx(s, ph, t + ONE) * size, LF)
                    buf[b, t, s] += bufs[ph - ONE][b, TWO, s, pl.ds(off, size)]
                else:
                    @pl.loop(ZERO, CH, step=ADD_ROWS)
                    def _(r):
                        at_r = pl.ds(pl.multiple_of(r, ADD_ROWS), ADD_ROWS)
                        buf[b, t, s, at_r] += stage[slot, s, at_r]
                if k == RS - ONE:
                    off = pl.multiple_of(own(s, ONE) * SB + own(s, TWO) * LF, LF)
                    gath[b, s, pl.ds(off, LF)] = bufc[b, TWO, s]
                send(b, s, k + ONE)

        batches(step)
        if k < SIX and k % TWO == ZERO:
            lp = k // TWO
            for d in peers:
                ln_copy(lp, d).wait()
            lnbuf[lp + ONE, THREE] = ln_sum(lp)
            for d in peers if lp < TWO else (ONE,):
                ln_copy(lp + ONE, d).start()

    def hand_over(b, s, j, src, start):
        pltpu.make_async_remote_copy(src_ref=src, dst_ref=frows(s, start, CH), send_sem=psem.at[b, j], recv_sem=qsem.at[b, j],
                                     device_id=partner, device_id_type=MESH).start()

    for k in range(RS, LAST):
        def step(b, k=k):
            wait_for(same_bytes(b, k), rsem.at[b, k])
            piece = k - (LAST - FOUR)
            for s in range(NS):
                if k < LAST - ONE:
                    send(b, s, k + ONE)
                if piece >= ZERO:
                    start = base(b) + idx(s, ZERO, piece - ONE) * CH
                    if piece:
                        hand_over(b, s, piece, frows(s, start, CH), start)
                    else:
                        pltpu.make_async_copy(gath.at[b, s], frows(s, start, CH), csem.at[b]).start()
                        hand_over(b, s, piece, gath.at[b, s], start)
        batches(step)

    ln_copy(THREE, ONE).wait()
    lnout_ref[...] = lnbuf[THREE, THREE] + lnbuf[THREE, ZERO]

    def finish(b):
        for k in range(LAST):
            wait_for(same_bytes(b, k), ssem.at[b, k])
        for j in range(FOUR):
            wait_for(gath.at[b], psem.at[b, j])
            wait_for(gath.at[b], qsem.at[b, j])
        wait_for(gath.at[b], csem.at[b])
    batches(finish)


def ring_all_reduce(g, ln, cid):
    vmem = pl.BlockSpec(memory_space=pltpu.VMEM)
    return pl.pallas_call(
        ring_body,
        in_specs=[ANY, vmem],
        out_specs=[ANY, vmem],
        out_shape=[sds((TWO, RING_ROWS, DM), F32), sds(ln.shape, F32)],
        scratch_shapes=[
            pltpu.VMEM((NB, THREE, NS, CH, LANE), F32), pltpu.VMEM((NB, THREE, NS, SB, LANE), F32),
            pltpu.VMEM((NB, THREE, NS, LF, LANE), F32), pltpu.VMEM((NB, NS, CH, LANE), F32),
            pltpu.VMEM((TWO, NS, CH, LANE), F32),
            pltpu.VMEM((FOUR, FOUR) + ln.shape, F32),
            DMA((NB, LAST)), DMA((NB, LAST)), DMA((NB, FOUR)), DMA((NB, FOUR)), DMA((NB,)), DMA((TWO,)),
            DMA((FOUR, THREE)), DMA((FOUR, THREE)),
        ],
        compiler_params=pltpu.CompilerParams(collective_id=cid, has_side_effects=True, vmem_limit_bytes=60 * MIB),
        cost_estimate=pl.CostEstimate(flops=MIB * MIB // FOUR, bytes_accessed=200 * MIB, transcendentals=ZERO),
        name="ring_all_reduce",
    )(g, ln)


SLOTS, LAG = 8, 4
NTURN = TWO * THREE
OUT_SHAPE, IN_SHAPE = (TWO, FF, DM), (TWO, DM, TWO * FF)


def stream(pieces, buf, turned, isem, osem):
    def loads(i):
        slot, srcs = i % SLOTS, pieces[i][ZERO]
        n = srcs[ZERO].shape[ZERO]
        return [pltpu.make_async_copy(src, buf.at[slot, k * n:k * n + n], isem.at[slot, k]) for k, src in enumerate(srcs)]

    def store(i):
        _, dst, turn = pieces[i]
        src = buf.at[i % SLOTS, :dst.shape[ZERO]] if turn is None else turned.at[turn]
        return pltpu.make_async_copy(src, dst, osem.at[i % SLOTS])

    total = len(pieces)
    for i in range(total + LAG):
        if i < total:
            if i >= SLOTS:
                store(i - SLOTS).wait()
            for cp in loads(i):
                cp.start()
        k = i - LAG
        if k >= ZERO:
            for cp in loads(k):
                cp.wait()
            turn = pieces[k][TWO]
            if turn is not None:
                for n in CHUNKS:
                    rows, col = LANE * n, RB * n
                    turned[turn, :, col:col + LANE] = buf[k % SLOTS, rows:rows + LANE].T
                    turned[turn, :, col + LANE:col + RB] = buf[k % SLOTS, PROJ + rows:PROJ + rows + LANE].T
            store(k).start()
    for i in range(max(total - SLOTS, ZERO), total):
        store(i).wait()


def unpack_ring_body(f, g_qkv, g_proj, g_in, g_out, *scratch):
    def block(c, row, n=DM):
        return f.at[c, row:row + n]

    pieces = []
    for c in range(TWO):
        for n in range(NDOWN):
            pieces.append(([block(c, ATT_ROWS + DM * n)], g_out.at[ZERO, DOWN * c + DM * n:DOWN * c + DM * n + DM], None))
        for n in range(FOUR):
            col = UP * c + DM * n
            pieces.append(([block(c, ATT_ROWS + DOWN + DM * n)], g_in.at[ZERO, :, col:col + DM], None))
    for l in range(TWO):
        first = (ONE - l) * (ATT_ROWS + MLP_ROWS)
        for n in range(THREE):
            row = first + PROJ * (n + ONE)
            pieces.append(([block(c, row, PROJ) for c in range(TWO)], g_qkv.at[l, :, DM * n:DM * n + DM], THREE * l + n))
        for c in range(TWO):
            pieces.append(([block(c, first, PROJ)], g_proj.at[l, PROJ * c:PROJ * c + PROJ], None))
    stream(pieces, *scratch)


def unpack_mlp_body(own, other, in_0, out_0, g_in, g_out, *scratch):
    core = lax.axis_index('core')
    pieces = []
    for src, side in ((own, core), (other, ONE - core)):
        for n in range(NDOWN):
            row = pl.multiple_of(DOWN * side + DM * n, DM)
            pieces.append(([src.at[DM * n:DM * n + DM]], g_out.at[ONE, pl.ds(row, DM)], None))
        for n in range(FOUR):
            col = pl.multiple_of(UP * side + DM * n, DM)
            pieces.append(([src.at[DOWN + DM * n:DOWN + DM * n + DM]], g_in.at[ONE, :, pl.ds(col, DM)], None))
    stream(pieces, *scratch)


def unpack_call(body, args, outs, alias, name):
    return pl.pallas_call(
        body, in_specs=[ANY] * len(args), out_specs=[ANY] * len(outs), out_shape=[sds(shape, F32) for shape in outs],
        scratch_shapes=[pltpu.VMEM((SLOTS, DM, DM), F32), pltpu.VMEM((NTURN, DM, DM), F32), DMA((SLOTS, TWO)), DMA((SLOTS,))],
        input_output_aliases=alias,
        compiler_params=pltpu.CompilerParams(vmem_limit_bytes=60 * MIB),
        cost_estimate=pl.CostEstimate(flops=MIB * MIB // RB, bytes_accessed=75 * MIB, transcendentals=ZERO), name=name,
    )(*args)


def rope_tables(pos, base):
    inv_freq = base ** (jnp.arange(HALF).astype(F32) * (-TWO / HEAD))
    angles = inv_freq[:, None] * pos.astype(F32)[None, :]
    return jnp.cos(angles), jnp.sin(angles)


def solution(mesh):
    n_sp = mesh.shape['sp']
    by_core = mesh.devices.reshape(n_sp, mesh.shape['dp'] // TWO, TWO)
    mesh = Mesh(by_core, ('sp', 'zy', 'core'))
    dp_axes = ('zy', 'core')
    row_axes = dp_axes + ('sp',)
    token_spec = P(row_axes, None)
    to_right = [(i, i + ONE) for i in range(n_sp - ONE)]
    to_left = [(i + ONE, i) for i in range(n_sp - ONE)]
    swap_cores = [(ZERO, ONE), (ONE, ZERO)]
    cids = list(range(RS))

    def halo_swap(arr):
        from_left = lax.ppermute(arr[..., TOK - LANE:], 'sp', to_right)
        from_right = lax.ppermute(arr[..., :LANE], 'sp', to_left)
        return from_left, from_right

    def exchange(arr):
        return lax.all_to_all(arr, 'sp', ZERO, ZERO, tiled=True)

    def device_step(x_loc, cu_loc, pos_loc, w_qkv, w_proj, w_in, w_out, ln_attn, ln_mlp, d_out):
        sp = lax.axis_index('sp')
        cu = cu_loc[ZERO][:, None]

        def bounds_of(tok):
            start = jnp.max(jnp.where(cu <= tok, cu, ZERO), axis=ZERO)
            return start, jnp.min(jnp.where(cu > tok, cu, GRP), axis=ZERO)

        start, stop = bounds_of(jnp.arange(GRP)[None, :])
        tiles = start[::QT] // QT, (stop[QT - ONE::QT] + QT - ONE) // QT
        rows = start[None, :], stop[None, :]
        shift = sp * TOK - LANE
        tok_x = jnp.arange(EXT) + shift
        start_x, stop_x = bounds_of(tok_x[None, :])
        inside = (tok_x >= ZERO) & (tok_x < GRP)
        near = (jnp.where(inside, jnp.maximum(start_x, tok_x - WIN) - shift, ZERO)[None, :],
                jnp.where(inside, jnp.minimum(stop_x, tok_x + WIN + ONE) - shift, ZERO)[None, :])
        tab0, tab1 = [rope_tables(pos_loc, base) for base in BASES]
        la0, la1, lm0, lm1 = ln_attn[:ONE], ln_attn[ONE:], ln_mlp[:ONE], ln_mlp[ONE:]

        w_mlp = (w_in, w_out)
        h0, qkv0, h0r = qkv_fwd(x_loc, la0, w_qkv, ZERO, *tab0, True, cids[ONE])
        qkv0 = exchange(qkv0)
        oh0, lse0 = attn0_fwd(*tiles, qkv0, *rows)
        f0 = mlp_call(ZERO, cids[TWO], True, False, w_proj, lm0, *w_mlp, x=x_loc, o_t=exchange(oh0))
        x1 = f0.y
        h1, qkv1, h1r = qkv_fwd(x1, la1, w_qkv, ONE, *tab1, False, cids[THREE])
        qkv1 = qkv1.reshape((THREE * NHEAD, HEAD, TOK))
        kv_halo = halo_swap(qkv1[NHEAD:])
        o1, lse1 = attn1_fwd(qkv1, *kv_halo, *near)
        f1 = mlp_call(ONE, cids[FOUR], True, True, w_proj, lm1, *w_mlp, x=x1, o_t=o1, dy=d_out, oshape=(NHEAD, HEAD, TOK))
        g_side = grad_mlp(None, f1.m_m, f1.m_r, d_out, f1.dy_r, f1.h, f1.h_r, f1.du_m, f1.du_r, ZERO, MLP_ROWS)
        d_o1, g_side = lax.optimization_barrier((f1.d_o, g_side))
        g_side = lax.psum(g_side, ('sp', 'zy'))
        d_halo = halo_swap(jnp.concatenate([qkv1[:NHEAD], d_o1], axis=ZERO))
        stats = jnp.concatenate([lse1.reshape(NHEAD, TOK), f1.delta[:NHEAD]], axis=ZERO)
        from_left, from_right = halo_swap(stats)
        lse_x, del_x = jnp.concatenate([from_left, stats, from_right], axis=ONE).reshape(TWO, NHEAD, ONE, EXT)
        dqkv1 = attn1_bwd(qkv1, d_o1, *kv_halo, *d_halo, lse_x, del_x, *near)
        dx1, gga1, dt1, dt1r = qkv_bwd(dqkv1.reshape(THREE, THREE, FOUR, HEAD, TOK), *tab1, w_qkv, x1, la1, f1.dmid,
                                       ONE, False, cids[SIX])
        b0 = mlp_call(ZERO, cids[5], False, True, w_proj, lm0, *w_mlp, dy=dx1, x1=f0.x1, u=f0.u, oshape=oh0.shape)
        dqkv0 = exchange(attn0_bwd(*tiles, qkv0, oh0, exchange(b0.d_o), lse0, *rows))
        grads = grad_att(None, f1.of_m, f1.of_r, f1.dmid, f1.dmid_r, dt1, dt1r, h1, h1r, ZERO)
        grads = grad_mlp(grads, f0.m_m, f0.m_r, dx1, b0.dy_r, f0.h, f0.h_r, b0.du_m, b0.du_r, ATT_ROWS, RING_ROWS)
        dx0, gga0, dt0, dt0r = qkv_bwd(dqkv0, *tab0, w_qkv, x_loc, la0, b0.dmid, ZERO, True, cids[7])
        grads = grad_att(grads, f0.of_m, f0.of_r, b0.dmid, b0.dmid_r, dt0, dt0r, h0, h0r, ATT_ROWS + MLP_ROWS)

        gains = jnp.concatenate([gga0, gga1, b0.gg, f1.gg, jnp.zeros((FOUR, DM), F32)], axis=ZERO)
        summed, gains = ring_all_reduce(grads, gains, cids[ZERO])
        summed, g_side = lax.optimization_barrier((summed, g_side))
        from_partner = lax.ppermute(g_side, 'core', swap_cores)
        shapes = [(TWO, DM, THREE * DM), (TWO, DM, DM), IN_SHAPE, OUT_SHAPE]
        g_qkv, g_proj, g_in, g_out = unpack_call(unpack_ring_body, (summed,), shapes, {}, "unpack_ring")
        g_in, g_out = unpack_call(unpack_mlp_body, (g_side, from_partner, g_in, g_out), shapes[TWO:],
                                  {TWO: ZERO, THREE: ONE}, "unpack_mlp")
        return f1.y, dx0, g_qkv, g_proj, g_in, g_out, gains[:TWO], gains[TWO:FOUR]

    in_specs = (token_spec, P(dp_axes, None), P(row_axes)) + (P(),) * SIX + (token_spec,)
    out_specs = (token_spec, token_spec) + (P(),) * SIX
    return jax.shard_map(device_step, mesh=mesh, in_specs=in_specs, out_specs=out_specs, check_vma=False)
```

```python
import functools
import math
import jax
import jax.numpy as jnp
from jax import lax
from jax.experimental import pallas as pl
from jax.experimental.pallas import tpu as pltpu
from jax.sharding import Mesh, PartitionSpec as P

ZERO, ONE, TWO, THREE, FOUR = range(5)
SIX, TWELVE = 6, 12
HEAD = 64
HALF = 32
NHEAD = 12
DM = 768
FF = 3072
TOK = 512
GRP = 2048
WIN = 64
LANE = 128
EPS = 1e-5
NEG = -1e30
SCALE = 0.125
BASES = (160000.0, 10000.0)
F32 = jnp.float32
BF = jnp.bfloat16
QT = 256
FT = 512
NFT = FF // FT
QTILES = GRP // QT
MIB = 1024 * 1024
ALLTOK = (TOK, DM)
PROJ = DM // 2
ALLDM = (DM, DM)
ANY = pl.BlockSpec(memory_space=pl.ANY)
DMA = pltpu.SemaphoreType.DMA
MESH = pl.DeviceIdType.MESH


def dot(a, b, ca, cb):
    return lax.dot_general(a, b, (((ca,), (cb,)), ((), ())), preferred_element_type=F32)


def mm(a, b):
    return dot(a, b, ONE, ZERO)


def mm_nt(a, b):
    return dot(a, b, ONE, ONE)


def mm_tn(a, b):
    return dot(a, b, ZERO, ZERO)


def call(body, grid, in_specs, out_specs, out_shape, scratch=(), prefetch=ZERO, flops=ZERO, nbytes=ZERO, name=None,
         cid=None, alias=None):
    extra = {} if cid is None else dict(collective_id=cid, has_side_effects=True)
    return pl.pallas_call(
        body,
        grid_spec=pltpu.PrefetchScalarGridSpec(
            num_scalar_prefetch=prefetch, grid=grid, in_specs=in_specs, out_specs=out_specs, scratch_shapes=scratch),
        out_shape=out_shape,
        input_output_aliases=alias or {},
        compiler_params=pltpu.CompilerParams(vmem_limit_bytes=60 * MIB, **extra),
        cost_estimate=pl.CostEstimate(flops=int(flops), bytes_accessed=int(nbytes), transcendentals=ZERO),
        name=name,
    )


def sds(shape, dtype):
    return jax.ShapeDtypeStruct(shape, dtype)


def spec(shape, *idx):
    idx = idx or (ZERO,) * len(shape)
    return pl.BlockSpec(shape, lambda *g: tuple(i(*g) if callable(i) else i for i in idx))


def step_of(s, *_):
    return s


def core_and_partner():
    core = lax.axis_index('core')
    return core, {'core': ONE - core}


def meet(*devices):
    bar = pltpu.get_barrier_semaphore()
    for dev in devices:
        pl.semaphore_signal(bar, inc=ONE, device_id=dev, device_id_type=MESH)
    pl.semaphore_wait(bar, len(devices))


def sp_peer(d):
    return lax.rem(lax.axis_index('sp') + d, FOUR)


PEERS = range(ONE, FOUR)


class Swaps:
    def __init__(self, ssem, rsem, lsem):
        self.sems, self.waits, self.n = (ssem, rsem, lsem), [], ZERO
        self.core, self.partner = core_and_partner()
        self.other = ONE - self.core
        self.me = lax.axis_index('sp')

    def remote(self, src, dst, dev=None):
        ssem, rsem, _ = self.sems
        return self.later(pltpu.make_async_remote_copy(
            src_ref=src, dst_ref=dst, send_sem=ssem.at[self.n], recv_sem=rsem.at[self.n],
            device_id=self.partner if dev is None else dev, device_id_type=MESH))

    def local(self, src, dst):
        return self.later(pltpu.make_async_copy(src, dst, self.sems[TWO].at[self.n]))

    def later(self, cp):
        self.n += ONE
        self.waits.append(cp)
        return cp

    def to_all(self, src_of, dst_of):
        return [self.remote(src_of(sp_peer(d)), dst_of(self.me), {'sp': sp_peer(d)}) for d in PEERS] + [
            self.local(src_of(self.me), dst_of(self.me))]

    def to_sides(self, left_src, right_src, from_left, from_right):
        return [self.remote(right_src, from_left, {'sp': sp_peer(ONE)}), self.remote(left_src, from_right, {'sp': sp_peer(THREE)})]

    def wait(self, some=None):
        some = self.waits if some is None else some
        done = {id(cp) for cp in some}
        for cp in some:
            cp.wait()
        self.waits = [cp for cp in self.waits if id(cp) not in done]


def meet_row(sw):
    meet(sw.partner, *[{'sp': sp_peer(d)} for d in PEERS])


def meet_sides():
    meet({'sp': sp_peer(ONE)}, {'sp': sp_peer(THREE)})


def swap_sems(n):
    return [DMA((n,))] * THREE


def norm_parts(x_bf):
    rows = x_bf.astype(F32)
    cen = rows - jnp.mean(rows, axis=ONE, keepdims=True)
    var = jnp.mean(cen * cen, axis=ONE, keepdims=True)
    return cen, lax.rsqrt(var + EPS)


def norm_rows(x_bf, gain):
    cen, inv = norm_parts(x_bf)
    return (cen * inv * gain).astype(BF)


def norm_rows_grad(x_bf, gain, d_bf):
    cen, inv = norm_parts(x_bf)
    hat = cen * inv
    d_out = d_bf.astype(F32)
    g_gain = jnp.sum(d_out * hat, axis=ZERO, keepdims=True)
    d_hat = d_out * gain
    d_x = inv * (d_hat - jnp.mean(d_hat, axis=ONE, keepdims=True) - hat * jnp.mean(d_hat * hat, axis=ONE, keepdims=True))
    return d_x.astype(BF), g_gain


def add_bf(a, b):
    return (a.astype(F32) + b.astype(F32)).astype(BF)


RB = 256
CHUNKS = range(DM // RB)


def head_rows(ref, chunk, head):
    return ref.at[head, ZERO, chunk] if ref.shape[ZERO] == FOUR else ref.at[ZERO, chunk, head]


def heads_spec(dest_major):
    if dest_major:
        return spec((FOUR, ONE, THREE, HEAD, TOK), ZERO, step_of, ZERO, ZERO, ZERO)
    return spec((ONE, THREE, FOUR, HEAD, TOK), step_of, ZERO, ZERO, ZERO, ZERO)


def weight_cols(layer, width, first=ZERO):
    return spec((None, DM, width), layer, ZERO, lambda s: first + s)


def qkv_fwd_body(x_ref, g_ref, w_ref, cos_ref, sin_ref, h_ref, out_ref, hr_ref, *rest, whole_group):
    step = pl.program_id(ZERO)
    if whole_group:
        out_s, *sems = rest
    else:
        left_ref, right_ref, edge_s, *sems = rest
    sw = Swaps(*sems)
    swap_h = sw.remote(h_ref, hr_ref)
    if whole_group:
        sends = [[sw.to_all(lambda dev: out_s.at[p, dev, chunk], lambda dev: out_ref.at[dev, p, chunk]) for chunk in CHUNKS]
                 for p in range(THREE)]
    else:
        edges = sw.to_sides(edge_s.at[ZERO], edge_s.at[ONE], left_ref, right_ref)

    @pl.when(step == ZERO)
    def _():
        h_ref[...] = norm_rows(x_ref[...], g_ref[...])
        meet_row(sw)
        swap_h.start()

    def head_block(p, chunk, head):
        return out_s.at[p, head, chunk] if whole_group else out_ref.at[ZERO, chunk, head]

    for p in range(THREE):
        @pl.when(step == p)
        def _(p=p):
            for chunk in CHUNKS:
                t_rows = mm(h_ref[...], w_ref[:, RB * chunk:RB * chunk + RB]).astype(BF).astype(F32).T
                for head in range(FOUR):
                    at = HEAD * head
                    a, b = t_rows[at:at + HALF], t_rows[at + HALF:at + HEAD]
                    if p < TWO:
                        cos, sin = cos_ref[...], sin_ref[...]
                        a, b = a * cos - b * sin, b * cos + a * sin
                    out = head_block(p, chunk, head)
                    out[:HALF] = a.astype(BF)
                    out[HALF:] = b.astype(BF)
                    if p and not whole_group:
                        n, lane = FOUR * chunk + head, WIN * (p - ONE)
                        blk = out[...]
                        edge_s[ZERO, n, :, lane:lane + WIN] = blk[:, :WIN]
                        edge_s[ONE, n, :, lane:lane + WIN] = blk[:, TOK - WIN:]
                if whole_group:
                    for cp in sends[p][chunk]:
                        cp.start()

    @pl.when(step == TWO)
    def _():
        if not whole_group:
            for cp in edges:
                cp.start()
        sw.wait()


GROUP_QKV = (FOUR, THREE, THREE, HEAD, TOK)
EDGE = (NHEAD, HEAD, LANE)


def qkv_fwd(x, gain, w_qkv, layer, cos_t, sin_t, whole_group, cid):
    table = spec((HALF, TOK))
    if whole_group:
        outs, specs, scratch, n = [sds(GROUP_QKV, BF)], [ANY], [pltpu.VMEM((THREE, FOUR, THREE, HEAD, TOK), BF)], 37
    else:
        outs, specs, scratch, n = [sds((THREE, THREE, FOUR, HEAD, TOK), BF)], [heads_spec(False)], [pltpu.VMEM((TWO,) + EDGE, BF)], THREE
    toks = sds(ALLTOK, BF)
    extra = [] if whole_group else [sds(EDGE, BF)] * TWO
    return call(
        functools.partial(qkv_fwd_body, whole_group=whole_group), (THREE,),
        [spec(ALLTOK), spec((ONE, DM)), weight_cols(layer, DM), table, table],
        [spec(ALLTOK)] + specs + [ANY] * (ONE + len(extra)),
        [toks] + outs + [toks] + extra,
        scratch=scratch + swap_sems(n),
        flops=TWO * TOK * DM * THREE * DM, nbytes=8 * MIB, name="qkv_fwd", cid=cid,
    )(x, gain, w_qkv, cos_t, sin_t)


def tile_src(i, *_):
    return i // TWO


def tile_side(i, *_):
    return i % TWO


Q_SPEC = spec((ONE, ONE, THREE, HEAD, QT), tile_src, ZERO, ZERO, ZERO, tile_side)
O_SPEC = spec((ONE, THREE, HEAD, QT), tile_src, ZERO, ZERO, tile_side)
ROW_SPEC = spec((ONE, QT), ZERO, step_of)
STAT_SPEC = spec((8, QT), ZERO, step_of)


def kv_spec(part):
    return spec((FOUR, ONE, THREE, HEAD, TOK), ZERO, part, ZERO, ZERO, ZERO)


def key_tile(kt):
    return kt // TWO, pl.ds(pl.multiple_of((kt % TWO) * QT, QT), QT)


def key_rows(dst, k_ref):
    for src in range(FOUR):
        for h in range(THREE):
            dst[h, TOK * src:TOK * src + TOK] = k_ref[src, ZERO, h].T


def row_tile(kt):
    return pl.ds(pl.multiple_of(kt * QT, QT), QT)


def attn0_fwd_body(lo_s, hi_s, q_ref, k_ref, v_ref, st_ref, en_ref, o_ref, lse_ref, m_s, l_s, acc_s, kr_s, s_s, p_s):
    tile = pl.program_id(ZERO)
    heads, pair = range(THREE), range(TWO)

    @pl.when(tile == ZERO)
    def _():
        key_rows(kr_s, k_ref)

    m_s[...] = jnp.full(m_s.shape, NEG, F32)
    l_s[...] = jnp.zeros(l_s.shape, F32)
    acc_s[...] = jnp.zeros(acc_s.shape, F32)
    st, en = st_ref[...], en_ref[...]
    io = lax.broadcasted_iota(jnp.int32, (QT, QT), ZERO)
    q_t = [q_ref[ZERO, ZERO, h] * SCALE for h in heads]
    first, n_tiles = lo_s[tile], hi_s[tile] - lo_s[tile]

    def body(g, carry):
        kts = [first + TWO * g + a for a in pair]
        safe = [jnp.minimum(kt, QTILES - ONE) for kt in kts]
        for h in heads:
            for a in pair:
                s_s[h, a] = mm(kr_s[h, row_tile(safe[a])], q_t[h])
        for h in heads:
            row = slice(h, h + ONE)
            s = [jnp.where((io >= st - kts[a] * QT) & (io < en - kts[a] * QT), s_s[h, a], NEG) for a in pair]
            m_old = m_s[row]
            m_new = m_old
            for a in pair:
                m_new = jnp.maximum(m_new, jnp.max(s[a], axis=ZERO, keepdims=True))
            alpha = jnp.exp(m_old - m_new)
            total = l_s[row] * alpha
            for a in pair:
                p = jnp.exp(s[a] - m_new)
                total += jnp.sum(p, axis=ZERO, keepdims=True)
                p_s[h, a] = p.astype(BF)
            l_s[row] = total
            m_s[row] = m_new
            acc_s[h] = acc_s[h] * alpha
        for h in heads:
            part = acc_s[h]
            for a in pair:
                src, cols = key_tile(safe[a])
                part += mm(v_ref[src, ZERO, h, :, cols], p_s[h, a])
            acc_s[h] = part
        return carry

    lax.fori_loop(ZERO, (n_tiles + ONE) // TWO, body, ZERO)
    for h in heads:
        row = slice(h, h + ONE)
        o_ref[ZERO, h] = (acc_s[h] / l_s[row]).astype(BF)
        lse_ref[row] = m_s[row] + jnp.log(l_s[row])


def attn0_fwd(lo, hi, qkv, st, en):
    stat = pltpu.VMEM((8, QT), F32)
    return call(
        attn0_fwd_body, (QTILES,),
        [Q_SPEC, kv_spec(ONE), kv_spec(TWO), ROW_SPEC, ROW_SPEC],
        [O_SPEC, STAT_SPEC],
        [sds((FOUR, THREE, HEAD, TOK), BF), sds((8, GRP), F32)],
        scratch=[stat, stat, pltpu.VMEM((THREE, HEAD, QT), F32), pltpu.VMEM((THREE, GRP, HEAD), BF),
                 pltpu.VMEM((THREE, TWO, QT, QT), F32), pltpu.VMEM((THREE, TWO, QT, QT), BF)],
        prefetch=TWO, flops=TWELVE * GRP * GRP * HEAD, nbytes=6 * MIB, name="attn0_fwd",
    )(lo, hi, qkv, qkv, qkv, st, en)


def attn0_bwd_body(lo_s, hi_s, q_ref, k_ref, v_ref, o_ref, do_ref, lse_ref, st_ref, en_ref, out_ref,
                   dk_s, dv_s, dq_s, kr_s, vr_s, s_s, d_s, p_s, t_s):
    tile = pl.program_id(ZERO)
    heads = range(THREE)

    @pl.when(tile == ZERO)
    def _():
        dk_s[...] = jnp.zeros(dk_s.shape, F32)
        dv_s[...] = jnp.zeros(dv_s.shape, F32)
        key_rows(kr_s, k_ref)
        key_rows(vr_s, v_ref)

    dq_s[...] = jnp.zeros(dq_s.shape, F32)
    st, en = st_ref[...], en_ref[...]
    io = lax.broadcasted_iota(jnp.int32, (QT, QT), ZERO)
    q_t = [q_ref[ZERO, ZERO, h] * SCALE for h in heads]
    do_t = [do_ref[ZERO, h] for h in heads]
    q_rows, do_rows = [q_t[h].T for h in heads], [do_t[h].T for h in heads]
    delta = [jnp.sum(do_t[h].astype(F32) * o_ref[ZERO, h].astype(F32), axis=ZERO, keepdims=True) for h in heads]
    lse = [lse_ref[h:h + ONE] for h in heads]

    def body(kt, carry):
        base = kt * QT
        src, cols = key_tile(kt)
        rows = row_tile(kt)
        ok = (io >= st - base) & (io < en - base)
        for h in heads:
            s_s[h] = mm(kr_s[h, rows], q_t[h])
            d_s[h] = mm(vr_s[h, rows], do_t[h])
        for h in heads:
            p = jnp.exp(jnp.where(ok, s_s[h] - lse[h], NEG))
            p_s[h] = p.astype(BF)
            t_s[h] = (p * (d_s[h] - delta[h])).astype(BF)
        for h in heads:
            dv_s[h, rows] += mm(p_s[h], do_rows[h])
            dk_s[h, rows] += mm(t_s[h], q_rows[h])
            dq_s[h] += mm(k_ref[src, ZERO, h, :, cols], t_s[h])
        return carry

    lax.fori_loop(lo_s[tile], hi_s[tile], body, ZERO)
    src, cols = key_tile(tile)
    for h in heads:
        out_ref[src, ZERO, h, :, cols] = (dq_s[h] * SCALE).astype(BF)

    @pl.when(tile == QTILES - ONE)
    def _():
        for src in range(FOUR):
            for h in heads:
                out_ref[src, ONE, h] = dk_s[h, TOK * src:TOK * src + TOK].T.astype(BF)
                out_ref[src, TWO, h] = dv_s[h, TOK * src:TOK * src + TOK].T.astype(BF)


def attn0_bwd(lo, hi, qkv, o_t, do_t, lse, st, en):
    acc, rows = pltpu.VMEM((THREE, GRP, HEAD), F32), pltpu.VMEM((THREE, GRP, HEAD), BF)
    sq32, sq16 = pltpu.VMEM((THREE, QT, QT), F32), pltpu.VMEM((THREE, QT, QT), BF)
    return call(
        attn0_bwd_body, (QTILES,),
        [Q_SPEC, kv_spec(ONE), kv_spec(TWO), O_SPEC, O_SPEC, STAT_SPEC, ROW_SPEC, ROW_SPEC],
        spec(GROUP_QKV), sds(GROUP_QKV, BF),
        scratch=[acc, acc, pltpu.VMEM((THREE, HEAD, QT), F32), rows, rows, sq32, sq32, sq16, sq16],
        prefetch=TWO, flops=30 * GRP * GRP * HEAD, nbytes=TWELVE * MIB, name="attn0_bwd",
    )(lo, hi, qkv, qkv, qkv, o_t, do_t, lse, st, en)


NBLK = TOK // LANE
EXT = TOK + TWO * WIN
XBLK = EXT // LANE
REACH = LANE + TWO * WIN
AHEAD_FWD, AHEAD_BWD = 4, 2
HPS = 4
HSTEPS = NHEAD // HPS


def heads_of(width, part):
    return spec((HPS, HEAD, width), lambda n: HSTEPS * part + n, ZERO, ZERO)


def own_head(part):
    return heads_of(TOK, part)


def row_of(width):
    return spec((HPS, ONE, width), step_of, ZERO, ZERO)


LOW, HIGH = slice(None, WIN), slice(WIN, None)


def joined(left, mid, right, h, left_lanes=HIGH, right_lanes=LOW):
    return jnp.concatenate([left[h][:, left_lanes], mid[h], right[h][:, right_lanes]], axis=ONE)


def blocks(first, last):
    return slice(LANE * first, LANE * last)


def in_bounds(lo_ref, hi_ref, cols, first, n):
    io = lax.broadcasted_iota(jnp.int32, (n, LANE), ZERO) + first
    return (io >= lo_ref[:, cols]) & (io < hi_ref[:, cols])


def every_head(fn, ahead):
    def body(g, c):
        fn([ahead * g + a for a in range(ahead)])
        return c
    lax.fori_loop(ZERO, HPS // ahead, body, ZERO)


def attn1_fwd_body(q_ref, k_ref, v_ref, left_ref, right_ref, lo_ref, hi_ref, o_ref, lse_ref, s_s, p_s):
    def some(heads):
        v_all = []
        for a, h in enumerate(heads):
            q_t = q_ref[h] * SCALE
            k_rows = joined(left_ref, k_ref, right_ref, h, LOW, LOW).T
            v_all.append(joined(left_ref, v_ref, right_ref, h, HIGH, HIGH))
            for i in range(NBLK):
                s_s[a, i] = mm(k_rows[LANE * i:LANE * i + REACH], q_t[:, blocks(i, i + ONE)])
        for a, h in enumerate(heads):
            for i in range(NBLK):
                cols = blocks(i, i + ONE)
                s = jnp.where(in_bounds(lo_ref, hi_ref, cols, LANE * i, REACH), s_s[a, i], NEG)
                m = jnp.max(s, axis=ZERO, keepdims=True)
                e = jnp.exp(s - m)
                l = jnp.sum(e, axis=ZERO, keepdims=True)
                p_s[a, i] = (e * (ONE / l)).astype(BF)
                lse_ref[h, :, cols] = m + jnp.log(l)
        for a, h in enumerate(heads):
            for i in range(NBLK):
                o_ref[h, :, blocks(i, i + ONE)] = mm(v_all[a][:, LANE * i:LANE * i + REACH], p_s[a, i]).astype(BF)
    every_head(some, AHEAD_FWD)


def attn1_fwd(qkv, left, right, lo, hi):
    bound, tile = spec((ONE, TOK)), (AHEAD_FWD, NBLK, REACH, LANE)
    edge = heads_of(LANE, ZERO)
    return call(
        attn1_fwd_body, (HSTEPS,),
        [own_head(ZERO), own_head(ONE), own_head(TWO), edge, edge, bound, bound],
        [own_head(ZERO), row_of(TOK)],
        [sds((NHEAD, HEAD, TOK), BF), sds((NHEAD, ONE, TOK), F32)],
        scratch=[pltpu.VMEM(tile, F32), pltpu.VMEM(tile, BF)],
        flops=NHEAD * FOUR * TOK * REACH * HEAD, nbytes=FOUR * MIB, name="attn1_fwd",
    )(qkv, qkv, qkv, left, right, lo, hi)


def attn1_bwd_body(q_ref, k_ref, v_ref, do_ref, lse_ref, del_ref, kvl, kvr, ql, qr, dl, dr, ll, lr, el, er,
                   lo_ref, hi_ref, out_ref, s_s, d_s, p_s, t_s):
    def window(e):
        first, last = max(LANE * e - WIN, ZERO), min(LANE * e + LANE + WIN, EXT)
        return first, last - first

    def parts(h):
        q_t = joined(ql, q_ref, qr, h) * SCALE
        return q_t, joined(dl, do_ref, dr, h), joined(kvl, k_ref, kvr, h, LOW, LOW)

    def some(heads):
        for a, h in enumerate(heads):
            q_t, do_t, k_t = parts(h)
            k_rows, v_rows = k_t.T, joined(kvl, v_ref, kvr, h, HIGH, HIGH).T
            for e in range(XBLK):
                first, n = window(e)
                cols = blocks(e, e + ONE)
                s_s[a, e, :n] = mm(k_rows[first:first + n], q_t[:, cols])
                d_s[a, e, :n] = mm(v_rows[first:first + n], do_t[:, cols])
        for a, h in enumerate(heads):
            lse, delta = joined(ll, lse_ref, lr, h), joined(el, del_ref, er, h)
            for e in range(XBLK):
                first, n = window(e)
                cols = blocks(e, e + ONE)
                ok = in_bounds(lo_ref, hi_ref, cols, first, n)
                p = jnp.exp(jnp.where(ok, s_s[a, e, :n] - lse[:, cols], NEG))
                p_s[a, first:first + n, cols] = p.astype(BF)
                t_s[a, first:first + n, cols] = (p * (d_s[a, e, :n] - delta[:, cols])).astype(BF)
        for a, h in enumerate(heads):
            q_t, do_t, k_t = parts(h)
            got = [[], [], []]
            for b in range(XBLK):
                here, wide = blocks(b, b + ONE), blocks(max(b - ONE, ZERO), min(b + TWO, XBLK))
                got[ZERO].append(mm(k_t[:, wide], t_s[a, wide, here]) * SCALE)
                got[ONE].append(mm_nt(q_t[:, wide], t_s[a, here, wide]))
                got[TWO].append(mm_nt(do_t[:, wide], p_s[a, here, wide]))
            for n in range(THREE):
                out_ref[n, h] = jnp.concatenate([g.astype(BF) for g in got[n]], axis=ONE)[:, WIN:WIN + TOK]

    @pl.when(pl.program_id(ZERO) == ZERO)
    def _():
        p_s[...] = jnp.zeros(p_s.shape, BF)
        t_s[...] = jnp.zeros(t_s.shape, BF)

    every_head(some, AHEAD_BWD)


def attn1_bwd(qkv, do_t, lse, delta, kv_edges, far, lo, hi):
    bound, edge, row = spec((ONE, EXT)), heads_of(LANE, ZERO), row_of(LANE)
    return call(
        attn1_bwd_body, (HSTEPS,),
        [own_head(ZERO), own_head(ONE), own_head(TWO), own_head(ZERO), row_of(TOK), row_of(TOK)]
        + [edge] * SIX + [row] * FOUR + [bound, bound],
        spec((THREE, HPS, HEAD, TOK), ZERO, step_of, ZERO, ZERO),
        sds((THREE, NHEAD, HEAD, TOK), BF),
        scratch=[pltpu.VMEM((AHEAD_BWD, XBLK, REACH, LANE), F32)] * TWO + [pltpu.VMEM((AHEAD_BWD, EXT, EXT), BF)] * TWO,
        flops=NHEAD * 10 * TOK * REACH * HEAD, nbytes=8 * MIB, name="attn1_bwd",
    )(qkv, qkv, qkv, do_t, lse, delta, *kv_edges, *far, lo, hi)


ROWBLK = [slice(r, r + RB) for r in range(ZERO, TOK, RB)]
HALFT = NFT // TWO
SQRT_HALF = math.sqrt(SCALE * FOUR)
PDF_SCALE = SQRT_HALF / math.sqrt(math.pi)


def normal_cdf(a):
    return SQRT_HALF * SQRT_HALF * (ONE + lax.erf(a * SQRT_HALF))


def half_rows(ref, which):
    n = ref.shape[ZERO] // TWO
    return ref.at[pl.ds(pl.multiple_of(which * n, n), n)]


def col_tile(ref, n):
    return ref.at[:, pl.ds(pl.multiple_of(n * FT, FT), FT)]


class Refs:
    def __init__(self, names, refs):
        self.__dict__.update(zip(names, refs))


def mlp_body(*refs, names, fwd, bwd):
    r = Refs(names, refs)
    step = pl.program_id(ZERO)
    sw = Swaps(r.ssem, r.rsem, r.lsem)
    start = []
    whole_group = not (fwd and bwd)
    if fwd:
        start = [sw.remote(r.h, r.h_r), sw.remote(half_rows(r.of, sw.other), r.of_r),
                 sw.local(half_rows(r.of, sw.core), r.of_m)]
        if whole_group:
            o_in = sw.to_all(lambda dev: r.o.at[dev], lambda dev: r.o_s.at[dev])
        m_out = [(sw.remote(r.m_s.at[HALFT * sw.other + n], col_tile(r.m_r, n)),
                  sw.local(r.m_s.at[HALFT * sw.core + n], col_tile(r.m_m, n))) for n in range(HALFT)]
    if bwd:
        start.append(sw.remote(r.dy, r.dy_r))
        dmid_out = sw.remote(r.dmid, r.dmid_r)
        du_out = [(sw.remote(r.du_s.at[n, sw.other], col_tile(r.du_r, n)),
                   sw.local(r.du_s.at[n, sw.core], col_tile(r.du_m, n))) for n in range(NFT)]

    if bwd and whole_group:
        do_out = sw.to_all(lambda dev: r.do_s.at[dev], lambda dev: r.d_o.at[dev])

    @pl.when(step == ZERO)
    def _():
        if whole_group:
            meet_row(sw)
        else:
            meet(sw.partner)
        if fwd:
            if whole_group:
                for cp in o_in:
                    cp.start()
                sw.wait(o_in)
            for n in range(NHEAD):
                r.of[HEAD * n:HEAD * n + HEAD, :] = (r.o_s[n % FOUR, n // FOUR] if whole_group else r.o[n])
            x1 = (r.x[...].astype(F32) + mm_tn(r.of[...], r.wp[...])).astype(BF)
            r.x1[...] = x1
            r.h[...] = norm_rows(x1, r.g[...])
            r.acc[...] = x1.astype(F32)
        if bwd:
            r.dacc[...] = jnp.zeros(r.dacc.shape, F32)
        for cp in start:
            cp.start()

    for rows in ROWBLK:
        if fwd:
            ua = mm(r.h[rows], r.wa[...]).astype(BF)
            ub = mm(r.h[rows], r.wb[...]).astype(BF)
            if not bwd:
                r.u[ZERO, rows] = ua
                r.u[ONE, rows] = ub
        else:
            ua, ub = r.u[ZERO, rows], r.u[ONE, rows]
        a, b = ua.astype(F32), ub.astype(F32)
        cdf = normal_cdf(a)
        gate = a * cdf
        if fwd:
            m = (gate * b).astype(BF)
            r.m_s[step, rows] = m
            r.acc[rows] += mm(m, r.wo[...])
        if bwd:
            dm = mm_nt(r.dy[rows], r.wo[...]).astype(BF).astype(F32)
            pdf = jnp.exp(a * a * (SCALE * FOUR - ONE)) * PDF_SCALE
            db = (dm * gate).astype(BF)
            da = (dm * b * (cdf + a * pdf)).astype(BF)
            r.du_s[step, ZERO, rows] = da
            r.du_s[step, ONE, rows] = db
            r.dacc[rows] += mm_nt(da, r.wa[...]) + mm_nt(db, r.wb[...])

    for n in range(NFT):
        @pl.when(step == n)
        def _(n=n):
            if fwd:
                there, here = m_out[n % HALFT]

                @pl.when(sw.core == n // HALFT)
                def _():
                    here.start()

                @pl.when(sw.other == n // HALFT)
                def _():
                    there.start()
            if bwd:
                for cp in du_out[n]:
                    cp.start()

    @pl.when(step == NFT - ONE)
    def _():
        if fwd:
            r.y[...] = r.acc[...].astype(BF)
        if bwd:
            d_ln, gg = norm_rows_grad(r.x1[...], r.g[...], r.dacc[...].astype(BF))
            r.gg[...] = gg
            d_mid = add_bf(r.dy[...], d_ln)
            r.dmid[...] = d_mid
            dmid_out.start()
            d_att = mm_nt(r.wp[...], d_mid).astype(BF)
            for n in range(NHEAD):
                rows = slice(HEAD * n, HEAD * n + HEAD)
                blk = d_att[rows]
                if whole_group:
                    r.do_s[n % FOUR, n // FOUR] = blk
                else:
                    r.d_o[n] = blk
                    r.delta[n] = jnp.sum(blk.astype(F32) * r.of[rows].astype(F32), axis=ZERO, keepdims=True)
            if whole_group:
                for cp in do_out:
                    cp.start()
        sw.wait()


def mlp_call(layer, cid, fwd, bwd, w_proj, gain, w_in, w_out, x=None, o_t=None, dy=None, x1=None, u=None, oshape=None):
    toks, tok_spec, vec = sds(ALLTOK, BF), spec(ALLTOK), spec((ONE, DM))
    u_spec = spec((TWO, TOK, FT), ZERO, ZERO, step_of)
    half_o = sds((DM // TWO, TOK), BF)
    half_m, half_u = sds((TOK, FF // TWO), BF), sds((TOK, FF), BF)
    ins = [('wp', w_proj, spec((None, DM, DM), layer, ZERO, ZERO)), ('g', gain, vec),
           ('wa', w_in, weight_cols(layer, FT)), ('wb', w_in, weight_cols(layer, FT, NFT)),
           ('wo', w_out, spec((None, FT, DM), layer, step_of, ZERO))]
    outs, scratch = [], []
    if fwd:
        ins += [('x', x, tok_spec), ('o', o_t, spec(o_t.shape) if bwd else ANY)]
        outs += [('y', toks, tok_spec), ('h', toks, tok_spec), ('h_r', toks, ANY), ('of_m', half_o, ANY), ('of_r', half_o, ANY),
                 ('m_m', half_m, ANY), ('m_r', half_m, ANY)]
        scratch += [('acc', pltpu.VMEM(ALLTOK, F32)), ('of', pltpu.VMEM((DM, TOK), BF)), ('m_s', pltpu.VMEM((NFT, TOK, FT), BF))]
    if fwd and not bwd:
        outs += [('x1', toks, tok_spec), ('u', sds((TWO, TOK, FF), BF), u_spec)]
        scratch += [('o_s', pltpu.VMEM(o_t.shape, BF))]
    if bwd:
        ins += [('dy', dy, tok_spec)]
        outs += [('dmid', toks, tok_spec), ('gg', sds((ONE, DM), F32), vec), ('d_o', sds(oshape, BF), spec(oshape) if fwd else ANY),
                 ('dy_r', toks, ANY), ('dmid_r', toks, ANY), ('du_m', half_u, ANY), ('du_r', half_u, ANY)]
        scratch += [('dacc', pltpu.VMEM(ALLTOK, F32)), ('du_s', pltpu.VMEM((NFT, TWO, TOK, FT), BF))]
    if fwd and bwd:
        outs += [('delta', sds((NHEAD, ONE, TOK), F32), spec((NHEAD, ONE, TOK)))]
        scratch += [('x1', pltpu.VMEM(ALLTOK, BF))]
    if not fwd:
        ins += [('x1', x1, tok_spec), ('u', u, u_spec)]
        scratch += [('do_s', pltpu.VMEM(oshape, BF))]
    sems = DMA((FOUR * NFT,))
    scratch += [('ssem', sems), ('rsem', sems), ('lsem', sems)]
    names = [n for n, *_ in ins + outs + scratch]
    name = "mlp_" + "fwd" * fwd + "bwd" * bwd
    got = call(
        functools.partial(mlp_body, names=names, fwd=fwd, bwd=bwd), (NFT,),
        [sp for *_, sp in ins], [sp for *_, sp in outs], [sh for _, sh, _ in outs], scratch=[sh for _, sh in scratch],
        flops=TWO * TOK * DM * (DM + THREE * FF) * (fwd + bwd), nbytes=26 * MIB, name=name, cid=cid,
    )(*[arr for _, arr, _ in ins])
    return Refs([n for n, *_ in outs], got)


def qkv_bwd_body(d_ref, cos_ref, sin_ref, w_ref, x_ref, g_ref, dmid_ref, dx_ref, gg_ref, dtm_ref, dtr_ref,
                 acc, dt_s, dt_all, ssem, rsem, lsem):
    step = pl.program_id(ZERO)
    core, partner = core_and_partner()

    def dst(ref, n):
        rows = PROJ
        return ref.at[pl.ds(pl.multiple_of(n * rows, rows), rows)]

    def copies(n):
        return (pltpu.make_async_remote_copy(src_ref=dt_s.at[ONE - core, n], dst_ref=dst(dtr_ref, n), send_sem=ssem.at[n],
                                             recv_sem=rsem.at[n], device_id=partner, device_id_type=MESH),
                pltpu.make_async_copy(dt_s.at[core, n], dst(dtm_ref, n), lsem.at[n]))

    @pl.when(step == ZERO)
    def _():
        acc[...] = jnp.zeros(acc.shape, F32)
        meet(partner)

    def put(chunk, head, row, val):
        at = LANE * chunk + row + HEAD * (head % TWO)
        dt_s[head // TWO, step, at:at + val.shape[ZERO]] = val
        at = RB * chunk + row + HEAD * head
        dt_all[at:at + val.shape[ZERO]] = val

    @pl.when(step < TWO)
    def _():
        cos, sin = cos_ref[...], sin_ref[...]
        for chunk in CHUNKS:
            for head in range(FOUR):
                d_head = head_rows(d_ref, chunk, head)[...].astype(F32)
                da, db = d_head[:HALF], d_head[HALF:]
                put(chunk, head, ZERO, (da * cos + db * sin).astype(BF))
                put(chunk, head, HALF, (db * cos - da * sin).astype(BF))

    @pl.when(step == TWO)
    def _():
        for chunk in CHUNKS:
            for head in range(FOUR):
                put(chunk, head, ZERO, head_rows(d_ref, chunk, head)[...])

    for cp in copies(step):
        cp.start()
    acc[...] += mm(w_ref[...], dt_all[...])

    @pl.when(step == TWO)
    def _():
        d_ln, gg = norm_rows_grad(x_ref[...], g_ref[...], acc[...].T.astype(BF))
        gg_ref[...] = gg
        dx_ref[...] = add_bf(dmid_ref[...], d_ln)
        for n in range(THREE):
            for cp in copies(n):
                cp.wait()


def qkv_bwd(d_qkv, cos_t, sin_t, w_qkv, x, gain, d_mid, layer, dest_major, cid):
    table = spec((HALF, TOK))
    half = sds((THREE * PROJ, TOK), BF)
    return call(
        qkv_bwd_body, (THREE,),
        [heads_spec(dest_major), table, table, weight_cols(layer, DM), spec(ALLTOK), spec((ONE, DM)), spec(ALLTOK)],
        [spec(ALLTOK), spec((ONE, DM)), ANY, ANY],
        [sds(ALLTOK, BF), sds((ONE, DM), F32), half, half],
        scratch=[pltpu.VMEM((DM, TOK), F32), pltpu.VMEM((TWO, THREE, PROJ, TOK), BF), pltpu.VMEM((DM, TOK), BF),
                 DMA((THREE,)), DMA((THREE,)), DMA((THREE,))],
        flops=TWO * TOK * DM * THREE * DM, nbytes=10 * MIB, name="qkv_bwd", cid=cid,
    )(d_qkv, cos_t, sin_t, w_qkv, x, gain, d_mid)


DOWN = FF // TWO
UP = FF
QKV = THREE * PROJ
MLP_ROWS = DOWN + UP
ATT_ROWS = PROJ + QKV
RING_ROWS = TWO * ATT_ROWS + MLP_ROWS
NDOWN = DOWN // DM


def grad_call(body, grads, steps, in_specs, args, rows, first_row, total, scratch=(), edges=(), cid=None):
    shared = [] if grads is None else [grads]
    first = first_row // rows
    more = [sds(arr.shape[:TWO] + (LANE,), arr.dtype) for arr in edges for _ in range(TWO)]
    return call(
        functools.partial(body, edges=len(edges)) if edges else body, (steps,), [ANY] * len(shared + list(edges)) + in_specs,
        [spec((rows, DM), lambda s: first + s, ZERO)] + [ANY] * len(more), [sds((total, DM), F32)] + more, scratch=scratch,
        flops=FOUR * steps * rows * TOK * DM, nbytes=20 * MIB, name=getattr(body, "__name__"), cid=cid,
        alias={ZERO: ZERO} if shared else None,
    )(*shared, *edges, *args)


GRAD_INS = 8


def grad_mlp_body(*refs, edges=ZERO):
    step = pl.program_id(ZERO)
    if edges:
        srcs, refs, (h_t, *sems) = refs[:edges], refs[edges:-FOUR], refs[-FOUR:]
        refs, outs = refs[:GRAD_INS + ONE], refs[GRAD_INS + ONE:]
        sw = Swaps(*sems)
        for n, src in enumerate(srcs):
            view = src.at[:NHEAD]
            sw.to_sides(view.at[:, :, :LANE], view.at[:, :, TOK - LANE:], outs[TWO * n].at[:NHEAD], outs[TWO * n + ONE].at[:NHEAD])

        @pl.when(step == ZERO)
        def _():
            meet_sides()
            for cp in sw.waits:
                cp.start()
    else:
        refs, h_t = refs[:-ONE], refs[-ONE]
    ma, mb, dya, dyb, ha, hb, dua, dub, out_ref = refs[-GRAD_INS - ONE:]

    @pl.when(step < NDOWN)
    def _():
        out_ref[...] = mm_tn(ma[...], dya[...]) + mm_tn(mb[...], dyb[...])

    @pl.when(step == NDOWN)
    def _():
        h_t[ZERO] = ha[...].T
        h_t[ONE] = hb[...].T

    @pl.when(step >= NDOWN)
    def _():
        out_ref[...] = mm(h_t[ZERO], dua[...]) + mm(h_t[ONE], dub[...])

    if edges:
        @pl.when(step == NDOWN + UP // DM - ONE)
        def _():
            sw.wait()


def grad_mlp(grads, m, m_r, dy, dy_r, h, h_r, du, du_r, first_row, total, edges=(), cid=None):
    toks = spec(ALLTOK)
    m_col = spec(ALLTOK, ZERO, lambda s: jnp.minimum(s, NDOWN - ONE))
    du_col = spec(ALLTOK, ZERO, lambda s: jnp.maximum(s - NDOWN, ZERO))
    return grad_call(grad_mlp_body, grads, NDOWN + UP // DM, [m_col, m_col, toks, toks, toks, toks, du_col, du_col],
                     (m, m_r, dy, dy_r, h, h_r, du, du_r), DM, first_row, total, edges=edges, cid=cid,
                     scratch=[pltpu.VMEM((TWO, DM, TOK), BF)] + (swap_sems(TWO * len(edges)) if edges else []))


def grad_att_body(*refs):
    oa, ob, dma, dmb, ta, tb, ha, hb, out_ref = refs[-GRAD_INS - ONE:]
    step = pl.program_id(ZERO)

    @pl.when(step == ZERO)
    def _():
        out_ref[...] = mm(oa[...], dma[...]) + mm(ob[...], dmb[...])

    @pl.when(step > ZERO)
    def _():
        out_ref[...] = mm(ta[...], ha[...]) + mm(tb[...], hb[...])


def grad_att(grads, of, of_r, dmid, dmid_r, dt, dt_r, h, h_r, first_row):
    toks = spec(ALLTOK)
    blk = (PROJ, TOK)
    dt_row = spec(blk, lambda s: jnp.maximum(s - ONE, ZERO), ZERO)
    return grad_call(grad_att_body, grads, ONE + QKV // PROJ, [spec(blk), spec(blk), toks, toks, dt_row, dt_row, toks, toks],
                     (of, of_r, dmid, dmid_r, dt, dt_r, h, h_r), PROJ, first_row, RING_ROWS)


NB, NS = 5, 6
CH = RING_ROWS // (NB * FOUR)
SB, LF = CH // FOUR, CH // 16
RS = 9
LAST = RS + RS
ADD_ROWS = 96


def ring_body(g_ref, ln_ref, f_ref, lnout_ref, bufa, bufb, bufc, gath, stage, lnbuf,
              ssem, rsem, psem, qsem, csem, stsem, lns, lnr):
    core, partner = core_and_partner()
    zy = lax.axis_index('zy')
    pos = (lax.axis_index('sp'), lax.rem(zy, FOUR), zy // FOUR)
    streams = [(c, sg) for c in range(THREE) for sg in (ONE, -ONE)]
    bufs, sizes = (bufa, bufb, bufc), (CH, SB, LF)
    peers = range(ONE, FOUR)

    def mod4(v):
        return lax.rem(v + 8, FOUR)

    def at(axis, val):
        if axis == ZERO:
            return {'sp': val}
        yz = (val, pos[TWO]) if axis == ONE else (pos[ONE], val)
        return {'zy': yz[ONE] * FOUR + yz[ZERO]}

    def shifted(axis, d):
        return at(axis, mod4(pos[axis] + d))

    def axis_of(s, ph):
        return (streams[s][ZERO] + ph) % THREE

    def idx(s, ph, t):
        return mod4(pos[axis_of(s, ph)] - streams[s][ONE] * t)

    def own(s, ph):
        return idx(s, ph, -ONE)

    def base(b):
        return b * (FOUR * CH)

    bar = pltpu.get_barrier_semaphore()
    for ax in range(THREE):
        for d in peers:
            pl.semaphore_signal(bar, inc=ONE, device_id=shifted(ax, d), device_id_type=MESH)
    pl.semaphore_signal(bar, inc=ONE, device_id=partner, device_id_type=MESH)
    pl.semaphore_wait(bar, 10)

    def rows(ref, start, n):
        return ref.at[pl.ds(pl.multiple_of(start, LF), n)]

    def grows(s, start, n):
        return g_ref.at[pl.ds(pl.multiple_of(start, LF), n), LANE * s:LANE * s + LANE]

    def frows(s, start, n):
        return f_ref.at[core, pl.ds(pl.multiple_of(start, LF), n), LANE * s:LANE * s + LANE]

    def same_bytes(b, k):
        if k < RS:
            return bufs[k // THREE].at[b, k % THREE]
        n = sizes[TWO - (k - RS) // THREE]
        return gath.at[b] if n == CH else gath.at[b, :, pl.ds(ZERO, n)]

    def wait_for(ref, sem):
        pltpu.make_async_copy(ref, ref, sem).wait()

    def send(b, s, k):
        ph = k // THREE if k < RS else TWO - (k - RS) // THREE
        t = k % THREE
        n = sizes[ph]
        if k < RS:
            dst = bufs[ph].at[b, t, s]
            if t:
                src = bufs[ph].at[b, t - ONE, s]
            elif ph:
                src = rows(bufs[ph - ONE].at[b, TWO, s], idx(s, ph, ZERO) * n, n)
            else:
                src = grows(s, base(b) + idx(s, ZERO, ZERO) * n, n)
        elif ph:
            off = own(s, ONE) * SB if ph == TWO else ZERO
            src = dst = rows(gath.at[b, s], off + idx(s, ph, t - ONE) * n, n)
        else:
            dst = frows(s, base(b) + idx(s, ZERO, t - ONE) * n, n)
            src = dst if t else gath.at[b, s]
        pltpu.make_async_remote_copy(src_ref=src, dst_ref=dst, send_sem=ssem.at[b, k], recv_sem=rsem.at[b, k],
                                     device_id=shifted(axis_of(s, ph), streams[s][ONE]), device_id_type=MESH).start()

    def stage_load(n):
        t, b, slot = n // NB, lax.rem(n, NB), lax.rem(n, TWO)
        for s in range(NS):
            pltpu.make_async_copy(grows(s, base(b) + idx(s, ZERO, t + ONE) * CH, CH), stage.at[slot, s],
                                  stsem.at[slot]).start()

    def ln_copy(ph, d):
        return pltpu.make_async_remote_copy(
            src_ref=lnbuf.at[ph, THREE] if ph else ln_ref, dst_ref=lnbuf.at[ph, d - ONE], send_sem=lns.at[ph, d - ONE],
            recv_sem=lnr.at[ph, d - ONE], device_id=shifted(ph, d) if ph < THREE else partner, device_id_type=MESH)

    def ln_sum(ph):
        vals = [lnbuf[ph, THREE] if ph else ln_ref[...]] + [lnbuf[ph, d - ONE] for d in peers]
        total = jnp.zeros_like(vals[ZERO])
        for p in range(FOUR):
            term = vals[ZERO]
            for d in peers:
                term = jnp.where(mod4(pos[ph] - d) == p, vals[d], term)
            total = total + term
        return total

    def batches(fn, start=ZERO):
        def body(b, c):
            fn(b)
            return c
        lax.fori_loop(start, NB, body, ZERO)

    def first(b):
        for s in range(NS):
            send(b, s, ZERO)

    first(ZERO)
    stage_load(jnp.int32(ZERO))
    for d in peers:
        ln_copy(ZERO, d).start()
    batches(first, ONE)

    for k in range(RS):
        ph, t = k // THREE, k % THREE
        buf, size = bufs[ph], sizes[ph]

        def step(b, k=k, ph=ph, t=t, buf=buf, size=size):
            n = k * NB + b
            slot = lax.rem(n, TWO)
            if not ph:
                @pl.when(n < THREE * NB - ONE)
                def _():
                    stage_load(n + ONE)
                wait_for(stage.at[slot], stsem.at[slot])
            wait_for(same_bytes(b, k), rsem.at[b, k])
            for s in range(NS):
                if ph:
                    off = pl.multiple_of(idx(s, ph, t + ONE) * size, LF)
                    buf[b, t, s] += bufs[ph - ONE][b, TWO, s, pl.ds(off, size)]
                else:
                    @pl.loop(ZERO, CH, step=ADD_ROWS)
                    def _(r):
                        at_r = pl.ds(pl.multiple_of(r, ADD_ROWS), ADD_ROWS)
                        buf[b, t, s, at_r] += stage[slot, s, at_r]
                if k == RS - ONE:
                    off = pl.multiple_of(own(s, ONE) * SB + own(s, TWO) * LF, LF)
                    gath[b, s, pl.ds(off, LF)] = bufc[b, TWO, s]
                send(b, s, k + ONE)

        batches(step)
        if k < SIX and k % TWO == ZERO:
            lp = k // TWO
            for d in peers:
                ln_copy(lp, d).wait()
            lnbuf[lp + ONE, THREE] = ln_sum(lp)
            for d in peers if lp < TWO else (ONE,):
                ln_copy(lp + ONE, d).start()

    def hand_over(b, s, j, src, start):
        pltpu.make_async_remote_copy(src_ref=src, dst_ref=frows(s, start, CH), send_sem=psem.at[b, j], recv_sem=qsem.at[b, j],
                                     device_id=partner, device_id_type=MESH).start()

    for k in range(RS, LAST):
        def step(b, k=k):
            wait_for(same_bytes(b, k), rsem.at[b, k])
            piece = k - (LAST - FOUR)
            for s in range(NS):
                if k < LAST - ONE:
                    send(b, s, k + ONE)
                if piece >= ZERO:
                    start = base(b) + idx(s, ZERO, piece - ONE) * CH
                    if piece:
                        hand_over(b, s, piece, frows(s, start, CH), start)
                    else:
                        pltpu.make_async_copy(gath.at[b, s], frows(s, start, CH), csem.at[b]).start()
                        hand_over(b, s, piece, gath.at[b, s], start)
        batches(step)

    ln_copy(THREE, ONE).wait()
    lnout_ref[...] = lnbuf[THREE, THREE] + lnbuf[THREE, ZERO]

    def finish(b):
        for k in range(LAST):
            wait_for(same_bytes(b, k), ssem.at[b, k])
        for j in range(FOUR):
            wait_for(gath.at[b], psem.at[b, j])
            wait_for(gath.at[b], qsem.at[b, j])
        wait_for(gath.at[b], csem.at[b])
    batches(finish)


def ring_all_reduce(g, ln, cid):
    vmem = pl.BlockSpec(memory_space=pltpu.VMEM)
    return pl.pallas_call(
        ring_body,
        in_specs=[ANY, vmem],
        out_specs=[ANY, vmem],
        out_shape=[sds((TWO, RING_ROWS, DM), F32), sds(ln.shape, F32)],
        scratch_shapes=[
            pltpu.VMEM((NB, THREE, NS, CH, LANE), F32), pltpu.VMEM((NB, THREE, NS, SB, LANE), F32),
            pltpu.VMEM((NB, THREE, NS, LF, LANE), F32), pltpu.VMEM((NB, NS, CH, LANE), F32),
            pltpu.VMEM((TWO, NS, CH, LANE), F32),
            pltpu.VMEM((FOUR, FOUR) + ln.shape, F32),
            DMA((NB, LAST)), DMA((NB, LAST)), DMA((NB, FOUR)), DMA((NB, FOUR)), DMA((NB,)), DMA((TWO,)),
            DMA((FOUR, THREE)), DMA((FOUR, THREE)),
        ],
        compiler_params=pltpu.CompilerParams(collective_id=cid, has_side_effects=True, vmem_limit_bytes=60 * MIB),
        cost_estimate=pl.CostEstimate(flops=MIB * MIB // FOUR, bytes_accessed=200 * MIB, transcendentals=ZERO),
        name="ring_all_reduce",
    )(g, ln)


SLOTS, LAG = 8, 4
NTURN = TWO * THREE
OUT_SHAPE, IN_SHAPE = (TWO, FF, DM), (TWO, DM, TWO * FF)


def stream(pieces, buf, turned, isem, osem):
    def loads(i):
        slot, srcs = i % SLOTS, pieces[i][ZERO]
        n = srcs[ZERO].shape[ZERO]
        return [pltpu.make_async_copy(src, buf.at[slot, k * n:k * n + n], isem.at[slot, k]) for k, src in enumerate(srcs)]

    def store(i):
        _, dst, turn = pieces[i]
        src = buf.at[i % SLOTS, :dst.shape[ZERO]] if turn is None else turned.at[turn]
        return pltpu.make_async_copy(src, dst, osem.at[i % SLOTS])

    total = len(pieces)
    for i in range(total + LAG):
        if i < total:
            if i >= SLOTS:
                store(i - SLOTS).wait()
            for cp in loads(i):
                cp.start()
        k = i - LAG
        if k >= ZERO:
            for cp in loads(k):
                cp.wait()
            turn = pieces[k][TWO]
            if turn is not None:
                for n in CHUNKS:
                    rows, col = LANE * n, RB * n
                    turned[turn, :, col:col + LANE] = buf[k % SLOTS, rows:rows + LANE].T
                    turned[turn, :, col + LANE:col + RB] = buf[k % SLOTS, PROJ + rows:PROJ + rows + LANE].T
            store(k).start()
    for i in range(max(total - SLOTS, ZERO), total):
        store(i).wait()


def unpack_ring_body(f, g_qkv, g_proj, g_in, g_out, *scratch):
    def block(c, row, n=DM):
        return f.at[c, row:row + n]

    pieces = []
    for c in range(TWO):
        for n in range(NDOWN):
            pieces.append(([block(c, ATT_ROWS + DM * n)], g_out.at[ZERO, DOWN * c + DM * n:DOWN * c + DM * n + DM], None))
        for n in range(FOUR):
            col = UP * c + DM * n
            pieces.append(([block(c, ATT_ROWS + DOWN + DM * n)], g_in.at[ZERO, :, col:col + DM], None))
    for l in range(TWO):
        first = (ONE - l) * (ATT_ROWS + MLP_ROWS)
        for n in range(THREE):
            row = first + PROJ * (n + ONE)
            pieces.append(([block(c, row, PROJ) for c in range(TWO)], g_qkv.at[l, :, DM * n:DM * n + DM], THREE * l + n))
        for c in range(TWO):
            pieces.append(([block(c, first, PROJ)], g_proj.at[l, PROJ * c:PROJ * c + PROJ], None))
    stream(pieces, *scratch)


def unpack_mlp_body(own, other, in_0, out_0, g_in, g_out, *scratch):
    core = lax.axis_index('core')
    pieces = []
    for src, side in ((own, core), (other, ONE - core)):
        for n in range(NDOWN):
            row = pl.multiple_of(DOWN * side + DM * n, DM)
            pieces.append(([src.at[DM * n:DM * n + DM]], g_out.at[ONE, pl.ds(row, DM)], None))
        for n in range(FOUR):
            col = pl.multiple_of(UP * side + DM * n, DM)
            pieces.append(([src.at[DOWN + DM * n:DOWN + DM * n + DM]], g_in.at[ONE, :, pl.ds(col, DM)], None))
    stream(pieces, *scratch)


def unpack_call(body, args, outs, alias, name):
    return pl.pallas_call(
        body, in_specs=[ANY] * len(args), out_specs=[ANY] * len(outs), out_shape=[sds(shape, F32) for shape in outs],
        scratch_shapes=[pltpu.VMEM((SLOTS, DM, DM), F32), pltpu.VMEM((NTURN, DM, DM), F32), DMA((SLOTS, TWO)), DMA((SLOTS,))],
        input_output_aliases=alias,
        compiler_params=pltpu.CompilerParams(vmem_limit_bytes=60 * MIB),
        cost_estimate=pl.CostEstimate(flops=MIB * MIB // RB, bytes_accessed=75 * MIB, transcendentals=ZERO), name=name,
    )(*args)


def rope_tables(pos, base):
    inv_freq = base ** (jnp.arange(HALF).astype(F32) * (-TWO / HEAD))
    angles = inv_freq[:, None] * pos.astype(F32)[None, :]
    return jnp.cos(angles), jnp.sin(angles)


def solution(mesh):
    n_sp = mesh.shape['sp']
    by_core = mesh.devices.reshape(n_sp, mesh.shape['dp'] // TWO, TWO)
    mesh = Mesh(by_core, ('sp', 'zy', 'core'))
    dp_axes = ('zy', 'core')
    row_axes = dp_axes + ('sp',)
    token_spec = P(row_axes, None)
    swap_cores = [(ZERO, ONE), (ONE, ZERO)]
    cids = list(range(RS))

    def exchange(arr):
        return lax.all_to_all(arr, 'sp', ZERO, ZERO, tiled=True)

    def device_step(x_loc, cu_loc, pos_loc, w_qkv, w_proj, w_in, w_out, ln_attn, ln_mlp, d_out):
        sp = lax.axis_index('sp')
        cu = cu_loc[ZERO][:, None]

        def bounds_of(tok):
            start = jnp.max(jnp.where(cu <= tok, cu, ZERO), axis=ZERO)
            return start, jnp.min(jnp.where(cu > tok, cu, GRP), axis=ZERO)

        start, stop = bounds_of(jnp.arange(GRP)[None, :])
        tiles = start[::QT] // QT, (stop[QT - ONE::QT] + QT - ONE) // QT
        rows = start[None, :], stop[None, :]
        shift = sp * TOK - WIN
        tok_x = jnp.arange(EXT) + shift
        start_x, stop_x = bounds_of(tok_x[None, :])
        inside = (tok_x >= ZERO) & (tok_x < GRP)
        near = (jnp.where(inside, jnp.maximum(start_x, tok_x - WIN) - shift, ZERO)[None, :],
                jnp.where(inside, jnp.minimum(stop_x, tok_x + WIN + ONE) - shift, ZERO)[None, :])
        near_own = [b[:, WIN:WIN + TOK] for b in near]
        tab0, tab1 = [rope_tables(pos_loc, base) for base in BASES]
        la0, la1, lm0, lm1 = ln_attn[:ONE], ln_attn[ONE:], ln_mlp[:ONE], ln_mlp[ONE:]

        w_mlp = (w_in, w_out)
        h0, qkv0, h0r = qkv_fwd(x_loc, la0, w_qkv, ZERO, *tab0, True, cids[ONE])
        oh0, lse0 = attn0_fwd(*tiles, qkv0, *rows)
        f0 = mlp_call(ZERO, cids[TWO], True, False, w_proj, lm0, *w_mlp, x=x_loc, o_t=oh0)
        x1 = f0.y
        h1, qkv1, h1r, *kv_edges = qkv_fwd(x1, la1, w_qkv, ONE, *tab1, False, cids[THREE])
        qkv1 = qkv1.reshape((THREE * NHEAD, HEAD, TOK))
        o1, lse1 = attn1_fwd(qkv1, *kv_edges, *near_own)
        f1 = mlp_call(ONE, cids[FOUR], True, True, w_proj, lm1, *w_mlp, x=x1, o_t=o1, dy=d_out, oshape=(NHEAD, HEAD, TOK))
        g_side, *far = grad_mlp(None, f1.m_m, f1.m_r, d_out, f1.dy_r, f1.h, f1.h_r, f1.du_m, f1.du_r, ZERO, MLP_ROWS,
                                edges=(qkv1, f1.d_o, lse1, f1.delta), cid=cids[8])
        g_side = lax.psum(g_side, ('sp', 'zy'))
        dqkv1 = attn1_bwd(qkv1, f1.d_o, lse1, f1.delta, kv_edges, far, *near)
        dx1, gga1, dt1, dt1r = qkv_bwd(dqkv1.reshape(THREE, THREE, FOUR, HEAD, TOK), *tab1, w_qkv, x1, la1, f1.dmid,
                                       ONE, False, cids[SIX])
        b0 = mlp_call(ZERO, cids[5], False, True, w_proj, lm0, *w_mlp, dy=dx1, x1=f0.x1, u=f0.u, oshape=oh0.shape)
        dqkv0 = exchange(attn0_bwd(*tiles, qkv0, oh0, b0.d_o, lse0, *rows))
        grads, = grad_att(None, f1.of_m, f1.of_r, f1.dmid, f1.dmid_r, dt1, dt1r, h1, h1r, ZERO)
        grads, = grad_mlp(grads, f0.m_m, f0.m_r, dx1, b0.dy_r, f0.h, f0.h_r, b0.du_m, b0.du_r, ATT_ROWS, RING_ROWS)
        dx0, gga0, dt0, dt0r = qkv_bwd(dqkv0, *tab0, w_qkv, x_loc, la0, b0.dmid, ZERO, True, cids[7])
        grads, = grad_att(grads, f0.of_m, f0.of_r, b0.dmid, b0.dmid_r, dt0, dt0r, h0, h0r, ATT_ROWS + MLP_ROWS)

        gains = jnp.concatenate([gga0, gga1, b0.gg, f1.gg, jnp.zeros((FOUR, DM), F32)], axis=ZERO)
        summed, gains = ring_all_reduce(grads, gains, cids[ZERO])
        summed, g_side = lax.optimization_barrier((summed, g_side))
        from_partner = lax.ppermute(g_side, 'core', swap_cores)
        shapes = [(TWO, DM, THREE * DM), (TWO, DM, DM), IN_SHAPE, OUT_SHAPE]
        g_qkv, g_proj, g_in, g_out = unpack_call(unpack_ring_body, (summed,), shapes, {}, "unpack_ring")
        g_in, g_out = unpack_call(unpack_mlp_body, (g_side, from_partner, g_in, g_out), shapes[TWO:],
                                  {TWO: ZERO, THREE: ONE}, "unpack_mlp")
        return f1.y, dx0, g_qkv, g_proj, g_in, g_out, gains[:TWO], gains[TWO:FOUR]

    in_specs = (token_spec, P(dp_axes, None), P(row_axes)) + (P(),) * SIX + (token_spec,)
    out_specs = (token_spec, token_spec) + (P(),) * SIX
    return jax.shard_map(device_step, mesh=mesh, in_specs=in_specs, out_specs=out_specs, check_vma=False)
```

```python
import functools
import math
import jax
import jax.numpy as jnp
from jax import lax
from jax.experimental import pallas as pl
from jax.experimental.pallas import tpu as pltpu
from jax.sharding import Mesh, PartitionSpec as P

ZERO, ONE, TWO, THREE, FOUR = range(5)
SIX, TWELVE = 6, 12
HEAD = 64
HALF = 32
NHEAD = 12
DM = 768
FF = 3072
TOK = 512
GRP = 2048
WIN = 64
NDOC = 8
LANE = 128
EPS = 1e-5
NEG = -1e30
SCALE = 0.125
BASES = (160000.0, 10000.0)
F32 = jnp.float32
BF = jnp.bfloat16
QT = 256
FT = 512
NFT = FF // FT
QTILES = GRP // QT
MIB = 1024 * 1024
ALLTOK = (TOK, DM)
PROJ = DM // 2
DOWN = FF // 2
UP = FF
QKV = 3 * PROJ
MLP_ROWS = DOWN + UP
ATT_ROWS = PROJ + QKV
RING_ROWS = 2 * ATT_ROWS + MLP_ROWS
ANY = pl.BlockSpec(memory_space=pl.ANY)
DMA = pltpu.SemaphoreType.DMA
MESH = pl.DeviceIdType.MESH


def dot(a, b, ca, cb):
    return lax.dot_general(a, b, (((ca,), (cb,)), ((), ())), preferred_element_type=F32)


def mm(a, b):
    return dot(a, b, ONE, ZERO)


def mm_nt(a, b):
    return dot(a, b, ONE, ONE)


def mm_tn(a, b):
    return dot(a, b, ZERO, ZERO)


def call(body, grid, in_specs, out_specs, out_shape, scratch=(), prefetch=ZERO, flops=ZERO, nbytes=ZERO, name=None,
         cid=None, alias=None):
    extra = {} if cid is None else dict(collective_id=cid, has_side_effects=True)
    return pl.pallas_call(
        body,
        grid_spec=pltpu.PrefetchScalarGridSpec(
            num_scalar_prefetch=prefetch, grid=grid, in_specs=in_specs, out_specs=out_specs, scratch_shapes=scratch),
        out_shape=out_shape,
        input_output_aliases=alias or {},
        compiler_params=pltpu.CompilerParams(vmem_limit_bytes=60 * MIB, **extra),
        cost_estimate=pl.CostEstimate(flops=int(flops), bytes_accessed=int(nbytes), transcendentals=ZERO),
        name=name,
    )


def sds(shape, dtype):
    return jax.ShapeDtypeStruct(shape, dtype)


def spec(shape, *idx):
    idx = idx or (ZERO,) * len(shape)
    return pl.BlockSpec(shape, lambda *g: tuple(i(*g) if callable(i) else i for i in idx))


def step_of(s, *_):
    return s


def core_and_partner():
    core = lax.axis_index('core')
    return core, {'core': ONE - core}


def meet(*devices):
    bar = pltpu.get_barrier_semaphore()
    for dev in devices:
        pl.semaphore_signal(bar, inc=ONE, device_id=dev, device_id_type=MESH)
    pl.semaphore_wait(bar, len(devices))


def sp_peer(d):
    return lax.rem(lax.axis_index('sp') + d, FOUR)


PEERS = range(ONE, FOUR)


class Swaps:
    def __init__(self, ssem, rsem, lsem):
        self.sems, self.waits, self.n = (ssem, rsem, lsem), [], ZERO
        self.core, self.partner = core_and_partner()
        self.other = ONE - self.core
        self.me = lax.axis_index('sp')

    def remote(self, src, dst, dev=None):
        ssem, rsem, _ = self.sems
        return self.later(pltpu.make_async_remote_copy(
            src_ref=src, dst_ref=dst, send_sem=ssem.at[self.n], recv_sem=rsem.at[self.n],
            device_id=self.partner if dev is None else dev, device_id_type=MESH))

    def local(self, src, dst):
        return self.later(pltpu.make_async_copy(src, dst, self.sems[TWO].at[self.n]))

    def later(self, cp):
        self.n += ONE
        self.waits.append(cp)
        return cp

    def to_all(self, src_of, dst_of):
        return [self.remote(src_of(sp_peer(d)), dst_of(self.me), {'sp': sp_peer(d)}) for d in PEERS] + [
            self.local(src_of(self.me), dst_of(self.me))]

    def to_sides(self, left_src, right_src, from_left, from_right):
        return [self.remote(right_src, from_left, {'sp': sp_peer(ONE)}), self.remote(left_src, from_right, {'sp': sp_peer(THREE)})]

    def wait(self, some=None):
        some = self.waits if some is None else some
        done = {id(cp) for cp in some}
        for cp in some:
            cp.wait()
        self.waits = [cp for cp in self.waits if id(cp) not in done]


def row_peers():
    return [core_and_partner()[ONE]] + [{'sp': sp_peer(d)} for d in PEERS]


def side_peers():
    return [{'sp': sp_peer(ONE)}, {'sp': sp_peer(THREE)}]


def partner_peer():
    return [core_and_partner()[ONE]]


def swap_sems(n):
    return [DMA((n,))] * THREE


def named_sems(n):
    return list(zip(('ssem', 'rsem', 'lsem'), swap_sems(n)))


class Refs:
    def __init__(self, named):
        self.__dict__.update(named)


class Stage:
    def __init__(self, body, steps, ins, outs, scratch, links=None, alias=()):
        self.body, self.steps, self.ins, self.outs, self.scratch = body, steps, ins, outs, scratch
        self.links, self.alias = links or {}, alias


def shifted(block, first, steps):
    if block.index_map is None:
        return block
    return pl.BlockSpec(block.block_shape, lambda g: block.index_map(jnp.clip(g - first, ZERO, steps - ONE)))


def run(name, cid, peers, *stages):
    firsts = [sum(st.steps for st in stages[:k]) for k in range(len(stages))]

    def flat(kind):
        return [(k, entry) for k, st in enumerate(stages) for entry in getattr(st, kind)]

    ins, outs, scratch = flat('ins'), flat('outs'), flat('scratch')
    keys = [(k, entry[ZERO]) for k, entry in ins + outs + scratch]

    def body(*refs):
        pid = pl.program_id(ZERO)
        have = dict(zip(keys, refs))

        @pl.when(pid == ZERO)
        def _():
            meet(*peers())

        for k, st in enumerate(stages):
            r = Refs({n: ref for (at, n), ref in have.items() if at == k})
            for n, source in st.links.items():
                setattr(r, n, have[source])

            @pl.when((pid >= firsts[k]) & (pid < firsts[k] + st.steps))
            def _(st=st, r=r, k=k):
                st.body(r, pid - firsts[k])

    def placed(entries):
        return [shifted(entry[TWO], firsts[k], stages[k].steps) for k, entry in entries]

    alias = {[e[ZERO] for _, e in ins].index(a): [e[ZERO] for _, e in outs].index(b) for st in stages for a, b in st.alias}
    got = call(body, (sum(st.steps for st in stages),), placed(ins), placed(outs), [e[ONE] for _, e in outs],
               scratch=[e[ONE] for _, e in scratch], flops=16 * TOK * DM * FF, nbytes=30 * MIB, name=name, cid=cid,
               alias=alias)(*[e[ONE] for _, e in ins])
    out = [{} for _ in stages]
    for (k, e), arr in zip(outs, got):
        out[k][e[ZERO]] = arr
    return [Refs(named) for named in out]


def norm_parts(x_bf):
    rows = x_bf.astype(F32)
    cen = rows - jnp.mean(rows, axis=ONE, keepdims=True)
    var = jnp.mean(cen * cen, axis=ONE, keepdims=True)
    return cen, lax.rsqrt(var + EPS)


def norm_rows(x_bf, gain):
    cen, inv = norm_parts(x_bf)
    return (cen * inv * gain).astype(BF)


def norm_rows_grad(x_bf, gain, d_bf):
    cen, inv = norm_parts(x_bf)
    hat = cen * inv
    d_out = d_bf.astype(F32)
    g_gain = jnp.sum(d_out * hat, axis=ZERO, keepdims=True)
    d_hat = d_out * gain
    d_x = inv * (d_hat - jnp.mean(d_hat, axis=ONE, keepdims=True) - hat * jnp.mean(d_hat * hat, axis=ONE, keepdims=True))
    return d_x.astype(BF), g_gain


def add_bf(a, b):
    return (a.astype(F32) + b.astype(F32)).astype(BF)


RB = 256
CHUNKS = range(DM // RB)


def head_rows(ref, chunk, head):
    return ref.at[head, ZERO, chunk] if ref.shape[ZERO] == FOUR else ref.at[ZERO, chunk, head]


def weight_cols(layer, width, first=ZERO):
    return spec((None, DM, width), layer, ZERO, lambda s: first + s)


def gain_spec(layer):
    return spec((None, ONE, DM), layer, ZERO, ZERO)


GROUP_QKV = (FOUR, THREE, THREE, HEAD, TOK)
OWN_QKV = (THREE * NHEAD, HEAD, TOK)
EDGE = (NHEAD, HEAD, LANE)
TOKS = jax.ShapeDtypeStruct(ALLTOK, BF)
TOK_SPEC = spec(ALLTOK)
TOK_VMEM = pltpu.VMEM(ALLTOK, BF)
TABLE = spec((HALF, TOK))


def qkv_fwd_body(r, step, whole_group):
    sw = Swaps(r.ssem, r.rsem, r.lsem)
    start = [sw.remote(r.h, r.h_r), sw.local(r.h, r.h_m)]
    if whole_group:
        sends = [[sw.to_all(lambda dev: r.out_s.at[p, dev, chunk], lambda dev: r.out.at[dev, p, chunk]) for chunk in CHUNKS]
                 for p in range(THREE)]
    else:
        edges = sw.to_sides(r.edge_s.at[ZERO], r.edge_s.at[ONE], r.left, r.right)

    @pl.when(step == ZERO)
    def _():
        r.h[...] = norm_rows(r.x[...], r.g[...])
        for cp in start:
            cp.start()

    for p in range(THREE):
        @pl.when(step == p)
        def _(p=p):
            for chunk in CHUNKS:
                t_rows = mm(r.h[...], r.w[:, RB * chunk:RB * chunk + RB]).astype(BF).astype(F32).T
                for head in range(FOUR):
                    at, n = HEAD * head, FOUR * chunk + head
                    a, b = t_rows[at:at + HALF], t_rows[at + HALF:at + HEAD]
                    if p < TWO:
                        cos, sin = r.cos[...], r.sin[...]
                        a, b = a * cos - b * sin, b * cos + a * sin
                    out = r.out_s.at[p, head, chunk] if whole_group else r.out.at[n]
                    out[:HALF] = a.astype(BF)
                    out[HALF:] = b.astype(BF)
                    if p and not whole_group:
                        lane = WIN * (p - ONE)
                        blk = out[...]
                        r.edge_s[ZERO, n, :, lane:lane + WIN] = blk[:, :WIN]
                        r.edge_s[ONE, n, :, lane:lane + WIN] = blk[:, TOK - WIN:]
                if whole_group:
                    for cp in sends[p][chunk]:
                        cp.start()

    @pl.when(step == TWO)
    def _():
        if not whole_group:
            for cp in edges:
                cp.start()
        sw.wait()


def qkv_fwd_stage(layer, whole_group, gain, w_qkv, tables, x=None, link=None):
    ins = [('g', gain, gain_spec(layer)), ('w', w_qkv, weight_cols(layer, DM)), ('cos', tables[ZERO], TABLE), ('sin', tables[ONE], TABLE)]
    outs = [('h_m', TOKS, ANY), ('h_r', TOKS, ANY)]
    scratch = [('h', TOK_VMEM)]
    if whole_group:
        outs += [('out', sds(GROUP_QKV, BF), ANY)]
        scratch += [('out_s', pltpu.VMEM((THREE, FOUR, THREE, HEAD, TOK), BF))]
    else:
        outs += [('out', sds(OWN_QKV, BF), spec((NHEAD, HEAD, TOK), step_of, ZERO, ZERO))]
        outs += [('left', sds(EDGE, BF), ANY), ('right', sds(EDGE, BF), ANY)]
        scratch += [('edge_s', pltpu.VMEM((TWO,) + EDGE, BF))]
    if link is None:
        ins += [('x', x, TOK_SPEC)]
    n = len(PEERS) * 16
    return Stage(functools.partial(qkv_fwd_body, whole_group=whole_group), THREE, ins, outs, scratch + named_sems(n),
                 {} if link is None else {'x': link})


def tile_src(i, *_):
    return i // TWO


def tile_side(i, *_):
    return i % TWO


Q_SPEC = spec((ONE, ONE, THREE, HEAD, QT), tile_src, ZERO, ZERO, ZERO, tile_side)
O_SPEC = spec((ONE, THREE, HEAD, QT), tile_src, ZERO, ZERO, tile_side)
STAT_SPEC = spec((8, QT), ZERO, step_of)


def kv_spec(part):
    return spec((FOUR, ONE, THREE, HEAD, TOK), ZERO, part, ZERO, ZERO, ZERO)


def key_tile(kt):
    return kt // TWO, pl.ds(pl.multiple_of((kt % TWO) * QT, QT), QT)


def key_rows(dst, k_ref):
    for src in range(FOUR):
        for h in range(THREE):
            dst[h, TOK * src:TOK * src + TOK] = k_ref[src, ZERO, h].T


def row_tile(kt):
    return pl.ds(pl.multiple_of(kt * QT, QT), QT)


def doc_start(cu_ref, tok):
    start = jnp.zeros_like(tok)
    for d in range(ONE, NDOC):
        start = jnp.where(cu_ref[ZERO, d] <= tok, cu_ref[ZERO, d], start)
    return start


def doc_stop(cu_ref, tok):
    stop = jnp.full_like(tok, GRP)
    for d in range(NDOC - ONE, ZERO, -ONE):
        stop = jnp.where(cu_ref[ZERO, d] > tok, cu_ref[ZERO, d], stop)
    return stop


def tile_bounds(cu_ref, tile):
    first = tile * QT
    tok = lax.broadcasted_iota(jnp.int32, (ONE, QT), ONE) + first
    lo = doc_start(cu_ref, first) // QT
    hi = (doc_stop(cu_ref, first + QT - ONE) + QT - ONE) // QT
    return lo, hi, doc_start(cu_ref, tok), doc_stop(cu_ref, tok)


def attn0_fwd_body(cu_ref, q_ref, k_ref, v_ref, o_ref, lse_ref, m_s, l_s, acc_s, kr_s, s_s, p_s):
    tile = pl.program_id(ZERO)
    first, last, st, en = tile_bounds(cu_ref, tile)
    heads, pair = range(THREE), range(TWO)

    @pl.when(tile == ZERO)
    def _():
        key_rows(kr_s, k_ref)

    m_s[...] = jnp.full(m_s.shape, NEG, F32)
    l_s[...] = jnp.zeros(l_s.shape, F32)
    acc_s[...] = jnp.zeros(acc_s.shape, F32)
    io = lax.broadcasted_iota(jnp.int32, (QT, QT), ZERO)
    q_t = [q_ref[ZERO, ZERO, h] * SCALE for h in heads]
    n_tiles = last - first

    def body(g, carry):
        kts = [first + TWO * g + a for a in pair]
        safe = [jnp.minimum(kt, QTILES - ONE) for kt in kts]
        for h in heads:
            for a in pair:
                s_s[h, a] = mm(kr_s[h, row_tile(safe[a])], q_t[h])
        for h in heads:
            row = slice(h, h + ONE)
            s = [jnp.where((io >= st - kts[a] * QT) & (io < en - kts[a] * QT), s_s[h, a], NEG) for a in pair]
            m_old = m_s[row]
            m_new = m_old
            for a in pair:
                m_new = jnp.maximum(m_new, jnp.max(s[a], axis=ZERO, keepdims=True))
            alpha = jnp.exp(m_old - m_new)
            total = l_s[row] * alpha
            for a in pair:
                p = jnp.exp(s[a] - m_new)
                total += jnp.sum(p, axis=ZERO, keepdims=True)
                p_s[h, a] = p.astype(BF)
            l_s[row] = total
            m_s[row] = m_new
            acc_s[h] = acc_s[h] * alpha
        for h in heads:
            part = acc_s[h]
            for a in pair:
                src, cols = key_tile(safe[a])
                part += mm(v_ref[src, ZERO, h, :, cols], p_s[h, a])
            acc_s[h] = part
        return carry

    lax.fori_loop(ZERO, (n_tiles + ONE) // TWO, body, ZERO)
    for h in heads:
        row = slice(h, h + ONE)
        o_ref[ZERO, h] = (acc_s[h] / l_s[row]).astype(BF)
        lse_ref[row] = m_s[row] + jnp.log(l_s[row])


def attn0_fwd(cu, qkv):
    stat = pltpu.VMEM((8, QT), F32)
    return call(
        attn0_fwd_body, (QTILES,),
        [Q_SPEC, kv_spec(ONE), kv_spec(TWO)],
        [O_SPEC, STAT_SPEC],
        [sds((FOUR, THREE, HEAD, TOK), BF), sds((8, GRP), F32)],
        scratch=[stat, stat, pltpu.VMEM((THREE, HEAD, QT), F32), pltpu.VMEM((THREE, GRP, HEAD), BF),
                 pltpu.VMEM((THREE, TWO, QT, QT), F32), pltpu.VMEM((THREE, TWO, QT, QT), BF)],
        prefetch=ONE, flops=TWELVE * GRP * GRP * HEAD, nbytes=6 * MIB, name="attn0_fwd",
    )(cu, qkv, qkv, qkv)


def attn0_bwd_body(cu_ref, q_ref, k_ref, v_ref, o_ref, do_ref, lse_ref, out_ref,
                   dk_s, dv_s, dq_s, kr_s, vr_s, s_s, d_s, p_s, t_s):
    tile = pl.program_id(ZERO)
    first, last, st, en = tile_bounds(cu_ref, tile)
    heads = range(THREE)

    @pl.when(tile == ZERO)
    def _():
        dk_s[...] = jnp.zeros(dk_s.shape, F32)
        dv_s[...] = jnp.zeros(dv_s.shape, F32)
        key_rows(kr_s, k_ref)
        key_rows(vr_s, v_ref)

    dq_s[...] = jnp.zeros(dq_s.shape, F32)
    io = lax.broadcasted_iota(jnp.int32, (QT, QT), ZERO)
    q_t = [q_ref[ZERO, ZERO, h] * SCALE for h in heads]
    do_t = [do_ref[ZERO, h] for h in heads]
    q_rows, do_rows = [q_t[h].T for h in heads], [do_t[h].T for h in heads]
    delta = [jnp.sum(do_t[h].astype(F32) * o_ref[ZERO, h].astype(F32), axis=ZERO, keepdims=True) for h in heads]
    lse = [lse_ref[h:h + ONE] for h in heads]

    def body(kt, carry):
        base = kt * QT
        src, cols = key_tile(kt)
        rows = row_tile(kt)
        ok = (io >= st - base) & (io < en - base)
        for h in heads:
            s_s[h] = mm(kr_s[h, rows], q_t[h])
            d_s[h] = mm(vr_s[h, rows], do_t[h])
        for h in heads:
            p = jnp.exp(jnp.where(ok, s_s[h] - lse[h], NEG))
            p_s[h] = p.astype(BF)
            t_s[h] = (p * (d_s[h] - delta[h])).astype(BF)
        for h in heads:
            dv_s[h, rows] += mm(p_s[h], do_rows[h])
            dk_s[h, rows] += mm(t_s[h], q_rows[h])
            dq_s[h] += mm(k_ref[src, ZERO, h, :, cols], t_s[h])
        return carry

    lax.fori_loop(first, last, body, ZERO)
    src, cols = key_tile(tile)
    for h in heads:
        out_ref[src, ZERO, h, :, cols] = (dq_s[h] * SCALE).astype(BF)

    @pl.when(tile == QTILES - ONE)
    def _():
        for src in range(FOUR):
            for h in heads:
                out_ref[src, ONE, h] = dk_s[h, TOK * src:TOK * src + TOK].T.astype(BF)
                out_ref[src, TWO, h] = dv_s[h, TOK * src:TOK * src + TOK].T.astype(BF)


def attn0_bwd(cu, qkv, o_t, do_t, lse):
    acc, rows = pltpu.VMEM((THREE, GRP, HEAD), F32), pltpu.VMEM((THREE, GRP, HEAD), BF)
    sq32, sq16 = pltpu.VMEM((THREE, QT, QT), F32), pltpu.VMEM((THREE, QT, QT), BF)
    return call(
        attn0_bwd_body, (QTILES,),
        [Q_SPEC, kv_spec(ONE), kv_spec(TWO), O_SPEC, O_SPEC, STAT_SPEC],
        spec(GROUP_QKV), sds(GROUP_QKV, BF),
        scratch=[acc, acc, pltpu.VMEM((THREE, HEAD, QT), F32), rows, rows, sq32, sq32, sq16, sq16],
        prefetch=ONE, flops=30 * GRP * GRP * HEAD, nbytes=TWELVE * MIB, name="attn0_bwd",
    )(cu, qkv, qkv, qkv, o_t, do_t, lse)


NBLK = TOK // LANE
EXT = TOK + TWO * WIN
XBLK = EXT // LANE
REACH = LANE + TWO * WIN
AHEAD_FWD, AHEAD_BWD = 4, 2
HPS = 4
HSTEPS = NHEAD // HPS


def heads_of(width, part):
    return spec((HPS, HEAD, width), lambda n: HSTEPS * part + n, ZERO, ZERO)


def own_head(part):
    return heads_of(TOK, part)


def row_of(width):
    return spec((HPS, ONE, width), step_of, ZERO, ZERO)


LOW, HIGH = slice(None, WIN), slice(WIN, None)


def joined(left, mid, right, h, left_lanes=HIGH, right_lanes=LOW):
    return jnp.concatenate([left[h][:, left_lanes], mid[h], right[h][:, right_lanes]], axis=ONE)


def blocks(first, last):
    return slice(LANE * first, LANE * last)


def near_bounds(cu_ref, before, width):
    shift = lax.axis_index('sp') * TOK
    tok = lax.broadcasted_iota(jnp.int32, (ONE, width), ONE) + (shift - before)
    inside = (tok >= ZERO) & (tok < GRP)
    lo = jnp.maximum(doc_start(cu_ref, tok), tok - WIN) - (shift - WIN)
    hi = jnp.minimum(doc_stop(cu_ref, tok), tok + WIN + ONE) - (shift - WIN)
    return jnp.where(inside, lo, ZERO), jnp.where(inside, hi, ZERO)


def in_bounds(bounds, cols, first, n):
    io = lax.broadcasted_iota(jnp.int32, (n, LANE), ZERO) + first
    return (io >= bounds[ZERO][:, cols]) & (io < bounds[ONE][:, cols])


def every_head(fn, ahead):
    def body(g, c):
        fn([ahead * g + a for a in range(ahead)])
        return c
    lax.fori_loop(ZERO, HPS // ahead, body, ZERO)


CU_SPEC = pl.BlockSpec(memory_space=pltpu.SMEM)


def attn1_fwd_body(r, step):
    bounds = near_bounds(r.cu, ZERO, TOK)

    def some(heads):
        v_all = []
        for a, h in enumerate(heads):
            q_t = r.q[h] * SCALE
            k_rows = joined(r.left, r.k, r.right, h, LOW, LOW).T
            v_all.append(joined(r.left, r.v, r.right, h, HIGH, HIGH))
            for i in range(NBLK):
                r.s_s[a, i] = mm(k_rows[LANE * i:LANE * i + REACH], q_t[:, blocks(i, i + ONE)])
        for a, h in enumerate(heads):
            for i in range(NBLK):
                cols = blocks(i, i + ONE)
                s = jnp.where(in_bounds(bounds, cols, LANE * i, REACH), r.s_s[a, i], NEG)
                m = jnp.max(s, axis=ZERO, keepdims=True)
                e = jnp.exp(s - m)
                l = jnp.sum(e, axis=ZERO, keepdims=True)
                r.p_s[a, i] = (e * (ONE / l)).astype(BF)
                r.lse[h, :, cols] = m + jnp.log(l)
        for a, h in enumerate(heads):
            for i in range(NBLK):
                out = mm(v_all[a][:, LANE * i:LANE * i + REACH], r.p_s[a, i]).astype(BF)
                r.o[HPS * step + h, :, blocks(i, i + ONE)] = out
    every_head(some, AHEAD_FWD)


def attn1_fwd_stage(cu, qkv, left, right):
    tile, edge = (AHEAD_FWD, NBLK, REACH, LANE), heads_of(LANE, ZERO)
    return Stage(
        attn1_fwd_body, HSTEPS,
        [('cu', cu, CU_SPEC), ('q', qkv, own_head(ZERO)), ('k', qkv, own_head(ONE)), ('v', qkv, own_head(TWO)),
         ('left', left, edge), ('right', right, edge)],
        [('lse', sds((NHEAD, ONE, TOK), F32), row_of(TOK))],
        [('o', pltpu.VMEM((NHEAD, HEAD, TOK), BF)), ('s_s', pltpu.VMEM(tile, F32)), ('p_s', pltpu.VMEM(tile, BF))])


def attn1_bwd_body(r, step):
    bounds = near_bounds(r.cu, WIN, EXT)

    def window(e):
        first, last = max(LANE * e - WIN, ZERO), min(LANE * e + LANE + WIN, EXT)
        return first, last - first

    def parts(h):
        q_t = joined(r.ql, r.q, r.qr, h) * SCALE
        return q_t, joined(r.dl, r.d, r.dr, h), joined(r.left, r.k, r.right, h, LOW, LOW)

    def some(heads):
        for a, h in enumerate(heads):
            q_t, do_t, k_t = parts(h)
            k_rows, v_rows = k_t.T, joined(r.left, r.v, r.right, h, HIGH, HIGH).T
            for e in range(XBLK):
                first, n = window(e)
                cols = blocks(e, e + ONE)
                r.s_s[a, e, :n] = mm(k_rows[first:first + n], q_t[:, cols])
                r.d_s[a, e, :n] = mm(v_rows[first:first + n], do_t[:, cols])
        for a, h in enumerate(heads):
            lse, delta = joined(r.ll, r.lse, r.lr, h), joined(r.el, r.delta, r.er, h)
            for e in range(XBLK):
                first, n = window(e)
                cols = blocks(e, e + ONE)
                ok = in_bounds(bounds, cols, first, n)
                p = jnp.exp(jnp.where(ok, r.s_s[a, e, :n] - lse[:, cols], NEG))
                r.p_s[a, first:first + n, cols] = p.astype(BF)
                r.t_s[a, first:first + n, cols] = (p * (r.d_s[a, e, :n] - delta[:, cols])).astype(BF)
        for a, h in enumerate(heads):
            q_t, do_t, k_t = parts(h)
            got = [[], [], []]
            for b in range(XBLK):
                here, wide = blocks(b, b + ONE), blocks(max(b - ONE, ZERO), min(b + TWO, XBLK))
                got[ZERO].append(mm(k_t[:, wide], r.t_s[a, wide, here]) * SCALE)
                got[ONE].append(mm_nt(q_t[:, wide], r.t_s[a, here, wide]))
                got[TWO].append(mm_nt(do_t[:, wide], r.p_s[a, here, wide]))
            for n in range(THREE):
                own = jnp.concatenate([g.astype(BF) for g in got[n]], axis=ONE)[:, WIN:WIN + TOK]
                r.out[n, HPS * step + h] = own

    @pl.when(step == ZERO)
    def _():
        r.p_s[...] = jnp.zeros(r.p_s.shape, BF)
        r.t_s[...] = jnp.zeros(r.t_s.shape, BF)

    every_head(some, AHEAD_BWD)


def attn1_bwd_stage(cu, qkv, do_t, lse, delta, edges, far):
    edge, row = heads_of(LANE, ZERO), row_of(LANE)
    blk = (AHEAD_BWD, XBLK, REACH, LANE)
    square = pltpu.VMEM((AHEAD_BWD, EXT, EXT), BF)
    names = ('left', 'right', 'ql', 'qr', 'dl', 'dr')
    return Stage(
        attn1_bwd_body, HSTEPS,
        [('cu', cu, CU_SPEC), ('q', qkv, own_head(ZERO)), ('k', qkv, own_head(ONE)), ('v', qkv, own_head(TWO)), ('d', do_t, own_head(ZERO)),
         ('lse', lse, row_of(TOK)), ('delta', delta, row_of(TOK))]
        + [(n, arr, edge) for n, arr in zip(names, list(edges) + far[:FOUR])]
        + [(n, arr, row) for n, arr in zip(('ll', 'lr', 'el', 'er'), far[FOUR:])],
        [], [('out', pltpu.VMEM((THREE, NHEAD, HEAD, TOK), BF)), ('s_s', pltpu.VMEM(blk, F32)), ('d_s', pltpu.VMEM(blk, F32)),
             ('p_s', square), ('t_s', square)])


ROWBLK = [slice(r, r + RB) for r in range(ZERO, TOK, RB)]
HALFT = NFT // TWO
SQRT_HALF = math.sqrt(SCALE * FOUR)
PDF_SCALE = SQRT_HALF / math.sqrt(math.pi)


def normal_cdf(a):
    return SQRT_HALF * SQRT_HALF * (ONE + lax.erf(a * SQRT_HALF))


def half_rows(ref, which):
    n = ref.shape[ZERO] // TWO
    return ref.at[pl.ds(pl.multiple_of(which * n, n), n)]


def col_tile(ref, n):
    return ref.at[:, pl.ds(pl.multiple_of(n * FT, FT), FT)]


def mlp_body(r, step, fwd, bwd):
    sw = Swaps(r.ssem, r.rsem, r.lsem)
    start = []
    whole_group = not (fwd and bwd)
    if fwd:
        start = [sw.remote(r.h, r.h_r), sw.remote(half_rows(r.of, sw.other), r.of_r),
                 sw.local(half_rows(r.of, sw.core), r.of_m), sw.local(r.h, r.h_m)]
        if whole_group:
            o_in = sw.to_all(lambda dev: r.o.at[dev], lambda dev: r.o_s.at[dev])
            start.append(sw.local(r.x1, r.x1_m))
        m_out = [(sw.remote(r.m_s.at[HALFT * sw.other + n], col_tile(r.m_r, n)),
                  sw.local(r.m_s.at[HALFT * sw.core + n], col_tile(r.m_m, n))) for n in range(HALFT)]
    if bwd:
        start.append(sw.remote(r.dy, r.dy_r))
        dmid_out = sw.remote(r.dmid, r.dmid_r)
        du_out = [(sw.remote(r.du_s.at[n, sw.other], col_tile(r.du_r, n)),
                   sw.local(r.du_s.at[n, sw.core], col_tile(r.du_m, n))) for n in range(NFT)]

    if bwd and whole_group:
        do_out = sw.to_all(lambda dev: r.do_s.at[dev], lambda dev: r.d_o.at[dev])

    @pl.when(step == ZERO)
    def _():
        if fwd:
            if whole_group:
                for cp in o_in:
                    cp.start()
                sw.wait(o_in)
            for n in range(NHEAD):
                r.of[HEAD * n:HEAD * n + HEAD, :] = (r.o_s[n % FOUR, n // FOUR] if whole_group else r.o[n])
            x1 = (r.x[...].astype(F32) + mm_tn(r.of[...], r.wp[...])).astype(BF)
            r.x1[...] = x1
            r.h[...] = norm_rows(x1, r.g[...])
            r.acc[...] = x1.astype(F32)
        if bwd:
            r.dacc[...] = jnp.zeros(r.dacc.shape, F32)
        for cp in start:
            cp.start()

    for rows in ROWBLK:
        if fwd:
            ua = mm(r.h[rows], r.wa[...]).astype(BF)
            ub = mm(r.h[rows], r.wb[...]).astype(BF)
            if not bwd:
                r.u[ZERO, rows] = ua
                r.u[ONE, rows] = ub
        else:
            ua, ub = r.u[ZERO, rows], r.u[ONE, rows]
        a, b = ua.astype(F32), ub.astype(F32)
        cdf = normal_cdf(a)
        gate = a * cdf
        if fwd:
            m = (gate * b).astype(BF)
            r.m_s[step, rows] = m
            r.acc[rows] += mm(m, r.wo[...])
        if bwd:
            dm = mm_nt(r.dy[rows], r.wo[...]).astype(BF).astype(F32)
            pdf = jnp.exp(a * a * (SCALE * FOUR - ONE)) * PDF_SCALE
            db = (dm * gate).astype(BF)
            da = (dm * b * (cdf + a * pdf)).astype(BF)
            r.du_s[step, ZERO, rows] = da
            r.du_s[step, ONE, rows] = db
            r.dacc[rows] += mm_nt(da, r.wa[...]) + mm_nt(db, r.wb[...])

    for n in range(NFT):
        @pl.when(step == n)
        def _(n=n):
            if fwd:
                there, here = m_out[n % HALFT]

                @pl.when(sw.core == n // HALFT)
                def _():
                    here.start()

                @pl.when(sw.other == n // HALFT)
                def _():
                    there.start()
            if bwd:
                for cp in du_out[n]:
                    cp.start()

    @pl.when(step == NFT - ONE)
    def _():
        if fwd:
            r.y[...] = r.acc[...].astype(BF)
        if bwd:
            d_ln, gg = norm_rows_grad(r.x1[...], r.g[...], r.dacc[...].astype(BF))
            r.gg[...] = gg
            d_mid = add_bf(r.dy[...], d_ln)
            r.dmid[...] = d_mid
            dmid_out.start()
            d_att = mm_nt(r.wp[...], d_mid).astype(BF)
            for n in range(NHEAD):
                rows = slice(HEAD * n, HEAD * n + HEAD)
                blk = d_att[rows]
                if whole_group:
                    r.do_s[n % FOUR, n // FOUR] = blk
                else:
                    r.d_o[n] = blk
                    r.delta[n] = jnp.sum(blk.astype(F32) * r.of[rows].astype(F32), axis=ZERO, keepdims=True)
            if whole_group:
                for cp in do_out:
                    cp.start()
        sw.wait()


def mlp_stage(layer, fwd, bwd, w_proj, gain, w_in, w_out, links=None, **arrays):
    u_spec = spec((TWO, TOK, FT), ZERO, ZERO, step_of)
    half_o = sds((DM // TWO, TOK), BF)
    half_m, half_u = sds((TOK, FF // TWO), BF), sds((TOK, FF), BF)
    heads, by_owner = (NHEAD, HEAD, TOK), (FOUR, THREE, HEAD, TOK)
    sums = pltpu.VMEM(ALLTOK, F32)
    links = links or {}
    ins = [('wp', w_proj, spec((None, DM, DM), layer, ZERO, ZERO)), ('g', gain, gain_spec(layer)),
           ('wa', w_in, weight_cols(layer, FT)), ('wb', w_in, weight_cols(layer, FT, NFT)),
           ('wo', w_out, spec((None, FT, DM), layer, step_of, ZERO))]
    kinds = dict(x=TOK_SPEC, o=ANY, dy=TOK_SPEC, x1=TOK_SPEC, u=u_spec)
    ins += [(n, arr, kinds[n]) for n, arr in arrays.items()]
    outs, scratch = [], []
    if fwd:
        outs += [('y', TOKS, TOK_SPEC), ('h_m', TOKS, ANY), ('h_r', TOKS, ANY), ('of_m', half_o, ANY), ('of_r', half_o, ANY),
                 ('m_m', half_m, ANY), ('m_r', half_m, ANY)]
        scratch += [('acc', sums), ('of', pltpu.VMEM((DM, TOK), BF)), ('m_s', pltpu.VMEM((NFT, TOK, FT), BF)), ('h', TOK_VMEM),
                    ('x1', TOK_VMEM)]
    if fwd and not bwd:
        outs += [('x1_m', TOKS, ANY), ('u', sds((TWO, TOK, FF), BF), u_spec)]
        scratch += [('o_s', pltpu.VMEM(by_owner, BF))]
    if bwd:
        shape = heads if fwd else by_owner
        outs += [('dmid', TOKS, TOK_SPEC), ('gg', sds((ONE, DM), F32), spec((ONE, DM))), ('d_o', sds(shape, BF), spec(shape) if fwd else ANY),
                 ('dy_r', TOKS, ANY), ('dmid_r', TOKS, ANY), ('du_m', half_u, ANY), ('du_r', half_u, ANY)]
        scratch += [('dacc', sums), ('du_s', pltpu.VMEM((NFT, TWO, TOK, FT), BF))]
    if fwd and bwd:
        outs += [('delta', sds((NHEAD, ONE, TOK), F32), spec((NHEAD, ONE, TOK)))]
    if not fwd:
        scratch += [('do_s', pltpu.VMEM(by_owner, BF))]
    return Stage(functools.partial(mlp_body, fwd=fwd, bwd=bwd), NFT, ins, outs, scratch + named_sems(FOUR * NFT), links)


NAMED = ('ha', 'hb', 'oa', 'ob', 'dma', 'dmb')


def qkv_bwd_body(r, step, grads):
    sw = Swaps(r.ssem, r.rsem, r.lsem)
    half = PROJ

    def rows(ref, n):
        return ref.at[half * n:half * n + half]

    copies = [[sw.remote(r.dt_s.at[sw.other, n], rows(r.dt_r, n))] for n in range(THREE)]
    if grads:
        loads = [sw.local(getattr(r, n + '_in'), getattr(r, n)) for n in NAMED]
    else:
        for n in range(THREE):
            copies[n].append(sw.local(r.dt_s.at[sw.core, n], rows(r.dt_m, n)))

    @pl.when(step == ZERO)
    def _():
        r.acc[...] = jnp.zeros(r.acc.shape, F32)
        if grads:
            for cp in loads:
                cp.start()

    for p in range(THREE):
        @pl.when(step == p)
        def _(p=p):
            cos, sin = r.cos[...], r.sin[...]
            for chunk in CHUNKS:
                for head in range(FOUR):
                    blk = r.d[head, ZERO, chunk] if grads else r.d[p, FOUR * chunk + head]
                    a, b = blk[:HALF], blk[HALF:]
                    if p < TWO:
                        a, b = a.astype(F32), b.astype(F32)
                        a, b = (a * cos + b * sin).astype(BF), (b * cos - a * sin).astype(BF)
                    at, full = LANE * chunk + HEAD * (head % TWO), RB * chunk + HEAD * head
                    for n, val in ((ZERO, a), (HALF, b)):
                        r.dt_s[head // TWO, p, at + n:at + n + HALF] = val
                        r.dt_all[full + n:full + n + HALF] = val
            for cp in copies[p]:
                cp.start()
            r.acc[...] += mm(r.w[...], r.dt_all[...])

    @pl.when(step == TWO)
    def _():
        d_ln, gg = norm_rows_grad(r.x[...], r.g[...], r.acc[...].T.astype(BF))
        r.gg[...] = gg
        r.dx[...] = add_bf(r.dmid[...], d_ln)
        if not grads:
            sw.wait()

    if grads:
        @pl.when(step == THREE)
        def _():
            sw.wait()
            r.out[...] = mm(r.oa[...], r.dma[...]) + mm(r.ob[...], r.dmb[...])

        for p in range(THREE):
            @pl.when(step == p + FOUR)
            def _(p=p):
                r.out[...] = mm(r.dt_s[sw.core, p], r.ha[...]) + mm(rows(r.dt_r, p)[...], r.hb[...])


def qkv_bwd_stage(layer, tables, w_qkv, x, gain, d_mid, d=None, link=None, grads=None, pairs=()):
    part = lambda s: jnp.minimum(s, TWO)
    ins = [('cos', tables[ZERO], TABLE), ('sin', tables[ONE], TABLE), ('w', w_qkv, spec((None, DM, DM), layer, ZERO, part)),
           ('x', x, TOK_SPEC), ('g', gain, gain_spec(layer)), ('dmid', d_mid, TOK_SPEC)]
    outs = [('dx', TOKS, TOK_SPEC), ('gg', sds((ONE, DM), F32), spec((ONE, DM)))]
    feats = (THREE * PROJ, TOK)
    scratch = [('acc', pltpu.VMEM((DM, TOK), F32)), ('dt_s', pltpu.VMEM((TWO, THREE, PROJ, TOK), BF)), ('dt_all', pltpu.VMEM((DM, TOK), BF))]
    steps, alias = THREE, ()
    if grads is None:
        outs += [('dt_m', sds(feats, BF), ANY), ('dt_r', sds(feats, BF), ANY)]
    else:
        first = (ATT_ROWS + MLP_ROWS) // PROJ
        ins += [('d', d, spec((FOUR, ONE, THREE, HEAD, TOK), ZERO, part, ZERO, ZERO, ZERO)), ('grads', grads, ANY)]
        ins += [(n + '_in', arr, ANY) for n, arr in zip(NAMED, pairs)]
        outs += [('out', sds(grads.shape, F32), spec((PROJ, DM), lambda s: first + jnp.maximum(s - THREE, ZERO), ZERO))]
        scratch += [('dt_r', pltpu.VMEM(feats, BF))] + [(n, pltpu.VMEM(arr.shape, BF)) for n, arr in zip(NAMED, pairs)]
        steps, alias = steps + FOUR, (('grads', 'out'),)
    return Stage(functools.partial(qkv_bwd_body, grads=grads is not None), steps, ins, outs, scratch + named_sems(TWELVE),
                 {} if link is None else {'d': link}, alias)


NDOWN = DOWN // DM


def grad_call(body, grads, steps, in_specs, args, rows, first_row, total, scratch=(), edges=(), cid=None):
    shared = [] if grads is None else [grads]
    first = first_row // rows
    more = [sds(arr.shape[:TWO] + (LANE,), arr.dtype) for arr in edges for _ in range(TWO)]
    return call(
        functools.partial(body, edges=len(edges)) if edges else body, (steps,), [ANY] * len(shared + list(edges)) + in_specs,
        [spec((rows, DM), lambda s: first + s, ZERO)] + [ANY] * len(more), [sds((total, DM), F32)] + more, scratch=scratch,
        flops=FOUR * steps * rows * TOK * DM, nbytes=20 * MIB, name=getattr(body, "__name__"), cid=cid,
        alias={ZERO: ZERO} if shared else None,
    )(*shared, *edges, *args)


GRAD_INS = 8


def grad_mlp_body(*refs, edges=ZERO):
    step = pl.program_id(ZERO)
    if edges:
        srcs, refs, (h_t, *sems) = refs[:edges], refs[edges:-FOUR], refs[-FOUR:]
        refs, outs = refs[:GRAD_INS + ONE], refs[GRAD_INS + ONE:]
        sw = Swaps(*sems)
        for n, src in enumerate(srcs):
            view = src.at[:NHEAD]
            sw.to_sides(view.at[:, :, :LANE], view.at[:, :, TOK - LANE:], outs[TWO * n].at[:NHEAD], outs[TWO * n + ONE].at[:NHEAD])

        @pl.when(step == ZERO)
        def _():
            meet(*side_peers())
            for cp in sw.waits:
                cp.start()
    else:
        refs, h_t = refs[:-ONE], refs[-ONE]
    ma, mb, dya, dyb, ha, hb, dua, dub, out_ref = refs[-GRAD_INS - ONE:]

    @pl.when(step < NDOWN)
    def _():
        out_ref[...] = mm_tn(ma[...], dya[...]) + mm_tn(mb[...], dyb[...])

    @pl.when(step == NDOWN)
    def _():
        h_t[ZERO] = ha[...].T
        h_t[ONE] = hb[...].T

    @pl.when(step >= NDOWN)
    def _():
        out_ref[...] = mm(h_t[ZERO], dua[...]) + mm(h_t[ONE], dub[...])

    if edges:
        @pl.when(step == NDOWN + UP // DM - ONE)
        def _():
            sw.wait()


def grad_mlp(grads, m, m_r, dy, dy_r, h, h_r, du, du_r, first_row, total, edges=(), cid=None):
    toks = spec(ALLTOK)
    m_col = spec(ALLTOK, ZERO, lambda s: jnp.minimum(s, NDOWN - ONE))
    du_col = spec(ALLTOK, ZERO, lambda s: jnp.maximum(s - NDOWN, ZERO))
    return grad_call(grad_mlp_body, grads, NDOWN + UP // DM, [m_col, m_col, toks, toks, toks, toks, du_col, du_col],
                     (m, m_r, dy, dy_r, h, h_r, du, du_r), DM, first_row, total, edges=edges, cid=cid,
                     scratch=[pltpu.VMEM((TWO, DM, TOK), BF)] + (swap_sems(TWO * len(edges)) if edges else []))


def grad_att_body(*refs):
    oa, ob, dma, dmb, ta, tb, ha, hb, out_ref = refs[-GRAD_INS - ONE:]
    step = pl.program_id(ZERO)

    @pl.when(step == ZERO)
    def _():
        out_ref[...] = mm(oa[...], dma[...]) + mm(ob[...], dmb[...])

    @pl.when(step > ZERO)
    def _():
        out_ref[...] = mm(ta[...], ha[...]) + mm(tb[...], hb[...])


def grad_att(grads, of, of_r, dmid, dmid_r, dt, dt_r, h, h_r, first_row):
    toks = spec(ALLTOK)
    blk = (PROJ, TOK)
    dt_row = spec(blk, lambda s: jnp.maximum(s - ONE, ZERO), ZERO)
    return grad_call(grad_att_body, grads, ONE + QKV // PROJ, [spec(blk), spec(blk), toks, toks, dt_row, dt_row, toks, toks],
                     (of, of_r, dmid, dmid_r, dt, dt_r, h, h_r), PROJ, first_row, RING_ROWS)


NB, NS = 5, 6
CH = RING_ROWS // (NB * FOUR)
SB, LF = CH // FOUR, CH // 16
RS = 9
LAST = RS + RS
ADD_ROWS = 96


def ring_body(g_ref, ln_ref, f_ref, lnout_ref, bufa, bufb, bufc, gath, stage, lnbuf,
              ssem, rsem, psem, qsem, csem, stsem, lns, lnr):
    core, partner = core_and_partner()
    zy = lax.axis_index('zy')
    pos = (lax.axis_index('sp'), lax.rem(zy, FOUR), zy // FOUR)
    streams = [(c, sg) for c in range(THREE) for sg in (ONE, -ONE)]
    bufs, sizes = (bufa, bufb, bufc), (CH, SB, LF)
    peers = range(ONE, FOUR)

    def mod4(v):
        return lax.rem(v + 8, FOUR)

    def at(axis, val):
        if axis == ZERO:
            return {'sp': val}
        yz = (val, pos[TWO]) if axis == ONE else (pos[ONE], val)
        return {'zy': yz[ONE] * FOUR + yz[ZERO]}

    def shifted(axis, d):
        return at(axis, mod4(pos[axis] + d))

    def axis_of(s, ph):
        return (streams[s][ZERO] + ph) % THREE

    def idx(s, ph, t):
        return mod4(pos[axis_of(s, ph)] - streams[s][ONE] * t)

    def own(s, ph):
        return idx(s, ph, -ONE)

    def base(b):
        return b * (FOUR * CH)

    bar = pltpu.get_barrier_semaphore()
    for ax in range(THREE):
        for d in peers:
            pl.semaphore_signal(bar, inc=ONE, device_id=shifted(ax, d), device_id_type=MESH)
    pl.semaphore_signal(bar, inc=ONE, device_id=partner, device_id_type=MESH)
    pl.semaphore_wait(bar, 10)

    def rows(ref, start, n):
        return ref.at[pl.ds(pl.multiple_of(start, LF), n)]

    def grows(s, start, n):
        return g_ref.at[pl.ds(pl.multiple_of(start, LF), n), LANE * s:LANE * s + LANE]

    def frows(s, start, n):
        return f_ref.at[core, pl.ds(pl.multiple_of(start, LF), n), LANE * s:LANE * s + LANE]

    def same_bytes(b, k):
        if k < RS:
            return bufs[k // THREE].at[b, k % THREE]
        n = sizes[TWO - (k - RS) // THREE]
        return gath.at[b] if n == CH else gath.at[b, :, pl.ds(ZERO, n)]

    def wait_for(ref, sem):
        pltpu.make_async_copy(ref, ref, sem).wait()

    def send(b, s, k):
        ph = k // THREE if k < RS else TWO - (k - RS) // THREE
        t = k % THREE
        n = sizes[ph]
        if k < RS:
            dst = bufs[ph].at[b, t, s]
            if t:
                src = bufs[ph].at[b, t - ONE, s]
            elif ph:
                src = rows(bufs[ph - ONE].at[b, TWO, s], idx(s, ph, ZERO) * n, n)
            else:
                src = grows(s, base(b) + idx(s, ZERO, ZERO) * n, n)
        elif ph:
            off = own(s, ONE) * SB if ph == TWO else ZERO
            src = dst = rows(gath.at[b, s], off + idx(s, ph, t - ONE) * n, n)
        else:
            dst = frows(s, base(b) + idx(s, ZERO, t - ONE) * n, n)
            src = dst if t else gath.at[b, s]
        pltpu.make_async_remote_copy(src_ref=src, dst_ref=dst, send_sem=ssem.at[b, k], recv_sem=rsem.at[b, k],
                                     device_id=shifted(axis_of(s, ph), streams[s][ONE]), device_id_type=MESH).start()

    def stage_load(n):
        t, b, slot = n // NB, lax.rem(n, NB), lax.rem(n, TWO)
        for s in range(NS):
            pltpu.make_async_copy(grows(s, base(b) + idx(s, ZERO, t + ONE) * CH, CH), stage.at[slot, s],
                                  stsem.at[slot]).start()

    def ln_copy(ph, d):
        return pltpu.make_async_remote_copy(
            src_ref=lnbuf.at[ph, THREE] if ph else ln_ref, dst_ref=lnbuf.at[ph, d - ONE], send_sem=lns.at[ph, d - ONE],
            recv_sem=lnr.at[ph, d - ONE], device_id=shifted(ph, d) if ph < THREE else partner, device_id_type=MESH)

    def ln_sum(ph):
        vals = [lnbuf[ph, THREE] if ph else ln_ref[...]] + [lnbuf[ph, d - ONE] for d in peers]
        total = jnp.zeros_like(vals[ZERO])
        for p in range(FOUR):
            term = vals[ZERO]
            for d in peers:
                term = jnp.where(mod4(pos[ph] - d) == p, vals[d], term)
            total = total + term
        return total

    def batches(fn, start=ZERO):
        def body(b, c):
            fn(b)
            return c
        lax.fori_loop(start, NB, body, ZERO)

    def first(b):
        for s in range(NS):
            send(b, s, ZERO)

    first(ZERO)
    stage_load(jnp.int32(ZERO))
    for d in peers:
        ln_copy(ZERO, d).start()
    batches(first, ONE)

    for k in range(RS):
        ph, t = k // THREE, k % THREE
        buf, size = bufs[ph], sizes[ph]

        def step(b, k=k, ph=ph, t=t, buf=buf, size=size):
            n = k * NB + b
            slot = lax.rem(n, TWO)
            if not ph:
                @pl.when(n < THREE * NB - ONE)
                def _():
                    stage_load(n + ONE)
                wait_for(stage.at[slot], stsem.at[slot])
            wait_for(same_bytes(b, k), rsem.at[b, k])
            for s in range(NS):
                if ph:
                    off = pl.multiple_of(idx(s, ph, t + ONE) * size, LF)
                    buf[b, t, s] += bufs[ph - ONE][b, TWO, s, pl.ds(off, size)]
                else:
                    @pl.loop(ZERO, CH, step=ADD_ROWS)
                    def _(r):
                        at_r = pl.ds(pl.multiple_of(r, ADD_ROWS), ADD_ROWS)
                        buf[b, t, s, at_r] += stage[slot, s, at_r]
                if k == RS - ONE:
                    off = pl.multiple_of(own(s, ONE) * SB + own(s, TWO) * LF, LF)
                    gath[b, s, pl.ds(off, LF)] = bufc[b, TWO, s]
                send(b, s, k + ONE)

        batches(step)
        if k < SIX and k % TWO == ZERO:
            lp = k // TWO
            for d in peers:
                ln_copy(lp, d).wait()
            lnbuf[lp + ONE, THREE] = ln_sum(lp)
            for d in peers if lp < TWO else (ONE,):
                ln_copy(lp + ONE, d).start()

    def hand_over(b, s, j, src, start):
        pltpu.make_async_remote_copy(src_ref=src, dst_ref=frows(s, start, CH), send_sem=psem.at[b, j], recv_sem=qsem.at[b, j],
                                     device_id=partner, device_id_type=MESH).start()

    for k in range(RS, LAST):
        def step(b, k=k):
            wait_for(same_bytes(b, k), rsem.at[b, k])
            piece = k - (LAST - FOUR)
            for s in range(NS):
                if k < LAST - ONE:
                    send(b, s, k + ONE)
                if piece >= ZERO:
                    start = base(b) + idx(s, ZERO, piece - ONE) * CH
                    if piece:
                        hand_over(b, s, piece, frows(s, start, CH), start)
                    else:
                        pltpu.make_async_copy(gath.at[b, s], frows(s, start, CH), csem.at[b]).start()
                        hand_over(b, s, piece, gath.at[b, s], start)
        batches(step)

    ln_copy(THREE, ONE).wait()
    lnout_ref[...] = lnbuf[THREE, THREE] + lnbuf[THREE, ZERO]

    def finish(b):
        for k in range(LAST):
            wait_for(same_bytes(b, k), ssem.at[b, k])
        for j in range(FOUR):
            wait_for(gath.at[b], psem.at[b, j])
            wait_for(gath.at[b], qsem.at[b, j])
        wait_for(gath.at[b], csem.at[b])
    batches(finish)


def ring_all_reduce(g, ln, cid):
    vmem = pl.BlockSpec(memory_space=pltpu.VMEM)
    return pl.pallas_call(
        ring_body,
        in_specs=[ANY, vmem],
        out_specs=[ANY, vmem],
        out_shape=[sds((TWO, RING_ROWS, DM), F32), sds(ln.shape, F32)],
        scratch_shapes=[
            pltpu.VMEM((NB, THREE, NS, CH, LANE), F32), pltpu.VMEM((NB, THREE, NS, SB, LANE), F32),
            pltpu.VMEM((NB, THREE, NS, LF, LANE), F32), pltpu.VMEM((NB, NS, CH, LANE), F32),
            pltpu.VMEM((TWO, NS, CH, LANE), F32),
            pltpu.VMEM((FOUR, FOUR) + ln.shape, F32),
            DMA((NB, LAST)), DMA((NB, LAST)), DMA((NB, FOUR)), DMA((NB, FOUR)), DMA((NB,)), DMA((TWO,)),
            DMA((FOUR, THREE)), DMA((FOUR, THREE)),
        ],
        compiler_params=pltpu.CompilerParams(collective_id=cid, has_side_effects=True, vmem_limit_bytes=60 * MIB),
        cost_estimate=pl.CostEstimate(flops=MIB * MIB // FOUR, bytes_accessed=200 * MIB, transcendentals=ZERO),
        name="ring_all_reduce",
    )(g, ln)


SLOTS, LAG = 8, 4
NTURN = TWO * THREE
OUT_SHAPE, IN_SHAPE = (TWO, FF, DM), (TWO, DM, TWO * FF)


def stream(pieces, buf, turned, isem, osem):
    def loads(i):
        slot, srcs = i % SLOTS, pieces[i][ZERO]
        n = srcs[ZERO].shape[ZERO]
        return [pltpu.make_async_copy(src, buf.at[slot, k * n:k * n + n], isem.at[slot, k]) for k, src in enumerate(srcs)]

    def store(i):
        _, dst, turn = pieces[i]
        src = buf.at[i % SLOTS, :dst.shape[ZERO]] if turn is None else turned.at[turn]
        return pltpu.make_async_copy(src, dst, osem.at[i % SLOTS])

    total = len(pieces)
    for i in range(total + LAG):
        if i < total:
            if i >= SLOTS:
                store(i - SLOTS).wait()
            for cp in loads(i):
                cp.start()
        k = i - LAG
        if k >= ZERO:
            for cp in loads(k):
                cp.wait()
            turn = pieces[k][TWO]
            if turn is not None:
                for n in CHUNKS:
                    rows, col = LANE * n, RB * n
                    turned[turn, :, col:col + LANE] = buf[k % SLOTS, rows:rows + LANE].T
                    turned[turn, :, col + LANE:col + RB] = buf[k % SLOTS, PROJ + rows:PROJ + rows + LANE].T
            store(k).start()
    for i in range(max(total - SLOTS, ZERO), total):
        store(i).wait()


def unpack_ring_body(f, g_qkv, g_proj, g_in, g_out, *scratch):
    def block(c, row, n=DM):
        return f.at[c, row:row + n]

    pieces = []
    for c in range(TWO):
        for n in range(NDOWN):
            pieces.append(([block(c, ATT_ROWS + DM * n)], g_out.at[ZERO, DOWN * c + DM * n:DOWN * c + DM * n + DM], None))
        for n in range(FOUR):
            col = UP * c + DM * n
            pieces.append(([block(c, ATT_ROWS + DOWN + DM * n)], g_in.at[ZERO, :, col:col + DM], None))
    for l in range(TWO):
        first = (ONE - l) * (ATT_ROWS + MLP_ROWS)
        for n in range(THREE):
            row = first + PROJ * (n + ONE)
            pieces.append(([block(c, row, PROJ) for c in range(TWO)], g_qkv.at[l, :, DM * n:DM * n + DM], THREE * l + n))
        for c in range(TWO):
            pieces.append(([block(c, first, PROJ)], g_proj.at[l, PROJ * c:PROJ * c + PROJ], None))
    stream(pieces, *scratch)


def unpack_mlp_body(own, other, in_0, out_0, g_in, g_out, *scratch):
    core = lax.axis_index('core')
    pieces = []
    for src, side in ((own, core), (other, ONE - core)):
        for n in range(NDOWN):
            row = pl.multiple_of(DOWN * side + DM * n, DM)
            pieces.append(([src.at[DM * n:DM * n + DM]], g_out.at[ONE, pl.ds(row, DM)], None))
        for n in range(FOUR):
            col = pl.multiple_of(UP * side + DM * n, DM)
            pieces.append(([src.at[DOWN + DM * n:DOWN + DM * n + DM]], g_in.at[ONE, :, pl.ds(col, DM)], None))
    stream(pieces, *scratch)


def unpack_call(body, args, outs, alias, name):
    return pl.pallas_call(
        body, in_specs=[ANY] * len(args), out_specs=[ANY] * len(outs), out_shape=[sds(shape, F32) for shape in outs],
        scratch_shapes=[pltpu.VMEM((SLOTS, DM, DM), F32), pltpu.VMEM((NTURN, DM, DM), F32), DMA((SLOTS, TWO)), DMA((SLOTS,))],
        input_output_aliases=alias,
        compiler_params=pltpu.CompilerParams(vmem_limit_bytes=60 * MIB),
        cost_estimate=pl.CostEstimate(flops=MIB * MIB // RB, bytes_accessed=75 * MIB, transcendentals=ZERO), name=name,
    )(*args)


def rope_tables(pos, base):
    inv_freq = base ** (jnp.arange(HALF).astype(F32) * (-TWO / HEAD))
    angles = inv_freq[:, None] * pos.astype(F32)[None, :]
    return jnp.cos(angles), jnp.sin(angles)


def solution(mesh):
    n_sp = mesh.shape['sp']
    by_core = mesh.devices.reshape(n_sp, mesh.shape['dp'] // TWO, TWO)
    mesh = Mesh(by_core, ('sp', 'zy', 'core'))
    dp_axes = ('zy', 'core')
    row_axes = dp_axes + ('sp',)
    token_spec = P(row_axes, None)
    swap_cores = [(ZERO, ONE), (ONE, ZERO)]
    cids = list(range(RS))

    def exchange(arr):
        return lax.all_to_all(arr, 'sp', ZERO, ZERO, tiled=True)

    def device_step(x_loc, cu_loc, pos_loc, w_qkv, w_proj, w_in, w_out, ln_attn, ln_mlp, d_out):
        tab0, tab1 = [rope_tables(pos_loc, base) for base in BASES]
        ln_attn, ln_mlp = [g.reshape(TWO, ONE, DM) for g in (ln_attn, ln_mlp)]
        mlp_args, w_mlp = (w_proj, ln_mlp), (w_in, w_out)

        q0, = run("qkv0", cids[ONE], row_peers, qkv_fwd_stage(ZERO, True, ln_attn, w_qkv, tab0, x=x_loc))
        oh0, lse0 = attn0_fwd(cu_loc, q0.out)
        f0, q1 = run("mlp0_qkv1", cids[TWO], row_peers,
                     mlp_stage(ZERO, True, False, *mlp_args, *w_mlp, x=x_loc, o=oh0),
                     qkv_fwd_stage(ONE, False, ln_attn, w_qkv, tab1, link=(ZERO, 'y')))
        kv_edges = (q1.left, q1.right)
        a1, f1 = run("attn1_mlp1", cids[THREE], partner_peer, attn1_fwd_stage(cu_loc, q1.out, *kv_edges),
                     mlp_stage(ONE, True, True, *mlp_args, *w_mlp, links={'o': (ZERO, 'o')}, x=f0.y, dy=d_out))
        g_side, *far = grad_mlp(None, f1.m_m, f1.m_r, d_out, f1.dy_r, f1.h_m, f1.h_r, f1.du_m, f1.du_r, ZERO, MLP_ROWS,
                                edges=(q1.out, f1.d_o, a1.lse, f1.delta), cid=cids[FOUR])
        g_side = lax.psum(g_side, ('sp', 'zy'))
        _, t1, b0 = run("attn1_qkv1_mlp0", cids[5], row_peers,
                        attn1_bwd_stage(cu_loc, q1.out, f1.d_o, a1.lse, f1.delta, kv_edges, far),
                        qkv_bwd_stage(ONE, tab1, w_qkv, f0.y, ln_attn, f1.dmid, link=(ZERO, 'out')),
                        mlp_stage(ZERO, False, True, *mlp_args, *w_mlp, links={'dy': (ONE, 'dx')}, x1=f0.x1_m, u=f0.u))
        dqkv0 = exchange(attn0_bwd(cu_loc, q0.out, oh0, b0.d_o, lse0))
        grads, = grad_att(None, f1.of_m, f1.of_r, f1.dmid, f1.dmid_r, t1.dt_m, t1.dt_r, q1.h_m, q1.h_r, ZERO)
        grads, = grad_mlp(grads, f0.m_m, f0.m_r, t1.dx, b0.dy_r, f0.h_m, f0.h_r, b0.du_m, b0.du_r, ATT_ROWS, RING_ROWS)
        t0, = run("qkv0_grads", cids[SIX], partner_peer, qkv_bwd_stage(
            ZERO, tab0, w_qkv, x_loc, ln_attn, b0.dmid, d=dqkv0, grads=grads,
            pairs=(q0.h_m, q0.h_r, f0.of_m, f0.of_r, b0.dmid, b0.dmid_r)))

        gains = jnp.concatenate([t0.gg, t1.gg, b0.gg, f1.gg, jnp.zeros((FOUR, DM), F32)], axis=ZERO)
        summed, gains = ring_all_reduce(t0.out, gains, cids[ZERO])
        summed, g_side = lax.optimization_barrier((summed, g_side))
        from_partner = lax.ppermute(g_side, 'core', swap_cores)
        shapes = [(TWO, DM, THREE * DM), (TWO, DM, DM), IN_SHAPE, OUT_SHAPE]
        g_qkv, g_proj, g_in, g_out = unpack_call(unpack_ring_body, (summed,), shapes, {}, "unpack_ring")
        g_in, g_out = unpack_call(unpack_mlp_body, (g_side, from_partner, g_in, g_out), shapes[TWO:],
                                  {TWO: ZERO, THREE: ONE}, "unpack_mlp")
        return f1.y, t0.dx, g_qkv, g_proj, g_in, g_out, gains[:TWO], gains[TWO:FOUR]

    in_specs = (token_spec, P(dp_axes, None), P(row_axes)) + (P(),) * SIX + (token_spec,)
    out_specs = (token_spec, token_spec) + (P(),) * SIX
    return jax.shard_map(device_step, mesh=mesh, in_specs=in_specs, out_specs=out_specs, check_vma=False)
```

```python
import functools
import math
import jax
import jax.numpy as jnp
from jax import lax
from jax.experimental import pallas as pl
from jax.experimental.pallas import tpu as pltpu
from jax.sharding import Mesh, PartitionSpec as P

ZERO, ONE, TWO, THREE, FOUR = range(5)
SIX, TWELVE = 6, 12
HEAD = 64
HALF = 32
NHEAD = 12
DM = 768
FF = 3072
TOK = 512
GRP = 2048
WIN = 64
NDOC = 8
LANE = 128
EPS = 1e-5
NEG = -1e30
SCALE = 0.125
BASES = (160000.0, 10000.0)
F32 = jnp.float32
BF = jnp.bfloat16
QT = 256
FT = 512
NFT = FF // FT
QTILES = GRP // QT
MIB = 1024 * 1024
ALLTOK = (TOK, DM)
PROJ = DM // 2
DOWN = FF // 2
UP = FF
QKV = 3 * PROJ
MLP_ROWS = DOWN + UP
ATT_ROWS = PROJ + QKV
RING_ROWS = 2 * ATT_ROWS + MLP_ROWS
ANY = pl.BlockSpec(memory_space=pl.ANY)
DMA = pltpu.SemaphoreType.DMA
MESH = pl.DeviceIdType.MESH


def dot(a, b, ca, cb):
    return lax.dot_general(a, b, (((ca,), (cb,)), ((), ())), preferred_element_type=F32)


def mm(a, b):
    return dot(a, b, ONE, ZERO)


def mm_nt(a, b):
    return dot(a, b, ONE, ONE)


def mm_tn(a, b):
    return dot(a, b, ZERO, ZERO)


def call(body, grid, in_specs, out_specs, out_shape, scratch=(), prefetch=ZERO, flops=ZERO, nbytes=ZERO, name=None,
         cid=None, alias=None):
    extra = {} if cid is None else dict(collective_id=cid, has_side_effects=True)
    return pl.pallas_call(
        body,
        grid_spec=pltpu.PrefetchScalarGridSpec(
            num_scalar_prefetch=prefetch, grid=grid, in_specs=in_specs, out_specs=out_specs, scratch_shapes=scratch),
        out_shape=out_shape,
        input_output_aliases=alias or {},
        compiler_params=pltpu.CompilerParams(vmem_limit_bytes=60 * MIB, **extra),
        cost_estimate=pl.CostEstimate(flops=int(flops), bytes_accessed=int(nbytes), transcendentals=ZERO),
        name=name,
    )


def sds(shape, dtype):
    return jax.ShapeDtypeStruct(shape, dtype)


def spec(shape, *idx):
    idx = idx or (ZERO,) * len(shape)
    return pl.BlockSpec(shape, lambda *g: tuple(i(*g) if callable(i) else i for i in idx))


def step_of(s, *_):
    return s


def core_and_partner():
    core = lax.axis_index('core')
    return core, {'core': ONE - core}


def greet(devices):
    for dev in devices:
        pl.semaphore_signal(pltpu.get_barrier_semaphore(), inc=ONE, device_id=dev, device_id_type=MESH)


def all_here(devices):
    pl.semaphore_wait(pltpu.get_barrier_semaphore(), len(devices))


def sp_peer(d):
    return lax.rem(lax.axis_index('sp') + d, FOUR)


PEERS = range(ONE, FOUR)


class Swaps:
    def __init__(self, ssem, rsem, lsem):
        self.sems, self.waits, self.n = (ssem, rsem, lsem), [], ZERO
        self.core, self.partner = core_and_partner()
        self.other = ONE - self.core
        self.me = lax.axis_index('sp')

    def remote(self, src, dst, dev=None):
        ssem, rsem, _ = self.sems
        return self.later(pltpu.make_async_remote_copy(
            src_ref=src, dst_ref=dst, send_sem=ssem.at[self.n], recv_sem=rsem.at[self.n],
            device_id=self.partner if dev is None else dev, device_id_type=MESH))

    def local(self, src, dst):
        return self.later(pltpu.make_async_copy(src, dst, self.sems[TWO].at[self.n]))

    def later(self, cp):
        self.n += ONE
        self.waits.append(cp)
        return cp

    def to_all(self, src_of, dst_of):
        return [self.remote(src_of(sp_peer(d)), dst_of(self.me), {'sp': sp_peer(d)}) for d in PEERS] + [
            self.local(src_of(self.me), dst_of(self.me))]

    def to_sides(self, left_src, right_src, from_left, from_right):
        return [self.remote(right_src, from_left, {'sp': sp_peer(ONE)}), self.remote(left_src, from_right, {'sp': sp_peer(THREE)})]

    def early(self, some):
        gone = {id(cp) for cp in some}
        self.waits = [cp for cp in self.waits if id(cp) not in gone]
        return some

    def wait(self):
        for cp in self.waits:
            cp.wait()


def start_all(copies):
    for cp in copies:
        cp.start()


def wait_all(copies):
    for cp in copies:
        cp.wait()


def row_peers():
    return [core_and_partner()[ONE]] + [{'sp': sp_peer(d)} for d in PEERS]


def side_peers():
    return [{'sp': sp_peer(ONE)}, {'sp': sp_peer(THREE)}]


def partner_peer():
    return [core_and_partner()[ONE]]


def swap_sems(n):
    return [DMA((n,))] * THREE


def named_sems(n):
    return list(zip(('ssem', 'rsem', 'lsem'), swap_sems(n)))


class Refs:
    def __init__(self, named):
        self.__dict__.update(named)


class Stage:
    def __init__(self, body, steps, ins, outs, scratch, copies=None, links=None, alias=()):
        self.body, self.steps, self.ins, self.outs, self.scratch = body, steps, ins, outs, scratch
        self.copies, self.links, self.alias = copies, links or {}, alias


def shifted(block, first, steps):
    if block.index_map is None:
        return block
    return pl.BlockSpec(block.block_shape, lambda g: block.index_map(jnp.clip(g - first, ZERO, steps - ONE)))


def run(name, cid, peers, *stages):
    firsts = [sum(st.steps for st in stages[:k]) for k in range(len(stages))]

    def flat(kind):
        return [(k, entry) for k, st in enumerate(stages) for entry in getattr(st, kind)]

    ins, outs, scratch = flat('ins'), flat('outs'), flat('scratch')
    keys = [(k, entry[ZERO]) for k, entry in ins + outs + scratch]

    def body(*refs):
        pid = pl.program_id(ZERO)
        have = dict(zip(keys, refs))

        @pl.when(pid == ZERO)
        def _():
            greet(peers())

        talking = [k for k, st in enumerate(stages) if st.copies]
        views = []
        for k, st in enumerate(stages):
            r = Refs({n: ref for (at, n), ref in have.items() if at == k})
            for n, source in st.links.items():
                setattr(r, n, have[source])
            r.arrive = lambda k=k: all_here(peers()) if k == talking[ZERO] else None
            views.append(r)

            @pl.when((pid >= firsts[k]) & (pid < firsts[k] + st.steps))
            def _(st=st, r=r, k=k):
                st.body(r, pid - firsts[k])

        @pl.when(pid == firsts[-ONE] + stages[-ONE].steps - ONE)
        def _():
            for k in talking:
                stages[k].copies(views[k]).sw.wait()

    def placed(entries):
        return [shifted(entry[TWO], firsts[k], stages[k].steps) for k, entry in entries]

    alias = {[e[ZERO] for _, e in ins].index(a): [e[ZERO] for _, e in outs].index(b) for st in stages for a, b in st.alias}
    got = call(body, (sum(st.steps for st in stages),), placed(ins), placed(outs), [e[ONE] for _, e in outs],
               scratch=[e[ONE] for _, e in scratch], flops=16 * TOK * DM * FF, nbytes=30 * MIB, name=name, cid=cid,
               alias=alias)(*[e[ONE] for _, e in ins])
    out = [{} for _ in stages]
    for (k, e), arr in zip(outs, got):
        out[k][e[ZERO]] = arr
    return [Refs(named) for named in out]


def norm_parts(x_bf):
    rows = x_bf.astype(F32)
    cen = rows - jnp.mean(rows, axis=ONE, keepdims=True)
    var = jnp.mean(cen * cen, axis=ONE, keepdims=True)
    return cen, lax.rsqrt(var + EPS)


def norm_rows(x_bf, gain):
    cen, inv = norm_parts(x_bf)
    return (cen * inv * gain).astype(BF)


def norm_rows_grad(x_bf, gain, d_bf):
    cen, inv = norm_parts(x_bf)
    hat = cen * inv
    d_out = d_bf.astype(F32)
    g_gain = jnp.sum(d_out * hat, axis=ZERO, keepdims=True)
    d_hat = d_out * gain
    d_x = inv * (d_hat - jnp.mean(d_hat, axis=ONE, keepdims=True) - hat * jnp.mean(d_hat * hat, axis=ONE, keepdims=True))
    return d_x.astype(BF), g_gain


def add_bf(a, b):
    return (a.astype(F32) + b.astype(F32)).astype(BF)


RB = 256
ROPED = 6
CHUNKS = range(DM // RB)


def head_rows(ref, chunk, head):
    return ref.at[head, ZERO, chunk] if ref.shape[ZERO] == FOUR else ref.at[ZERO, chunk, head]


def weight_cols(layer, width, first=ZERO):
    return spec((None, DM, width), layer, ZERO, lambda s: first + s)


GAINS = spec((TWO, DM))


GROUP_QKV = (FOUR, THREE, THREE, HEAD, TOK)
OWN_QKV = (THREE * NHEAD, HEAD, TOK)
EDGE = (NHEAD, HEAD, LANE)
TOKS = jax.ShapeDtypeStruct(ALLTOK, BF)
TOK_SPEC = spec(ALLTOK)
TOK_VMEM = pltpu.VMEM(ALLTOK, BF)
TABLE = spec((HALF, TOK))
CU_SPEC = pl.BlockSpec(memory_space=pltpu.SMEM)


def rotated(a, b, r):
    cos, sin = r.cos[...], r.sin[...]
    return a * cos - b * sin, b * cos + a * sin


def qkv_chunk(r, w):
    return mm(r.h[...], w).astype(BF).astype(F32).T


def head_halves(t_rows, head):
    at = HEAD * head
    return t_rows[at:at + HALF], t_rows[at + HALF:at + HEAD]


def qkv_fwd_copies(r):
    sw = Swaps(r.ssem, r.rsem, r.lsem)
    return Refs(dict(sw=sw, start=[sw.remote(r.h, r.h_r), sw.local(r.h, r.h_m)],
                     edges=sw.to_sides(r.edge_s.at[ZERO], r.edge_s.at[ONE], r.left, r.right)))


def qkv_fwd_body(r, step, layer):
    cps = qkv_fwd_copies(r)

    @pl.when(step == ZERO)
    def _():
        r.h[...] = norm_rows(r.x[...], r.g[layer:layer + ONE])
        r.arrive()
        start_all(cps.start)

    for p in range(THREE):
        @pl.when(step == p)
        def _(p=p):
            for chunk in CHUNKS:
                t_rows = qkv_chunk(r, r.w[:, RB * chunk:RB * chunk + RB])
                for head in range(FOUR):
                    a, b = head_halves(t_rows, head)
                    if p < TWO:
                        a, b = rotated(a, b, r)
                    n = FOUR * chunk + head
                    out = r.out.at[n]
                    out[:HALF] = a.astype(BF)
                    out[HALF:] = b.astype(BF)
                    if p:
                        lane = WIN * (p - ONE)
                        blk = out[...]
                        r.edge_s[ZERO, n, :, lane:lane + WIN] = blk[:, :WIN]
                        r.edge_s[ONE, n, :, lane:lane + WIN] = blk[:, TOK - WIN:]

    @pl.when(step == TWO)
    def _():
        start_all(cps.edges)


def qkv_fwd_stage(layer, gain, w_qkv, tables, link):
    ins = [('g', gain, GAINS), ('w', w_qkv, weight_cols(layer, DM)), ('cos', tables[ZERO], TABLE), ('sin', tables[ONE], TABLE)]
    outs = [('h_m', TOKS, ANY), ('h_r', TOKS, ANY), ('out', sds(OWN_QKV, BF), spec((NHEAD, HEAD, TOK), step_of, ZERO, ZERO)),
            ('left', sds(EDGE, BF), ANY), ('right', sds(EDGE, BF), ANY)]
    scratch = [('h', TOK_VMEM), ('edge_s', pltpu.VMEM((TWO,) + EDGE, BF))]
    return Stage(functools.partial(qkv_fwd_body, layer=layer), THREE, ins, outs, scratch + named_sems(FOUR),
                 qkv_fwd_copies, {'x': link})


def tile_src(i, *_):
    return i // TWO


def tile_side(i, *_):
    return i % TWO


Q_SPEC = spec((ONE, ONE, THREE, HEAD, QT), tile_src, ZERO, ZERO, ZERO, tile_side)
O_SPEC = spec((ONE, THREE, HEAD, QT), tile_src, ZERO, ZERO, tile_side)
STAT_SPEC = spec((8, QT), ZERO, step_of)


def kv_spec(part):
    return spec((FOUR, ONE, THREE, HEAD, TOK), ZERO, part, ZERO, ZERO, ZERO)


def key_tile(kt):
    return kt // TWO, pl.ds(pl.multiple_of((kt % TWO) * QT, QT), QT)


def key_rows(dst, k_ref):
    for src in range(FOUR):
        for h in range(THREE):
            dst[h, TOK * src:TOK * src + TOK] = k_ref[src, ZERO, h].T


def row_tile(kt):
    return pl.ds(pl.multiple_of(kt * QT, QT), QT)


def doc_start(cu_ref, tok):
    start = jnp.zeros_like(tok)
    for d in range(ONE, NDOC):
        start = jnp.where(cu_ref[ZERO, d] <= tok, cu_ref[ZERO, d], start)
    return start


def doc_stop(cu_ref, tok):
    stop = jnp.full_like(tok, GRP)
    for d in range(NDOC - ONE, ZERO, -ONE):
        stop = jnp.where(cu_ref[ZERO, d] > tok, cu_ref[ZERO, d], stop)
    return stop


def tile_bounds(cu_ref, tile):
    first = tile * QT
    tok = lax.broadcasted_iota(jnp.int32, (ONE, QT), ONE) + first
    lo = doc_start(cu_ref, first) // QT
    hi = (doc_stop(cu_ref, first + QT - ONE) + QT - ONE) // QT
    return lo, hi, doc_start(cu_ref, tok), doc_stop(cu_ref, tok)


BY_OWNER = (FOUR, THREE, HEAD, TOK)


def group_copies(r):
    sw = Swaps(r.ssem, r.rsem, r.lsem)

    def head_parts(c):
        return [cp for p in range(THREE) for cp in sw.to_all(lambda dev: r.out_s.at[p, dev, c], lambda dev: r.got.at[dev, p, c])]

    start = [sw.remote(r.h, r.h_r), sw.local(r.h, r.h_m)]
    parts = [sw.early(head_parts(c)) for c in range(THREE)]
    heads = [sw.early(sw.to_all(lambda dev: r.o_s.at[dev, c], lambda dev: r.o_r.at[dev, c])) for c in range(THREE)]
    return Refs(dict(sw=sw, start=start, parts=parts, heads=heads, keep=[sw.local(r.got, r.out), sw.local(r.o_s, r.o_m)]))


def group_fwd_body(r, step):
    cps = group_copies(r)
    tiles = range(QTILES)

    @pl.when(step == ZERO)
    def _():
        r.h[...] = norm_rows(r.x[...], r.g[:ONE])
        r.arrive()
        start_all(cps.start)

    for c in range(THREE):
        @pl.when(step == c)
        def _(c=c):
            for p, w in enumerate((r.wq, r.wk, r.wv)):
                t_rows = qkv_chunk(r, w[...])
                for head in range(FOUR):
                    a, b = head_halves(t_rows, head)
                    if p < TWO:
                        a, b = rotated(a, b, r)
                    out = r.out_s.at[p, head, c]
                    out[:HALF] = a.astype(BF)
                    out[HALF:] = b.astype(BF)
            start_all(cps.parts[c])

        @pl.when(step == c + THREE)
        def _(c=c):
            wait_all(cps.parts[c])
            for src in range(FOUR):
                r.kr_s[TOK * src:TOK * src + TOK] = r.got[src, ONE, c].T
            io = lax.broadcasted_iota(jnp.int32, (QT, QT), ZERO)

            def q_tile(t, carry):
                src, cols = key_tile(t)
                tok = lax.broadcasted_iota(jnp.int32, (ONE, QT), ONE) + t * QT
                st, en = doc_start(r.cu, tok), doc_stop(r.cu, tok)
                q_t = r.got[src, ZERO, c, :, cols] * SCALE
                for k in tiles:
                    r.s_s[k] = mm(r.kr_s[QT * k:QT * k + QT], q_t)
                m = jnp.full((ONE, QT), NEG, F32)
                for k in tiles:
                    s = jnp.where((io >= st - QT * k) & (io < en - QT * k), r.s_s[k], NEG)
                    r.s_s[k] = s
                    m = jnp.maximum(m, jnp.max(s, axis=ZERO, keepdims=True))
                total = jnp.zeros((ONE, QT), F32)
                for k in tiles:
                    p = jnp.exp(r.s_s[k] - m)
                    total += jnp.sum(p, axis=ZERO, keepdims=True)
                    r.p_s[QT * k:QT * k + QT] = p.astype(BF)
                acc = jnp.zeros((HEAD, QT), F32)
                for k in range(FOUR):
                    acc += mm(r.got[k, TWO, c], r.p_s[TOK * k:TOK * k + TOK])
                r.o_s[src, c, :, cols] = (acc / total).astype(BF)
                r.lse[c:c + ONE, row_tile(t)] = m + jnp.log(total)
                return carry

            lax.fori_loop(ZERO, QTILES, q_tile, ZERO)
            start_all(cps.heads[c])

    @pl.when(step == ROPED - ONE)
    def _():
        start_all(cps.keep)
        for c in range(THREE):
            wait_all(cps.heads[c])


def group_fwd_stage(cu, gain, w_qkv, tables, x):
    part = lambda p: spec((None, DM, RB), ZERO, ZERO, lambda s: THREE * p + jnp.minimum(s, TWO))
    ins = [('cu', cu, CU_SPEC), ('g', gain, GAINS), ('wq', w_qkv, part(ZERO)), ('wk', w_qkv, part(ONE)), ('wv', w_qkv, part(TWO)),
           ('cos', tables[ZERO], TABLE), ('sin', tables[ONE], TABLE), ('x', x, TOK_SPEC)]
    outs = [('h_m', TOKS, ANY), ('h_r', TOKS, ANY), ('out', sds(GROUP_QKV, BF), ANY), ('o_m', sds(BY_OWNER, BF), ANY),
            ('lse', sds((8, GRP), F32), spec((8, GRP)))]
    owner = pltpu.VMEM(BY_OWNER, BF)
    scratch = [('h', TOK_VMEM), ('out_s', pltpu.VMEM((THREE, FOUR, THREE, HEAD, TOK), BF)), ('got', pltpu.VMEM(GROUP_QKV, BF)),
               ('kr_s', pltpu.VMEM((GRP, HEAD), BF)), ('s_s', pltpu.VMEM((QTILES, QT, QT), F32)), ('p_s', pltpu.VMEM((GRP, QT), BF)),
               ('o_s', owner), ('o_r', owner)]
    return Stage(group_fwd_body, ROPED, ins, outs, scratch + named_sems(FOUR * 16), group_copies)


def attn0_bwd_body(cu_ref, q_ref, k_ref, v_ref, o_ref, do_ref, lse_ref, out_ref,
                   dk_s, dv_s, dq_s, kr_s, vr_s, s_s, d_s, p_s, t_s):
    tile = pl.program_id(ZERO)
    first, last, st, en = tile_bounds(cu_ref, tile)
    heads = range(THREE)

    @pl.when(tile == ZERO)
    def _():
        dk_s[...] = jnp.zeros(dk_s.shape, F32)
        dv_s[...] = jnp.zeros(dv_s.shape, F32)
        key_rows(kr_s, k_ref)
        key_rows(vr_s, v_ref)

    dq_s[...] = jnp.zeros(dq_s.shape, F32)
    io = lax.broadcasted_iota(jnp.int32, (QT, QT), ZERO)
    q_t = [q_ref[ZERO, ZERO, h] * SCALE for h in heads]
    do_t = [do_ref[ZERO, h] for h in heads]
    q_rows, do_rows = [q_t[h].T for h in heads], [do_t[h].T for h in heads]
    delta = [jnp.sum(do_t[h].astype(F32) * o_ref[ZERO, h].astype(F32), axis=ZERO, keepdims=True) for h in heads]
    lse = [lse_ref[h:h + ONE] for h in heads]

    def body(kt, carry):
        base = kt * QT
        src, cols = key_tile(kt)
        rows = row_tile(kt)
        ok = (io >= st - base) & (io < en - base)
        for h in heads:
            s_s[h] = mm(kr_s[h, rows], q_t[h])
            d_s[h] = mm(vr_s[h, rows], do_t[h])
        for h in heads:
            p = jnp.exp(jnp.where(ok, s_s[h] - lse[h], NEG))
            p_s[h] = p.astype(BF)
            t_s[h] = (p * (d_s[h] - delta[h])).astype(BF)
        for h in heads:
            dv_s[h, rows] += mm(p_s[h], do_rows[h])
            dk_s[h, rows] += mm(t_s[h], q_rows[h])
            dq_s[h] += mm(k_ref[src, ZERO, h, :, cols], t_s[h])
        return carry

    lax.fori_loop(first, last, body, ZERO)
    src, cols = key_tile(tile)
    for h in heads:
        out_ref[src, ZERO, h, :, cols] = (dq_s[h] * SCALE).astype(BF)

    @pl.when(tile == QTILES - ONE)
    def _():
        for src in range(FOUR):
            for h in heads:
                out_ref[src, ONE, h] = dk_s[h, TOK * src:TOK * src + TOK].T.astype(BF)
                out_ref[src, TWO, h] = dv_s[h, TOK * src:TOK * src + TOK].T.astype(BF)


def attn0_bwd(cu, qkv, o_t, do_t, lse):
    acc, rows = pltpu.VMEM((THREE, GRP, HEAD), F32), pltpu.VMEM((THREE, GRP, HEAD), BF)
    sq32, sq16 = pltpu.VMEM((THREE, QT, QT), F32), pltpu.VMEM((THREE, QT, QT), BF)
    return call(
        attn0_bwd_body, (QTILES,),
        [Q_SPEC, kv_spec(ONE), kv_spec(TWO), O_SPEC, O_SPEC, STAT_SPEC],
        spec(GROUP_QKV), sds(GROUP_QKV, BF),
        scratch=[acc, acc, pltpu.VMEM((THREE, HEAD, QT), F32), rows, rows, sq32, sq32, sq16, sq16],
        prefetch=ONE, flops=30 * GRP * GRP * HEAD, nbytes=TWELVE * MIB, name="attn0_bwd",
    )(cu, qkv, qkv, qkv, o_t, do_t, lse)


NBLK = TOK // LANE
EXT = TOK + TWO * WIN
XBLK = EXT // LANE
REACH = LANE + TWO * WIN
AHEAD_FWD, AHEAD_BWD = 4, 2
HPS = 4
HSTEPS = NHEAD // HPS


def heads_of(width, part):
    return spec((HPS, HEAD, width), lambda n: HSTEPS * part + n, ZERO, ZERO)


def own_head(part):
    return heads_of(TOK, part)


def row_of(width):
    return spec((HPS, ONE, width), step_of, ZERO, ZERO)


LOW, HIGH = slice(None, WIN), slice(WIN, None)


def joined(left, mid, right, h, left_lanes=HIGH, right_lanes=LOW):
    return jnp.concatenate([left[h][:, left_lanes], mid[h], right[h][:, right_lanes]], axis=ONE)


def blocks(first, last):
    return slice(LANE * first, LANE * last)


def near_bounds(cu_ref, before, width):
    shift = lax.axis_index('sp') * TOK
    tok = lax.broadcasted_iota(jnp.int32, (ONE, width), ONE) + (shift - before)
    inside = (tok >= ZERO) & (tok < GRP)
    lo = jnp.maximum(doc_start(cu_ref, tok), tok - WIN) - (shift - WIN)
    hi = jnp.minimum(doc_stop(cu_ref, tok), tok + WIN + ONE) - (shift - WIN)
    return jnp.where(inside, lo, ZERO), jnp.where(inside, hi, ZERO)


def in_bounds(bounds, cols, first, n):
    io = lax.broadcasted_iota(jnp.int32, (n, LANE), ZERO) + first
    return (io >= bounds[ZERO][:, cols]) & (io < bounds[ONE][:, cols])


def every_head(fn, ahead):
    def body(g, c):
        fn([ahead * g + a for a in range(ahead)])
        return c
    lax.fori_loop(ZERO, HPS // ahead, body, ZERO)


def attn1_fwd_body(r, step):
    bounds = near_bounds(r.cu, ZERO, TOK)

    def some(heads):
        v_all = []
        for a, h in enumerate(heads):
            q_t = r.q[h] * SCALE
            k_rows = joined(r.left, r.k, r.right, h, LOW, LOW).T
            v_all.append(joined(r.left, r.v, r.right, h, HIGH, HIGH))
            for i in range(NBLK):
                r.s_s[a, i] = mm(k_rows[LANE * i:LANE * i + REACH], q_t[:, blocks(i, i + ONE)])
        for a, h in enumerate(heads):
            for i in range(NBLK):
                cols = blocks(i, i + ONE)
                s = jnp.where(in_bounds(bounds, cols, LANE * i, REACH), r.s_s[a, i], NEG)
                m = jnp.max(s, axis=ZERO, keepdims=True)
                e = jnp.exp(s - m)
                l = jnp.sum(e, axis=ZERO, keepdims=True)
                r.p_s[a, i] = (e * (ONE / l)).astype(BF)
                r.lse[h, :, cols] = m + jnp.log(l)
        for a, h in enumerate(heads):
            for i in range(NBLK):
                out = mm(v_all[a][:, LANE * i:LANE * i + REACH], r.p_s[a, i]).astype(BF)
                r.o[HPS * step + h, :, blocks(i, i + ONE)] = out
    every_head(some, AHEAD_FWD)


def attn1_fwd_stage(cu, qkv, left, right):
    tile, edge = (AHEAD_FWD, NBLK, REACH, LANE), heads_of(LANE, ZERO)
    return Stage(
        attn1_fwd_body, HSTEPS,
        [('cu', cu, CU_SPEC), ('q', qkv, own_head(ZERO)), ('k', qkv, own_head(ONE)), ('v', qkv, own_head(TWO)),
         ('left', left, edge), ('right', right, edge)],
        [('lse', sds((NHEAD, ONE, TOK), F32), row_of(TOK))],
        [('o', pltpu.VMEM((NHEAD, HEAD, TOK), BF)), ('s_s', pltpu.VMEM(tile, F32)), ('p_s', pltpu.VMEM(tile, BF))])


def attn1_bwd_body(r, step):
    bounds = near_bounds(r.cu, WIN, EXT)

    def window(e):
        first, last = max(LANE * e - WIN, ZERO), min(LANE * e + LANE + WIN, EXT)
        return first, last - first

    def parts(h):
        q_t = joined(r.ql, r.q, r.qr, h) * SCALE
        return q_t, joined(r.dl, r.d, r.dr, h), joined(r.left, r.k, r.right, h, LOW, LOW)

    def some(heads):
        for a, h in enumerate(heads):
            q_t, do_t, k_t = parts(h)
            k_rows, v_rows = k_t.T, joined(r.left, r.v, r.right, h, HIGH, HIGH).T
            for e in range(XBLK):
                first, n = window(e)
                cols = blocks(e, e + ONE)
                r.s_s[a, e, :n] = mm(k_rows[first:first + n], q_t[:, cols])
                r.d_s[a, e, :n] = mm(v_rows[first:first + n], do_t[:, cols])
        for a, h in enumerate(heads):
            lse, delta = joined(r.ll, r.lse, r.lr, h), joined(r.el, r.delta, r.er, h)
            for e in range(XBLK):
                first, n = window(e)
                cols = blocks(e, e + ONE)
                ok = in_bounds(bounds, cols, first, n)
                p = jnp.exp(jnp.where(ok, r.s_s[a, e, :n] - lse[:, cols], NEG))
                r.p_s[a, first:first + n, cols] = p.astype(BF)
                r.t_s[a, first:first + n, cols] = (p * (r.d_s[a, e, :n] - delta[:, cols])).astype(BF)
        for a, h in enumerate(heads):
            q_t, do_t, k_t = parts(h)
            got = [[], [], []]
            for b in range(XBLK):
                here, wide = blocks(b, b + ONE), blocks(max(b - ONE, ZERO), min(b + TWO, XBLK))
                got[ZERO].append(mm(k_t[:, wide], r.t_s[a, wide, here]) * SCALE)
                got[ONE].append(mm_nt(q_t[:, wide], r.t_s[a, here, wide]))
                got[TWO].append(mm_nt(do_t[:, wide], r.p_s[a, here, wide]))
            for n in range(THREE):
                own = jnp.concatenate([g.astype(BF) for g in got[n]], axis=ONE)[:, WIN:WIN + TOK]
                r.out[n, HPS * step + h] = own

    @pl.when(step == ZERO)
    def _():
        r.p_s[...] = jnp.zeros(r.p_s.shape, BF)
        r.t_s[...] = jnp.zeros(r.t_s.shape, BF)

    every_head(some, AHEAD_BWD)


def attn1_bwd_stage(cu, qkv, do_t, lse, delta, edges, far):
    edge, row = heads_of(LANE, ZERO), row_of(LANE)
    blk = (AHEAD_BWD, XBLK, REACH, LANE)
    square = pltpu.VMEM((AHEAD_BWD, EXT, EXT), BF)
    names = ('left', 'right', 'ql', 'qr', 'dl', 'dr')
    return Stage(
        attn1_bwd_body, HSTEPS,
        [('cu', cu, CU_SPEC), ('q', qkv, own_head(ZERO)), ('k', qkv, own_head(ONE)), ('v', qkv, own_head(TWO)), ('d', do_t, own_head(ZERO)),
         ('lse', lse, row_of(TOK)), ('delta', delta, row_of(TOK))]
        + [(n, arr, edge) for n, arr in zip(names, list(edges) + far[:FOUR])]
        + [(n, arr, row) for n, arr in zip(('ll', 'lr', 'el', 'er'), far[FOUR:])],
        [], [('out', pltpu.VMEM((THREE, NHEAD, HEAD, TOK), BF)), ('s_s', pltpu.VMEM(blk, F32)), ('d_s', pltpu.VMEM(blk, F32)),
             ('p_s', square), ('t_s', square)])


ROWBLK = [slice(r, r + RB) for r in range(ZERO, TOK, RB)]
HALFT = NFT // TWO
SQRT_HALF = math.sqrt(SCALE * FOUR)
PDF_SCALE = SQRT_HALF / math.sqrt(math.pi)


def normal_cdf(a):
    return SQRT_HALF * SQRT_HALF * (ONE + lax.erf(a * SQRT_HALF))


def half_rows(ref, which):
    n = ref.shape[ZERO] // TWO
    return ref.at[pl.ds(pl.multiple_of(which * n, n), n)]


def col_tile(ref, n):
    return ref.at[:, pl.ds(pl.multiple_of(n * FT, FT), FT)]


def mlp_copies(r, fwd, bwd):
    sw = Swaps(r.ssem, r.rsem, r.lsem)
    c = Refs(dict(sw=sw, start=[]))
    if fwd:
        c.start += [sw.remote(r.h, r.h_r), sw.remote(half_rows(r.of, sw.other), r.of_r),
                    sw.local(half_rows(r.of, sw.core), r.of_m), sw.local(r.h, r.h_m)]
        c.m_out = [(sw.remote(r.m_s.at[HALFT * sw.other + n], col_tile(r.m_r, n)),
                    sw.local(r.m_s.at[HALFT * sw.core + n], col_tile(r.m_m, n))) for n in range(HALFT)]
    if fwd and not bwd:
        c.start.append(sw.local(r.x1, r.x1_m))
    if bwd:
        c.start.append(sw.remote(r.dy, r.dy_r))
        c.dmid_out = sw.remote(r.dmid, r.dmid_r)
        c.du_out = [(sw.remote(r.du_s.at[n, sw.other], col_tile(r.du_r, n)),
                     sw.local(r.du_s.at[n, sw.core], col_tile(r.du_m, n))) for n in range(NFT)]
    if bwd and not fwd:
        c.do_out = sw.to_all(lambda dev: r.do_s.at[dev], lambda dev: r.d_o.at[dev])
    return c


def mlp_body(r, step, layer, fwd, bwd):
    cps = mlp_copies(r, fwd, bwd)
    sw, start, whole_group = cps.sw, cps.start, not (fwd and bwd)
    if fwd:
        m_out = cps.m_out
    if bwd:
        dmid_out, du_out = cps.dmid_out, cps.du_out

    @pl.when(step == ZERO)
    def _():
        if fwd:
            for n in range(NHEAD):
                r.of[HEAD * n:HEAD * n + HEAD, :] = (r.o[n % FOUR, n // FOUR] if whole_group else r.o[n])
            x1 = (r.x[...].astype(F32) + mm_tn(r.of[...], r.wp[...])).astype(BF)
            r.x1[...] = x1
            r.h[...] = norm_rows(x1, r.g[layer:layer + ONE])
            r.acc[...] = x1.astype(F32)
        if bwd:
            r.dacc[...] = jnp.zeros(r.dacc.shape, F32)
        r.arrive()
        start_all(start)

    for rows in ROWBLK:
        if fwd:
            ua = mm(r.h[rows], r.wa[...]).astype(BF)
            ub = mm(r.h[rows], r.wb[...]).astype(BF)
            if not bwd:
                r.u[ZERO, rows] = ua
                r.u[ONE, rows] = ub
        else:
            ua, ub = r.u[ZERO, rows], r.u[ONE, rows]
        a, b = ua.astype(F32), ub.astype(F32)
        cdf = normal_cdf(a)
        gate = a * cdf
        if fwd:
            m = (gate * b).astype(BF)
            r.m_s[step, rows] = m
            r.acc[rows] += mm(m, r.wo[...])
        if bwd:
            dm = mm_nt(r.dy[rows], r.wo[...]).astype(BF).astype(F32)
            pdf = jnp.exp(a * a * (SCALE * FOUR - ONE)) * PDF_SCALE
            db = (dm * gate).astype(BF)
            da = (dm * b * (cdf + a * pdf)).astype(BF)
            r.du_s[step, ZERO, rows] = da
            r.du_s[step, ONE, rows] = db
            r.dacc[rows] += mm_nt(da, r.wa[...]) + mm_nt(db, r.wb[...])

    for n in range(NFT):
        @pl.when(step == n)
        def _(n=n):
            if fwd:
                there, here = m_out[n % HALFT]

                @pl.when(sw.core == n // HALFT)
                def _():
                    here.start()

                @pl.when(sw.other == n // HALFT)
                def _():
                    there.start()
            if bwd:
                for cp in du_out[n]:
                    cp.start()

    @pl.when(step == NFT - ONE)
    def _():
        if fwd:
            r.y[...] = r.acc[...].astype(BF)
        if bwd:
            d_ln, gg = norm_rows_grad(r.x1[...], r.g[layer:layer + ONE], r.dacc[...].astype(BF))
            r.gg[...] = gg
            d_mid = add_bf(r.dy[...], d_ln)
            r.dmid[...] = d_mid
            dmid_out.start()
            d_att = mm_nt(r.wp[...], d_mid).astype(BF)
            for n in range(NHEAD):
                rows = slice(HEAD * n, HEAD * n + HEAD)
                blk = d_att[rows]
                if whole_group:
                    r.do_s[n % FOUR, n // FOUR] = blk
                else:
                    r.d_o[n] = blk
                    r.delta[n] = jnp.sum(blk.astype(F32) * r.of[rows].astype(F32), axis=ZERO, keepdims=True)
            if whole_group:
                start_all(cps.do_out)


def mlp_stage(layer, fwd, bwd, w_proj, gain, w_in, w_out, links=None, **arrays):
    u_spec = spec((TWO, TOK, FT), ZERO, ZERO, step_of)
    half_o = sds((DM // TWO, TOK), BF)
    half_m, half_u = sds((TOK, FF // TWO), BF), sds((TOK, FF), BF)
    heads = (NHEAD, HEAD, TOK)
    sums = pltpu.VMEM(ALLTOK, F32)
    links = links or {}
    ins = [('wp', w_proj, spec((None, DM, DM), layer, ZERO, ZERO)), ('g', gain, GAINS),
           ('wa', w_in, weight_cols(layer, FT)), ('wb', w_in, weight_cols(layer, FT, NFT)),
           ('wo', w_out, spec((None, FT, DM), layer, step_of, ZERO))]
    kinds = dict(x=TOK_SPEC, dy=TOK_SPEC, x1=TOK_SPEC, u=u_spec)
    ins += [(n, arr, kinds[n]) for n, arr in arrays.items()]
    outs, scratch = [], []
    if fwd:
        outs += [('y', TOKS, TOK_SPEC), ('h_m', TOKS, ANY), ('h_r', TOKS, ANY), ('of_m', half_o, ANY), ('of_r', half_o, ANY),
                 ('m_m', half_m, ANY), ('m_r', half_m, ANY)]
        scratch += [('acc', sums), ('of', pltpu.VMEM((DM, TOK), BF)), ('m_s', pltpu.VMEM((NFT, TOK, FT), BF)), ('h', TOK_VMEM),
                    ('x1', TOK_VMEM)]
    if fwd and not bwd:
        outs += [('x1_m', TOKS, ANY), ('u', sds((TWO, TOK, FF), BF), u_spec)]
    if bwd:
        shape = heads if fwd else BY_OWNER
        outs += [('dmid', TOKS, TOK_SPEC), ('gg', sds((ONE, DM), F32), spec((ONE, DM))), ('d_o', sds(shape, BF), spec(shape) if fwd else ANY),
                 ('dy_r', TOKS, ANY), ('dmid_r', TOKS, ANY), ('du_m', half_u, ANY), ('du_r', half_u, ANY)]
        scratch += [('dacc', sums), ('du_s', pltpu.VMEM((NFT, TWO, TOK, FT), BF))]
    if fwd and bwd:
        outs += [('delta', sds((NHEAD, ONE, TOK), F32), spec((NHEAD, ONE, TOK)))]
    if not fwd:
        scratch += [('do_s', pltpu.VMEM(BY_OWNER, BF))]
    return Stage(functools.partial(mlp_body, layer=layer, fwd=fwd, bwd=bwd), NFT, ins, outs, scratch + named_sems(FOUR * NFT),
                 functools.partial(mlp_copies, fwd=fwd, bwd=bwd), links)


NAMED = ('ha', 'hb', 'oa', 'ob', 'dma', 'dmb')


def third(ref, n):
    return ref.at[PROJ * n:PROJ * n + PROJ]


def qkv_bwd_copies(r, grads):
    sw = Swaps(r.ssem, r.rsem, r.lsem)
    c = Refs(dict(sw=sw, parts=[[sw.remote(r.dt_s.at[sw.other, n], third(r.dt_r, n))] for n in range(THREE)]))
    if grads:
        c.loads = sw.early([sw.local(getattr(r, n + '_in'), getattr(r, n)) for n in NAMED])
        for part in c.parts:
            sw.early(part)
    else:
        for n in range(THREE):
            c.parts[n].append(sw.local(r.dt_s.at[sw.core, n], third(r.dt_m, n)))
    return c


def qkv_bwd_body(r, step, layer, grads):
    cps = qkv_bwd_copies(r, grads)
    sw, copies = cps.sw, cps.parts

    @pl.when(step == ZERO)
    def _():
        r.acc[...] = jnp.zeros(r.acc.shape, F32)
        if grads:
            start_all(cps.loads)

    for p in range(THREE):
        @pl.when(step == p)
        def _(p=p):
            cos, sin = r.cos[...], r.sin[...]
            for chunk in CHUNKS:
                for head in range(FOUR):
                    blk = r.d[head, ZERO, chunk] if grads else r.d[p, FOUR * chunk + head]
                    a, b = blk[:HALF], blk[HALF:]
                    if p < TWO:
                        a, b = a.astype(F32), b.astype(F32)
                        a, b = (a * cos + b * sin).astype(BF), (b * cos - a * sin).astype(BF)
                    at, full = LANE * chunk + HEAD * (head % TWO), RB * chunk + HEAD * head
                    for n, val in ((ZERO, a), (HALF, b)):
                        r.dt_s[head // TWO, p, at + n:at + n + HALF] = val
                        r.dt_all[full + n:full + n + HALF] = val
            if p == ZERO:
                r.arrive()
            start_all(copies[p])
            r.acc[...] += mm(r.w[...], r.dt_all[...])

    @pl.when(step == TWO)
    def _():
        d_ln, gg = norm_rows_grad(r.x[...], r.g[layer:layer + ONE], r.acc[...].T.astype(BF))
        r.gg[...] = gg
        r.dx[...] = add_bf(r.dmid[...], d_ln)

    if grads:
        @pl.when(step == THREE)
        def _():
            wait_all(cps.loads)
            for part in copies:
                wait_all(part)
            r.out[...] = mm(r.oa[...], r.dma[...]) + mm(r.ob[...], r.dmb[...])

        for p in range(THREE):
            @pl.when(step == p + FOUR)
            def _(p=p):
                r.out[...] = mm(r.dt_s[sw.core, p], r.ha[...]) + mm(third(r.dt_r, p)[...], r.hb[...])


def qkv_bwd_stage(layer, tables, w_qkv, x, gain, d_mid, d=None, link=None, grads=None, pairs=()):
    part = lambda s: jnp.minimum(s, TWO)
    ins = [('cos', tables[ZERO], TABLE), ('sin', tables[ONE], TABLE), ('w', w_qkv, spec((None, DM, DM), layer, ZERO, part)),
           ('x', x, TOK_SPEC), ('g', gain, GAINS), ('dmid', d_mid, TOK_SPEC)]
    outs = [('dx', TOKS, TOK_SPEC), ('gg', sds((ONE, DM), F32), spec((ONE, DM)))]
    feats = (THREE * PROJ, TOK)
    scratch = [('acc', pltpu.VMEM((DM, TOK), F32)), ('dt_s', pltpu.VMEM((TWO, THREE, PROJ, TOK), BF)), ('dt_all', pltpu.VMEM((DM, TOK), BF))]
    steps, alias = THREE, ()
    if grads is None:
        outs += [('dt_m', sds(feats, BF), ANY), ('dt_r', sds(feats, BF), ANY)]
    else:
        first = (ATT_ROWS + MLP_ROWS) // PROJ
        ins += [('d', d, spec((FOUR, ONE, THREE, HEAD, TOK), ZERO, part, ZERO, ZERO, ZERO)), ('grads', grads, ANY)]
        ins += [(n + '_in', arr, ANY) for n, arr in zip(NAMED, pairs)]
        outs += [('out', sds(grads.shape, F32), spec((PROJ, DM), lambda s: first + jnp.maximum(s - THREE, ZERO), ZERO))]
        scratch += [('dt_r', pltpu.VMEM(feats, BF))] + [(n, pltpu.VMEM(arr.shape, BF)) for n, arr in zip(NAMED, pairs)]
        steps, alias = steps + FOUR, (('grads', 'out'),)
    flag = grads is not None
    return Stage(functools.partial(qkv_bwd_body, layer=layer, grads=flag), steps, ins, outs, scratch + named_sems(TWELVE),
                 functools.partial(qkv_bwd_copies, grads=flag), {} if link is None else {'d': link}, alias)


NDOWN = DOWN // DM


def grad_call(body, grads, steps, in_specs, args, rows, first_row, total, scratch=(), edges=(), cid=None):
    shared = [] if grads is None else [grads]
    first = first_row // rows
    more = [sds(arr.shape[:TWO] + (LANE,), arr.dtype) for arr in edges for _ in range(TWO)]
    return call(
        functools.partial(body, edges=len(edges)) if edges else body, (steps,), [ANY] * len(shared + list(edges)) + in_specs,
        [spec((rows, DM), lambda s: first + s, ZERO)] + [ANY] * len(more), [sds((total, DM), F32)] + more, scratch=scratch,
        flops=FOUR * steps * rows * TOK * DM, nbytes=20 * MIB, name=getattr(body, "__name__"), cid=cid,
        alias={ZERO: ZERO} if shared else None,
    )(*shared, *edges, *args)


GRAD_INS = 8


def grad_mlp_body(*refs, edges=ZERO):
    step = pl.program_id(ZERO)
    if edges:
        srcs, refs, (h_t, *sems) = refs[:edges], refs[edges:-FOUR], refs[-FOUR:]
        refs, outs = refs[:GRAD_INS + ONE], refs[GRAD_INS + ONE:]
        sw = Swaps(*sems)
        for n, src in enumerate(srcs):
            view = src.at[:NHEAD]
            sw.to_sides(view.at[:, :, :LANE], view.at[:, :, TOK - LANE:], outs[TWO * n].at[:NHEAD], outs[TWO * n + ONE].at[:NHEAD])

        @pl.when(step == ZERO)
        def _():
            greet(side_peers())
            all_here(side_peers())
            for cp in sw.waits:
                cp.start()
    else:
        refs, h_t = refs[:-ONE], refs[-ONE]
    ma, mb, dya, dyb, ha, hb, dua, dub, out_ref = refs[-GRAD_INS - ONE:]

    @pl.when(step < NDOWN)
    def _():
        out_ref[...] = mm_tn(ma[...], dya[...]) + mm_tn(mb[...], dyb[...])

    @pl.when(step == NDOWN)
    def _():
        h_t[ZERO] = ha[...].T
        h_t[ONE] = hb[...].T

    @pl.when(step >= NDOWN)
    def _():
        out_ref[...] = mm(h_t[ZERO], dua[...]) + mm(h_t[ONE], dub[...])

    if edges:
        @pl.when(step == NDOWN + UP // DM - ONE)
        def _():
            sw.wait()


def grad_mlp(grads, m, m_r, dy, dy_r, h, h_r, du, du_r, first_row, total, edges=(), cid=None):
    toks = spec(ALLTOK)
    m_col = spec(ALLTOK, ZERO, lambda s: jnp.minimum(s, NDOWN - ONE))
    du_col = spec(ALLTOK, ZERO, lambda s: jnp.maximum(s - NDOWN, ZERO))
    return grad_call(grad_mlp_body, grads, NDOWN + UP // DM, [m_col, m_col, toks, toks, toks, toks, du_col, du_col],
                     (m, m_r, dy, dy_r, h, h_r, du, du_r), DM, first_row, total, edges=edges, cid=cid,
                     scratch=[pltpu.VMEM((TWO, DM, TOK), BF)] + (swap_sems(TWO * len(edges)) if edges else []))


def grad_att_body(*refs):
    oa, ob, dma, dmb, ta, tb, ha, hb, out_ref = refs[-GRAD_INS - ONE:]
    step = pl.program_id(ZERO)

    @pl.when(step == ZERO)
    def _():
        out_ref[...] = mm(oa[...], dma[...]) + mm(ob[...], dmb[...])

    @pl.when(step > ZERO)
    def _():
        out_ref[...] = mm(ta[...], ha[...]) + mm(tb[...], hb[...])


def grad_att(grads, of, of_r, dmid, dmid_r, dt, dt_r, h, h_r, first_row):
    toks = spec(ALLTOK)
    blk = (PROJ, TOK)
    dt_row = spec(blk, lambda s: jnp.maximum(s - ONE, ZERO), ZERO)
    return grad_call(grad_att_body, grads, ONE + QKV // PROJ, [spec(blk), spec(blk), toks, toks, dt_row, dt_row, toks, toks],
                     (of, of_r, dmid, dmid_r, dt, dt_r, h, h_r), PROJ, first_row, RING_ROWS)


NB, NS = 5, 6
CH = RING_ROWS // (NB * FOUR)
SB, LF = CH // FOUR, CH // 16
RS = 9
LAST = RS + RS
ADD_ROWS = 96


def ring_body(g_ref, ln_ref, f_ref, lnout_ref, bufa, bufb, bufc, gath, stage, lnbuf,
              ssem, rsem, psem, qsem, csem, stsem, lns, lnr):
    core, partner = core_and_partner()
    zy = lax.axis_index('zy')
    pos = (lax.axis_index('sp'), lax.rem(zy, FOUR), zy // FOUR)
    streams = [(c, sg) for c in range(THREE) for sg in (ONE, -ONE)]
    bufs, sizes = (bufa, bufb, bufc), (CH, SB, LF)
    peers = range(ONE, FOUR)

    def mod4(v):
        return lax.rem(v + 8, FOUR)

    def at(axis, val):
        if axis == ZERO:
            return {'sp': val}
        yz = (val, pos[TWO]) if axis == ONE else (pos[ONE], val)
        return {'zy': yz[ONE] * FOUR + yz[ZERO]}

    def shifted(axis, d):
        return at(axis, mod4(pos[axis] + d))

    def axis_of(s, ph):
        return (streams[s][ZERO] + ph) % THREE

    def idx(s, ph, t):
        return mod4(pos[axis_of(s, ph)] - streams[s][ONE] * t)

    def own(s, ph):
        return idx(s, ph, -ONE)

    def base(b):
        return b * (FOUR * CH)

    bar = pltpu.get_barrier_semaphore()
    for ax in range(THREE):
        for d in peers:
            pl.semaphore_signal(bar, inc=ONE, device_id=shifted(ax, d), device_id_type=MESH)
    pl.semaphore_signal(bar, inc=ONE, device_id=partner, device_id_type=MESH)
    pl.semaphore_wait(bar, 10)

    def rows(ref, start, n):
        return ref.at[pl.ds(pl.multiple_of(start, LF), n)]

    def grows(s, start, n):
        return g_ref.at[pl.ds(pl.multiple_of(start, LF), n), LANE * s:LANE * s + LANE]

    def frows(s, start, n):
        return f_ref.at[core, pl.ds(pl.multiple_of(start, LF), n), LANE * s:LANE * s + LANE]

    def same_bytes(b, k):
        if k < RS:
            return bufs[k // THREE].at[b, k % THREE]
        n = sizes[TWO - (k - RS) // THREE]
        return gath.at[b] if n == CH else gath.at[b, :, pl.ds(ZERO, n)]

    def wait_for(ref, sem):
        pltpu.make_async_copy(ref, ref, sem).wait()

    def send(b, s, k):
        ph = k // THREE if k < RS else TWO - (k - RS) // THREE
        t = k % THREE
        n = sizes[ph]
        if k < RS:
            dst = bufs[ph].at[b, t, s]
            if t:
                src = bufs[ph].at[b, t - ONE, s]
            elif ph:
                src = rows(bufs[ph - ONE].at[b, TWO, s], idx(s, ph, ZERO) * n, n)
            else:
                src = grows(s, base(b) + idx(s, ZERO, ZERO) * n, n)
        elif ph:
            off = own(s, ONE) * SB if ph == TWO else ZERO
            src = dst = rows(gath.at[b, s], off + idx(s, ph, t - ONE) * n, n)
        else:
            dst = frows(s, base(b) + idx(s, ZERO, t - ONE) * n, n)
            src = dst if t else gath.at[b, s]
        pltpu.make_async_remote_copy(src_ref=src, dst_ref=dst, send_sem=ssem.at[b, k], recv_sem=rsem.at[b, k],
                                     device_id=shifted(axis_of(s, ph), streams[s][ONE]), device_id_type=MESH).start()

    def stage_load(n):
        t, b, slot = n // NB, lax.rem(n, NB), lax.rem(n, TWO)
        for s in range(NS):
            pltpu.make_async_copy(grows(s, base(b) + idx(s, ZERO, t + ONE) * CH, CH), stage.at[slot, s],
                                  stsem.at[slot]).start()

    def ln_copy(ph, d):
        return pltpu.make_async_remote_copy(
            src_ref=lnbuf.at[ph, THREE] if ph else ln_ref, dst_ref=lnbuf.at[ph, d - ONE], send_sem=lns.at[ph, d - ONE],
            recv_sem=lnr.at[ph, d - ONE], device_id=shifted(ph, d) if ph < THREE else partner, device_id_type=MESH)

    def ln_sum(ph):
        vals = [lnbuf[ph, THREE] if ph else ln_ref[...]] + [lnbuf[ph, d - ONE] for d in peers]
        total = jnp.zeros_like(vals[ZERO])
        for p in range(FOUR):
            term = vals[ZERO]
            for d in peers:
                term = jnp.where(mod4(pos[ph] - d) == p, vals[d], term)
            total = total + term
        return total

    def batches(fn, start=ZERO):
        def body(b, c):
            fn(b)
            return c
        lax.fori_loop(start, NB, body, ZERO)

    def first(b):
        for s in range(NS):
            send(b, s, ZERO)

    first(ZERO)
    stage_load(jnp.int32(ZERO))
    for d in peers:
        ln_copy(ZERO, d).start()
    batches(first, ONE)

    for k in range(RS):
        ph, t = k // THREE, k % THREE
        buf, size = bufs[ph], sizes[ph]

        def step(b, k=k, ph=ph, t=t, buf=buf, size=size):
            n = k * NB + b
            slot = lax.rem(n, TWO)
            if not ph:
                @pl.when(n < THREE * NB - ONE)
                def _():
                    stage_load(n + ONE)
                wait_for(stage.at[slot], stsem.at[slot])
            wait_for(same_bytes(b, k), rsem.at[b, k])
            for s in range(NS):
                if ph:
                    off = pl.multiple_of(idx(s, ph, t + ONE) * size, LF)
                    buf[b, t, s] += bufs[ph - ONE][b, TWO, s, pl.ds(off, size)]
                else:
                    @pl.loop(ZERO, CH, step=ADD_ROWS)
                    def _(r):
                        at_r = pl.ds(pl.multiple_of(r, ADD_ROWS), ADD_ROWS)
                        buf[b, t, s, at_r] += stage[slot, s, at_r]
                if k == RS - ONE:
                    off = pl.multiple_of(own(s, ONE) * SB + own(s, TWO) * LF, LF)
                    gath[b, s, pl.ds(off, LF)] = bufc[b, TWO, s]
                send(b, s, k + ONE)

        batches(step)
        if k < SIX and k % TWO == ZERO:
            lp = k // TWO
            for d in peers:
                ln_copy(lp, d).wait()
            lnbuf[lp + ONE, THREE] = ln_sum(lp)
            for d in peers if lp < TWO else (ONE,):
                ln_copy(lp + ONE, d).start()

    def hand_over(b, s, j, src, start):
        pltpu.make_async_remote_copy(src_ref=src, dst_ref=frows(s, start, CH), send_sem=psem.at[b, j], recv_sem=qsem.at[b, j],
                                     device_id=partner, device_id_type=MESH).start()

    for k in range(RS, LAST):
        def step(b, k=k):
            wait_for(same_bytes(b, k), rsem.at[b, k])
            piece = k - (LAST - FOUR)
            for s in range(NS):
                if k < LAST - ONE:
                    send(b, s, k + ONE)
                if piece >= ZERO:
                    start = base(b) + idx(s, ZERO, piece - ONE) * CH
                    if piece:
                        hand_over(b, s, piece, frows(s, start, CH), start)
                    else:
                        pltpu.make_async_copy(gath.at[b, s], frows(s, start, CH), csem.at[b]).start()
                        hand_over(b, s, piece, gath.at[b, s], start)
        batches(step)

    ln_copy(THREE, ONE).wait()
    lnout_ref[...] = lnbuf[THREE, THREE] + lnbuf[THREE, ZERO]

    def finish(b):
        for k in range(LAST):
            wait_for(same_bytes(b, k), ssem.at[b, k])
        for j in range(FOUR):
            wait_for(gath.at[b], psem.at[b, j])
            wait_for(gath.at[b], qsem.at[b, j])
        wait_for(gath.at[b], csem.at[b])
    batches(finish)


def ring_all_reduce(g, ln, cid):
    vmem = pl.BlockSpec(memory_space=pltpu.VMEM)
    return pl.pallas_call(
        ring_body,
        in_specs=[ANY, vmem],
        out_specs=[ANY, vmem],
        out_shape=[sds((TWO, RING_ROWS, DM), F32), sds(ln.shape, F32)],
        scratch_shapes=[
            pltpu.VMEM((NB, THREE, NS, CH, LANE), F32), pltpu.VMEM((NB, THREE, NS, SB, LANE), F32),
            pltpu.VMEM((NB, THREE, NS, LF, LANE), F32), pltpu.VMEM((NB, NS, CH, LANE), F32),
            pltpu.VMEM((TWO, NS, CH, LANE), F32),
            pltpu.VMEM((FOUR, FOUR) + ln.shape, F32),
            DMA((NB, LAST)), DMA((NB, LAST)), DMA((NB, FOUR)), DMA((NB, FOUR)), DMA((NB,)), DMA((TWO,)),
            DMA((FOUR, THREE)), DMA((FOUR, THREE)),
        ],
        compiler_params=pltpu.CompilerParams(collective_id=cid, has_side_effects=True, vmem_limit_bytes=60 * MIB),
        cost_estimate=pl.CostEstimate(flops=MIB * MIB // FOUR, bytes_accessed=200 * MIB, transcendentals=ZERO),
        name="ring_all_reduce",
    )(g, ln)


SLOTS, LAG = 8, 4
NTURN = TWO * THREE
OUT_SHAPE, IN_SHAPE = (TWO, FF, DM), (TWO, DM, TWO * FF)


def stream(pieces, buf, turned, isem, osem):
    def loads(i):
        slot, srcs = i % SLOTS, pieces[i][ZERO]
        n = srcs[ZERO].shape[ZERO]
        return [pltpu.make_async_copy(src, buf.at[slot, k * n:k * n + n], isem.at[slot, k]) for k, src in enumerate(srcs)]

    def store(i):
        _, dst, turn = pieces[i]
        src = buf.at[i % SLOTS, :dst.shape[ZERO]] if turn is None else turned.at[turn]
        return pltpu.make_async_copy(src, dst, osem.at[i % SLOTS])

    total = len(pieces)
    for i in range(total + LAG):
        if i < total:
            if i >= SLOTS:
                store(i - SLOTS).wait()
            for cp in loads(i):
                cp.start()
        k = i - LAG
        if k >= ZERO:
            for cp in loads(k):
                cp.wait()
            turn = pieces[k][TWO]
            if turn is not None:
                for n in CHUNKS:
                    rows, col = LANE * n, RB * n
                    turned[turn, :, col:col + LANE] = buf[k % SLOTS, rows:rows + LANE].T
                    turned[turn, :, col + LANE:col + RB] = buf[k % SLOTS, PROJ + rows:PROJ + rows + LANE].T
            store(k).start()
    for i in range(max(total - SLOTS, ZERO), total):
        store(i).wait()


def unpack_ring_body(f, g_qkv, g_proj, g_in, g_out, *scratch):
    def block(c, row, n=DM):
        return f.at[c, row:row + n]

    pieces = []
    for c in range(TWO):
        for n in range(NDOWN):
            pieces.append(([block(c, ATT_ROWS + DM * n)], g_out.at[ZERO, DOWN * c + DM * n:DOWN * c + DM * n + DM], None))
        for n in range(FOUR):
            col = UP * c + DM * n
            pieces.append(([block(c, ATT_ROWS + DOWN + DM * n)], g_in.at[ZERO, :, col:col + DM], None))
    for l in range(TWO):
        first = (ONE - l) * (ATT_ROWS + MLP_ROWS)
        for n in range(THREE):
            row = first + PROJ * (n + ONE)
            pieces.append(([block(c, row, PROJ) for c in range(TWO)], g_qkv.at[l, :, DM * n:DM * n + DM], THREE * l + n))
        for c in range(TWO):
            pieces.append(([block(c, first, PROJ)], g_proj.at[l, PROJ * c:PROJ * c + PROJ], None))
    stream(pieces, *scratch)


def unpack_mlp_body(own, other, in_0, out_0, g_in, g_out, *scratch):
    core = lax.axis_index('core')
    pieces = []
    for src, side in ((own, core), (other, ONE - core)):
        for n in range(NDOWN):
            row = pl.multiple_of(DOWN * side + DM * n, DM)
            pieces.append(([src.at[DM * n:DM * n + DM]], g_out.at[ONE, pl.ds(row, DM)], None))
        for n in range(FOUR):
            col = pl.multiple_of(UP * side + DM * n, DM)
            pieces.append(([src.at[DOWN + DM * n:DOWN + DM * n + DM]], g_in.at[ONE, :, pl.ds(col, DM)], None))
    stream(pieces, *scratch)


def unpack_call(body, args, outs, alias, name):
    return pl.pallas_call(
        body, in_specs=[ANY] * len(args), out_specs=[ANY] * len(outs), out_shape=[sds(shape, F32) for shape in outs],
        scratch_shapes=[pltpu.VMEM((SLOTS, DM, DM), F32), pltpu.VMEM((NTURN, DM, DM), F32), DMA((SLOTS, TWO)), DMA((SLOTS,))],
        input_output_aliases=alias,
        compiler_params=pltpu.CompilerParams(vmem_limit_bytes=60 * MIB),
        cost_estimate=pl.CostEstimate(flops=MIB * MIB // RB, bytes_accessed=75 * MIB, transcendentals=ZERO), name=name,
    )(*args)


def rope_tables(pos, base):
    inv_freq = base ** (jnp.arange(HALF).astype(F32) * (-TWO / HEAD))
    angles = inv_freq[:, None] * pos.astype(F32)[None, :]
    return jnp.cos(angles), jnp.sin(angles)


def solution(mesh):
    n_sp = mesh.shape['sp']
    by_core = mesh.devices.reshape(n_sp, mesh.shape['dp'] // TWO, TWO)
    mesh = Mesh(by_core, ('sp', 'zy', 'core'))
    dp_axes = ('zy', 'core')
    row_axes = dp_axes + ('sp',)
    token_spec = P(row_axes, None)
    swap_cores = [(ZERO, ONE), (ONE, ZERO)]
    cids = list(range(RS))

    def exchange(arr):
        return lax.all_to_all(arr, 'sp', ZERO, ZERO, tiled=True)

    def device_step(x_loc, cu_loc, pos_loc, w_qkv, w_proj, w_in, w_out, ln_attn, ln_mlp, d_out):
        tab0, tab1 = [rope_tables(pos_loc, base) for base in BASES]
        mlp_args, w_mlp = (w_proj, ln_mlp), (w_in, w_out)

        q0, f0, q1 = run("layer0_qkv1", cids[ONE], row_peers, group_fwd_stage(cu_loc, ln_attn, w_qkv, tab0, x_loc),
                         mlp_stage(ZERO, True, False, *mlp_args, *w_mlp, links={'o': (ZERO, 'o_r')}, x=x_loc),
                         qkv_fwd_stage(ONE, ln_attn, w_qkv, tab1, (ONE, 'y')))
        kv_edges = (q1.left, q1.right)
        a1, f1 = run("attn1_mlp1", cids[THREE], partner_peer, attn1_fwd_stage(cu_loc, q1.out, *kv_edges),
                     mlp_stage(ONE, True, True, *mlp_args, *w_mlp, links={'o': (ZERO, 'o')}, x=f0.y, dy=d_out))
        g_side, *far = grad_mlp(None, f1.m_m, f1.m_r, d_out, f1.dy_r, f1.h_m, f1.h_r, f1.du_m, f1.du_r, ZERO, MLP_ROWS,
                                edges=(q1.out, f1.d_o, a1.lse, f1.delta), cid=cids[FOUR])
        g_side = lax.psum(g_side, ('sp', 'zy'))
        _, t1, b0 = run("attn1_qkv1_mlp0", cids[5], row_peers,
                        attn1_bwd_stage(cu_loc, q1.out, f1.d_o, a1.lse, f1.delta, kv_edges, far),
                        qkv_bwd_stage(ONE, tab1, w_qkv, f0.y, ln_attn, f1.dmid, link=(ZERO, 'out')),
                        mlp_stage(ZERO, False, True, *mlp_args, *w_mlp, links={'dy': (ONE, 'dx')}, x1=f0.x1_m, u=f0.u))
        dqkv0 = exchange(attn0_bwd(cu_loc, q0.out, q0.o_m, b0.d_o, q0.lse))
        grads, = grad_att(None, f1.of_m, f1.of_r, f1.dmid, f1.dmid_r, t1.dt_m, t1.dt_r, q1.h_m, q1.h_r, ZERO)
        grads, = grad_mlp(grads, f0.m_m, f0.m_r, t1.dx, b0.dy_r, f0.h_m, f0.h_r, b0.du_m, b0.du_r, ATT_ROWS, RING_ROWS)
        t0, = run("qkv0_grads", cids[SIX], partner_peer, qkv_bwd_stage(
            ZERO, tab0, w_qkv, x_loc, ln_attn, b0.dmid, d=dqkv0, grads=grads,
            pairs=(q0.h_m, q0.h_r, f0.of_m, f0.of_r, b0.dmid, b0.dmid_r)))

        gains = jnp.concatenate([t0.gg, t1.gg, b0.gg, f1.gg, jnp.zeros((FOUR, DM), F32)], axis=ZERO)
        summed, gains = ring_all_reduce(t0.out, gains, cids[ZERO])
        summed, g_side = lax.optimization_barrier((summed, g_side))
        from_partner = lax.ppermute(g_side, 'core', swap_cores)
        shapes = [(TWO, DM, THREE * DM), (TWO, DM, DM), IN_SHAPE, OUT_SHAPE]
        g_qkv, g_proj, g_in, g_out = unpack_call(unpack_ring_body, (summed,), shapes, {}, "unpack_ring")
        g_in, g_out = unpack_call(unpack_mlp_body, (g_side, from_partner, g_in, g_out), shapes[TWO:],
                                  {TWO: ZERO, THREE: ONE}, "unpack_mlp")
        return f1.y, t0.dx, g_qkv, g_proj, g_in, g_out, gains[:TWO], gains[TWO:FOUR]

    in_specs = (token_spec, P(dp_axes, None), P(row_axes)) + (P(),) * SIX + (token_spec,)
    out_specs = (token_spec, token_spec) + (P(),) * SIX
    return jax.shard_map(device_step, mesh=mesh, in_specs=in_specs, out_specs=out_specs, check_vma=False)
```

```python
import functools
import math
import jax
import jax.numpy as jnp
from jax import lax
from jax.experimental import pallas as pl
from jax.experimental.pallas import tpu as pltpu
from jax.sharding import Mesh, PartitionSpec as P

ZERO, ONE, TWO, THREE, FOUR = range(5)
SIX, TWELVE = 6, 12
HEAD = 64
HALF = 32
NHEAD = 12
DM = 768
FF = 3072
TOK = 512
GRP = 2048
WIN = 64
NDOC = 8
LANE = 128
EPS = 1e-5
NEG = -1e30
SCALE = 0.125
BASES = (160000.0, 10000.0)
F32 = jnp.float32
BF = jnp.bfloat16
QT = 256
FT = 768
NFT = FF // FT
QTILES = GRP // QT
MIB = 1024 * 1024
ALLTOK = (TOK, DM)
ALLDM = (DM, DM)
PROJ = DM // 2
DOWN = FF // 2
UP = FF
QKV = 3 * PROJ
MLP_ROWS = DOWN + UP
ATT_ROWS = PROJ + QKV
RING_ROWS = 2 * ATT_ROWS + MLP_ROWS
ANY = pl.BlockSpec(memory_space=pl.ANY)
DMA = pltpu.SemaphoreType.DMA
MESH = pl.DeviceIdType.MESH


def dot(a, b, ca, cb):
    return lax.dot_general(a, b, (((ca,), (cb,)), ((), ())), preferred_element_type=F32)


def mm(a, b):
    return dot(a, b, ONE, ZERO)


def mm_nt(a, b):
    return dot(a, b, ONE, ONE)


def mm_tn(a, b):
    return dot(a, b, ZERO, ZERO)


def call(body, grid, in_specs, out_specs, out_shape, scratch=(), prefetch=ZERO, flops=ZERO, nbytes=ZERO, name=None,
         cid=None, alias=None):
    extra = {} if cid is None else dict(collective_id=cid, has_side_effects=True)
    return pl.pallas_call(
        body,
        grid_spec=pltpu.PrefetchScalarGridSpec(
            num_scalar_prefetch=prefetch, grid=grid, in_specs=in_specs, out_specs=out_specs, scratch_shapes=scratch),
        out_shape=out_shape,
        input_output_aliases=alias or {},
        compiler_params=pltpu.CompilerParams(vmem_limit_bytes=60 * MIB, **extra),
        cost_estimate=pl.CostEstimate(flops=int(flops), bytes_accessed=int(nbytes), transcendentals=ZERO),
        name=name,
    )


def sds(shape, dtype):
    return jax.ShapeDtypeStruct(shape, dtype)


def spec(shape, *idx):
    idx = idx or (ZERO,) * len(shape)
    return pl.BlockSpec(shape, lambda *g: tuple(i(*g) if callable(i) else i for i in idx))


def step_of(s, *_):
    return s


def core_and_partner():
    core = lax.axis_index('core')
    return core, {'core': ONE - core}


def greet(devices):
    for dev in devices:
        pl.semaphore_signal(pltpu.get_barrier_semaphore(), inc=ONE, device_id=dev, device_id_type=MESH)


def all_here(devices):
    pl.semaphore_wait(pltpu.get_barrier_semaphore(), len(devices))


def sp_peer(d):
    return lax.rem(lax.axis_index('sp') + d, FOUR)


PEERS = range(ONE, FOUR)


class Swaps:
    def __init__(self, ssem, rsem, lsem):
        self.sems, self.waits, self.n = (ssem, rsem, lsem), [], ZERO
        self.core, self.partner = core_and_partner()
        self.other = ONE - self.core
        self.me = lax.axis_index('sp')

    def remote(self, src, dst, dev=None):
        ssem, rsem, _ = self.sems
        return self.later(pltpu.make_async_remote_copy(
            src_ref=src, dst_ref=dst, send_sem=ssem.at[self.n], recv_sem=rsem.at[self.n],
            device_id=self.partner if dev is None else dev, device_id_type=MESH))

    def local(self, src, dst):
        return self.later(pltpu.make_async_copy(src, dst, self.sems[TWO].at[self.n]))

    def later(self, cp):
        self.n += ONE
        self.waits.append(cp)
        return cp

    def to_all(self, src_of, dst_of):
        return [self.remote(src_of(sp_peer(d)), dst_of(self.me), {'sp': sp_peer(d)}) for d in PEERS] + [
            self.local(src_of(self.me), dst_of(self.me))]

    def to_sides(self, left_src, right_src, from_left, from_right):
        return [self.remote(right_src, from_left, {'sp': sp_peer(ONE)}), self.remote(left_src, from_right, {'sp': sp_peer(THREE)})]

    def early(self, some):
        gone = {id(cp) for cp in some}
        self.waits = [cp for cp in self.waits if id(cp) not in gone]
        return some

    def wait(self):
        for cp in self.waits:
            cp.wait()


def start_all(copies):
    for cp in copies:
        cp.start()


def wait_all(copies):
    for cp in copies:
        cp.wait()


def row_peers():
    return [core_and_partner()[ONE]] + [{'sp': sp_peer(d)} for d in PEERS]


def side_peers():
    return [{'sp': sp_peer(ONE)}, {'sp': sp_peer(THREE)}]


def partner_peer():
    return [core_and_partner()[ONE]]


def near_peers():
    return partner_peer() + side_peers()


def swap_sems(n):
    return [DMA((n,))] * THREE


def named_sems(n):
    return list(zip(('ssem', 'rsem', 'lsem'), swap_sems(n)))


class Refs:
    def __init__(self, named):
        self.__dict__.update(named)


class Stage:
    def __init__(self, body, steps, ins, outs, scratch, copies=None, links=None, alias=()):
        self.body, self.steps, self.ins, self.outs, self.scratch = body, steps, ins, outs, scratch
        self.copies, self.links, self.alias = copies, links or {}, alias


def shifted(block, first, steps):
    if block.index_map is None:
        return block
    return pl.BlockSpec(block.block_shape, lambda g: block.index_map(jnp.clip(g - first, ZERO, steps - ONE)))


def run(name, cid, peers, *stages):
    firsts = [sum(st.steps for st in stages[:k]) for k in range(len(stages))]

    def flat(kind):
        return [(k, entry) for k, st in enumerate(stages) for entry in getattr(st, kind)]

    ins, outs, scratch = flat('ins'), flat('outs'), flat('scratch')
    keys = [(k, entry[ZERO]) for k, entry in ins + outs + scratch]

    def body(*refs):
        pid = pl.program_id(ZERO)
        have = dict(zip(keys, refs))

        @pl.when(pid == ZERO)
        def _():
            greet(peers())

        talking = [k for k, st in enumerate(stages) if st.copies]
        views = []
        for k, st in enumerate(stages):
            r = Refs({n: ref for (at, n), ref in have.items() if at == k})
            for n, source in st.links.items():
                setattr(r, n, have[source])
            r.arrive = lambda k=k: all_here(peers()) if k == talking[ZERO] else None
            views.append(r)

            @pl.when((pid >= firsts[k]) & (pid < firsts[k] + st.steps))
            def _(st=st, r=r, k=k):
                st.body(r, pid - firsts[k])

        @pl.when(pid == firsts[-ONE] + stages[-ONE].steps - ONE)
        def _():
            for k in talking:
                stages[k].copies(views[k]).sw.wait()

    def placed(entries):
        return [shifted(entry[TWO], firsts[k], stages[k].steps) for k, entry in entries]

    alias = {[e[ZERO] for _, e in ins].index(a): [e[ZERO] for _, e in outs].index(b) for st in stages for a, b in st.alias}
    got = call(body, (sum(st.steps for st in stages),), placed(ins), placed(outs), [e[ONE] for _, e in outs],
               scratch=[e[ONE] for _, e in scratch], flops=16 * TOK * DM * FF, nbytes=30 * MIB, name=name, cid=cid,
               alias=alias)(*[e[ONE] for _, e in ins])
    out = [{} for _ in stages]
    for (k, e), arr in zip(outs, got):
        out[k][e[ZERO]] = arr
    return [Refs(named) for named in out]


def norm_parts(x_bf):
    rows = x_bf.astype(F32)
    cen = rows - jnp.mean(rows, axis=ONE, keepdims=True)
    var = jnp.mean(cen * cen, axis=ONE, keepdims=True)
    return cen, lax.rsqrt(var + EPS)


def norm_rows(x_bf, gain):
    cen, inv = norm_parts(x_bf)
    return (cen * inv * gain).astype(BF)


def norm_rows_grad(x_bf, gain, d_bf):
    cen, inv = norm_parts(x_bf)
    hat = cen * inv
    d_out = d_bf.astype(F32)
    g_gain = jnp.sum(d_out * hat, axis=ZERO, keepdims=True)
    d_hat = d_out * gain
    d_x = inv * (d_hat - jnp.mean(d_hat, axis=ONE, keepdims=True) - hat * jnp.mean(d_hat * hat, axis=ONE, keepdims=True))
    return d_x.astype(BF), g_gain


def add_bf(a, b):
    return (a.astype(F32) + b.astype(F32)).astype(BF)


RB = 256
ROPED = 6
CHUNKS = range(DM // RB)


def head_rows(ref, chunk, head):
    return ref.at[head, ZERO, chunk] if ref.shape[ZERO] == FOUR else ref.at[ZERO, chunk, head]


def weight_cols(layer, width, first=ZERO):
    return spec((None, DM, width), layer, ZERO, lambda s: first + s)


GAINS = spec((TWO, DM))


GROUP_QKV = (FOUR, THREE, THREE, HEAD, TOK)
OWN_QKV = (THREE * NHEAD, HEAD, TOK)
EDGE = (NHEAD, HEAD, LANE)
TOKS = jax.ShapeDtypeStruct(ALLTOK, BF)
TOK_SPEC = spec(ALLTOK)
TOK_VMEM = pltpu.VMEM(ALLTOK, BF)
TABLE = spec((HALF, TOK))
CU_SPEC = pl.BlockSpec(memory_space=pltpu.SMEM)


def rotated(a, b, r):
    cos, sin = r.cos[...], r.sin[...]
    return a * cos - b * sin, b * cos + a * sin


def qkv_chunk(r, w):
    return mm(r.h[...], w).astype(BF).astype(F32).T


def head_halves(t_rows, head):
    at = HEAD * head
    return t_rows[at:at + HALF], t_rows[at + HALF:at + HEAD]


def qkv_fwd_copies(r):
    sw = Swaps(r.ssem, r.rsem, r.lsem)
    return Refs(dict(sw=sw, start=[sw.remote(r.h, r.h_r), sw.local(r.h, r.h_m)],
                     edges=sw.to_sides(r.edge_s.at[ZERO], r.edge_s.at[ONE], r.left, r.right)))


def qkv_fwd_body(r, step, layer):
    cps = qkv_fwd_copies(r)

    @pl.when(step == ZERO)
    def _():
        r.h[...] = norm_rows(r.x[...], r.g[layer:layer + ONE])
        r.arrive()
        start_all(cps.start)

    for p in range(THREE):
        @pl.when(step == p)
        def _(p=p):
            for chunk in CHUNKS:
                t_rows = qkv_chunk(r, r.w[:, RB * chunk:RB * chunk + RB])
                for head in range(FOUR):
                    a, b = head_halves(t_rows, head)
                    if p < TWO:
                        a, b = rotated(a, b, r)
                    n = FOUR * chunk + head
                    out = r.out.at[n]
                    out[:HALF] = a.astype(BF)
                    out[HALF:] = b.astype(BF)
                    if p:
                        lane = WIN * (p - ONE)
                        blk = out[...]
                        r.edge_s[ZERO, n, :, lane:lane + WIN] = blk[:, :WIN]
                        r.edge_s[ONE, n, :, lane:lane + WIN] = blk[:, TOK - WIN:]

    @pl.when(step == TWO)
    def _():
        start_all(cps.edges)


def qkv_fwd_stage(layer, gain, w_qkv, tables, link):
    ins = [('g', gain, GAINS), ('w', w_qkv, weight_cols(layer, DM)), ('cos', tables[ZERO], TABLE), ('sin', tables[ONE], TABLE)]
    outs = [('h_m', TOKS, ANY), ('h_r', TOKS, ANY), ('out', sds(OWN_QKV, BF), spec((NHEAD, HEAD, TOK), step_of, ZERO, ZERO)),
            ('left', sds(EDGE, BF), ANY), ('right', sds(EDGE, BF), ANY)]
    scratch = [('h', TOK_VMEM), ('edge_s', pltpu.VMEM((TWO,) + EDGE, BF))]
    return Stage(functools.partial(qkv_fwd_body, layer=layer), THREE, ins, outs, scratch + named_sems(FOUR),
                 qkv_fwd_copies, {'x': link})


def tile_src(i, *_):
    return i // TWO


def tile_side(i, *_):
    return i % TWO


Q_SPEC = spec((ONE, ONE, THREE, HEAD, QT), tile_src, ZERO, ZERO, ZERO, tile_side)
O_SPEC = spec((ONE, THREE, HEAD, QT), tile_src, ZERO, ZERO, tile_side)
STAT_SPEC = spec((8, QT), ZERO, step_of)


def kv_spec(part):
    return spec((FOUR, ONE, THREE, HEAD, TOK), ZERO, part, ZERO, ZERO, ZERO)


def key_tile(kt):
    return kt // TWO, pl.ds(pl.multiple_of((kt % TWO) * QT, QT), QT)


def key_rows(dst, k_ref):
    for src in range(FOUR):
        for h in range(THREE):
            dst[h, TOK * src:TOK * src + TOK] = k_ref[src, ZERO, h].T


def row_tile(kt):
    return pl.ds(pl.multiple_of(kt * QT, QT), QT)


def doc_start(cu_ref, tok):
    start = jnp.zeros_like(tok)
    for d in range(ONE, NDOC):
        start = jnp.where(cu_ref[ZERO, d] <= tok, cu_ref[ZERO, d], start)
    return start


def doc_stop(cu_ref, tok):
    stop = jnp.full_like(tok, GRP)
    for d in range(NDOC - ONE, ZERO, -ONE):
        stop = jnp.where(cu_ref[ZERO, d] > tok, cu_ref[ZERO, d], stop)
    return stop


def tile_bounds(cu_ref, tile):
    first = tile * QT
    tok = lax.broadcasted_iota(jnp.int32, (ONE, QT), ONE) + first
    lo = doc_start(cu_ref, first) // QT
    hi = (doc_stop(cu_ref, first + QT - ONE) + QT - ONE) // QT
    return lo, hi, doc_start(cu_ref, tok), doc_stop(cu_ref, tok)


BY_OWNER = (FOUR, THREE, HEAD, TOK)


def group_copies(r):
    sw = Swaps(r.ssem, r.rsem, r.lsem)

    def head_parts(c):
        return [cp for p in range(THREE) for cp in sw.to_all(lambda dev: r.out_s.at[p, dev, c], lambda dev: r.got.at[dev, p, c])]

    start = [sw.remote(r.h, r.h_r), sw.local(r.h, r.h_m)]
    parts = [sw.early(head_parts(c)) for c in range(THREE)]
    heads = [sw.early(sw.to_all(lambda dev: r.o_s.at[dev, c], lambda dev: r.o_r.at[dev, c])) for c in range(THREE)]
    return Refs(dict(sw=sw, start=start, parts=parts, heads=heads, keep=[sw.local(r.got, r.out), sw.local(r.o_s, r.o_m)]))


def group_fwd_body(r, step):
    cps = group_copies(r)
    tiles = range(QTILES)

    @pl.when(step == ZERO)
    def _():
        r.h[...] = norm_rows(r.x[...], r.g[:ONE])
        r.arrive()
        start_all(cps.start)

    for c in range(THREE):
        @pl.when(step == c)
        def _(c=c):
            for p, w in enumerate((r.wq, r.wk, r.wv)):
                t_rows = qkv_chunk(r, w[...])
                for head in range(FOUR):
                    a, b = head_halves(t_rows, head)
                    if p < TWO:
                        a, b = rotated(a, b, r)
                    out = r.out_s.at[p, head, c]
                    out[:HALF] = a.astype(BF)
                    out[HALF:] = b.astype(BF)
            start_all(cps.parts[c])

        @pl.when(step == c + THREE)
        def _(c=c):
            wait_all(cps.parts[c])
            for src in range(FOUR):
                r.kr_s[TOK * src:TOK * src + TOK] = r.got[src, ONE, c].T
            io = lax.broadcasted_iota(jnp.int32, (QT, QT), ZERO)

            def q_pair(src, carry):
                pair = range(TWO)
                cols = [slice(QT * a, QT * a + QT) for a in pair]
                toks = [lax.broadcasted_iota(jnp.int32, (ONE, QT), ONE) + src * TOK + QT * a for a in pair]
                st, en = [doc_start(r.cu, tok) for tok in toks], [doc_stop(r.cu, tok) for tok in toks]
                for a in pair:
                    q_t = r.got[src, ZERO, c, :, cols[a]] * SCALE
                    for k in tiles:
                        r.s_s[a, k] = mm(r.kr_s[QT * k:QT * k + QT], q_t)
                top, total = [], []
                for a in pair:
                    m = jnp.full((ONE, QT), NEG, F32)
                    for k in tiles:
                        s = jnp.where((io >= st[a] - QT * k) & (io < en[a] - QT * k), r.s_s[a, k], NEG)
                        r.s_s[a, k] = s
                        m = jnp.maximum(m, jnp.max(s, axis=ZERO, keepdims=True))
                    top.append(m)
                for a in pair:
                    part = jnp.zeros((ONE, QT), F32)
                    for k in tiles:
                        p = jnp.exp(r.s_s[a, k] - top[a])
                        part += jnp.sum(p, axis=ZERO, keepdims=True)
                        r.p_s[a, QT * k:QT * k + QT] = p.astype(BF)
                    total.append(part)
                for a in pair:
                    acc = jnp.zeros((HEAD, QT), F32)
                    for k in range(FOUR):
                        acc += mm(r.got[k, TWO, c], r.p_s[a, TOK * k:TOK * k + TOK])
                    r.o_s[src, c, :, cols[a]] = (acc / total[a]).astype(BF)
                    r.lse[c:c + ONE, row_tile(TWO * src + a)] = top[a] + jnp.log(total[a])
                return carry

            lax.fori_loop(ZERO, FOUR, q_pair, ZERO)
            start_all(cps.heads[c])

    @pl.when(step == ROPED - ONE)
    def _():
        start_all(cps.keep)
        for c in range(THREE):
            wait_all(cps.heads[c])


def group_fwd_stage(cu, gain, w_qkv, tables, x):
    part = lambda p: spec((None, DM, RB), ZERO, ZERO, lambda s: THREE * p + jnp.minimum(s, TWO))
    ins = [('cu', cu, CU_SPEC), ('g', gain, GAINS), ('wq', w_qkv, part(ZERO)), ('wk', w_qkv, part(ONE)), ('wv', w_qkv, part(TWO)),
           ('cos', tables[ZERO], TABLE), ('sin', tables[ONE], TABLE), ('x', x, TOK_SPEC)]
    outs = [('h_m', TOKS, ANY), ('h_r', TOKS, ANY), ('out', sds(GROUP_QKV, BF), ANY), ('o_m', sds(BY_OWNER, BF), ANY),
            ('lse', sds((8, GRP), F32), spec((8, GRP)))]
    owner = pltpu.VMEM(BY_OWNER, BF)
    scratch = [('h', TOK_VMEM), ('out_s', pltpu.VMEM((THREE, FOUR, THREE, HEAD, TOK), BF)), ('got', pltpu.VMEM(GROUP_QKV, BF)),
               ('kr_s', pltpu.VMEM((GRP, HEAD), BF)), ('s_s', pltpu.VMEM((TWO, QTILES, QT, QT), F32)), ('p_s', pltpu.VMEM((TWO, GRP, QT), BF)),
               ('o_s', owner), ('o_r', owner)]
    return Stage(group_fwd_body, ROPED, ins, outs, scratch + named_sems(FOUR * 16), group_copies)


def attn0_bwd_body(cu_ref, q_ref, k_ref, v_ref, o_ref, do_ref, lse_ref, out_ref,
                   dk_s, dv_s, dq_s, kr_s, vr_s, s_s, d_s, p_s, t_s):
    tile = pl.program_id(ZERO)
    first, last, st, en = tile_bounds(cu_ref, tile)
    heads = range(THREE)

    @pl.when(tile == ZERO)
    def _():
        dk_s[...] = jnp.zeros(dk_s.shape, F32)
        dv_s[...] = jnp.zeros(dv_s.shape, F32)
        key_rows(kr_s, k_ref)
        key_rows(vr_s, v_ref)

    dq_s[...] = jnp.zeros(dq_s.shape, F32)
    io = lax.broadcasted_iota(jnp.int32, (QT, QT), ZERO)
    q_t = [q_ref[ZERO, ZERO, h] * SCALE for h in heads]
    do_t = [do_ref[ZERO, h] for h in heads]
    q_rows, do_rows = [q_t[h].T for h in heads], [do_t[h].T for h in heads]
    delta = [jnp.sum(do_t[h].astype(F32) * o_ref[ZERO, h].astype(F32), axis=ZERO, keepdims=True) for h in heads]
    lse = [lse_ref[h:h + ONE] for h in heads]

    def body(kt, carry):
        base = kt * QT
        src, cols = key_tile(kt)
        rows = row_tile(kt)
        ok = (io >= st - base) & (io < en - base)
        for h in heads:
            s_s[h] = mm(kr_s[h, rows], q_t[h])
            d_s[h] = mm(vr_s[h, rows], do_t[h])
        for h in heads:
            p = jnp.exp(jnp.where(ok, s_s[h] - lse[h], NEG))
            p_s[h] = p.astype(BF)
            t_s[h] = (p * (d_s[h] - delta[h])).astype(BF)
        for h in heads:
            dv_s[h, rows] += mm(p_s[h], do_rows[h])
            dk_s[h, rows] += mm(t_s[h], q_rows[h])
            dq_s[h] += mm(k_ref[src, ZERO, h, :, cols], t_s[h])
        return carry

    lax.fori_loop(first, last, body, ZERO)
    src, cols = key_tile(tile)
    for h in heads:
        out_ref[src, ZERO, h, :, cols] = (dq_s[h] * SCALE).astype(BF)

    @pl.when(tile == QTILES - ONE)
    def _():
        for src in range(FOUR):
            for h in heads:
                out_ref[src, ONE, h] = dk_s[h, TOK * src:TOK * src + TOK].T.astype(BF)
                out_ref[src, TWO, h] = dv_s[h, TOK * src:TOK * src + TOK].T.astype(BF)


def attn0_bwd(cu, qkv, o_t, do_t, lse):
    acc, rows = pltpu.VMEM((THREE, GRP, HEAD), F32), pltpu.VMEM((THREE, GRP, HEAD), BF)
    sq32, sq16 = pltpu.VMEM((THREE, QT, QT), F32), pltpu.VMEM((THREE, QT, QT), BF)
    return call(
        attn0_bwd_body, (QTILES,),
        [Q_SPEC, kv_spec(ONE), kv_spec(TWO), O_SPEC, O_SPEC, STAT_SPEC],
        spec(GROUP_QKV), sds(GROUP_QKV, BF),
        scratch=[acc, acc, pltpu.VMEM((THREE, HEAD, QT), F32), rows, rows, sq32, sq32, sq16, sq16],
        prefetch=ONE, flops=30 * GRP * GRP * HEAD, nbytes=TWELVE * MIB, name="attn0_bwd",
    )(cu, qkv, qkv, qkv, o_t, do_t, lse)


NBLK = TOK // LANE
EXT = TOK + TWO * WIN
XBLK = EXT // LANE
REACH = LANE + TWO * WIN
AHEAD_FWD, AHEAD_BWD = 4, 2
HPS = 4
HSTEPS = NHEAD // HPS


def heads_of(width, part):
    return spec((HPS, HEAD, width), lambda n: HSTEPS * part + n, ZERO, ZERO)


def own_head(part):
    return heads_of(TOK, part)


def row_of(width):
    return spec((HPS, ONE, width), step_of, ZERO, ZERO)


LOW, HIGH = slice(None, WIN), slice(WIN, None)
STAT = jax.ShapeDtypeStruct((NHEAD, ONE, TOK), F32)
STAT_BLOCK = spec((NHEAD, ONE, TOK))


def joined(left, mid, right, h, left_lanes=HIGH, right_lanes=LOW):
    return jnp.concatenate([left[h][:, left_lanes], mid[h], right[h][:, right_lanes]], axis=ONE)


def blocks(first, last):
    return slice(LANE * first, LANE * last)


def near_bounds(cu_ref, before, width):
    shift = lax.axis_index('sp') * TOK
    tok = lax.broadcasted_iota(jnp.int32, (ONE, width), ONE) + (shift - before)
    inside = (tok >= ZERO) & (tok < GRP)
    lo = jnp.maximum(doc_start(cu_ref, tok), tok - WIN) - (shift - WIN)
    hi = jnp.minimum(doc_stop(cu_ref, tok), tok + WIN + ONE) - (shift - WIN)
    return jnp.where(inside, lo, ZERO), jnp.where(inside, hi, ZERO)


def in_bounds(bounds, cols, first, n):
    io = lax.broadcasted_iota(jnp.int32, (n, LANE), ZERO) + first
    return (io >= bounds[ZERO][:, cols]) & (io < bounds[ONE][:, cols])


def every_head(fn, ahead):
    def body(g, c):
        fn([ahead * g + a for a in range(ahead)])
        return c
    lax.fori_loop(ZERO, HPS // ahead, body, ZERO)


def attn1_fwd_body(r, step):
    bounds = near_bounds(r.cu, ZERO, TOK)

    def some(heads):
        v_all = []
        for a, h in enumerate(heads):
            q_t = r.q[h] * SCALE
            k_rows = joined(r.left, r.k, r.right, h, LOW, LOW).T
            v_all.append(joined(r.left, r.v, r.right, h, HIGH, HIGH))
            for i in range(NBLK):
                r.s_s[a, i] = mm(k_rows[LANE * i:LANE * i + REACH], q_t[:, blocks(i, i + ONE)])
        for a, h in enumerate(heads):
            for i in range(NBLK):
                cols = blocks(i, i + ONE)
                s = jnp.where(in_bounds(bounds, cols, LANE * i, REACH), r.s_s[a, i], NEG)
                m = jnp.max(s, axis=ZERO, keepdims=True)
                e = jnp.exp(s - m)
                l = jnp.sum(e, axis=ZERO, keepdims=True)
                r.p_s[a, i] = (e * (ONE / l)).astype(BF)
                r.lse[HPS * step + h, :, cols] = m + jnp.log(l)
        for a, h in enumerate(heads):
            for i in range(NBLK):
                out = mm(v_all[a][:, LANE * i:LANE * i + REACH], r.p_s[a, i]).astype(BF)
                r.o[HPS * step + h, :, blocks(i, i + ONE)] = out
    every_head(some, AHEAD_FWD)


def attn1_fwd_stage(cu, qkv, left, right):
    tile, edge = (AHEAD_FWD, NBLK, REACH, LANE), heads_of(LANE, ZERO)
    return Stage(
        attn1_fwd_body, HSTEPS,
        [('cu', cu, CU_SPEC), ('q', qkv, own_head(ZERO)), ('k', qkv, own_head(ONE)), ('v', qkv, own_head(TWO)),
         ('left', left, edge), ('right', right, edge)],
        [('lse', STAT, STAT_BLOCK)],
        [('o', pltpu.VMEM((NHEAD, HEAD, TOK), BF)), ('s_s', pltpu.VMEM(tile, F32)), ('p_s', pltpu.VMEM(tile, BF))])


def attn1_bwd_body(r, step):
    bounds = near_bounds(r.cu, WIN, EXT)

    def window(e):
        first, last = max(LANE * e - WIN, ZERO), min(LANE * e + LANE + WIN, EXT)
        return first, last - first

    def parts(h):
        q_t = joined(r.ql, r.q, r.qr, h) * SCALE
        return q_t, joined(r.dl, r.d, r.dr, h), joined(r.left, r.k, r.right, h, LOW, LOW)

    def some(heads):
        for a, h in enumerate(heads):
            q_t, do_t, k_t = parts(h)
            k_rows, v_rows = k_t.T, joined(r.left, r.v, r.right, h, HIGH, HIGH).T
            for e in range(XBLK):
                first, n = window(e)
                cols = blocks(e, e + ONE)
                r.s_s[a, e, :n] = mm(k_rows[first:first + n], q_t[:, cols])
                r.d_s[a, e, :n] = mm(v_rows[first:first + n], do_t[:, cols])
        for a, h in enumerate(heads):
            lse, delta = joined(r.ll, r.lse, r.lr, h), joined(r.el, r.delta, r.er, h)
            for e in range(XBLK):
                first, n = window(e)
                cols = blocks(e, e + ONE)
                ok = in_bounds(bounds, cols, first, n)
                p = jnp.exp(jnp.where(ok, r.s_s[a, e, :n] - lse[:, cols], NEG))
                r.p_s[a, first:first + n, cols] = p.astype(BF)
                r.t_s[a, first:first + n, cols] = (p * (r.d_s[a, e, :n] - delta[:, cols])).astype(BF)
        for a, h in enumerate(heads):
            q_t, do_t, k_t = parts(h)
            got = [[], [], []]
            for b in range(XBLK):
                here, wide = blocks(b, b + ONE), blocks(max(b - ONE, ZERO), min(b + TWO, XBLK))
                got[ZERO].append(mm(k_t[:, wide], r.t_s[a, wide, here]) * SCALE)
                got[ONE].append(mm_nt(q_t[:, wide], r.t_s[a, here, wide]))
                got[TWO].append(mm_nt(do_t[:, wide], r.p_s[a, here, wide]))
            for n in range(THREE):
                own = jnp.concatenate([g.astype(BF) for g in got[n]], axis=ONE)[:, WIN:WIN + TOK]
                r.out[n, HPS * step + h] = own

    @pl.when(step == ZERO)
    def _():
        r.p_s[...] = jnp.zeros(r.p_s.shape, BF)
        r.t_s[...] = jnp.zeros(r.t_s.shape, BF)

    every_head(some, AHEAD_BWD)


def attn1_bwd_stage(cu, qkv, do_t, lse, delta, edges, far):
    edge, row = heads_of(LANE, ZERO), row_of(LANE)
    blk = (AHEAD_BWD, XBLK, REACH, LANE)
    square = pltpu.VMEM((AHEAD_BWD, EXT, EXT), BF)
    names = ('left', 'right', 'ql', 'qr', 'dl', 'dr')
    return Stage(
        attn1_bwd_body, HSTEPS,
        [('cu', cu, CU_SPEC), ('q', qkv, own_head(ZERO)), ('k', qkv, own_head(ONE)), ('v', qkv, own_head(TWO)), ('d', do_t, own_head(ZERO)),
         ('lse', lse, row_of(TOK)), ('delta', delta, row_of(TOK))]
        + [(n, arr, edge) for n, arr in zip(names, list(edges) + far[:FOUR])]
        + [(n, arr, row) for n, arr in zip(('ll', 'lr', 'el', 'er'), far[FOUR:])],
        [], [('out', pltpu.VMEM((THREE, NHEAD, HEAD, TOK), BF)), ('s_s', pltpu.VMEM(blk, F32)), ('d_s', pltpu.VMEM(blk, F32)),
             ('p_s', square), ('t_s', square)])


ROWBLK = [slice(r, r + RB) for r in range(ZERO, TOK, RB)]
HALFT = NFT // TWO
SQRT_HALF = math.sqrt(SCALE * FOUR)
PDF_SCALE = SQRT_HALF / math.sqrt(math.pi)


def normal_cdf(a):
    return SQRT_HALF * SQRT_HALF * (ONE + lax.erf(a * SQRT_HALF))


def half_rows(ref, which):
    n = ref.shape[ZERO] // TWO
    return ref.at[pl.ds(pl.multiple_of(which * n, n), n)]


def col_tile(ref, n):
    return ref.at[:, pl.ds(pl.multiple_of(n * FT, FT), FT)]


def mlp_copies(r, fwd, bwd):
    sw = Swaps(r.ssem, r.rsem, r.lsem)
    both = fwd and bwd
    c = Refs(dict(sw=sw, start=[], first=[], second=[]))
    if fwd:
        c.start += [sw.remote(r.h, r.h_r), sw.remote(half_rows(r.of, sw.other), r.of_r), sw.local(half_rows(r.of, sw.core), r.of_m)]
        there = [sw.remote(r.m_s.at[HALFT * sw.other + n], r.m_r.at[n] if both else col_tile(r.m_r, n)) for n in range(HALFT)]
        here = [None] * HALFT
        if not both:
            c.start += [sw.local(r.h, r.h_m), sw.local(r.x1, r.x1_m)]
            here = [sw.local(r.m_s.at[HALFT * sw.core + n], col_tile(r.m_m, n)) for n in range(HALFT)]
        c.m_out = list(zip(there, here))
    if bwd:
        c.start.append(sw.remote(r.dy, r.dy_r))
        c.dmid_out = sw.remote(r.dmid, r.dmid_r)
        c.du_out = [[sw.remote(r.du_s.at[n, sw.other], r.du_r.at[n] if both else col_tile(r.du_r, n))] for n in range(NFT)]
        if not both:
            for n in range(NFT):
                c.du_out[n].append(sw.local(r.du_s.at[n, sw.core], col_tile(r.du_m, n)))
            c.do_out = sw.to_all(lambda dev: r.do_s.at[dev], lambda dev: r.d_o.at[dev])
    if both:
        c.first = sw.early([c.start[ZERO], c.start[-ONE]] + there)
        c.second = sw.early([cp for part in c.du_out for cp in part])
    return c


def mlp_body(r, step, layer, fwd, bwd):
    cps = mlp_copies(r, fwd, bwd)
    sw, start, whole_group = cps.sw, cps.start, not (fwd and bwd)
    if fwd:
        m_out = cps.m_out
    if bwd:
        dmid_out, du_out = cps.dmid_out, cps.du_out

    @pl.when(step == ZERO)
    def _():
        if fwd:
            for n in range(NHEAD):
                r.of[HEAD * n:HEAD * n + HEAD, :] = (r.o[n % FOUR, n // FOUR] if whole_group else r.o[n])
            x1 = (r.x[...].astype(F32) + mm_tn(r.of[...], r.wp[...])).astype(BF)
            r.x1[...] = x1
            r.h[...] = norm_rows(x1, r.g[layer:layer + ONE])
            r.acc[...] = x1.astype(F32)
        if bwd:
            r.dacc[...] = jnp.zeros(r.dacc.shape, F32)
        r.arrive()
        start_all(start)

    for rows in ROWBLK:
        if fwd:
            ua = mm(r.h[rows], r.wa[...]).astype(BF)
            ub = mm(r.h[rows], r.wb[...]).astype(BF)
            if not bwd:
                r.u[ZERO, rows] = ua
                r.u[ONE, rows] = ub
        else:
            ua, ub = r.u[ZERO, rows], r.u[ONE, rows]
        a, b = ua.astype(F32), ub.astype(F32)
        cdf = normal_cdf(a)
        gate = a * cdf
        if fwd:
            m = (gate * b).astype(BF)
            r.m_s[step, rows] = m
            r.acc[rows] += mm(m, r.wo[...])
        if bwd:
            dm = mm_nt(r.dy[rows], r.wo[...]).astype(BF).astype(F32)
            pdf = jnp.exp(a * a * (SCALE * FOUR - ONE)) * PDF_SCALE
            db = (dm * gate).astype(BF)
            da = (dm * b * (cdf + a * pdf)).astype(BF)
            r.du_s[step, ZERO, rows] = da
            r.du_s[step, ONE, rows] = db
            r.dacc[rows] += mm_nt(da, r.wa[...]) + mm_nt(db, r.wb[...])

    for n in range(NFT):
        @pl.when(step == n)
        def _(n=n):
            if fwd:
                there, here = m_out[n % HALFT]

                if here:
                    @pl.when(sw.core == n // HALFT)
                    def _():
                        here.start()

                @pl.when(sw.other == n // HALFT)
                def _():
                    there.start()
            if bwd:
                for cp in du_out[n]:
                    cp.start()

    @pl.when(step == NFT - ONE)
    def _():
        if fwd:
            r.y[...] = r.acc[...].astype(BF)
        if bwd:
            d_ln, gg = norm_rows_grad(r.x1[...], r.g[layer:layer + ONE], r.dacc[...].astype(BF))
            r.gg[...] = gg
            d_mid = add_bf(r.dy[...], d_ln)
            r.dmid[...] = d_mid
            dmid_out.start()
            d_att = mm_nt(r.wp[...], d_mid).astype(BF)
            for n in range(NHEAD):
                rows = slice(HEAD * n, HEAD * n + HEAD)
                blk = d_att[rows]
                if whole_group:
                    r.do_s[n % FOUR, n // FOUR] = blk
                else:
                    r.d_o[n] = blk
                    r.delta[n] = jnp.sum(blk.astype(F32) * r.of[rows].astype(F32), axis=ZERO, keepdims=True)
            if whole_group:
                start_all(cps.do_out)


def mlp_stage(layer, fwd, bwd, w_proj, gain, w_in, w_out, links=None, **arrays):
    u_spec = spec((TWO, TOK, FT), ZERO, ZERO, step_of)
    half_o = sds((DM // TWO, TOK), BF)
    half_m, half_u = sds((TOK, FF // TWO), BF), sds((TOK, FF), BF)
    heads = (NHEAD, HEAD, TOK)
    sums = pltpu.VMEM(ALLTOK, F32)
    links = links or {}
    ins = [('wp', w_proj, spec((None, DM, DM), layer, ZERO, ZERO)), ('g', gain, GAINS),
           ('wa', w_in, weight_cols(layer, FT)), ('wb', w_in, weight_cols(layer, FT, NFT)),
           ('wo', w_out, spec((None, FT, DM), layer, step_of, ZERO))]
    kinds = dict(x=TOK_SPEC, dy=TOK_SPEC, x1=TOK_SPEC, u=u_spec)
    ins += [(n, arr, kinds[n]) for n, arr in arrays.items()]
    outs, scratch, both = [], [], fwd and bwd
    own_tiles, far_tiles = pltpu.VMEM((HALFT, TOK, FT), BF), pltpu.VMEM((NFT, TOK, FT), BF)
    if fwd:
        outs += [('y', TOKS, TOK_SPEC), ('of_m', half_o, ANY), ('of_r', half_o, ANY)]
        scratch += [('acc', sums), ('of', pltpu.VMEM((DM, TOK), BF)), ('m_s', pltpu.VMEM((NFT, TOK, FT), BF)), ('h', TOK_VMEM),
                    ('x1', TOK_VMEM)]
    if fwd and not bwd:
        outs += [('h_m', TOKS, ANY), ('h_r', TOKS, ANY), ('m_m', half_m, ANY), ('m_r', half_m, ANY)]
        outs += [('x1_m', TOKS, ANY), ('u', sds((TWO, TOK, FF), BF), u_spec)]
    if bwd:
        shape = heads if fwd else BY_OWNER
        outs += [('dmid', TOKS, TOK_SPEC), ('gg', sds((ONE, DM), F32), spec((ONE, DM))), ('d_o', sds(shape, BF), spec(shape) if fwd else ANY),
                 ('dmid_r', TOKS, ANY)]
        scratch += [('dacc', sums), ('du_s', pltpu.VMEM((NFT, TWO, TOK, FT), BF))]
    if bwd and not fwd:
        outs += [('dy_r', TOKS, ANY), ('du_m', half_u, ANY), ('du_r', half_u, ANY)]
    if both:
        outs += [('delta', STAT, STAT_BLOCK)]
        scratch += [('h_r', TOK_VMEM), ('dy_r', TOK_VMEM), ('m_r', own_tiles), ('du_r', far_tiles)]
    if not fwd:
        scratch += [('do_s', pltpu.VMEM(BY_OWNER, BF))]
    return Stage(functools.partial(mlp_body, layer=layer, fwd=fwd, bwd=bwd), NFT, ins, outs, scratch + named_sems(FOUR * NFT),
                 functools.partial(mlp_copies, fwd=fwd, bwd=bwd), links)


def side_grad_copies(r):
    sw = Swaps(r.ssem, r.rsem, r.lsem)
    for n, src in enumerate((r.q_all.at[:NHEAD], r.d_o, r.lse, r.delta)):
        sw.to_sides(src.at[:, :, :LANE], src.at[:, :, TOK - LANE:], getattr(r, FAR[TWO * n]), getattr(r, FAR[TWO * n + ONE]))
    return Refs(dict(sw=sw))


def side_grad_body(r, step):
    sw = side_grad_copies(r).sw
    mlp = mlp_copies(Refs(dict(r.__dict__, ssem=r.mlp_ssem, rsem=r.mlp_rsem, lsem=r.mlp_lsem)), True, True)

    @pl.when(step == ZERO)
    def _():
        start_all(sw.waits)
        wait_all(mlp.first)

    @pl.when(step < HALFT)
    def _():
        r.out[...] = mm_tn(r.m_s[HALFT * sw.core + step], r.dy[...]) + mm_tn(r.m_r[step], r.dy_r[...])

    @pl.when(step == HALFT)
    def _():
        wait_all(mlp.second)
        r.h_t[ZERO] = r.h[...].T
        r.h_t[ONE] = r.h_r[...].T

    @pl.when(step >= HALFT)
    def _():
        n = step - HALFT
        r.out[...] = mm(r.h_t[ZERO], r.du_s[n, sw.core]) + mm(r.h_t[ONE], r.du_r[n])


FAR = ('ql', 'qr', 'dl', 'dr', 'll', 'lr', 'el', 'er')


def side_grad_stage(qkv):
    kinds = [(NHEAD, HEAD, LANE, BF)] * FOUR + [(NHEAD, ONE, LANE, F32)] * FOUR
    far = [(n, sds(shape, dtype), ANY) for n, (*shape, dtype) in zip(FAR, kinds)]
    names = ('m_s', 'du_s', 'h', 'h_r', 'dy', 'dy_r', 'm_r', 'du_r', 'd_o', 'delta', 'of', 'of_r', 'of_m', 'dmid', 'dmid_r')
    links = {n: (ONE, n) for n in names}
    links.update({'mlp_' + n: (ONE, n) for n in ('ssem', 'rsem', 'lsem')}, lse=(ZERO, 'lse'))
    return Stage(side_grad_body, HALFT + NFT, [('q_all', qkv, ANY)],
                 [('out', sds((MLP_ROWS, DM), F32), spec(ALLDM, step_of, ZERO))] + far,
                 [('h_t', pltpu.VMEM((TWO, DM, TOK), BF))] + named_sems(8), side_grad_copies, links)


NAMED = ('ha', 'hb', 'oa', 'ob', 'dma', 'dmb')


def third(ref, n):
    return ref.at[PROJ * n:PROJ * n + PROJ]


def qkv_bwd_copies(r, grads):
    sw = Swaps(r.ssem, r.rsem, r.lsem)
    c = Refs(dict(sw=sw, parts=[[sw.remote(r.dt_s.at[sw.other, n], third(r.dt_r, n))] for n in range(THREE)]))
    if grads:
        c.loads = sw.early([sw.local(getattr(r, n + '_in'), getattr(r, n)) for n in NAMED])
        for part in c.parts:
            sw.early(part)
    else:
        for n in range(THREE):
            c.parts[n].append(sw.local(r.dt_s.at[sw.core, n], third(r.dt_m, n)))
    return c


def qkv_bwd_body(r, step, layer, grads):
    cps = qkv_bwd_copies(r, grads)
    sw, copies = cps.sw, cps.parts

    @pl.when(step == ZERO)
    def _():
        r.acc[...] = jnp.zeros(r.acc.shape, F32)
        if grads:
            start_all(cps.loads)

    for p in range(THREE):
        @pl.when(step == p)
        def _(p=p):
            cos, sin = r.cos[...], r.sin[...]
            for chunk in CHUNKS:
                for head in range(FOUR):
                    blk = r.d[head, ZERO, chunk] if grads else r.d[p, FOUR * chunk + head]
                    a, b = blk[:HALF], blk[HALF:]
                    if p < TWO:
                        a, b = a.astype(F32), b.astype(F32)
                        a, b = (a * cos + b * sin).astype(BF), (b * cos - a * sin).astype(BF)
                    at, full = LANE * chunk + HEAD * (head % TWO), RB * chunk + HEAD * head
                    for n, val in ((ZERO, a), (HALF, b)):
                        r.dt_s[head // TWO, p, at + n:at + n + HALF] = val
                        r.dt_all[full + n:full + n + HALF] = val
            if p == ZERO:
                r.arrive()
            start_all(copies[p])
            r.acc[...] += mm(r.w[...], r.dt_all[...])

    @pl.when(step == TWO)
    def _():
        d_ln, gg = norm_rows_grad(r.x[...], r.g[layer:layer + ONE], r.acc[...].T.astype(BF))
        r.gg[...] = gg
        r.dx[...] = add_bf(r.dmid[...], d_ln)

    if grads:
        @pl.when(step == THREE)
        def _():
            wait_all(cps.loads)
            for part in copies:
                wait_all(part)
            r.out[...] = mm(r.oa[...], r.dma[...]) + mm(r.ob[...], r.dmb[...])

        for p in range(THREE):
            @pl.when(step == p + FOUR)
            def _(p=p):
                r.out[...] = mm(r.dt_s[sw.core, p], r.ha[...]) + mm(third(r.dt_r, p)[...], r.hb[...])


def qkv_bwd_stage(layer, tables, w_qkv, x, gain, d_mid, d=None, link=None, grads=None, pairs=()):
    part = lambda s: jnp.minimum(s, TWO)
    ins = [('cos', tables[ZERO], TABLE), ('sin', tables[ONE], TABLE), ('w', w_qkv, spec((None, DM, DM), layer, ZERO, part)),
           ('x', x, TOK_SPEC), ('g', gain, GAINS), ('dmid', d_mid, TOK_SPEC)]
    outs = [('dx', TOKS, TOK_SPEC), ('gg', sds((ONE, DM), F32), spec((ONE, DM)))]
    feats = (THREE * PROJ, TOK)
    scratch = [('acc', pltpu.VMEM((DM, TOK), F32)), ('dt_s', pltpu.VMEM((TWO, THREE, PROJ, TOK), BF)), ('dt_all', pltpu.VMEM((DM, TOK), BF))]
    steps, alias = THREE, ()
    if grads is None:
        outs += [('dt_m', sds(feats, BF), ANY), ('dt_r', sds(feats, BF), ANY)]
    else:
        first = (ATT_ROWS + MLP_ROWS) // PROJ
        ins += [('d', d, spec((FOUR, ONE, THREE, HEAD, TOK), ZERO, part, ZERO, ZERO, ZERO)), ('grads', grads, ANY)]
        ins += [(n + '_in', arr, ANY) for n, arr in zip(NAMED, pairs)]
        outs += [('out', sds(grads.shape, F32), spec((PROJ, DM), lambda s: first + jnp.maximum(s - THREE, ZERO), ZERO))]
        scratch += [('dt_r', pltpu.VMEM(feats, BF))] + [(n, pltpu.VMEM(arr.shape, BF)) for n, arr in zip(NAMED, pairs)]
        steps, alias = steps + FOUR, (('grads', 'out'),)
    flag = grads is not None
    return Stage(functools.partial(qkv_bwd_body, layer=layer, grads=flag), steps, ins, outs, scratch + named_sems(TWELVE),
                 functools.partial(qkv_bwd_copies, grads=flag), {} if link is None else {'d': link}, alias)


NDOWN = DOWN // DM


def grad_call(body, grads, steps, in_specs, args, rows, first_row, total, scratch=()):
    shared = [] if grads is None else [grads]
    first = first_row // rows
    return call(
        body, (steps,), [ANY] * len(shared) + in_specs,
        spec((rows, DM), lambda s: first + s, ZERO), sds((total, DM), F32), scratch=scratch,
        flops=FOUR * steps * rows * TOK * DM, nbytes=20 * MIB, name=body.__name__,
        alias={ZERO: ZERO} if shared else None,
    )(*shared, *args)


GRAD_INS = 8


def grad_mlp_body(*refs):
    ma, mb, dya, dyb, ha, hb, dua, dub, out_ref, h_t = refs[-GRAD_INS - TWO:]
    step = pl.program_id(ZERO)

    @pl.when(step < NDOWN)
    def _():
        out_ref[...] = mm_tn(ma[...], dya[...]) + mm_tn(mb[...], dyb[...])

    @pl.when(step == NDOWN)
    def _():
        h_t[ZERO] = ha[...].T
        h_t[ONE] = hb[...].T

    @pl.when(step >= NDOWN)
    def _():
        out_ref[...] = mm(h_t[ZERO], dua[...]) + mm(h_t[ONE], dub[...])


def grad_mlp(grads, m, m_r, dy, dy_r, h, h_r, du, du_r, first_row, total):
    toks = spec(ALLTOK)
    m_col = spec(ALLTOK, ZERO, lambda s: jnp.minimum(s, NDOWN - ONE))
    du_col = spec(ALLTOK, ZERO, lambda s: jnp.maximum(s - NDOWN, ZERO))
    return grad_call(grad_mlp_body, grads, NDOWN + UP // DM, [m_col, m_col, toks, toks, toks, toks, du_col, du_col],
                     (m, m_r, dy, dy_r, h, h_r, du, du_r), DM, first_row, total, scratch=[pltpu.VMEM((TWO, DM, TOK), BF)])


def grad_att_body(*refs):
    oa, ob, dma, dmb, ta, tb, ha, hb, out_ref = refs[-GRAD_INS - ONE:]
    step = pl.program_id(ZERO)

    @pl.when(step == ZERO)
    def _():
        out_ref[...] = mm(oa[...], dma[...]) + mm(ob[...], dmb[...])

    @pl.when(step > ZERO)
    def _():
        out_ref[...] = mm(ta[...], ha[...]) + mm(tb[...], hb[...])


def grad_att(grads, of, of_r, dmid, dmid_r, dt, dt_r, h, h_r, first_row):
    toks = spec(ALLTOK)
    blk = (PROJ, TOK)
    dt_row = spec(blk, lambda s: jnp.maximum(s - ONE, ZERO), ZERO)
    return grad_call(grad_att_body, grads, ONE + QKV // PROJ, [spec(blk), spec(blk), toks, toks, dt_row, dt_row, toks, toks],
                     (of, of_r, dmid, dmid_r, dt, dt_r, h, h_r), PROJ, first_row, RING_ROWS)


NB, NS = 5, 6
CH = RING_ROWS // (NB * FOUR)
SB, LF = CH // FOUR, CH // 16
RS = 9
LAST = RS + RS
ADD_ROWS = 96


def ring_body(g_ref, *refs):
    gains, refs = refs[:FOUR], refs[FOUR:]
    (f_ref, lnout_ref, bufa, bufb, bufc, gath, stage, lnbuf, ssem, rsem, psem, qsem, csem, stsem, lns, lnr) = refs
    core, partner = core_and_partner()
    zy = lax.axis_index('zy')
    pos = (lax.axis_index('sp'), lax.rem(zy, FOUR), zy // FOUR)
    streams = [(c, sg) for c in range(THREE) for sg in (ONE, -ONE)]
    bufs, sizes = (bufa, bufb, bufc), (CH, SB, LF)
    peers = range(ONE, FOUR)

    def mod4(v):
        return lax.rem(v + 8, FOUR)

    def at(axis, val):
        if axis == ZERO:
            return {'sp': val}
        yz = (val, pos[TWO]) if axis == ONE else (pos[ONE], val)
        return {'zy': yz[ONE] * FOUR + yz[ZERO]}

    def shifted(axis, d):
        return at(axis, mod4(pos[axis] + d))

    def axis_of(s, ph):
        return (streams[s][ZERO] + ph) % THREE

    def idx(s, ph, t):
        return mod4(pos[axis_of(s, ph)] - streams[s][ONE] * t)

    def own(s, ph):
        return idx(s, ph, -ONE)

    def base(b):
        return b * (FOUR * CH)

    bar = pltpu.get_barrier_semaphore()
    for ax in range(THREE):
        for d in peers:
            pl.semaphore_signal(bar, inc=ONE, device_id=shifted(ax, d), device_id_type=MESH)
    pl.semaphore_signal(bar, inc=ONE, device_id=partner, device_id_type=MESH)
    pl.semaphore_wait(bar, 10)

    def rows(ref, start, n):
        return ref.at[pl.ds(pl.multiple_of(start, LF), n)]

    def grows(s, start, n):
        return g_ref.at[pl.ds(pl.multiple_of(start, LF), n), LANE * s:LANE * s + LANE]

    def frows(s, start, n):
        return f_ref.at[core, pl.ds(pl.multiple_of(start, LF), n), LANE * s:LANE * s + LANE]

    def same_bytes(b, k):
        if k < RS:
            return bufs[k // THREE].at[b, k % THREE]
        n = sizes[TWO - (k - RS) // THREE]
        return gath.at[b] if n == CH else gath.at[b, :, pl.ds(ZERO, n)]

    def wait_for(ref, sem):
        pltpu.make_async_copy(ref, ref, sem).wait()

    def send(b, s, k):
        ph = k // THREE if k < RS else TWO - (k - RS) // THREE
        t = k % THREE
        n = sizes[ph]
        if k < RS:
            dst = bufs[ph].at[b, t, s]
            if t:
                src = bufs[ph].at[b, t - ONE, s]
            elif ph:
                src = rows(bufs[ph - ONE].at[b, TWO, s], idx(s, ph, ZERO) * n, n)
            else:
                src = grows(s, base(b) + idx(s, ZERO, ZERO) * n, n)
        elif ph:
            off = own(s, ONE) * SB if ph == TWO else ZERO
            src = dst = rows(gath.at[b, s], off + idx(s, ph, t - ONE) * n, n)
        else:
            dst = frows(s, base(b) + idx(s, ZERO, t - ONE) * n, n)
            src = dst if t else gath.at[b, s]
        pltpu.make_async_remote_copy(src_ref=src, dst_ref=dst, send_sem=ssem.at[b, k], recv_sem=rsem.at[b, k],
                                     device_id=shifted(axis_of(s, ph), streams[s][ONE]), device_id_type=MESH).start()

    def stage_load(n):
        t, b, slot = n // NB, lax.rem(n, NB), lax.rem(n, TWO)
        for s in range(NS):
            pltpu.make_async_copy(grows(s, base(b) + idx(s, ZERO, t + ONE) * CH, CH), stage.at[slot, s],
                                  stsem.at[slot]).start()

    def ln_copy(ph, d):
        return pltpu.make_async_remote_copy(
            src_ref=lnbuf.at[ph, THREE], dst_ref=lnbuf.at[ph, d - ONE], send_sem=lns.at[ph, d - ONE],
            recv_sem=lnr.at[ph, d - ONE], device_id=shifted(ph, d) if ph < THREE else partner, device_id_type=MESH)

    def ln_sum(ph):
        vals = [lnbuf[ph, THREE]] + [lnbuf[ph, d - ONE] for d in peers]
        total = jnp.zeros_like(vals[ZERO])
        for p in range(FOUR):
            term = vals[ZERO]
            for d in peers:
                term = jnp.where(mod4(pos[ph] - d) == p, vals[d], term)
            total = total + term
        return total

    def batches(fn, start=ZERO):
        def body(b, c):
            fn(b)
            return c
        lax.fori_loop(start, NB, body, ZERO)

    def first(b):
        for s in range(NS):
            send(b, s, ZERO)

    lnbuf[ZERO, THREE] = jnp.zeros(lnout_ref.shape, F32)
    for n, gain in enumerate(gains):
        lnbuf[ZERO, THREE, n:n + ONE] = gain[...]
    first(ZERO)
    stage_load(jnp.int32(ZERO))
    for d in peers:
        ln_copy(ZERO, d).start()
    batches(first, ONE)

    for k in range(RS):
        ph, t = k // THREE, k % THREE
        buf, size = bufs[ph], sizes[ph]

        def step(b, k=k, ph=ph, t=t, buf=buf, size=size):
            n = k * NB + b
            slot = lax.rem(n, TWO)
            if not ph:
                @pl.when(n < THREE * NB - ONE)
                def _():
                    stage_load(n + ONE)
                wait_for(stage.at[slot], stsem.at[slot])
            wait_for(same_bytes(b, k), rsem.at[b, k])
            for s in range(NS):
                if ph:
                    off = pl.multiple_of(idx(s, ph, t + ONE) * size, LF)
                    buf[b, t, s] += bufs[ph - ONE][b, TWO, s, pl.ds(off, size)]
                else:
                    @pl.loop(ZERO, CH, step=ADD_ROWS)
                    def _(r):
                        at_r = pl.ds(pl.multiple_of(r, ADD_ROWS), ADD_ROWS)
                        buf[b, t, s, at_r] += stage[slot, s, at_r]
                if k == RS - ONE:
                    off = pl.multiple_of(own(s, ONE) * SB + own(s, TWO) * LF, LF)
                    gath[b, s, pl.ds(off, LF)] = bufc[b, TWO, s]
                send(b, s, k + ONE)

        batches(step)
        if k < SIX and k % TWO == ZERO:
            lp = k // TWO
            for d in peers:
                ln_copy(lp, d).wait()
            lnbuf[lp + ONE, THREE] = ln_sum(lp)
            for d in peers if lp < TWO else (ONE,):
                ln_copy(lp + ONE, d).start()

    def hand_over(b, s, j, src, start):
        pltpu.make_async_remote_copy(src_ref=src, dst_ref=frows(s, start, CH), send_sem=psem.at[b, j], recv_sem=qsem.at[b, j],
                                     device_id=partner, device_id_type=MESH).start()

    for k in range(RS, LAST):
        def step(b, k=k):
            wait_for(same_bytes(b, k), rsem.at[b, k])
            piece = k - (LAST - FOUR)
            for s in range(NS):
                if k < LAST - ONE:
                    send(b, s, k + ONE)
                if piece >= ZERO:
                    start = base(b) + idx(s, ZERO, piece - ONE) * CH
                    if piece:
                        hand_over(b, s, piece, frows(s, start, CH), start)
                    else:
                        pltpu.make_async_copy(gath.at[b, s], frows(s, start, CH), csem.at[b]).start()
                        hand_over(b, s, piece, gath.at[b, s], start)
        batches(step)

    ln_copy(THREE, ONE).wait()
    lnout_ref[...] = lnbuf[THREE, THREE] + lnbuf[THREE, ZERO]

    def finish(b):
        for k in range(LAST):
            wait_for(same_bytes(b, k), ssem.at[b, k])
        for j in range(FOUR):
            wait_for(gath.at[b], psem.at[b, j])
            wait_for(gath.at[b], qsem.at[b, j])
        wait_for(gath.at[b], csem.at[b])
    batches(finish)


def ring_all_reduce(g, gains, cid):
    vmem = pl.BlockSpec(memory_space=pltpu.VMEM)
    ln = sds((8, DM), F32)
    return pl.pallas_call(
        ring_body,
        in_specs=[ANY] + [vmem] * FOUR,
        out_specs=[ANY, vmem],
        out_shape=[sds((TWO, RING_ROWS, DM), F32), ln],
        scratch_shapes=[
            pltpu.VMEM((NB, THREE, NS, CH, LANE), F32), pltpu.VMEM((NB, THREE, NS, SB, LANE), F32),
            pltpu.VMEM((NB, THREE, NS, LF, LANE), F32), pltpu.VMEM((NB, NS, CH, LANE), F32),
            pltpu.VMEM((TWO, NS, CH, LANE), F32),
            pltpu.VMEM((FOUR, FOUR) + ln.shape, F32),
            DMA((NB, LAST)), DMA((NB, LAST)), DMA((NB, FOUR)), DMA((NB, FOUR)), DMA((NB,)), DMA((TWO,)),
            DMA((FOUR, THREE)), DMA((FOUR, THREE)),
        ],
        compiler_params=pltpu.CompilerParams(collective_id=cid, has_side_effects=True, vmem_limit_bytes=60 * MIB),
        cost_estimate=pl.CostEstimate(flops=MIB * MIB // FOUR, bytes_accessed=200 * MIB, transcendentals=ZERO),
        name="ring_all_reduce",
    )(g, *gains)


SLOTS, LAG = 8, 4
NTURN = TWO * THREE
OUT_SHAPE, IN_SHAPE = (TWO, FF, DM), (TWO, DM, TWO * FF)


def stream(pieces, buf, turned, isem, osem):
    def loads(i):
        slot, srcs = i % SLOTS, pieces[i][ZERO]
        n = srcs[ZERO].shape[ZERO]
        return [pltpu.make_async_copy(src, buf.at[slot, k * n:k * n + n], isem.at[slot, k]) for k, src in enumerate(srcs)]

    def store(i):
        _, dst, turn = pieces[i]
        src = buf.at[i % SLOTS, :dst.shape[ZERO]] if turn is None else turned.at[turn]
        return pltpu.make_async_copy(src, dst, osem.at[i % SLOTS])

    total = len(pieces)
    for i in range(total + LAG):
        if i < total:
            if i >= SLOTS:
                store(i - SLOTS).wait()
            for cp in loads(i):
                cp.start()
        k = i - LAG
        if k >= ZERO:
            for cp in loads(k):
                cp.wait()
            turn = pieces[k][TWO]
            if turn is not None:
                for n in CHUNKS:
                    rows, col = LANE * n, RB * n
                    turned[turn, :, col:col + LANE] = buf[k % SLOTS, rows:rows + LANE].T
                    turned[turn, :, col + LANE:col + RB] = buf[k % SLOTS, PROJ + rows:PROJ + rows + LANE].T
            store(k).start()
    for i in range(max(total - SLOTS, ZERO), total):
        store(i).wait()


def unpack_ring_body(f, g_qkv, g_proj, g_in, g_out, *scratch):
    def block(c, row, n=DM):
        return f.at[c, row:row + n]

    pieces = []
    for c in range(TWO):
        for n in range(NDOWN):
            pieces.append(([block(c, ATT_ROWS + DM * n)], g_out.at[ZERO, DOWN * c + DM * n:DOWN * c + DM * n + DM], None))
        for n in range(FOUR):
            col = UP * c + DM * n
            pieces.append(([block(c, ATT_ROWS + DOWN + DM * n)], g_in.at[ZERO, :, col:col + DM], None))
    for l in range(TWO):
        first = (ONE - l) * (ATT_ROWS + MLP_ROWS)
        for n in range(THREE):
            row = first + PROJ * (n + ONE)
            pieces.append(([block(c, row, PROJ) for c in range(TWO)], g_qkv.at[l, :, DM * n:DM * n + DM], THREE * l + n))
        for c in range(TWO):
            pieces.append(([block(c, first, PROJ)], g_proj.at[l, PROJ * c:PROJ * c + PROJ], None))
    stream(pieces, *scratch)


def unpack_mlp_body(own, other, in_0, out_0, g_in, g_out, *scratch):
    core = lax.axis_index('core')
    pieces = []
    for src, side in ((own, core), (other, ONE - core)):
        for n in range(NDOWN):
            row = pl.multiple_of(DOWN * side + DM * n, DM)
            pieces.append(([src.at[DM * n:DM * n + DM]], g_out.at[ONE, pl.ds(row, DM)], None))
        for n in range(FOUR):
            col = pl.multiple_of(UP * side + DM * n, DM)
            pieces.append(([src.at[DOWN + DM * n:DOWN + DM * n + DM]], g_in.at[ONE, :, pl.ds(col, DM)], None))
    stream(pieces, *scratch)


def unpack_call(body, args, outs, alias, name):
    return pl.pallas_call(
        body, in_specs=[ANY] * len(args), out_specs=[ANY] * len(outs), out_shape=[sds(shape, F32) for shape in outs],
        scratch_shapes=[pltpu.VMEM((SLOTS, DM, DM), F32), pltpu.VMEM((NTURN, DM, DM), F32), DMA((SLOTS, TWO)), DMA((SLOTS,))],
        input_output_aliases=alias,
        compiler_params=pltpu.CompilerParams(vmem_limit_bytes=60 * MIB),
        cost_estimate=pl.CostEstimate(flops=MIB * MIB // RB, bytes_accessed=75 * MIB, transcendentals=ZERO), name=name,
    )(*args)


def rope_tables(pos, base):
    inv_freq = base ** (jnp.arange(HALF).astype(F32) * (-TWO / HEAD))
    angles = inv_freq[:, None] * pos.astype(F32)[None, :]
    return jnp.cos(angles), jnp.sin(angles)


def solution(mesh):
    n_sp = mesh.shape['sp']
    by_core = mesh.devices.reshape(n_sp, mesh.shape['dp'] // TWO, TWO)
    mesh = Mesh(by_core, ('sp', 'zy', 'core'))
    dp_axes = ('zy', 'core')
    row_axes = dp_axes + ('sp',)
    token_spec = P(row_axes, None)
    swap_cores = [(ZERO, ONE), (ONE, ZERO)]
    cids = list(range(RS))

    def exchange(arr):
        return lax.all_to_all(arr, 'sp', ZERO, ZERO, tiled=True)

    def device_step(x_loc, cu_loc, pos_loc, w_qkv, w_proj, w_in, w_out, ln_attn, ln_mlp, d_out):
        tab0, tab1 = [rope_tables(pos_loc, base) for base in BASES]
        mlp_args, w_mlp = (w_proj, ln_mlp), (w_in, w_out)

        q0, f0, q1 = run("layer0_qkv1", cids[ONE], row_peers, group_fwd_stage(cu_loc, ln_attn, w_qkv, tab0, x_loc),
                         mlp_stage(ZERO, True, False, *mlp_args, *w_mlp, links={'o': (ZERO, 'o_r')}, x=x_loc),
                         qkv_fwd_stage(ONE, ln_attn, w_qkv, tab1, (ONE, 'y')))
        kv_edges = (q1.left, q1.right)
        a1, f1, s1 = run("attn1_mlp1", cids[TWO], near_peers, attn1_fwd_stage(cu_loc, q1.out, *kv_edges),
                         mlp_stage(ONE, True, True, *mlp_args, *w_mlp, links={'o': (ZERO, 'o')}, x=f0.y, dy=d_out),
                         side_grad_stage(q1.out))
        g_side = lax.psum(s1.out, ('sp', 'zy'))
        far = [getattr(s1, n) for n in FAR]
        _, t1, b0 = run("attn1_qkv1_mlp0", cids[5], row_peers,
                        attn1_bwd_stage(cu_loc, q1.out, f1.d_o, a1.lse, f1.delta, kv_edges, far),
                        qkv_bwd_stage(ONE, tab1, w_qkv, f0.y, ln_attn, f1.dmid, link=(ZERO, 'out')),
                        mlp_stage(ZERO, False, True, *mlp_args, *w_mlp, links={'dy': (ONE, 'dx')}, x1=f0.x1_m, u=f0.u))
        dqkv0 = exchange(attn0_bwd(cu_loc, q0.out, q0.o_m, b0.d_o, q0.lse))
        grads = grad_att(None, f1.of_m, f1.of_r, f1.dmid, f1.dmid_r, t1.dt_m, t1.dt_r, q1.h_m, q1.h_r, ZERO)
        grads = grad_mlp(grads, f0.m_m, f0.m_r, t1.dx, b0.dy_r, f0.h_m, f0.h_r, b0.du_m, b0.du_r, ATT_ROWS, RING_ROWS)
        t0, = run("qkv0_grads", cids[SIX], partner_peer, qkv_bwd_stage(
            ZERO, tab0, w_qkv, x_loc, ln_attn, b0.dmid, d=dqkv0, grads=grads,
            pairs=(q0.h_m, q0.h_r, f0.of_m, f0.of_r, b0.dmid, b0.dmid_r)))

        gains = (t0.gg, t1.gg, b0.gg, f1.gg)
        summed, gains = ring_all_reduce(t0.out, gains, cids[ZERO])
        summed, g_side = lax.optimization_barrier((summed, g_side))
        from_partner = lax.ppermute(g_side, 'core', swap_cores)
        shapes = [(TWO, DM, THREE * DM), (TWO, DM, DM), IN_SHAPE, OUT_SHAPE]
        g_qkv, g_proj, g_in, g_out = unpack_call(unpack_ring_body, (summed,), shapes, {}, "unpack_ring")
        g_in, g_out = unpack_call(unpack_mlp_body, (g_side, from_partner, g_in, g_out), shapes[TWO:],
                                  {TWO: ZERO, THREE: ONE}, "unpack_mlp")
        return f1.y, t0.dx, g_qkv, g_proj, g_in, g_out, gains[:TWO], gains[TWO:FOUR]

    in_specs = (token_spec, P(dp_axes, None), P(row_axes)) + (P(),) * SIX + (token_spec,)
    out_specs = (token_spec, token_spec) + (P(),) * SIX
    return jax.shard_map(device_step, mesh=mesh, in_specs=in_specs, out_specs=out_specs, check_vma=False)
```

```python
import functools
import math
import jax
import jax.numpy as jnp
from jax import lax
from jax.experimental import pallas as pl
from jax.experimental.pallas import tpu as pltpu
from jax.sharding import Mesh, PartitionSpec as P

ZERO, ONE, TWO, THREE, FOUR = range(5)
SIX, TWELVE = 6, 12
HEAD = 64
HALF = 32
NHEAD = 12
DM = 768
FF = 3072
TOK = 512
GRP = 2048
WIN = 64
NDOC = 8
LANE = 128
EPS = 1e-5
NEG = -1e30
SCALE = 0.125
BASES = (160000.0, 10000.0)
F32 = jnp.float32
BF = jnp.bfloat16
QT = 256
FT = 768
NFT = FF // FT
QTILES = GRP // QT
MIB = 1024 * 1024
ALLTOK = (TOK, DM)
ALLDM = (DM, DM)
PROJ = DM // 2
DOWN = FF // 2
UP = FF
QKV = 3 * PROJ
MLP_ROWS = DOWN + UP
ATT_ROWS = PROJ + QKV
RING_ROWS = 2 * ATT_ROWS + MLP_ROWS
ANY = pl.BlockSpec(memory_space=pl.ANY)
DMA = pltpu.SemaphoreType.DMA
MESH = pl.DeviceIdType.MESH


def dot(a, b, ca, cb):
    return lax.dot_general(a, b, (((ca,), (cb,)), ((), ())), preferred_element_type=F32)


def mm(a, b):
    return dot(a, b, ONE, ZERO)


def mm_nt(a, b):
    return dot(a, b, ONE, ONE)


def mm_tn(a, b):
    return dot(a, b, ZERO, ZERO)


def call(body, grid, in_specs, out_specs, out_shape, scratch=(), prefetch=ZERO, flops=ZERO, nbytes=ZERO, name=None,
         cid=None, alias=None):
    extra = {} if cid is None else dict(collective_id=cid, has_side_effects=True)
    return pl.pallas_call(
        body,
        grid_spec=pltpu.PrefetchScalarGridSpec(
            num_scalar_prefetch=prefetch, grid=grid, in_specs=in_specs, out_specs=out_specs, scratch_shapes=scratch),
        out_shape=out_shape,
        input_output_aliases=alias or {},
        compiler_params=pltpu.CompilerParams(vmem_limit_bytes=60 * MIB, **extra),
        cost_estimate=pl.CostEstimate(flops=int(flops), bytes_accessed=int(nbytes), transcendentals=ZERO),
        name=name,
    )


def sds(shape, dtype):
    return jax.ShapeDtypeStruct(shape, dtype)


def spec(shape, *idx):
    idx = idx or (ZERO,) * len(shape)
    return pl.BlockSpec(shape, lambda *g: tuple(i(*g) if callable(i) else i for i in idx))


def step_of(s, *_):
    return s


def core_and_partner():
    core = lax.axis_index('core')
    return core, {'core': ONE - core}


def greet(devices):
    for dev in devices:
        pl.semaphore_signal(pltpu.get_barrier_semaphore(), inc=ONE, device_id=dev, device_id_type=MESH)


def all_here(devices):
    pl.semaphore_wait(pltpu.get_barrier_semaphore(), len(devices))


def sp_peer(d):
    return lax.rem(lax.axis_index('sp') + d, FOUR)


PEERS = range(ONE, FOUR)


class Swaps:
    def __init__(self, ssem, rsem, lsem):
        self.sems, self.waits, self.n = (ssem, rsem, lsem), [], ZERO
        self.core, self.partner = core_and_partner()
        self.other = ONE - self.core
        self.me = lax.axis_index('sp')

    def remote(self, src, dst, dev=None):
        ssem, rsem, _ = self.sems
        return self.later(pltpu.make_async_remote_copy(
            src_ref=src, dst_ref=dst, send_sem=ssem.at[self.n], recv_sem=rsem.at[self.n],
            device_id=self.partner if dev is None else dev, device_id_type=MESH))

    def local(self, src, dst):
        return self.later(pltpu.make_async_copy(src, dst, self.sems[TWO].at[self.n]))

    def later(self, cp):
        self.n += ONE
        self.waits.append(cp)
        return cp

    def to_all(self, src_of, dst_of):
        return [self.remote(src_of(sp_peer(d)), dst_of(self.me), {'sp': sp_peer(d)}) for d in PEERS] + [
            self.local(src_of(self.me), dst_of(self.me))]

    def to_sides(self, left_src, right_src, from_left, from_right):
        return [self.remote(right_src, from_left, {'sp': sp_peer(ONE)}), self.remote(left_src, from_right, {'sp': sp_peer(THREE)})]

    def early(self, some):
        gone = {id(cp) for cp in some}
        self.waits = [cp for cp in self.waits if id(cp) not in gone]
        return some

    def wait(self):
        for cp in self.waits:
            cp.wait()


def start_all(copies):
    for cp in copies:
        cp.start()


def wait_all(copies):
    for cp in copies:
        cp.wait()


def row_peers():
    return [core_and_partner()[ONE]] + [{'sp': sp_peer(d)} for d in PEERS]


def side_peers():
    return [{'sp': sp_peer(ONE)}, {'sp': sp_peer(THREE)}]


def partner_peer():
    return [core_and_partner()[ONE]]


def near_peers():
    return partner_peer() + side_peers()


def swap_sems(n):
    return [DMA((n,))] * THREE


def named_sems(n):
    return list(zip(('ssem', 'rsem', 'lsem'), swap_sems(n)))


class Refs:
    def __init__(self, named):
        self.__dict__.update(named)


class Stage:
    def __init__(self, body, steps, ins, outs, scratch, copies=None, links=None, alias=()):
        self.body, self.steps, self.ins, self.outs, self.scratch = body, steps, ins, outs, scratch
        self.copies, self.links, self.alias = copies, links or {}, alias


def shifted(block, first, steps):
    if block.index_map is None:
        return block
    return pl.BlockSpec(block.block_shape, lambda g: block.index_map(jnp.clip(g - first, ZERO, steps - ONE)))


def run(name, cid, peers, *stages):
    firsts = [sum(st.steps for st in stages[:k]) for k in range(len(stages))]

    def flat(kind):
        return [(k, entry) for k, st in enumerate(stages) for entry in getattr(st, kind)]

    ins, outs, scratch = flat('ins'), flat('outs'), flat('scratch')
    keys = [(k, entry[ZERO]) for k, entry in ins + outs + scratch]

    def body(*refs):
        pid = pl.program_id(ZERO)
        have = dict(zip(keys, refs))

        @pl.when(pid == ZERO)
        def _():
            greet(peers())

        talking = [k for k, st in enumerate(stages) if st.copies]
        views = []
        for k, st in enumerate(stages):
            r = Refs({n: ref for (at, n), ref in have.items() if at == k})
            for n, source in st.links.items():
                setattr(r, n, have[source])
            r.arrive = lambda k=k: all_here(peers()) if k == talking[ZERO] else None
            views.append(r)

            @pl.when((pid >= firsts[k]) & (pid < firsts[k] + st.steps))
            def _(st=st, r=r, k=k):
                st.body(r, pid - firsts[k])

        @pl.when(pid == firsts[-ONE] + stages[-ONE].steps - ONE)
        def _():
            for k in talking:
                stages[k].copies(views[k]).sw.wait()

    def placed(entries):
        return [shifted(entry[TWO], firsts[k], stages[k].steps) for k, entry in entries]

    alias = {[e[ZERO] for _, e in ins].index(a): [e[ZERO] for _, e in outs].index(b) for st in stages for a, b in st.alias}
    got = call(body, (sum(st.steps for st in stages),), placed(ins), placed(outs), [e[ONE] for _, e in outs],
               scratch=[e[ONE] for _, e in scratch], flops=16 * TOK * DM * FF, nbytes=30 * MIB, name=name, cid=cid,
               alias=alias)(*[e[ONE] for _, e in ins])
    out = [{} for _ in stages]
    for (k, e), arr in zip(outs, got):
        out[k][e[ZERO]] = arr
    return [Refs(named) for named in out]


def norm_parts(x_bf):
    rows = x_bf.astype(F32)
    cen = rows - jnp.mean(rows, axis=ONE, keepdims=True)
    var = jnp.mean(cen * cen, axis=ONE, keepdims=True)
    return cen, lax.rsqrt(var + EPS)


def norm_rows(x_bf, gain):
    cen, inv = norm_parts(x_bf)
    return (cen * inv * gain).astype(BF)


def norm_rows_grad(x_bf, gain, d_bf):
    cen, inv = norm_parts(x_bf)
    hat = cen * inv
    d_out = d_bf.astype(F32)
    g_gain = jnp.sum(d_out * hat, axis=ZERO, keepdims=True)
    d_hat = d_out * gain
    d_x = inv * (d_hat - jnp.mean(d_hat, axis=ONE, keepdims=True) - hat * jnp.mean(d_hat * hat, axis=ONE, keepdims=True))
    return d_x.astype(BF), g_gain


def add_bf(a, b):
    return (a.astype(F32) + b.astype(F32)).astype(BF)


RB = 256
ROPED = 6
CHUNKS = range(DM // RB)


def head_rows(ref, chunk, head):
    return ref.at[head, ZERO, chunk] if ref.shape[ZERO] == FOUR else ref.at[ZERO, chunk, head]


def weight_cols(layer, width, first=ZERO):
    return spec((None, DM, width), layer, ZERO, lambda s: first + s)


GAINS = spec((TWO, DM))


GROUP_QKV = (FOUR, THREE, THREE, HEAD, TOK)
OWN_QKV = (THREE * NHEAD, HEAD, TOK)
EDGE = (NHEAD, HEAD, LANE)
TOKS = jax.ShapeDtypeStruct(ALLTOK, BF)
TOK_SPEC = spec(ALLTOK)
TOK_VMEM = pltpu.VMEM(ALLTOK, BF)
TABLE = spec((HALF, TOK))
CU_SPEC = pl.BlockSpec(memory_space=pltpu.SMEM)


def rotated(a, b, r):
    cos, sin = r.cos[...], r.sin[...]
    return a * cos - b * sin, b * cos + a * sin


def qkv_chunk(r, w):
    return mm(r.h[...], w).astype(BF).astype(F32).T


def head_halves(t_rows, head):
    at = HEAD * head
    return t_rows[at:at + HALF], t_rows[at + HALF:at + HEAD]


def qkv_fwd_copies(r):
    sw = Swaps(r.ssem, r.rsem, r.lsem)
    return Refs(dict(sw=sw, start=[sw.remote(r.h, r.h_r), sw.local(r.h, r.h_m)],
                     edges=sw.to_sides(r.edge_s.at[ZERO], r.edge_s.at[ONE], r.left, r.right)))


def qkv_fwd_body(r, step, layer):
    cps = qkv_fwd_copies(r)

    @pl.when(step == ZERO)
    def _():
        r.h[...] = norm_rows(r.x[...], r.g[layer:layer + ONE])
        r.arrive()
        start_all(cps.start)

    for p in range(THREE):
        @pl.when(step == KVQ.index(p))
        def _(p=p):
            for chunk in CHUNKS:
                t_rows = qkv_chunk(r, r.w[:, RB * chunk:RB * chunk + RB])
                for head in range(FOUR):
                    a, b = head_halves(t_rows, head)
                    if p < TWO:
                        a, b = rotated(a, b, r)
                    n = FOUR * chunk + head
                    out = r.out.at[n]
                    out[:HALF] = a.astype(BF)
                    out[HALF:] = b.astype(BF)
                    if p:
                        lane = WIN * (p - ONE)
                        blk = out[...]
                        r.edge_s[ZERO, n, :, lane:lane + WIN] = blk[:, :WIN]
                        r.edge_s[ONE, n, :, lane:lane + WIN] = blk[:, TOK - WIN:]
            if p == TWO:
                start_all(cps.edges)


KVQ = (ONE, TWO, ZERO)


def kvq_part(s, *_):
    return (s + ONE) % THREE


def qkv_fwd_stage(layer, gain, w_qkv, tables, link):
    ins = [('g', gain, GAINS), ('w', w_qkv, spec((None, DM, DM), layer, ZERO, kvq_part)), ('cos', tables[ZERO], TABLE), ('sin', tables[ONE], TABLE)]
    outs = [('h_m', TOKS, ANY), ('h_r', TOKS, ANY), ('out', sds(OWN_QKV, BF), spec((NHEAD, HEAD, TOK), kvq_part, ZERO, ZERO)),
            ('left', sds(EDGE, BF), ANY), ('right', sds(EDGE, BF), ANY)]
    scratch = [('h', TOK_VMEM), ('edge_s', pltpu.VMEM((TWO,) + EDGE, BF))]
    return Stage(functools.partial(qkv_fwd_body, layer=layer), THREE, ins, outs, scratch + named_sems(FOUR),
                 qkv_fwd_copies, {'x': link})


def tile_src(i, *_):
    return i // TWO


def tile_side(i, *_):
    return i % TWO


Q_SPEC = spec((ONE, ONE, THREE, HEAD, QT), tile_src, ZERO, ZERO, ZERO, tile_side)
O_SPEC = spec((ONE, THREE, HEAD, QT), tile_src, ZERO, ZERO, tile_side)
STAT_SPEC = spec((8, QT), ZERO, step_of)


def kv_spec(part):
    return spec((FOUR, ONE, THREE, HEAD, TOK), ZERO, part, ZERO, ZERO, ZERO)


def key_tile(kt):
    return kt // TWO, pl.ds(pl.multiple_of((kt % TWO) * QT, QT), QT)


def key_rows(dst, k_ref):
    for src in range(FOUR):
        for h in range(THREE):
            dst[h, TOK * src:TOK * src + TOK] = k_ref[src, ZERO, h].T


def row_tile(kt):
    return pl.ds(pl.multiple_of(kt * QT, QT), QT)


def doc_start(cu_ref, tok):
    start = jnp.zeros_like(tok)
    for d in range(ONE, NDOC):
        start = jnp.where(cu_ref[ZERO, d] <= tok, cu_ref[ZERO, d], start)
    return start


def doc_stop(cu_ref, tok):
    stop = jnp.full_like(tok, GRP)
    for d in range(NDOC - ONE, ZERO, -ONE):
        stop = jnp.where(cu_ref[ZERO, d] > tok, cu_ref[ZERO, d], stop)
    return stop


def tile_bounds(cu_ref, tile):
    first = tile * QT
    tok = lax.broadcasted_iota(jnp.int32, (ONE, QT), ONE) + first
    lo = doc_start(cu_ref, first) // QT
    hi = (doc_stop(cu_ref, first + QT - ONE) + QT - ONE) // QT
    return lo, hi, doc_start(cu_ref, tok), doc_stop(cu_ref, tok)


BY_OWNER = (FOUR, THREE, HEAD, TOK)


def group_copies(r):
    sw = Swaps(r.ssem, r.rsem, r.lsem)

    def head_parts(c):
        return [cp for p in range(THREE) for cp in sw.to_all(lambda dev: r.out_s.at[p, dev, c], lambda dev: r.got.at[dev, p, c])]

    start = [sw.remote(r.h, r.h_r), sw.local(r.h, r.h_m)]
    parts = [sw.early(head_parts(c)) for c in range(THREE)]
    heads = [sw.early(sw.to_all(lambda dev: r.o_s.at[dev, c], lambda dev: r.o_r.at[dev, c])) for c in range(THREE)]
    return Refs(dict(sw=sw, start=start, parts=parts, heads=heads, keep=[sw.local(r.got, r.out), sw.local(r.o_s, r.o_m)]))


def group_fwd_body(r, step):
    cps = group_copies(r)
    tiles = range(QTILES)

    @pl.when(step == ZERO)
    def _():
        r.h[...] = norm_rows(r.x[...], r.g[:ONE])
        r.arrive()
        start_all(cps.start)

    for c in range(THREE):
        @pl.when(step == c)
        def _(c=c):
            for p, w in enumerate((r.wq, r.wk, r.wv)):
                t_rows = qkv_chunk(r, w[...])
                for head in range(FOUR):
                    a, b = head_halves(t_rows, head)
                    if p < TWO:
                        a, b = rotated(a, b, r)
                    out = r.out_s.at[p, head, c]
                    out[:HALF] = a.astype(BF)
                    out[HALF:] = b.astype(BF)
            start_all(cps.parts[c])

        @pl.when(step == c + THREE)
        def _(c=c):
            wait_all(cps.parts[c])
            for src in range(FOUR):
                r.kr_s[TOK * src:TOK * src + TOK] = r.got[src, ONE, c].T
            io = lax.broadcasted_iota(jnp.int32, (QT, QT), ZERO)

            def q_pair(n, carry):
                src = sp_peer(n + ONE)
                pair = range(TWO)
                cols = [slice(QT * a, QT * a + QT) for a in pair]
                toks = [lax.broadcasted_iota(jnp.int32, (ONE, QT), ONE) + src * TOK + QT * a for a in pair]
                st, en = [doc_start(r.cu, tok) for tok in toks], [doc_stop(r.cu, tok) for tok in toks]
                for a in pair:
                    q_t = r.got[src, ZERO, c, :, cols[a]] * SCALE
                    for k in tiles:
                        r.s_s[a, k] = mm(r.kr_s[QT * k:QT * k + QT], q_t)
                top, total = [], []
                for a in pair:
                    m = jnp.full((ONE, QT), NEG, F32)
                    for k in tiles:
                        s = jnp.where((io >= st[a] - QT * k) & (io < en[a] - QT * k), r.s_s[a, k], NEG)
                        r.s_s[a, k] = s
                        m = jnp.maximum(m, jnp.max(s, axis=ZERO, keepdims=True))
                    top.append(m)
                for a in pair:
                    part = jnp.zeros((ONE, QT), F32)
                    for k in tiles:
                        p = jnp.exp(r.s_s[a, k] - top[a])
                        part += jnp.sum(p, axis=ZERO, keepdims=True)
                        r.p_s[a, QT * k:QT * k + QT] = p.astype(BF)
                    total.append(part)
                for a in pair:
                    acc = jnp.zeros((HEAD, QT), F32)
                    for k in range(FOUR):
                        acc += mm(r.got[k, TWO, c], r.p_s[a, TOK * k:TOK * k + TOK])
                    r.o_s[src, c, :, cols[a]] = (acc / total[a]).astype(BF)
                    r.lse[c:c + ONE, row_tile(TWO * src + a)] = top[a] + jnp.log(total[a])
                for k, cp in enumerate(cps.heads[c]):
                    @pl.when(n == k)
                    def _(cp=cp):
                        cp.start()
                return carry

            lax.fori_loop(ZERO, FOUR, q_pair, ZERO)

    @pl.when(step == ROPED - ONE)
    def _():
        start_all(cps.keep)
        for c in range(THREE):
            wait_all(cps.heads[c])


def group_fwd_stage(cu, gain, w_qkv, tables, x):
    part = lambda p: spec((None, DM, RB), ZERO, ZERO, lambda s: THREE * p + jnp.minimum(s, TWO))
    ins = [('cu', cu, CU_SPEC), ('g', gain, GAINS), ('wq', w_qkv, part(ZERO)), ('wk', w_qkv, part(ONE)), ('wv', w_qkv, part(TWO)),
           ('cos', tables[ZERO], TABLE), ('sin', tables[ONE], TABLE), ('x', x, TOK_SPEC)]
    outs = [('h_m', TOKS, ANY), ('h_r', TOKS, ANY), ('out', sds(GROUP_QKV, BF), ANY), ('o_m', sds(BY_OWNER, BF), ANY),
            ('lse', sds((8, GRP), F32), spec((8, GRP)))]
    owner = pltpu.VMEM(BY_OWNER, BF)
    scratch = [('h', TOK_VMEM), ('out_s', pltpu.VMEM((THREE, FOUR, THREE, HEAD, TOK), BF)), ('got', pltpu.VMEM(GROUP_QKV, BF)),
               ('kr_s', pltpu.VMEM((GRP, HEAD), BF)), ('s_s', pltpu.VMEM((TWO, QTILES, QT, QT), F32)), ('p_s', pltpu.VMEM((TWO, GRP, QT), BF)),
               ('o_s', owner), ('o_r', owner)]
    return Stage(group_fwd_body, ROPED, ins, outs, scratch + named_sems(FOUR * 16), group_copies)


def attn0_bwd_body(cu_ref, q_ref, k_ref, v_ref, o_ref, do_ref, lse_ref, out_ref,
                   dk_s, dv_s, dq_s, kr_s, vr_s, s_s, d_s, p_s, t_s):
    tile = pl.program_id(ZERO)
    first, last, st, en = tile_bounds(cu_ref, tile)
    heads = range(THREE)

    @pl.when(tile == ZERO)
    def _():
        dk_s[...] = jnp.zeros(dk_s.shape, F32)
        dv_s[...] = jnp.zeros(dv_s.shape, F32)
        key_rows(kr_s, k_ref)
        key_rows(vr_s, v_ref)

    dq_s[...] = jnp.zeros(dq_s.shape, F32)
    io = lax.broadcasted_iota(jnp.int32, (QT, QT), ZERO)
    q_t = [q_ref[ZERO, ZERO, h] * SCALE for h in heads]
    do_t = [do_ref[ZERO, h] for h in heads]
    q_rows, do_rows = [q_t[h].T for h in heads], [do_t[h].T for h in heads]
    delta = [jnp.sum(do_t[h].astype(F32) * o_ref[ZERO, h].astype(F32), axis=ZERO, keepdims=True) for h in heads]
    lse = [lse_ref[h:h + ONE] for h in heads]

    def body(kt, carry):
        base = kt * QT
        src, cols = key_tile(kt)
        rows = row_tile(kt)
        ok = (io >= st - base) & (io < en - base)
        for h in heads:
            s_s[h] = mm(kr_s[h, rows], q_t[h])
            d_s[h] = mm(vr_s[h, rows], do_t[h])
        for h in heads:
            p = jnp.exp(jnp.where(ok, s_s[h] - lse[h], NEG))
            p_s[h] = p.astype(BF)
            t_s[h] = (p * (d_s[h] - delta[h])).astype(BF)
        for h in heads:
            dv_s[h, rows] += mm(p_s[h], do_rows[h])
            dk_s[h, rows] += mm(t_s[h], q_rows[h])
            dq_s[h] += mm(k_ref[src, ZERO, h, :, cols], t_s[h])
        return carry

    lax.fori_loop(first, last, body, ZERO)
    src, cols = key_tile(tile)
    for h in heads:
        out_ref[src, ZERO, h, :, cols] = (dq_s[h] * SCALE).astype(BF)

    @pl.when(tile == QTILES - ONE)
    def _():
        for src in range(FOUR):
            for h in heads:
                out_ref[src, ONE, h] = dk_s[h, TOK * src:TOK * src + TOK].T.astype(BF)
                out_ref[src, TWO, h] = dv_s[h, TOK * src:TOK * src + TOK].T.astype(BF)


def attn0_bwd(cu, qkv, o_t, do_t, lse):
    acc, rows = pltpu.VMEM((THREE, GRP, HEAD), F32), pltpu.VMEM((THREE, GRP, HEAD), BF)
    sq32, sq16 = pltpu.VMEM((THREE, QT, QT), F32), pltpu.VMEM((THREE, QT, QT), BF)
    return call(
        attn0_bwd_body, (QTILES,),
        [Q_SPEC, kv_spec(ONE), kv_spec(TWO), O_SPEC, O_SPEC, STAT_SPEC],
        spec(GROUP_QKV), sds(GROUP_QKV, BF),
        scratch=[acc, acc, pltpu.VMEM((THREE, HEAD, QT), F32), rows, rows, sq32, sq32, sq16, sq16],
        prefetch=ONE, flops=30 * GRP * GRP * HEAD, nbytes=TWELVE * MIB, name="attn0_bwd",
    )(cu, qkv, qkv, qkv, o_t, do_t, lse)


NBLK = TOK // LANE
EXT = TOK + TWO * WIN
XBLK = EXT // LANE
REACH = LANE + TWO * WIN
AHEAD_FWD, AHEAD_BWD = 4, 2
HPS = 4
HSTEPS = NHEAD // HPS


def heads_of(width, part):
    return spec((HPS, HEAD, width), lambda n: HSTEPS * part + n, ZERO, ZERO)


def own_head(part):
    return heads_of(TOK, part)


def row_of(width):
    return spec((HPS, ONE, width), step_of, ZERO, ZERO)


LOW, HIGH = slice(None, WIN), slice(WIN, None)
STAT = jax.ShapeDtypeStruct((NHEAD, ONE, TOK), F32)
STAT_BLOCK = spec((NHEAD, ONE, TOK))


def joined(left, mid, right, h, left_lanes=HIGH, right_lanes=LOW):
    return jnp.concatenate([left[h][:, left_lanes], mid[h], right[h][:, right_lanes]], axis=ONE)


def blocks(first, last):
    return slice(LANE * first, LANE * last)


def near_bounds(cu_ref, before, width):
    shift = lax.axis_index('sp') * TOK
    tok = lax.broadcasted_iota(jnp.int32, (ONE, width), ONE) + (shift - before)
    inside = (tok >= ZERO) & (tok < GRP)
    lo = jnp.maximum(doc_start(cu_ref, tok), tok - WIN) - (shift - WIN)
    hi = jnp.minimum(doc_stop(cu_ref, tok), tok + WIN + ONE) - (shift - WIN)
    return jnp.where(inside, lo, ZERO), jnp.where(inside, hi, ZERO)


def in_bounds(bounds, cols, first, n):
    io = lax.broadcasted_iota(jnp.int32, (n, LANE), ZERO) + first
    return (io >= bounds[ZERO][:, cols]) & (io < bounds[ONE][:, cols])


def every_head(fn, ahead):
    def body(g, c):
        fn([ahead * g + a for a in range(ahead)])
        return c
    lax.fori_loop(ZERO, HPS // ahead, body, ZERO)


def attn1_fwd_body(r, step):
    bounds = near_bounds(r.cu, ZERO, TOK)

    def some(heads):
        v_all = []
        for a, h in enumerate(heads):
            q_t = r.q[h] * SCALE
            k_rows = joined(r.left, r.k, r.right, h, LOW, LOW).T
            v_all.append(joined(r.left, r.v, r.right, h, HIGH, HIGH))
            for i in range(NBLK):
                r.s_s[a, i] = mm(k_rows[LANE * i:LANE * i + REACH], q_t[:, blocks(i, i + ONE)])
        for a, h in enumerate(heads):
            for i in range(NBLK):
                cols = blocks(i, i + ONE)
                s = jnp.where(in_bounds(bounds, cols, LANE * i, REACH), r.s_s[a, i], NEG)
                m = jnp.max(s, axis=ZERO, keepdims=True)
                e = jnp.exp(s - m)
                l = jnp.sum(e, axis=ZERO, keepdims=True)
                r.p_s[a, i] = (e * (ONE / l)).astype(BF)
                r.lse[HPS * step + h, :, cols] = m + jnp.log(l)
        for a, h in enumerate(heads):
            for i in range(NBLK):
                out = mm(v_all[a][:, LANE * i:LANE * i + REACH], r.p_s[a, i]).astype(BF)
                r.o[HPS * step + h, :, blocks(i, i + ONE)] = out
    every_head(some, AHEAD_FWD)


def attn1_fwd_stage(cu, qkv, left, right):
    tile, edge = (AHEAD_FWD, NBLK, REACH, LANE), heads_of(LANE, ZERO)
    return Stage(
        attn1_fwd_body, HSTEPS,
        [('cu', cu, CU_SPEC), ('q', qkv, own_head(ZERO)), ('k', qkv, own_head(ONE)), ('v', qkv, own_head(TWO)),
         ('left', left, edge), ('right', right, edge)],
        [('lse', STAT, STAT_BLOCK)],
        [('o', pltpu.VMEM((NHEAD, HEAD, TOK), BF)), ('s_s', pltpu.VMEM(tile, F32)), ('p_s', pltpu.VMEM(tile, BF))])


def attn1_bwd_body(r, step):
    bounds = near_bounds(r.cu, WIN, EXT)

    def window(e):
        first, last = max(LANE * e - WIN, ZERO), min(LANE * e + LANE + WIN, EXT)
        return first, last - first

    def parts(h):
        q_t = joined(r.ql, r.q, r.qr, h) * SCALE
        return q_t, joined(r.dl, r.d, r.dr, h), joined(r.left, r.k, r.right, h, LOW, LOW)

    def some(heads):
        for a, h in enumerate(heads):
            q_t, do_t, k_t = parts(h)
            for n, arr in enumerate((q_t, do_t, k_t)):
                r.x_s[a, n] = arr
            k_rows, v_rows = k_t.T, joined(r.left, r.v, r.right, h, HIGH, HIGH).T
            for e in range(XBLK):
                first, n = window(e)
                cols = blocks(e, e + ONE)
                r.s_s[a, e, :n] = mm(k_rows[first:first + n], q_t[:, cols])
                r.d_s[a, e, :n] = mm(v_rows[first:first + n], do_t[:, cols])
        for a, h in enumerate(heads):
            lse, delta = joined(r.ll, r.lse, r.lr, h), joined(r.el, r.delta, r.er, h)
            for e in range(XBLK):
                first, n = window(e)
                cols = blocks(e, e + ONE)
                ok = in_bounds(bounds, cols, first, n)
                p = jnp.exp(jnp.where(ok, r.s_s[a, e, :n] - lse[:, cols], NEG))
                r.p_s[a, first:first + n, cols] = p.astype(BF)
                r.t_s[a, first:first + n, cols] = (p * (r.d_s[a, e, :n] - delta[:, cols])).astype(BF)
        for a, h in enumerate(heads):
            got = [[], [], []]
            for b in range(XBLK):
                here, wide = blocks(b, b + ONE), blocks(max(b - ONE, ZERO), min(b + TWO, XBLK))
                got[ZERO].append(mm(r.x_s[a, TWO, :, wide], r.t_s[a, wide, here]) * SCALE)
                got[ONE].append(mm_nt(r.x_s[a, ZERO, :, wide], r.t_s[a, here, wide]))
                got[TWO].append(mm_nt(r.x_s[a, ONE, :, wide], r.p_s[a, here, wide]))
            for n in range(THREE):
                own = jnp.concatenate([g.astype(BF) for g in got[n]], axis=ONE)[:, WIN:WIN + TOK]
                r.out[n, HPS * step + h] = own

    @pl.when(step == ZERO)
    def _():
        r.p_s[...] = jnp.zeros(r.p_s.shape, BF)
        r.t_s[...] = jnp.zeros(r.t_s.shape, BF)

    every_head(some, AHEAD_BWD)


def attn1_bwd_stage(cu, qkv, do_t, lse, delta, edges, far):
    edge, row = heads_of(LANE, ZERO), row_of(LANE)
    blk = (AHEAD_BWD, XBLK, REACH, LANE)
    square = pltpu.VMEM((AHEAD_BWD, EXT, EXT), BF)
    names = ('left', 'right', 'ql', 'qr', 'dl', 'dr')
    return Stage(
        attn1_bwd_body, HSTEPS,
        [('cu', cu, CU_SPEC), ('q', qkv, own_head(ZERO)), ('k', qkv, own_head(ONE)), ('v', qkv, own_head(TWO)), ('d', do_t, own_head(ZERO)),
         ('lse', lse, row_of(TOK)), ('delta', delta, row_of(TOK))]
        + [(n, arr, edge) for n, arr in zip(names, list(edges) + far[:FOUR])]
        + [(n, arr, row) for n, arr in zip(('ll', 'lr', 'el', 'er'), far[FOUR:])],
        [], [('out', pltpu.VMEM((THREE, NHEAD, HEAD, TOK), BF)), ('s_s', pltpu.VMEM(blk, F32)), ('d_s', pltpu.VMEM(blk, F32)),
             ('p_s', square), ('t_s', square), ('x_s', pltpu.VMEM((AHEAD_BWD, THREE, HEAD, EXT), BF))])


ROWBLK = [slice(r, r + RB) for r in range(ZERO, TOK, RB)]
HALFT = NFT // TWO
SQRT_HALF = math.sqrt(SCALE * FOUR)
PDF_SCALE = SQRT_HALF / math.sqrt(math.pi)


def normal_cdf(a):
    return SQRT_HALF * SQRT_HALF * (ONE + lax.erf(a * SQRT_HALF))


def half_rows(ref, which):
    n = ref.shape[ZERO] // TWO
    return ref.at[pl.ds(pl.multiple_of(which * n, n), n)]


def col_tile(ref, n):
    return ref.at[:, pl.ds(pl.multiple_of(n * FT, FT), FT)]


def mlp_copies(r, fwd, bwd):
    sw = Swaps(r.ssem, r.rsem, r.lsem)
    both = fwd and bwd
    c = Refs(dict(sw=sw, start=[], first=[], second=[]))
    if fwd:
        c.start += [sw.remote(r.h, r.h_r), sw.remote(half_rows(r.of, sw.other), r.of_r), sw.local(half_rows(r.of, sw.core), r.of_m)]
        there = [sw.remote(r.m_s.at[HALFT * sw.other + n], r.m_r.at[n] if both else col_tile(r.m_r, n)) for n in range(HALFT)]
        here = [None] * HALFT
        if not both:
            c.start += [sw.local(r.h, r.h_m), sw.local(r.x1, r.x1_m)]
            here = [sw.local(r.m_s.at[HALFT * sw.core + n], col_tile(r.m_m, n)) for n in range(HALFT)]
        c.m_out = list(zip(there, here))
    if bwd:
        c.start.append(sw.remote(r.dy, r.dy_r))
        c.dmid_out = sw.remote(r.dmid, r.dmid_r)
        c.du_out = [[sw.remote(r.du_s.at[n, sw.other], r.du_r.at[n] if both else col_tile(r.du_r, n))] for n in range(NFT)]
        if not both:
            for n in range(NFT):
                c.du_out[n].append(sw.local(r.du_s.at[n, sw.core], col_tile(r.du_m, n)))
            c.do_out = sw.to_all(lambda dev: r.do_s.at[dev], lambda dev: r.d_o.at[dev])
    if both:
        c.first = sw.early([c.start[ZERO], c.start[-ONE]] + there)
        c.second = sw.early([cp for part in c.du_out for cp in part])
    return c


def mlp_body(r, step, layer, fwd, bwd):
    cps = mlp_copies(r, fwd, bwd)
    sw, start, whole_group = cps.sw, cps.start, not (fwd and bwd)
    if fwd:
        m_out = cps.m_out
    if bwd:
        dmid_out, du_out = cps.dmid_out, cps.du_out

    @pl.when(step == ZERO)
    def _():
        if fwd:
            for n in range(NHEAD):
                r.of[HEAD * n:HEAD * n + HEAD, :] = (r.o[n % FOUR, n // FOUR] if whole_group else r.o[n])
            x1 = (r.x[...].astype(F32) + mm_tn(r.of[...], r.wp[...])).astype(BF)
            r.x1[...] = x1
            r.h[...] = norm_rows(x1, r.g[layer:layer + ONE])
            r.acc[...] = x1.astype(F32)
        if bwd:
            r.dacc[...] = jnp.zeros(r.dacc.shape, F32)
        r.arrive()
        start_all(start)

    for rows in ROWBLK:
        if fwd:
            ua = mm(r.h[rows], r.wa[...]).astype(BF)
            ub = mm(r.h[rows], r.wb[...]).astype(BF)
            if not bwd:
                r.u[ZERO, rows] = ua
                r.u[ONE, rows] = ub
        else:
            ua, ub = r.u[ZERO, rows], r.u[ONE, rows]
        a, b = ua.astype(F32), ub.astype(F32)
        cdf = normal_cdf(a)
        gate = a * cdf
        if fwd:
            m = (gate * b).astype(BF)
            r.m_s[step, rows] = m
            r.acc[rows] += mm(m, r.wo[...])
        if bwd:
            dm = mm_nt(r.dy[rows], r.wo[...]).astype(BF).astype(F32)
            pdf = jnp.exp(a * a * (SCALE * FOUR - ONE)) * PDF_SCALE
            db = (dm * gate).astype(BF)
            da = (dm * b * (cdf + a * pdf)).astype(BF)
            r.du_s[step, ZERO, rows] = da
            r.du_s[step, ONE, rows] = db
            r.dacc[rows] += mm_nt(da, r.wa[...]) + mm_nt(db, r.wb[...])

    for n in range(NFT):
        @pl.when(step == n)
        def _(n=n):
            if fwd:
                there, here = m_out[n % HALFT]

                if here:
                    @pl.when(sw.core == n // HALFT)
                    def _():
                        here.start()

                @pl.when(sw.other == n // HALFT)
                def _():
                    there.start()
            if bwd:
                for cp in du_out[n]:
                    cp.start()

    @pl.when(step == NFT - ONE)
    def _():
        if fwd:
            r.y[...] = r.acc[...].astype(BF)
        if bwd:
            d_ln, gg = norm_rows_grad(r.x1[...], r.g[layer:layer + ONE], r.dacc[...].astype(BF))
            r.gg[...] = gg
            d_mid = add_bf(r.dy[...], d_ln)
            r.dmid[...] = d_mid
            dmid_out.start()
            d_att = mm_nt(r.wp[...], d_mid).astype(BF)
            for n in range(NHEAD):
                rows = slice(HEAD * n, HEAD * n + HEAD)
                blk = d_att[rows]
                if whole_group:
                    r.do_s[n % FOUR, n // FOUR] = blk
                else:
                    r.d_o[n] = blk
                    r.delta[n] = jnp.sum(blk.astype(F32) * r.of[rows].astype(F32), axis=ZERO, keepdims=True)
            if whole_group:
                start_all(cps.do_out)


def mlp_stage(layer, fwd, bwd, w_proj, gain, w_in, w_out, links=None, **arrays):
    u_spec = spec((TWO, TOK, FT), ZERO, ZERO, step_of)
    half_o = sds((DM // TWO, TOK), BF)
    half_m, half_u = sds((TOK, FF // TWO), BF), sds((TOK, FF), BF)
    heads = (NHEAD, HEAD, TOK)
    sums = pltpu.VMEM(ALLTOK, F32)
    links = links or {}
    ins = [('wp', w_proj, spec((None, DM, DM), layer, ZERO, ZERO)), ('g', gain, GAINS),
           ('wa', w_in, weight_cols(layer, FT)), ('wb', w_in, weight_cols(layer, FT, NFT)),
           ('wo', w_out, spec((None, FT, DM), layer, step_of, ZERO))]
    kinds = dict(x=TOK_SPEC, dy=TOK_SPEC, x1=TOK_SPEC, u=u_spec)
    ins += [(n, arr, kinds[n]) for n, arr in arrays.items()]
    outs, scratch, both = [], [], fwd and bwd
    own_tiles, far_tiles = pltpu.VMEM((HALFT, TOK, FT), BF), pltpu.VMEM((NFT, TOK, FT), BF)
    if fwd:
        outs += [('y', TOKS, TOK_SPEC), ('of_m', half_o, ANY), ('of_r', half_o, ANY)]
        scratch += [('acc', sums), ('of', pltpu.VMEM((DM, TOK), BF)), ('m_s', pltpu.VMEM((NFT, TOK, FT), BF)), ('h', TOK_VMEM),
                    ('x1', TOK_VMEM)]
    if fwd and not bwd:
        outs += [('h_m', TOKS, ANY), ('h_r', TOKS, ANY), ('m_m', half_m, ANY), ('m_r', half_m, ANY)]
        outs += [('x1_m', TOKS, ANY), ('u', sds((TWO, TOK, FF), BF), u_spec)]
    if bwd:
        shape = heads if fwd else BY_OWNER
        outs += [('dmid', TOKS, TOK_SPEC), ('gg', sds((ONE, DM), F32), spec((ONE, DM))), ('d_o', sds(shape, BF), spec(shape) if fwd else ANY),
                 ('dmid_r', TOKS, ANY)]
        scratch += [('dacc', sums), ('du_s', pltpu.VMEM((NFT, TWO, TOK, FT), BF))]
    if bwd and not fwd:
        outs += [('dy_r', TOKS, ANY), ('du_m', half_u, ANY), ('du_r', half_u, ANY)]
    if both:
        outs += [('delta', STAT, STAT_BLOCK)]
        scratch += [('h_r', TOK_VMEM), ('dy_r', TOK_VMEM), ('m_r', own_tiles), ('du_r', far_tiles)]
    if not fwd:
        scratch += [('do_s', pltpu.VMEM(BY_OWNER, BF))]
    return Stage(functools.partial(mlp_body, layer=layer, fwd=fwd, bwd=bwd), NFT, ins, outs, scratch + named_sems(FOUR * NFT),
                 functools.partial(mlp_copies, fwd=fwd, bwd=bwd), links)


def side_grad_copies(r):
    sw = Swaps(r.ssem, r.rsem, r.lsem)
    for n, src in enumerate((r.q_all.at[:NHEAD], r.d_o, r.lse, r.delta)):
        sw.to_sides(src.at[:, :, :LANE], src.at[:, :, TOK - LANE:], getattr(r, FAR[TWO * n]), getattr(r, FAR[TWO * n + ONE]))
    return Refs(dict(sw=sw))


def side_grad_body(r, step):
    sw = side_grad_copies(r).sw
    mlp = mlp_copies(Refs(dict(r.__dict__, ssem=r.mlp_ssem, rsem=r.mlp_rsem, lsem=r.mlp_lsem)), True, True)

    @pl.when(step == ZERO)
    def _():
        start_all(sw.waits)
        wait_all(mlp.first)

    @pl.when(step < HALFT)
    def _():
        r.out[...] = mm_tn(r.m_s[HALFT * sw.core + step], r.dy[...]) + mm_tn(r.m_r[step], r.dy_r[...])

    @pl.when(step == HALFT)
    def _():
        wait_all(mlp.second)
        r.h_t[ZERO] = r.h[...].T
        r.h_t[ONE] = r.h_r[...].T

    @pl.when(step >= HALFT)
    def _():
        n = step - HALFT
        r.out[...] = mm(r.h_t[ZERO], r.du_s[n, sw.core]) + mm(r.h_t[ONE], r.du_r[n])


FAR = ('ql', 'qr', 'dl', 'dr', 'll', 'lr', 'el', 'er')


def side_grad_stage(qkv):
    kinds = [(NHEAD, HEAD, LANE, BF)] * FOUR + [(NHEAD, ONE, LANE, F32)] * FOUR
    far = [(n, sds(shape, dtype), ANY) for n, (*shape, dtype) in zip(FAR, kinds)]
    names = ('m_s', 'du_s', 'h', 'h_r', 'dy', 'dy_r', 'm_r', 'du_r', 'd_o', 'delta', 'of', 'of_r', 'of_m', 'dmid', 'dmid_r')
    links = {n: (ONE, n) for n in names}
    links.update({'mlp_' + n: (ONE, n) for n in ('ssem', 'rsem', 'lsem')}, lse=(ZERO, 'lse'))
    return Stage(side_grad_body, HALFT + NFT, [('q_all', qkv, ANY)],
                 [('out', sds((MLP_ROWS, DM), F32), spec(ALLDM, step_of, ZERO))] + far,
                 [('h_t', pltpu.VMEM((TWO, DM, TOK), BF))] + named_sems(8), side_grad_copies, links)


NAMED = ('ha', 'hb', 'oa', 'ob', 'dma', 'dmb')


def third(ref, n):
    return ref.at[PROJ * n:PROJ * n + PROJ]


def qkv_bwd_copies(r, grads):
    sw = Swaps(r.ssem, r.rsem, r.lsem)
    c = Refs(dict(sw=sw, parts=[[sw.remote(r.dt_s.at[sw.other, n], third(r.dt_r, n))] for n in range(THREE)]))
    if grads:
        c.loads = sw.early([sw.local(getattr(r, n + '_in'), getattr(r, n)) for n in NAMED])
        for part in c.parts:
            sw.early(part)
    else:
        for n in range(THREE):
            c.parts[n].append(sw.local(r.dt_s.at[sw.core, n], third(r.dt_m, n)))
    return c


def qkv_bwd_body(r, step, layer, grads):
    cps = qkv_bwd_copies(r, grads)
    sw, copies = cps.sw, cps.parts

    @pl.when(step == ZERO)
    def _():
        r.acc[...] = jnp.zeros(r.acc.shape, F32)
        if grads:
            start_all(cps.loads)

    for p in range(THREE):
        @pl.when(step == p)
        def _(p=p):
            cos, sin = r.cos[...], r.sin[...]
            for chunk in CHUNKS:
                for head in range(FOUR):
                    blk = r.d[head, ZERO, chunk] if grads else r.d[p, FOUR * chunk + head]
                    a, b = blk[:HALF], blk[HALF:]
                    if p < TWO:
                        a, b = a.astype(F32), b.astype(F32)
                        a, b = (a * cos + b * sin).astype(BF), (b * cos - a * sin).astype(BF)
                    at, full = LANE * chunk + HEAD * (head % TWO), RB * chunk + HEAD * head
                    for n, val in ((ZERO, a), (HALF, b)):
                        r.dt_s[head // TWO, p, at + n:at + n + HALF] = val
                        r.dt_all[full + n:full + n + HALF] = val
            if p == ZERO:
                r.arrive()
            start_all(copies[p])
            r.acc[...] += mm(r.w[...], r.dt_all[...])

    @pl.when(step == TWO)
    def _():
        d_ln, gg = norm_rows_grad(r.x[...], r.g[layer:layer + ONE], r.acc[...].T.astype(BF))
        r.gg[...] = gg
        r.dx[...] = add_bf(r.dmid[...], d_ln)

    if grads:
        @pl.when(step == THREE)
        def _():
            wait_all(cps.loads)
            for part in copies:
                wait_all(part)
            r.out[...] = mm(r.oa[...], r.dma[...]) + mm(r.ob[...], r.dmb[...])

        for p in range(THREE):
            @pl.when(step == p + FOUR)
            def _(p=p):
                r.out[...] = mm(r.dt_s[sw.core, p], r.ha[...]) + mm(third(r.dt_r, p)[...], r.hb[...])


def qkv_bwd_stage(layer, tables, w_qkv, x, gain, d_mid, d=None, link=None, grads=None, pairs=()):
    part = lambda s: jnp.minimum(s, TWO)
    ins = [('cos', tables[ZERO], TABLE), ('sin', tables[ONE], TABLE), ('w', w_qkv, spec((None, DM, DM), layer, ZERO, part)),
           ('x', x, TOK_SPEC), ('g', gain, GAINS), ('dmid', d_mid, TOK_SPEC)]
    outs = [('dx', TOKS, TOK_SPEC), ('gg', sds((ONE, DM), F32), spec((ONE, DM)))]
    feats = (THREE * PROJ, TOK)
    scratch = [('acc', pltpu.VMEM((DM, TOK), F32)), ('dt_s', pltpu.VMEM((TWO, THREE, PROJ, TOK), BF)), ('dt_all', pltpu.VMEM((DM, TOK), BF))]
    steps, alias = THREE, ()
    if grads is None:
        outs += [('dt_m', sds(feats, BF), ANY), ('dt_r', sds(feats, BF), ANY)]
    else:
        first = (ATT_ROWS + MLP_ROWS) // PROJ
        ins += [('d', d, spec((FOUR, ONE, THREE, HEAD, TOK), ZERO, part, ZERO, ZERO, ZERO)), ('grads', grads, ANY)]
        ins += [(n + '_in', arr, ANY) for n, arr in zip(NAMED, pairs)]
        outs += [('out', sds(grads.shape, F32), spec((PROJ, DM), lambda s: first + jnp.maximum(s - THREE, ZERO), ZERO))]
        scratch += [('dt_r', pltpu.VMEM(feats, BF))] + [(n, pltpu.VMEM(arr.shape, BF)) for n, arr in zip(NAMED, pairs)]
        steps, alias = steps + FOUR, (('grads', 'out'),)
    flag = grads is not None
    return Stage(functools.partial(qkv_bwd_body, layer=layer, grads=flag), steps, ins, outs, scratch + named_sems(TWELVE),
                 functools.partial(qkv_bwd_copies, grads=flag), {} if link is None else {'d': link}, alias)


NDOWN = DOWN // DM


def grad_call(body, grads, steps, in_specs, args, rows, first_row, total, scratch=()):
    shared = [] if grads is None else [grads]
    first = first_row // rows
    return call(
        body, (steps,), [ANY] * len(shared) + in_specs,
        spec((rows, DM), lambda s: first + s, ZERO), sds((total, DM), F32), scratch=scratch,
        flops=FOUR * steps * rows * TOK * DM, nbytes=20 * MIB, name=body.__name__,
        alias={ZERO: ZERO} if shared else None,
    )(*shared, *args)


GRAD_INS = 8


def grad_mlp_body(*refs):
    ma, mb, dya, dyb, ha, hb, dua, dub, out_ref, h_t = refs[-GRAD_INS - TWO:]
    step = pl.program_id(ZERO)

    @pl.when(step < NDOWN)
    def _():
        out_ref[...] = mm_tn(ma[...], dya[...]) + mm_tn(mb[...], dyb[...])

    @pl.when(step == NDOWN)
    def _():
        h_t[ZERO] = ha[...].T
        h_t[ONE] = hb[...].T

    @pl.when(step >= NDOWN)
    def _():
        out_ref[...] = mm(h_t[ZERO], dua[...]) + mm(h_t[ONE], dub[...])


def grad_mlp(grads, m, m_r, dy, dy_r, h, h_r, du, du_r, first_row, total):
    toks = spec(ALLTOK)
    m_col = spec(ALLTOK, ZERO, lambda s: jnp.minimum(s, NDOWN - ONE))
    du_col = spec(ALLTOK, ZERO, lambda s: jnp.maximum(s - NDOWN, ZERO))
    return grad_call(grad_mlp_body, grads, NDOWN + UP // DM, [m_col, m_col, toks, toks, toks, toks, du_col, du_col],
                     (m, m_r, dy, dy_r, h, h_r, du, du_r), DM, first_row, total, scratch=[pltpu.VMEM((TWO, DM, TOK), BF)])


def grad_att_body(*refs):
    oa, ob, dma, dmb, ta, tb, ha, hb, out_ref = refs[-GRAD_INS - ONE:]
    step = pl.program_id(ZERO)

    @pl.when(step == ZERO)
    def _():
        out_ref[...] = mm(oa[...], dma[...]) + mm(ob[...], dmb[...])

    @pl.when(step > ZERO)
    def _():
        out_ref[...] = mm(ta[...], ha[...]) + mm(tb[...], hb[...])


def grad_att(grads, of, of_r, dmid, dmid_r, dt, dt_r, h, h_r, first_row):
    toks = spec(ALLTOK)
    blk = (PROJ, TOK)
    dt_row = spec(blk, lambda s: jnp.maximum(s - ONE, ZERO), ZERO)
    return grad_call(grad_att_body, grads, ONE + QKV // PROJ, [spec(blk), spec(blk), toks, toks, dt_row, dt_row, toks, toks],
                     (of, of_r, dmid, dmid_r, dt, dt_r, h, h_r), PROJ, first_row, RING_ROWS)


NB, NS = 5, 6
CH = RING_ROWS // (NB * FOUR)
SB, LF = CH // FOUR, CH // 16
RS = 9
LAST = RS + RS
ADD_ROWS = 96


def ring_body(g_ref, *refs):
    gains, refs = refs[:FOUR], refs[FOUR:]
    (f_ref, lnout_ref, bufa, bufb, bufc, gath, stage, lnbuf, ssem, rsem, psem, qsem, csem, stsem, lns, lnr) = refs
    core, partner = core_and_partner()
    zy = lax.axis_index('zy')
    pos = (lax.axis_index('sp'), lax.rem(zy, FOUR), zy // FOUR)
    streams = [(c, sg) for c in range(THREE) for sg in (ONE, -ONE)]
    bufs, sizes = (bufa, bufb, bufc), (CH, SB, LF)
    peers = range(ONE, FOUR)

    def mod4(v):
        return lax.rem(v + 8, FOUR)

    def at(axis, val):
        if axis == ZERO:
            return {'sp': val}
        yz = (val, pos[TWO]) if axis == ONE else (pos[ONE], val)
        return {'zy': yz[ONE] * FOUR + yz[ZERO]}

    def shifted(axis, d):
        return at(axis, mod4(pos[axis] + d))

    def axis_of(s, ph):
        return (streams[s][ZERO] + ph) % THREE

    def idx(s, ph, t):
        return mod4(pos[axis_of(s, ph)] - streams[s][ONE] * t)

    def own(s, ph):
        return idx(s, ph, -ONE)

    def base(b):
        return b * (FOUR * CH)

    bar = pltpu.get_barrier_semaphore()
    for ax in range(THREE):
        for d in peers:
            pl.semaphore_signal(bar, inc=ONE, device_id=shifted(ax, d), device_id_type=MESH)
    pl.semaphore_signal(bar, inc=ONE, device_id=partner, device_id_type=MESH)
    pl.semaphore_wait(bar, 10)

    def rows(ref, start, n):
        return ref.at[pl.ds(pl.multiple_of(start, LF), n)]

    def grows(s, start, n):
        return g_ref.at[pl.ds(pl.multiple_of(start, LF), n), LANE * s:LANE * s + LANE]

    def frows(s, start, n):
        return f_ref.at[core, pl.ds(pl.multiple_of(start, LF), n), LANE * s:LANE * s + LANE]

    def same_bytes(b, k):
        if k < RS:
            return bufs[k // THREE].at[b, k % THREE]
        n = sizes[TWO - (k - RS) // THREE]
        return gath.at[b] if n == CH else gath.at[b, :, pl.ds(ZERO, n)]

    def wait_for(ref, sem):
        pltpu.make_async_copy(ref, ref, sem).wait()

    def send(b, s, k):
        ph = k // THREE if k < RS else TWO - (k - RS) // THREE
        t = k % THREE
        n = sizes[ph]
        if k < RS:
            dst = bufs[ph].at[b, t, s]
            if t:
                src = bufs[ph].at[b, t - ONE, s]
            elif ph:
                src = rows(bufs[ph - ONE].at[b, TWO, s], idx(s, ph, ZERO) * n, n)
            else:
                src = grows(s, base(b) + idx(s, ZERO, ZERO) * n, n)
        elif ph:
            off = own(s, ONE) * SB if ph == TWO else ZERO
            src = dst = rows(gath.at[b, s], off + idx(s, ph, t - ONE) * n, n)
        else:
            dst = frows(s, base(b) + idx(s, ZERO, t - ONE) * n, n)
            src = dst if t else gath.at[b, s]
        pltpu.make_async_remote_copy(src_ref=src, dst_ref=dst, send_sem=ssem.at[b, k], recv_sem=rsem.at[b, k],
                                     device_id=shifted(axis_of(s, ph), streams[s][ONE]), device_id_type=MESH).start()

    def stage_load(n):
        t, b, slot = n // NB, lax.rem(n, NB), lax.rem(n, TWO)
        for s in range(NS):
            pltpu.make_async_copy(grows(s, base(b) + idx(s, ZERO, t + ONE) * CH, CH), stage.at[slot, s],
                                  stsem.at[slot]).start()

    def ln_copy(ph, d):
        return pltpu.make_async_remote_copy(
            src_ref=lnbuf.at[ph, THREE], dst_ref=lnbuf.at[ph, d - ONE], send_sem=lns.at[ph, d - ONE],
            recv_sem=lnr.at[ph, d - ONE], device_id=shifted(ph, d) if ph < THREE else partner, device_id_type=MESH)

    def ln_sum(ph):
        vals = [lnbuf[ph, THREE]] + [lnbuf[ph, d - ONE] for d in peers]
        total = jnp.zeros_like(vals[ZERO])
        for p in range(FOUR):
            term = vals[ZERO]
            for d in peers:
                term = jnp.where(mod4(pos[ph] - d) == p, vals[d], term)
            total = total + term
        return total

    def batches(fn, start=ZERO):
        def body(b, c):
            fn(b)
            return c
        lax.fori_loop(start, NB, body, ZERO)

    def first(b):
        for s in range(NS):
            send(b, s, ZERO)

    lnbuf[ZERO, THREE] = jnp.zeros(lnout_ref.shape, F32)
    for n, gain in enumerate(gains):
        lnbuf[ZERO, THREE, n:n + ONE] = gain[...]
    first(ZERO)
    stage_load(jnp.int32(ZERO))
    for d in peers:
        ln_copy(ZERO, d).start()
    batches(first, ONE)

    for k in range(RS):
        ph, t = k // THREE, k % THREE
        buf, size = bufs[ph], sizes[ph]

        def step(b, k=k, ph=ph, t=t, buf=buf, size=size):
            n = k * NB + b
            slot = lax.rem(n, TWO)
            if not ph:
                @pl.when(n < THREE * NB - ONE)
                def _():
                    stage_load(n + ONE)
                wait_for(stage.at[slot], stsem.at[slot])
            wait_for(same_bytes(b, k), rsem.at[b, k])
            for s in range(NS):
                if ph:
                    off = pl.multiple_of(idx(s, ph, t + ONE) * size, LF)
                    buf[b, t, s] += bufs[ph - ONE][b, TWO, s, pl.ds(off, size)]
                else:
                    @pl.loop(ZERO, CH, step=ADD_ROWS)
                    def _(r):
                        at_r = pl.ds(pl.multiple_of(r, ADD_ROWS), ADD_ROWS)
                        buf[b, t, s, at_r] += stage[slot, s, at_r]
                if k == RS - ONE:
                    off = pl.multiple_of(own(s, ONE) * SB + own(s, TWO) * LF, LF)
                    gath[b, s, pl.ds(off, LF)] = bufc[b, TWO, s]
                send(b, s, k + ONE)

        batches(step)
        if k < SIX and k % TWO == ZERO:
            lp = k // TWO
            for d in peers:
                ln_copy(lp, d).wait()
            lnbuf[lp + ONE, THREE] = ln_sum(lp)
            for d in peers if lp < TWO else (ONE,):
                ln_copy(lp + ONE, d).start()

    def hand_over(b, s, j, src, start):
        pltpu.make_async_remote_copy(src_ref=src, dst_ref=frows(s, start, CH), send_sem=psem.at[b, j], recv_sem=qsem.at[b, j],
                                     device_id=partner, device_id_type=MESH).start()

    for k in range(RS, LAST):
        def step(b, k=k):
            wait_for(same_bytes(b, k), rsem.at[b, k])
            piece = k - (LAST - FOUR)
            for s in range(NS):
                if k < LAST - ONE:
                    send(b, s, k + ONE)
                if piece >= ZERO:
                    start = base(b) + idx(s, ZERO, piece - ONE) * CH
                    if piece:
                        hand_over(b, s, piece, frows(s, start, CH), start)
                    else:
                        pltpu.make_async_copy(gath.at[b, s], frows(s, start, CH), csem.at[b]).start()
                        hand_over(b, s, piece, gath.at[b, s], start)
        batches(step)

    ln_copy(THREE, ONE).wait()
    lnout_ref[...] = lnbuf[THREE, THREE] + lnbuf[THREE, ZERO]

    def finish(b):
        for k in range(LAST):
            wait_for(same_bytes(b, k), ssem.at[b, k])
        for j in range(FOUR):
            wait_for(gath.at[b], psem.at[b, j])
            wait_for(gath.at[b], qsem.at[b, j])
        wait_for(gath.at[b], csem.at[b])
    batches(finish)


def ring_all_reduce(g, gains, cid):
    vmem = pl.BlockSpec(memory_space=pltpu.VMEM)
    ln = sds((8, DM), F32)
    return pl.pallas_call(
        ring_body,
        in_specs=[ANY] + [vmem] * FOUR,
        out_specs=[ANY, vmem],
        out_shape=[sds((TWO, RING_ROWS, DM), F32), ln],
        scratch_shapes=[
            pltpu.VMEM((NB, THREE, NS, CH, LANE), F32), pltpu.VMEM((NB, THREE, NS, SB, LANE), F32),
            pltpu.VMEM((NB, THREE, NS, LF, LANE), F32), pltpu.VMEM((NB, NS, CH, LANE), F32),
            pltpu.VMEM((TWO, NS, CH, LANE), F32),
            pltpu.VMEM((FOUR, FOUR) + ln.shape, F32),
            DMA((NB, LAST)), DMA((NB, LAST)), DMA((NB, FOUR)), DMA((NB, FOUR)), DMA((NB,)), DMA((TWO,)),
            DMA((FOUR, THREE)), DMA((FOUR, THREE)),
        ],
        compiler_params=pltpu.CompilerParams(collective_id=cid, has_side_effects=True, vmem_limit_bytes=60 * MIB),
        cost_estimate=pl.CostEstimate(flops=MIB * MIB // FOUR, bytes_accessed=200 * MIB, transcendentals=ZERO),
        name="ring_all_reduce",
    )(g, *gains)


SLOTS, LAG = 8, 4
NTURN = TWO * THREE
OUT_SHAPE, IN_SHAPE = (TWO, FF, DM), (TWO, DM, TWO * FF)


def stream(pieces, buf, turned, isem, osem, between=None):
    def loads(i):
        slot, srcs = i % SLOTS, pieces[i][ZERO]
        n = srcs[ZERO].shape[ZERO]
        return [pltpu.make_async_copy(src, buf.at[slot, k * n:k * n + n], isem.at[slot, k]) for k, src in enumerate(srcs)]

    def store(i):
        _, dst, turn = pieces[i]
        src = buf.at[i % SLOTS, :dst.shape[ZERO]] if turn is None else turned.at[turn]
        return pltpu.make_async_copy(src, dst, osem.at[i % SLOTS])

    total = len(pieces)
    for i in range(total + LAG):
        if i == SLOTS and between:
            between()
        if i < total:
            if i >= SLOTS:
                store(i - SLOTS).wait()
            for cp in loads(i):
                cp.start()
        k = i - LAG
        if k >= ZERO:
            for cp in loads(k):
                cp.wait()
            turn = pieces[k][TWO]
            if turn is not None:
                for n in CHUNKS:
                    rows, col = LANE * n, RB * n
                    turned[turn, :, col:col + LANE] = buf[k % SLOTS, rows:rows + LANE].T
                    turned[turn, :, col + LANE:col + RB] = buf[k % SLOTS, PROJ + rows:PROJ + rows + LANE].T
            store(k).start()
    for i in range(max(total - SLOTS, ZERO), total):
        store(i).wait()


def unpack_ring_body(f, y_in, dx_in, gains, g_qkv, g_proj, g_in, g_out, y, dx, g_attn, g_mlp, y_s, dx_s, *scratch):
    small_in, small_out, *scratch = scratch
    loads = [pltpu.make_async_copy(src, dst, small_in.at[n]) for n, (src, dst) in enumerate(((y_in, y_s), (dx_in, dx_s)))]
    stores = [pltpu.make_async_copy(src, dst, small_out.at[n]) for n, (src, dst) in enumerate(((y_s, y), (dx_s, dx)))]
    start_all(loads)
    g_attn[...] = gains[:TWO]
    g_mlp[...] = gains[TWO:FOUR]

    def between():
        wait_all(loads)
        start_all(stores)

    def block(c, row, n=DM):
        return f.at[c, row:row + n]

    pieces = []
    for c in range(TWO):
        for n in range(NDOWN):
            pieces.append(([block(c, ATT_ROWS + DM * n)], g_out.at[ZERO, DOWN * c + DM * n:DOWN * c + DM * n + DM], None))
        for n in range(FOUR):
            col = UP * c + DM * n
            pieces.append(([block(c, ATT_ROWS + DOWN + DM * n)], g_in.at[ZERO, :, col:col + DM], None))
    for l in range(TWO):
        first = (ONE - l) * (ATT_ROWS + MLP_ROWS)
        for n in range(THREE):
            row = first + PROJ * (n + ONE)
            pieces.append(([block(c, row, PROJ) for c in range(TWO)], g_qkv.at[l, :, DM * n:DM * n + DM], THREE * l + n))
        for c in range(TWO):
            pieces.append(([block(c, first, PROJ)], g_proj.at[l, PROJ * c:PROJ * c + PROJ], None))
    stream(pieces, *scratch, between=between)
    wait_all(stores)


def unpack_mlp_body(own, other, in_0, out_0, g_in, g_out, *scratch):
    core = lax.axis_index('core')
    pieces = []
    for src, side in ((own, core), (other, ONE - core)):
        for n in range(NDOWN):
            row = pl.multiple_of(DOWN * side + DM * n, DM)
            pieces.append(([src.at[DM * n:DM * n + DM]], g_out.at[ONE, pl.ds(row, DM)], None))
        for n in range(FOUR):
            col = pl.multiple_of(UP * side + DM * n, DM)
            pieces.append(([src.at[DOWN + DM * n:DOWN + DM * n + DM]], g_in.at[ONE, :, pl.ds(col, DM)], None))
    stream(pieces, *scratch)


def unpack_call(body, args, outs, alias, name, in_specs=None, out_specs=None, small=()):
    return pl.pallas_call(
        body, in_specs=in_specs or [ANY] * len(args), out_specs=out_specs or [ANY] * len(outs), out_shape=outs,
        scratch_shapes=list(small) + [pltpu.VMEM((SLOTS, DM, DM), F32), pltpu.VMEM((NTURN, DM, DM), F32),
                                      DMA((SLOTS, TWO)), DMA((SLOTS,))],
        input_output_aliases=alias,
        compiler_params=pltpu.CompilerParams(vmem_limit_bytes=60 * MIB),
        cost_estimate=pl.CostEstimate(flops=MIB * MIB // RB, bytes_accessed=75 * MIB, transcendentals=ZERO), name=name,
    )(*args)


def rope_tables(pos, base):
    inv_freq = base ** (jnp.arange(HALF).astype(F32) * (-TWO / HEAD))
    angles = inv_freq[:, None] * pos.astype(F32)[None, :]
    return jnp.cos(angles), jnp.sin(angles)


def solution(mesh):
    n_sp = mesh.shape['sp']
    by_core = mesh.devices.reshape(n_sp, mesh.shape['dp'] // TWO, TWO)
    mesh = Mesh(by_core, ('sp', 'zy', 'core'))
    dp_axes = ('zy', 'core')
    row_axes = dp_axes + ('sp',)
    token_spec = P(row_axes, None)
    swap_cores = [(ZERO, ONE), (ONE, ZERO)]
    cids = list(range(RS))

    def exchange(arr):
        return lax.all_to_all(arr, 'sp', ZERO, ZERO, tiled=True)

    def device_step(x_loc, cu_loc, pos_loc, w_qkv, w_proj, w_in, w_out, ln_attn, ln_mlp, d_out):
        tab0, tab1 = [rope_tables(pos_loc, base) for base in BASES]
        mlp_args, w_mlp = (w_proj, ln_mlp), (w_in, w_out)

        q0, f0, q1 = run("layer0_qkv1", cids[ONE], row_peers, group_fwd_stage(cu_loc, ln_attn, w_qkv, tab0, x_loc),
                         mlp_stage(ZERO, True, False, *mlp_args, *w_mlp, links={'o': (ZERO, 'o_r')}, x=x_loc),
                         qkv_fwd_stage(ONE, ln_attn, w_qkv, tab1, (ONE, 'y')))
        kv_edges = (q1.left, q1.right)
        a1, f1, s1 = run("attn1_mlp1", cids[TWO], near_peers, attn1_fwd_stage(cu_loc, q1.out, *kv_edges),
                         mlp_stage(ONE, True, True, *mlp_args, *w_mlp, links={'o': (ZERO, 'o')}, x=f0.y, dy=d_out),
                         side_grad_stage(q1.out))
        g_side = lax.psum(s1.out, ('sp', 'zy'))
        far = [getattr(s1, n) for n in FAR]
        _, t1, b0 = run("attn1_qkv1_mlp0", cids[5], row_peers,
                        attn1_bwd_stage(cu_loc, q1.out, f1.d_o, a1.lse, f1.delta, kv_edges, far),
                        qkv_bwd_stage(ONE, tab1, w_qkv, f0.y, ln_attn, f1.dmid, link=(ZERO, 'out')),
                        mlp_stage(ZERO, False, True, *mlp_args, *w_mlp, links={'dy': (ONE, 'dx')}, x1=f0.x1_m, u=f0.u))
        dqkv0 = exchange(attn0_bwd(cu_loc, q0.out, q0.o_m, b0.d_o, q0.lse))
        grads = grad_att(None, f1.of_m, f1.of_r, f1.dmid, f1.dmid_r, t1.dt_m, t1.dt_r, q1.h_m, q1.h_r, ZERO)
        grads = grad_mlp(grads, f0.m_m, f0.m_r, t1.dx, b0.dy_r, f0.h_m, f0.h_r, b0.du_m, b0.du_r, ATT_ROWS, RING_ROWS)
        t0, = run("qkv0_grads", cids[SIX], partner_peer, qkv_bwd_stage(
            ZERO, tab0, w_qkv, x_loc, ln_attn, b0.dmid, d=dqkv0, grads=grads,
            pairs=(q0.h_m, q0.h_r, f0.of_m, f0.of_r, b0.dmid, b0.dmid_r)))

        gains = (t0.gg, t1.gg, b0.gg, f1.gg)
        summed, gains = ring_all_reduce(t0.out, gains, cids[ZERO])
        summed, g_side = lax.optimization_barrier((summed, g_side))
        from_partner = lax.ppermute(g_side, 'core', swap_cores)
        shapes = [sds(shape, F32) for shape in ((TWO, DM, THREE * DM), (TWO, DM, DM), IN_SHAPE, OUT_SHAPE)]
        vmem = pl.BlockSpec(memory_space=pltpu.VMEM)
        gain = sds((TWO, DM), F32)
        g_qkv, g_proj, g_in, g_out, y, dx, g_attn, g_mlp = unpack_call(
            unpack_ring_body, (summed, f1.y, t0.dx, gains), shapes + [TOKS, TOKS, gain, gain], {}, "unpack_ring",
            [ANY] * THREE + [vmem], [ANY] * SIX + [vmem] * TWO, [TOK_VMEM, TOK_VMEM, DMA((TWO,)), DMA((TWO,))])
        g_in, g_out = unpack_call(unpack_mlp_body, (g_side, from_partner, g_in, g_out), shapes[TWO:],
                                  {TWO: ZERO, THREE: ONE}, "unpack_mlp")
        return y, dx, g_qkv, g_proj, g_in, g_out, g_attn, g_mlp

    in_specs = (token_spec, P(dp_axes, None), P(row_axes)) + (P(),) * SIX + (token_spec,)
    out_specs = (token_spec, token_spec) + (P(),) * SIX
    return jax.shard_map(device_step, mesh=mesh, in_specs=in_specs, out_specs=out_specs, check_vma=False)
```

```python
import functools
import math
import jax
import jax.numpy as jnp
from jax import lax
from jax.experimental import pallas as pl
from jax.experimental.pallas import tpu as pltpu
from jax.sharding import Mesh, PartitionSpec as P

ZERO, ONE, TWO, THREE, FOUR = range(5)
SIX, TWELVE = 6, 12
HEAD = 64
HALF = 32
NHEAD = 12
DM = 768
FF = 3072
TOK = 512
GRP = 2048
WIN = 64
NDOC = 8
LANE = 128
EPS = 1e-5
NEG = -1e30
SCALE = 0.125
BASES = (160000.0, 10000.0)
F32 = jnp.float32
BF = jnp.bfloat16
QT = 256
FT = 768
NFT = FF // FT
QTILES = GRP // QT
MIB = 1024 * 1024
ALLTOK = (TOK, DM)
ALLDM = (DM, DM)
PROJ = DM // 2
DOWN = FF // 2
UP = FF
QKV = 3 * PROJ
MLP_ROWS = DOWN + UP
ATT_ROWS = PROJ + QKV
RING_ROWS = 2 * ATT_ROWS + MLP_ROWS
ANY = pl.BlockSpec(memory_space=pl.ANY)
DMA = pltpu.SemaphoreType.DMA
MESH = pl.DeviceIdType.MESH


def dot(a, b, ca, cb):
    return lax.dot_general(a, b, (((ca,), (cb,)), ((), ())), preferred_element_type=F32)


def mm(a, b):
    return dot(a, b, ONE, ZERO)


def mm_nt(a, b):
    return dot(a, b, ONE, ONE)


def mm_tn(a, b):
    return dot(a, b, ZERO, ZERO)


def call(body, grid, in_specs, out_specs, out_shape, scratch=(), prefetch=ZERO, flops=ZERO, nbytes=ZERO, name=None,
         cid=None, alias=None):
    extra = {} if cid is None else dict(collective_id=cid, has_side_effects=True)
    return pl.pallas_call(
        body,
        grid_spec=pltpu.PrefetchScalarGridSpec(
            num_scalar_prefetch=prefetch, grid=grid, in_specs=in_specs, out_specs=out_specs, scratch_shapes=scratch),
        out_shape=out_shape,
        input_output_aliases=alias or {},
        compiler_params=pltpu.CompilerParams(vmem_limit_bytes=60 * MIB, **extra),
        cost_estimate=pl.CostEstimate(flops=int(flops), bytes_accessed=int(nbytes), transcendentals=ZERO),
        name=name,
    )


def sds(shape, dtype):
    return jax.ShapeDtypeStruct(shape, dtype)


def spec(shape, *idx):
    idx = idx or (ZERO,) * len(shape)
    return pl.BlockSpec(shape, lambda *g: tuple(i(*g) if callable(i) else i for i in idx))


def step_of(s, *_):
    return s


def core_and_partner():
    core = lax.axis_index('core')
    return core, {'core': ONE - core}


def greet(devices):
    for dev in devices:
        pl.semaphore_signal(pltpu.get_barrier_semaphore(), inc=ONE, device_id=dev, device_id_type=MESH)


def all_here(devices):
    pl.semaphore_wait(pltpu.get_barrier_semaphore(), len(devices))


def sp_peer(d):
    return lax.rem(lax.axis_index('sp') + d, FOUR)


PEERS = range(ONE, FOUR)


class Swaps:
    def __init__(self, ssem, rsem, lsem):
        self.sems, self.waits, self.n = (ssem, rsem, lsem), [], ZERO
        self.core, self.partner = core_and_partner()
        self.other = ONE - self.core
        self.me = lax.axis_index('sp')

    def remote(self, src, dst, dev=None):
        ssem, rsem, _ = self.sems
        return self.later(pltpu.make_async_remote_copy(
            src_ref=src, dst_ref=dst, send_sem=ssem.at[self.n], recv_sem=rsem.at[self.n],
            device_id=self.partner if dev is None else dev, device_id_type=MESH))

    def local(self, src, dst):
        return self.later(pltpu.make_async_copy(src, dst, self.sems[TWO].at[self.n]))

    def later(self, cp):
        self.n += ONE
        self.waits.append(cp)
        return cp

    def to_all(self, src_of, dst_of):
        return [self.remote(src_of(sp_peer(d)), dst_of(self.me), {'sp': sp_peer(d)}) for d in PEERS] + [
            self.local(src_of(self.me), dst_of(self.me))]

    def to_sides(self, left_src, right_src, from_left, from_right):
        return [self.remote(right_src, from_left, {'sp': sp_peer(ONE)}), self.remote(left_src, from_right, {'sp': sp_peer(THREE)})]

    def early(self, some):
        gone = {id(cp) for cp in some}
        self.waits = [cp for cp in self.waits if id(cp) not in gone]
        return some

    def wait(self):
        for cp in self.waits:
            cp.wait()


def start_all(copies):
    for cp in copies:
        cp.start()


def wait_all(copies):
    for cp in copies:
        cp.wait()


def row_peers():
    return [core_and_partner()[ONE]] + [{'sp': sp_peer(d)} for d in PEERS]


def side_peers():
    return [{'sp': sp_peer(ONE)}, {'sp': sp_peer(THREE)}]


def partner_peer():
    return [core_and_partner()[ONE]]


def near_peers():
    return partner_peer() + side_peers()


def swap_sems(n):
    return [DMA((n,))] * THREE


def named_sems(n):
    return list(zip(('ssem', 'rsem', 'lsem'), swap_sems(n)))


class Refs:
    def __init__(self, named):
        self.__dict__.update(named)


class Stage:
    def __init__(self, body, steps, ins, outs, scratch, copies=None, links=None, alias=()):
        self.body, self.steps, self.ins, self.outs, self.scratch = body, steps, ins, outs, scratch
        self.copies, self.links, self.alias = copies, links or {}, alias


def shifted(block, first, steps):
    if block.index_map is None:
        return block
    return pl.BlockSpec(block.block_shape, lambda g: block.index_map(jnp.clip(g - first, ZERO, steps - ONE)))


def run(name, cid, peers, *stages):
    firsts = [sum(st.steps for st in stages[:k]) for k in range(len(stages))]

    def flat(kind):
        return [(k, entry) for k, st in enumerate(stages) for entry in getattr(st, kind)]

    ins, outs, scratch = flat('ins'), flat('outs'), flat('scratch')
    keys = [(k, entry[ZERO]) for k, entry in ins + outs + scratch]

    def body(*refs):
        pid = pl.program_id(ZERO)
        have = dict(zip(keys, refs))

        @pl.when(pid == ZERO)
        def _():
            greet(peers())

        talking = [k for k, st in enumerate(stages) if st.copies]
        views = []
        for k, st in enumerate(stages):
            r = Refs({n: ref for (at, n), ref in have.items() if at == k})
            for n, source in st.links.items():
                setattr(r, n, have[source])
            r.arrive = lambda k=k: all_here(peers()) if k == talking[ZERO] else None
            views.append(r)

            @pl.when((pid >= firsts[k]) & (pid < firsts[k] + st.steps))
            def _(st=st, r=r, k=k):
                st.body(r, pid - firsts[k])

        @pl.when(pid == firsts[-ONE] + stages[-ONE].steps - ONE)
        def _():
            for k in talking:
                stages[k].copies(views[k]).sw.wait()

    def placed(entries):
        return [shifted(entry[TWO], firsts[k], stages[k].steps) for k, entry in entries]

    alias = {[e[ZERO] for _, e in ins].index(a): [e[ZERO] for _, e in outs].index(b) for st in stages for a, b in st.alias}
    got = call(body, (sum(st.steps for st in stages),), placed(ins), placed(outs), [e[ONE] for _, e in outs],
               scratch=[e[ONE] for _, e in scratch], flops=16 * TOK * DM * FF, nbytes=30 * MIB, name=name, cid=cid,
               alias=alias)(*[e[ONE] for _, e in ins])
    out = [{} for _ in stages]
    for (k, e), arr in zip(outs, got):
        out[k][e[ZERO]] = arr
    return [Refs(named) for named in out]


def norm_parts(x_bf):
    rows = x_bf.astype(F32)
    cen = rows - jnp.mean(rows, axis=ONE, keepdims=True)
    var = jnp.mean(cen * cen, axis=ONE, keepdims=True)
    return cen, lax.rsqrt(var + EPS)


def norm_rows(x_bf, gain):
    cen, inv = norm_parts(x_bf)
    return (cen * inv * gain).astype(BF)


def norm_rows_grad(x_bf, gain, d_bf):
    cen, inv = norm_parts(x_bf)
    hat = cen * inv
    d_out = d_bf.astype(F32)
    g_gain = jnp.sum(d_out * hat, axis=ZERO, keepdims=True)
    d_hat = d_out * gain
    d_x = inv * (d_hat - jnp.mean(d_hat, axis=ONE, keepdims=True) - hat * jnp.mean(d_hat * hat, axis=ONE, keepdims=True))
    return d_x.astype(BF), g_gain


def add_bf(a, b):
    return (a.astype(F32) + b.astype(F32)).astype(BF)


RB = 256
ROPED = 6
CHUNKS = range(DM // RB)


def head_rows(ref, chunk, head):
    return ref.at[head, ZERO, chunk] if ref.shape[ZERO] == FOUR else ref.at[ZERO, chunk, head]


def weight_cols(layer, width, first=ZERO):
    return spec((None, DM, width), layer, ZERO, lambda s: first + s)


GAINS = spec((TWO, DM))


GROUP_QKV = (FOUR, THREE, THREE, HEAD, TOK)
OWN_QKV = (THREE * NHEAD, HEAD, TOK)
EDGE = (NHEAD, HEAD, LANE)
TOKS = jax.ShapeDtypeStruct(ALLTOK, BF)
TOK_SPEC = spec(ALLTOK)
TOK_VMEM = pltpu.VMEM(ALLTOK, BF)
TABLE = spec((HALF, TOK))
CU_SPEC = pl.BlockSpec(memory_space=pltpu.SMEM)


def rotated(a, b, r):
    cos, sin = r.cos[...], r.sin[...]
    return a * cos - b * sin, b * cos + a * sin


def qkv_chunk(r, w):
    return mm(r.h[...], w).astype(BF).astype(F32).T


def head_halves(t_rows, head):
    at = HEAD * head
    return t_rows[at:at + HALF], t_rows[at + HALF:at + HEAD]


def qkv_fwd_copies(r):
    sw = Swaps(r.ssem, r.rsem, r.lsem)
    return Refs(dict(sw=sw, start=[sw.remote(r.h, r.h_r), sw.local(r.h, r.h_m)],
                     edges=sw.to_sides(r.edge_s.at[ZERO], r.edge_s.at[ONE], r.left, r.right)))


def qkv_fwd_body(r, step, layer):
    cps = qkv_fwd_copies(r)

    @pl.when(step == ZERO)
    def _():
        r.h[...] = norm_rows(r.x[...], r.g[layer:layer + ONE])
        r.arrive()
        start_all(cps.start)

    for p in range(THREE):
        @pl.when(step == KVQ.index(p))
        def _(p=p):
            for chunk in CHUNKS:
                t_rows = qkv_chunk(r, r.w[:, RB * chunk:RB * chunk + RB])
                for head in range(FOUR):
                    a, b = head_halves(t_rows, head)
                    if p < TWO:
                        a, b = rotated(a, b, r)
                    n = FOUR * chunk + head
                    out = r.out.at[n]
                    out[:HALF] = a.astype(BF)
                    out[HALF:] = b.astype(BF)
                    if p:
                        lane = WIN * (p - ONE)
                        blk = out[...]
                        r.edge_s[ZERO, n, :, lane:lane + WIN] = blk[:, :WIN]
                        r.edge_s[ONE, n, :, lane:lane + WIN] = blk[:, TOK - WIN:]
            if p == TWO:
                start_all(cps.edges)


KVQ = (ONE, TWO, ZERO)


def kvq_part(s, *_):
    return (s + ONE) % THREE


def qkv_fwd_stage(layer, gain, w_qkv, tables, link):
    ins = [('g', gain, GAINS), ('w', w_qkv, spec((None, DM, DM), layer, ZERO, kvq_part)), ('cos', tables[ZERO], TABLE), ('sin', tables[ONE], TABLE)]
    outs = [('h_m', TOKS, ANY), ('h_r', TOKS, ANY), ('out', sds(OWN_QKV, BF), spec((NHEAD, HEAD, TOK), kvq_part, ZERO, ZERO)),
            ('left', sds(EDGE, BF), ANY), ('right', sds(EDGE, BF), ANY)]
    scratch = [('h', TOK_VMEM), ('edge_s', pltpu.VMEM((TWO,) + EDGE, BF))]
    return Stage(functools.partial(qkv_fwd_body, layer=layer), THREE, ins, outs, scratch + named_sems(FOUR),
                 qkv_fwd_copies, {'x': link})


def tile_src(i, *_):
    return i // TWO


def tile_side(i, *_):
    return i % TWO


Q_SPEC = spec((ONE, ONE, THREE, HEAD, QT), tile_src, ZERO, ZERO, ZERO, tile_side)
O_SPEC = spec((ONE, THREE, HEAD, QT), tile_src, ZERO, ZERO, tile_side)
STAT_SPEC = spec((8, QT), ZERO, step_of)


def kv_spec(part):
    return spec((FOUR, ONE, THREE, HEAD, TOK), ZERO, part, ZERO, ZERO, ZERO)


def key_tile(kt):
    return kt // TWO, pl.ds(pl.multiple_of((kt % TWO) * QT, QT), QT)


def key_rows(dst, k_ref):
    for src in range(FOUR):
        for h in range(THREE):
            dst[h, TOK * src:TOK * src + TOK] = k_ref[src, ZERO, h].T


def row_tile(kt):
    return pl.ds(pl.multiple_of(kt * QT, QT), QT)


def since(pos, start):
    return (pos - start).astype(jnp.uint32)


def doc_start(cu_ref, tok):
    start = jnp.zeros_like(tok)
    for d in range(ONE, NDOC):
        start = jnp.where(cu_ref[ZERO, d] <= tok, cu_ref[ZERO, d], start)
    return start


def doc_stop(cu_ref, tok):
    stop = jnp.full_like(tok, GRP)
    for d in range(NDOC - ONE, ZERO, -ONE):
        stop = jnp.where(cu_ref[ZERO, d] > tok, cu_ref[ZERO, d], stop)
    return stop


def tile_bounds(cu_ref, tile):
    first = tile * QT
    tok = lax.broadcasted_iota(jnp.int32, (ONE, QT), ONE) + first
    lo = doc_start(cu_ref, first) // QT
    hi = (doc_stop(cu_ref, first + QT - ONE) + QT - ONE) // QT
    return lo, hi, doc_start(cu_ref, tok), doc_stop(cu_ref, tok)


BY_OWNER = (FOUR, THREE, HEAD, TOK)


def group_copies(r):
    sw = Swaps(r.ssem, r.rsem, r.lsem)

    def head_parts(c):
        return [cp for p in range(THREE) for cp in sw.to_all(lambda dev: r.out_s.at[p, dev, c], lambda dev: r.got.at[dev, p, c])]

    start = [sw.remote(r.h, r.h_r), sw.local(r.h, r.h_m)]
    parts = [sw.early(head_parts(c)) for c in range(THREE)]
    heads = [sw.early(sw.to_all(lambda dev: r.o_s.at[dev, c], lambda dev: r.o_r.at[dev, c])) for c in range(THREE)]
    return Refs(dict(sw=sw, start=start, parts=parts, heads=heads, keep=[sw.local(r.got, r.out), sw.local(r.o_s, r.o_m)]))


def group_fwd_body(r, step):
    cps = group_copies(r)
    tiles = range(QTILES)

    @pl.when(step == ZERO)
    def _():
        r.h[...] = norm_rows(r.x[...], r.g[:ONE])
        r.arrive()
        start_all(cps.start)

    for c in range(THREE):
        @pl.when(step == c)
        def _(c=c):
            for p, w in enumerate((r.wq, r.wk, r.wv)):
                t_rows = qkv_chunk(r, w[...])
                for head in range(FOUR):
                    a, b = head_halves(t_rows, head)
                    if p < TWO:
                        a, b = rotated(a, b, r)
                    out = r.out_s.at[p, head, c]
                    out[:HALF] = a.astype(BF)
                    out[HALF:] = b.astype(BF)
            start_all(cps.parts[c])

        @pl.when(step == c + THREE)
        def _(c=c):
            wait_all(cps.parts[c])
            for src in range(FOUR):
                r.kr_s[TOK * src:TOK * src + TOK] = r.got[src, ONE, c].T
            io = lax.broadcasted_iota(jnp.int32, (QT, QT), ZERO)

            def q_pair(n, carry):
                src = sp_peer(n + ONE)
                pair = range(TWO)
                cols = [slice(QT * a, QT * a + QT) for a in pair]
                toks = [lax.broadcasted_iota(jnp.int32, (ONE, QT), ONE) + src * TOK + QT * a for a in pair]
                st, en = [doc_start(r.cu, tok) for tok in toks], [doc_stop(r.cu, tok) for tok in toks]
                for a in pair:
                    q_t = r.got[src, ZERO, c, :, cols[a]] * SCALE
                    for k in tiles:
                        r.s_s[a, k] = mm(r.kr_s[QT * k:QT * k + QT], q_t)
                top, total = [], []
                size = [(en[a] - st[a]).astype(jnp.uint32) for a in pair]
                for a in pair:
                    m = jnp.full((ONE, QT), NEG, F32)
                    for k in tiles:
                        s = jnp.where(since(io, st[a] - QT * k) < size[a], r.s_s[a, k], NEG)
                        r.s_s[a, k] = s
                        m = jnp.maximum(m, jnp.max(s, axis=ZERO, keepdims=True))
                    top.append(m)
                for a in pair:
                    part = jnp.zeros((ONE, QT), F32)
                    for k in tiles:
                        p = jnp.exp(r.s_s[a, k] - top[a])
                        part += jnp.sum(p, axis=ZERO, keepdims=True)
                        r.p_s[a, QT * k:QT * k + QT] = p.astype(BF)
                    total.append(part)
                for a in pair:
                    acc = jnp.zeros((HEAD, QT), F32)
                    for k in range(FOUR):
                        acc += mm(r.got[k, TWO, c], r.p_s[a, TOK * k:TOK * k + TOK])
                    r.o_s[src, c, :, cols[a]] = (acc / total[a]).astype(BF)
                    r.lse[c:c + ONE, row_tile(TWO * src + a)] = top[a] + jnp.log(total[a])
                for k, cp in enumerate(cps.heads[c]):
                    @pl.when(n == k)
                    def _(cp=cp):
                        cp.start()
                return carry

            lax.fori_loop(ZERO, FOUR, q_pair, ZERO)

    @pl.when(step == ROPED - ONE)
    def _():
        start_all(cps.keep)
        for c in range(THREE):
            wait_all(cps.heads[c])


def group_fwd_stage(cu, gain, w_qkv, tables, x):
    part = lambda p: spec((None, DM, RB), ZERO, ZERO, lambda s: THREE * p + jnp.minimum(s, TWO))
    ins = [('cu', cu, CU_SPEC), ('g', gain, GAINS), ('wq', w_qkv, part(ZERO)), ('wk', w_qkv, part(ONE)), ('wv', w_qkv, part(TWO)),
           ('cos', tables[ZERO], TABLE), ('sin', tables[ONE], TABLE), ('x', x, TOK_SPEC)]
    outs = [('h_m', TOKS, ANY), ('h_r', TOKS, ANY), ('out', sds(GROUP_QKV, BF), ANY), ('o_m', sds(BY_OWNER, BF), ANY),
            ('lse', sds((8, GRP), F32), spec((8, GRP)))]
    owner = pltpu.VMEM(BY_OWNER, BF)
    scratch = [('h', TOK_VMEM), ('out_s', pltpu.VMEM((THREE, FOUR, THREE, HEAD, TOK), BF)), ('got', pltpu.VMEM(GROUP_QKV, BF)),
               ('kr_s', pltpu.VMEM((GRP, HEAD), BF)), ('s_s', pltpu.VMEM((TWO, QTILES, QT, QT), F32)), ('p_s', pltpu.VMEM((TWO, GRP, QT), BF)),
               ('o_s', owner), ('o_r', owner)]
    return Stage(group_fwd_body, ROPED, ins, outs, scratch + named_sems(FOUR * 16), group_copies)


def attn0_bwd_body(cu_ref, q_ref, k_ref, v_ref, o_ref, do_ref, lse_ref, out_ref,
                   dk_s, dv_s, dq_s, kr_s, vr_s, s_s, d_s, p_s, t_s):
    tile = pl.program_id(ZERO)
    first, last, st, en = tile_bounds(cu_ref, tile)
    heads = range(THREE)

    @pl.when(tile == ZERO)
    def _():
        dk_s[...] = jnp.zeros(dk_s.shape, F32)
        dv_s[...] = jnp.zeros(dv_s.shape, F32)
        key_rows(kr_s, k_ref)
        key_rows(vr_s, v_ref)

    dq_s[...] = jnp.zeros(dq_s.shape, F32)
    io = lax.broadcasted_iota(jnp.int32, (QT, QT), ZERO)
    q_t = [q_ref[ZERO, ZERO, h] * SCALE for h in heads]
    do_t = [do_ref[ZERO, h] for h in heads]
    q_rows, do_rows = [q_t[h].T for h in heads], [do_t[h].T for h in heads]
    delta = [jnp.sum(do_t[h].astype(F32) * o_ref[ZERO, h].astype(F32), axis=ZERO, keepdims=True) for h in heads]
    lse = [lse_ref[h:h + ONE] for h in heads]
    size = (en - st).astype(jnp.uint32)

    def body(kt, carry):
        base = kt * QT
        src, cols = key_tile(kt)
        rows = row_tile(kt)
        ok = since(io, st - base) < size
        for h in heads:
            s_s[h] = mm(kr_s[h, rows], q_t[h])
            d_s[h] = mm(vr_s[h, rows], do_t[h])
        for h in heads:
            p = jnp.exp(jnp.where(ok, s_s[h] - lse[h], NEG))
            p_s[h] = p.astype(BF)
            t_s[h] = (p * (d_s[h] - delta[h])).astype(BF)
        for h in heads:
            dv_s[h, rows] += mm(p_s[h], do_rows[h])
            dk_s[h, rows] += mm(t_s[h], q_rows[h])
            dq_s[h] += mm(k_ref[src, ZERO, h, :, cols], t_s[h])
        return carry

    lax.fori_loop(first, last, body, ZERO)
    src, cols = key_tile(tile)
    for h in heads:
        out_ref[src, ZERO, h, :, cols] = (dq_s[h] * SCALE).astype(BF)

    @pl.when(tile == QTILES - ONE)
    def _():
        for src in range(FOUR):
            for h in heads:
                out_ref[src, ONE, h] = dk_s[h, TOK * src:TOK * src + TOK].T.astype(BF)
                out_ref[src, TWO, h] = dv_s[h, TOK * src:TOK * src + TOK].T.astype(BF)


def attn0_bwd(cu, qkv, o_t, do_t, lse):
    acc, rows = pltpu.VMEM((THREE, GRP, HEAD), F32), pltpu.VMEM((THREE, GRP, HEAD), BF)
    sq32, sq16 = pltpu.VMEM((THREE, QT, QT), F32), pltpu.VMEM((THREE, QT, QT), BF)
    return call(
        attn0_bwd_body, (QTILES,),
        [Q_SPEC, kv_spec(ONE), kv_spec(TWO), O_SPEC, O_SPEC, STAT_SPEC],
        spec(GROUP_QKV), sds(GROUP_QKV, BF),
        scratch=[acc, acc, pltpu.VMEM((THREE, HEAD, QT), F32), rows, rows, sq32, sq32, sq16, sq16],
        prefetch=ONE, flops=30 * GRP * GRP * HEAD, nbytes=TWELVE * MIB, name="attn0_bwd",
    )(cu, qkv, qkv, qkv, o_t, do_t, lse)


NBLK = TOK // LANE
EXT = TOK + TWO * WIN
XBLK = EXT // LANE
REACH = LANE + TWO * WIN
AHEAD_FWD, AHEAD_BWD = 4, 2
HPS = 4
HSTEPS = NHEAD // HPS


def heads_of(width, part):
    return spec((HPS, HEAD, width), lambda n: HSTEPS * part + n, ZERO, ZERO)


def own_head(part):
    return heads_of(TOK, part)


def row_of(width):
    return spec((HPS, ONE, width), step_of, ZERO, ZERO)


LOW, HIGH = slice(None, WIN), slice(WIN, None)
STAT = jax.ShapeDtypeStruct((NHEAD, ONE, TOK), F32)
STAT_BLOCK = spec((NHEAD, ONE, TOK))


def joined(left, mid, right, h, left_lanes=HIGH, right_lanes=LOW):
    return jnp.concatenate([left[h][:, left_lanes], mid[h], right[h][:, right_lanes]], axis=ONE)


def blocks(first, last):
    return slice(LANE * first, LANE * last)


def near_bounds(cu_ref, before, width):
    shift = lax.axis_index('sp') * TOK
    tok = lax.broadcasted_iota(jnp.int32, (ONE, width), ONE) + (shift - before)
    inside = (tok >= ZERO) & (tok < GRP)
    lo = jnp.maximum(doc_start(cu_ref, tok), tok - WIN) - (shift - WIN)
    hi = jnp.minimum(doc_stop(cu_ref, tok), tok + WIN + ONE) - (shift - WIN)
    return lo, jnp.where(inside, hi - lo, ZERO).astype(jnp.uint32)


def in_bounds(bounds, cols, first, n):
    io = lax.broadcasted_iota(jnp.int32, (n, LANE), ZERO)
    return since(io, bounds[ZERO][:, cols] - first) < bounds[ONE][:, cols]


def every_head(fn, ahead):
    def body(g, c):
        fn([ahead * g + a for a in range(ahead)])
        return c
    lax.fori_loop(ZERO, HPS // ahead, body, ZERO)


def attn1_fwd_body(r, step):
    bounds = near_bounds(r.cu, ZERO, TOK)

    def some(heads):
        v_all = []
        for a, h in enumerate(heads):
            q_t = r.q[h] * SCALE
            k_rows = joined(r.left, r.k, r.right, h, LOW, LOW).T
            v_all.append(joined(r.left, r.v, r.right, h, HIGH, HIGH))
            for i in range(NBLK):
                r.s_s[a, i] = mm(k_rows[LANE * i:LANE * i + REACH], q_t[:, blocks(i, i + ONE)])
        for a, h in enumerate(heads):
            for i in range(NBLK):
                cols = blocks(i, i + ONE)
                s = jnp.where(in_bounds(bounds, cols, LANE * i, REACH), r.s_s[a, i], NEG)
                m = jnp.max(s, axis=ZERO, keepdims=True)
                e = jnp.exp(s - m)
                l = jnp.sum(e, axis=ZERO, keepdims=True)
                r.p_s[a, i] = (e * (ONE / l)).astype(BF)
                r.lse[HPS * step + h, :, cols] = m + jnp.log(l)
        for a, h in enumerate(heads):
            for i in range(NBLK):
                out = mm(v_all[a][:, LANE * i:LANE * i + REACH], r.p_s[a, i]).astype(BF)
                r.o[HPS * step + h, :, blocks(i, i + ONE)] = out
    every_head(some, AHEAD_FWD)


def attn1_fwd_stage(cu, qkv, left, right):
    tile, edge = (AHEAD_FWD, NBLK, REACH, LANE), heads_of(LANE, ZERO)
    return Stage(
        attn1_fwd_body, HSTEPS,
        [('cu', cu, CU_SPEC), ('q', qkv, own_head(ZERO)), ('k', qkv, own_head(ONE)), ('v', qkv, own_head(TWO)),
         ('left', left, edge), ('right', right, edge)],
        [('lse', STAT, STAT_BLOCK)],
        [('o', pltpu.VMEM((NHEAD, HEAD, TOK), BF)), ('s_s', pltpu.VMEM(tile, F32)), ('p_s', pltpu.VMEM(tile, BF))])


def attn1_bwd_body(r, step):
    bounds = near_bounds(r.cu, WIN, EXT)

    def window(e):
        first, last = max(LANE * e - WIN, ZERO), min(LANE * e + LANE + WIN, EXT)
        return first, last - first

    def parts(h):
        q_t = joined(r.ql, r.q, r.qr, h) * SCALE
        return q_t, joined(r.dl, r.d, r.dr, h), joined(r.left, r.k, r.right, h, LOW, LOW)

    def some(heads):
        for a, h in enumerate(heads):
            q_t, do_t, k_t = parts(h)
            for n, arr in enumerate((q_t, do_t, k_t)):
                r.x_s[a, n] = arr
            k_rows, v_rows = k_t.T, joined(r.left, r.v, r.right, h, HIGH, HIGH).T
            for e in range(XBLK):
                first, n = window(e)
                cols = blocks(e, e + ONE)
                r.s_s[a, e, :n] = mm(k_rows[first:first + n], q_t[:, cols])
                r.d_s[a, e, :n] = mm(v_rows[first:first + n], do_t[:, cols])
        for a, h in enumerate(heads):
            lse, delta = joined(r.ll, r.lse, r.lr, h), joined(r.el, r.delta, r.er, h)
            for e in range(XBLK):
                first, n = window(e)
                cols = blocks(e, e + ONE)
                ok = in_bounds(bounds, cols, first, n)
                p = jnp.exp(jnp.where(ok, r.s_s[a, e, :n] - lse[:, cols], NEG))
                r.p_s[a, first:first + n, cols] = p.astype(BF)
                r.t_s[a, first:first + n, cols] = (p * (r.d_s[a, e, :n] - delta[:, cols])).astype(BF)
        for a, h in enumerate(heads):
            got = [[], [], []]
            for b in range(XBLK):
                here, wide = blocks(b, b + ONE), blocks(max(b - ONE, ZERO), min(b + TWO, XBLK))
                got[ZERO].append(mm(r.x_s[a, TWO, :, wide], r.t_s[a, wide, here]) * SCALE)
                got[ONE].append(mm_nt(r.x_s[a, ZERO, :, wide], r.t_s[a, here, wide]))
                got[TWO].append(mm_nt(r.x_s[a, ONE, :, wide], r.p_s[a, here, wide]))
            for n in range(THREE):
                own = jnp.concatenate([g.astype(BF) for g in got[n]], axis=ONE)[:, WIN:WIN + TOK]
                r.out[n, HPS * step + h] = own

    @pl.when(step == ZERO)
    def _():
        r.p_s[...] = jnp.zeros(r.p_s.shape, BF)
        r.t_s[...] = jnp.zeros(r.t_s.shape, BF)

    every_head(some, AHEAD_BWD)


def attn1_bwd_stage(cu, qkv, do_t, lse, delta, edges, far):
    edge, row = heads_of(LANE, ZERO), row_of(LANE)
    blk = (AHEAD_BWD, XBLK, REACH, LANE)
    square = pltpu.VMEM((AHEAD_BWD, EXT, EXT), BF)
    names = ('left', 'right', 'ql', 'qr', 'dl', 'dr')
    return Stage(
        attn1_bwd_body, HSTEPS,
        [('cu', cu, CU_SPEC), ('q', qkv, own_head(ZERO)), ('k', qkv, own_head(ONE)), ('v', qkv, own_head(TWO)), ('d', do_t, own_head(ZERO)),
         ('lse', lse, row_of(TOK)), ('delta', delta, row_of(TOK))]
        + [(n, arr, edge) for n, arr in zip(names, list(edges) + far[:FOUR])]
        + [(n, arr, row) for n, arr in zip(('ll', 'lr', 'el', 'er'), far[FOUR:])],
        [], [('out', pltpu.VMEM((THREE, NHEAD, HEAD, TOK), BF)), ('s_s', pltpu.VMEM(blk, F32)), ('d_s', pltpu.VMEM(blk, F32)),
             ('p_s', square), ('t_s', square), ('x_s', pltpu.VMEM((AHEAD_BWD, THREE, HEAD, EXT), BF))])


ROWBLK = [slice(r, r + RB) for r in range(ZERO, TOK, RB)]
HALFT = NFT // TWO
SQRT_HALF = math.sqrt(SCALE * FOUR)
PDF_SCALE = SQRT_HALF / math.sqrt(math.pi)


def normal_cdf(a):
    return SQRT_HALF * SQRT_HALF * (ONE + lax.erf(a * SQRT_HALF))


def half_rows(ref, which):
    n = ref.shape[ZERO] // TWO
    return ref.at[pl.ds(pl.multiple_of(which * n, n), n)]


def col_tile(ref, n):
    return ref.at[:, pl.ds(pl.multiple_of(n * FT, FT), FT)]


def mlp_copies(r, fwd, bwd):
    sw = Swaps(r.ssem, r.rsem, r.lsem)
    both = fwd and bwd
    c = Refs(dict(sw=sw, start=[], first=[], second=[]))
    if fwd:
        c.start += [sw.remote(r.h, r.h_r), sw.remote(half_rows(r.of, sw.other), r.of_r), sw.local(half_rows(r.of, sw.core), r.of_m)]
        there = [sw.remote(r.m_s.at[HALFT * sw.other + n], r.m_r.at[n] if both else col_tile(r.m_r, n)) for n in range(HALFT)]
        here = [None] * HALFT
        if not both:
            c.start += [sw.local(r.h, r.h_m), sw.local(r.x1, r.x1_m)]
            here = [sw.local(r.m_s.at[HALFT * sw.core + n], col_tile(r.m_m, n)) for n in range(HALFT)]
        c.m_out = list(zip(there, here))
    if bwd:
        c.start.append(sw.remote(r.dy, r.dy_r))
        c.dmid_out = sw.remote(r.dmid, r.dmid_r)
        c.du_out = [[sw.remote(r.du_s.at[n, sw.other], r.du_r.at[n] if both else col_tile(r.du_r, n))] for n in range(NFT)]
        if not both:
            for n in range(NFT):
                c.du_out[n].append(sw.local(r.du_s.at[n, sw.core], col_tile(r.du_m, n)))
            c.do_out = sw.to_all(lambda dev: r.do_s.at[dev], lambda dev: r.d_o.at[dev])
    if both:
        c.first = sw.early([c.start[ZERO], c.start[-ONE]] + there)
        c.second = sw.early([cp for part in c.du_out for cp in part])
    return c


def mlp_body(r, step, layer, fwd, bwd):
    cps = mlp_copies(r, fwd, bwd)
    sw, start, whole_group = cps.sw, cps.start, not (fwd and bwd)
    if fwd:
        m_out = cps.m_out
    if bwd:
        dmid_out, du_out = cps.dmid_out, cps.du_out

    @pl.when(step == ZERO)
    def _():
        if fwd:
            for n in range(NHEAD):
                r.of[HEAD * n:HEAD * n + HEAD, :] = (r.o[n % FOUR, n // FOUR] if whole_group else r.o[n])
            x1 = (r.x[...].astype(F32) + mm_tn(r.of[...], r.wp[...])).astype(BF)
            r.x1[...] = x1
            r.h[...] = norm_rows(x1, r.g[layer:layer + ONE])
            r.acc[...] = x1.astype(F32)
        if bwd:
            r.dacc[...] = jnp.zeros(r.dacc.shape, F32)
        r.arrive()
        start_all(start)

    for rows in ROWBLK:
        if fwd:
            ua = mm(r.h[rows], r.wa[...]).astype(BF)
            ub = mm(r.h[rows], r.wb[...]).astype(BF)
            if not bwd:
                r.u[ZERO, rows] = ua
                r.u[ONE, rows] = ub
        else:
            ua, ub = r.u[ZERO, rows], r.u[ONE, rows]
        a, b = ua.astype(F32), ub.astype(F32)
        cdf = normal_cdf(a)
        gate = a * cdf
        if fwd:
            m = (gate * b).astype(BF)
            r.m_s[step, rows] = m
            r.acc[rows] += mm(m, r.wo[...])
        if bwd:
            dm = mm_nt(r.dy[rows], r.wo[...]).astype(BF).astype(F32)
            pdf = jnp.exp(a * a * (SCALE * FOUR - ONE)) * PDF_SCALE
            db = (dm * gate).astype(BF)
            da = (dm * b * (cdf + a * pdf)).astype(BF)
            r.du_s[step, ZERO, rows] = da
            r.du_s[step, ONE, rows] = db
            r.dacc[rows] += mm_nt(da, r.wa[...]) + mm_nt(db, r.wb[...])

    for n in range(NFT):
        @pl.when(step == n)
        def _(n=n):
            if fwd:
                there, here = m_out[n % HALFT]

                if here:
                    @pl.when(sw.core == n // HALFT)
                    def _():
                        here.start()

                @pl.when(sw.other == n // HALFT)
                def _():
                    there.start()
            if bwd:
                for cp in du_out[n]:
                    cp.start()

    @pl.when(step == NFT - ONE)
    def _():
        if fwd:
            r.y[...] = r.acc[...].astype(BF)
        if bwd:
            d_ln, gg = norm_rows_grad(r.x1[...], r.g[layer:layer + ONE], r.dacc[...].astype(BF))
            r.gg[...] = gg
            d_mid = add_bf(r.dy[...], d_ln)
            r.dmid[...] = d_mid
            dmid_out.start()
            d_att = mm_nt(r.wp[...], d_mid).astype(BF)
            for n in range(NHEAD):
                rows = slice(HEAD * n, HEAD * n + HEAD)
                blk = d_att[rows]
                if whole_group:
                    r.do_s[n % FOUR, n // FOUR] = blk
                else:
                    r.d_o[n] = blk
                    r.delta[n] = jnp.sum(blk.astype(F32) * r.of[rows].astype(F32), axis=ZERO, keepdims=True)
            if whole_group:
                start_all(cps.do_out)


def mlp_stage(layer, fwd, bwd, w_proj, gain, w_in, w_out, links=None, **arrays):
    u_spec = spec((TWO, TOK, FT), ZERO, ZERO, step_of)
    half_o = sds((DM // TWO, TOK), BF)
    half_m, half_u = sds((TOK, FF // TWO), BF), sds((TOK, FF), BF)
    heads = (NHEAD, HEAD, TOK)
    sums = pltpu.VMEM(ALLTOK, F32)
    links = links or {}
    ins = [('wp', w_proj, spec((None, DM, DM), layer, ZERO, ZERO)), ('g', gain, GAINS),
           ('wa', w_in, weight_cols(layer, FT)), ('wb', w_in, weight_cols(layer, FT, NFT)),
           ('wo', w_out, spec((None, FT, DM), layer, step_of, ZERO))]
    kinds = dict(x=TOK_SPEC, dy=TOK_SPEC, x1=TOK_SPEC, u=u_spec)
    ins += [(n, arr, kinds[n]) for n, arr in arrays.items()]
    outs, scratch, both = [], [], fwd and bwd
    own_tiles, far_tiles = pltpu.VMEM((HALFT, TOK, FT), BF), pltpu.VMEM((NFT, TOK, FT), BF)
    if fwd:
        outs += [('y', TOKS, TOK_SPEC), ('of_m', half_o, ANY), ('of_r', half_o, ANY)]
        scratch += [('acc', sums), ('of', pltpu.VMEM((DM, TOK), BF)), ('m_s', pltpu.VMEM((NFT, TOK, FT), BF)), ('h', TOK_VMEM),
                    ('x1', TOK_VMEM)]
    if fwd and not bwd:
        outs += [('h_m', TOKS, ANY), ('h_r', TOKS, ANY), ('m_m', half_m, ANY), ('m_r', half_m, ANY)]
        outs += [('x1_m', TOKS, ANY), ('u', sds((TWO, TOK, FF), BF), u_spec)]
    if bwd:
        shape = heads if fwd else BY_OWNER
        outs += [('dmid', TOKS, TOK_SPEC), ('gg', sds((ONE, DM), F32), spec((ONE, DM))), ('d_o', sds(shape, BF), spec(shape) if fwd else ANY),
                 ('dmid_r', TOKS, ANY)]
        scratch += [('dacc', sums), ('du_s', pltpu.VMEM((NFT, TWO, TOK, FT), BF))]
    if bwd and not fwd:
        outs += [('dy_r', TOKS, ANY), ('du_m', half_u, ANY), ('du_r', half_u, ANY)]
    if both:
        outs += [('delta', STAT, STAT_BLOCK)]
        scratch += [('h_r', TOK_VMEM), ('dy_r', TOK_VMEM), ('m_r', own_tiles), ('du_r', far_tiles)]
    if not fwd:
        scratch += [('do_s', pltpu.VMEM(BY_OWNER, BF))]
    return Stage(functools.partial(mlp_body, layer=layer, fwd=fwd, bwd=bwd), NFT, ins, outs, scratch + named_sems(FOUR * NFT),
                 functools.partial(mlp_copies, fwd=fwd, bwd=bwd), links)


def side_grad_copies(r):
    sw = Swaps(r.ssem, r.rsem, r.lsem)
    for n, src in enumerate((r.q_all.at[:NHEAD], r.d_o, r.lse, r.delta)):
        sw.to_sides(src.at[:, :, :LANE], src.at[:, :, TOK - LANE:], getattr(r, FAR[TWO * n]), getattr(r, FAR[TWO * n + ONE]))
    return Refs(dict(sw=sw))


def side_grad_body(r, step):
    sw = side_grad_copies(r).sw
    mlp = mlp_copies(Refs(dict(r.__dict__, ssem=r.mlp_ssem, rsem=r.mlp_rsem, lsem=r.mlp_lsem)), True, True)

    @pl.when(step == ZERO)
    def _():
        start_all(sw.waits)
        wait_all(mlp.first)

    @pl.when(step < HALFT)
    def _():
        r.out[...] = mm_tn(r.m_s[HALFT * sw.core + step], r.dy[...]) + mm_tn(r.m_r[step], r.dy_r[...])

    @pl.when(step == HALFT)
    def _():
        wait_all(mlp.second)
        r.h_t[ZERO] = r.h[...].T
        r.h_t[ONE] = r.h_r[...].T

    @pl.when(step >= HALFT)
    def _():
        n = step - HALFT
        r.out[...] = mm(r.h_t[ZERO], r.du_s[n, sw.core]) + mm(r.h_t[ONE], r.du_r[n])


FAR = ('ql', 'qr', 'dl', 'dr', 'll', 'lr', 'el', 'er')


def side_grad_stage(qkv):
    kinds = [(NHEAD, HEAD, LANE, BF)] * FOUR + [(NHEAD, ONE, LANE, F32)] * FOUR
    far = [(n, sds(shape, dtype), ANY) for n, (*shape, dtype) in zip(FAR, kinds)]
    names = ('m_s', 'du_s', 'h', 'h_r', 'dy', 'dy_r', 'm_r', 'du_r', 'd_o', 'delta', 'of', 'of_r', 'of_m', 'dmid', 'dmid_r')
    links = {n: (ONE, n) for n in names}
    links.update({'mlp_' + n: (ONE, n) for n in ('ssem', 'rsem', 'lsem')}, lse=(ZERO, 'lse'))
    return Stage(side_grad_body, HALFT + NFT, [('q_all', qkv, ANY)],
                 [('out', sds((MLP_ROWS, DM), F32), spec(ALLDM, step_of, ZERO))] + far,
                 [('h_t', pltpu.VMEM((TWO, DM, TOK), BF))] + named_sems(8), side_grad_copies, links)


NAMED = ('ha', 'hb', 'oa', 'ob', 'dma', 'dmb')


def third(ref, n):
    return ref.at[PROJ * n:PROJ * n + PROJ]


def qkv_bwd_copies(r, grads):
    sw = Swaps(r.ssem, r.rsem, r.lsem)
    c = Refs(dict(sw=sw, parts=[[sw.remote(r.dt_s.at[sw.other, n], third(r.dt_r, n))] for n in range(THREE)]))
    if grads:
        c.loads = sw.early([sw.local(getattr(r, n + '_in'), getattr(r, n)) for n in NAMED])
        for part in c.parts:
            sw.early(part)
    else:
        for n in range(THREE):
            c.parts[n].append(sw.local(r.dt_s.at[sw.core, n], third(r.dt_m, n)))
    return c


def qkv_bwd_body(r, step, layer, grads):
    cps = qkv_bwd_copies(r, grads)
    sw, copies = cps.sw, cps.parts

    @pl.when(step == ZERO)
    def _():
        r.acc[...] = jnp.zeros(r.acc.shape, F32)
        if grads:
            start_all(cps.loads)

    for p in range(THREE):
        @pl.when(step == p)
        def _(p=p):
            cos, sin = r.cos[...], r.sin[...]
            for chunk in CHUNKS:
                for head in range(FOUR):
                    blk = r.d[head, ZERO, chunk] if grads else r.d[p, FOUR * chunk + head]
                    a, b = blk[:HALF], blk[HALF:]
                    if p < TWO:
                        a, b = a.astype(F32), b.astype(F32)
                        a, b = (a * cos + b * sin).astype(BF), (b * cos - a * sin).astype(BF)
                    at, full = LANE * chunk + HEAD * (head % TWO), RB * chunk + HEAD * head
                    for n, val in ((ZERO, a), (HALF, b)):
                        r.dt_s[head // TWO, p, at + n:at + n + HALF] = val
                        r.dt_all[full + n:full + n + HALF] = val
            if p == ZERO:
                r.arrive()
            start_all(copies[p])
            r.acc[...] += mm(r.w[...], r.dt_all[...])

    @pl.when(step == TWO)
    def _():
        d_ln, gg = norm_rows_grad(r.x[...], r.g[layer:layer + ONE], r.acc[...].T.astype(BF))
        r.gg[...] = gg
        r.dx[...] = add_bf(r.dmid[...], d_ln)

    if grads:
        @pl.when(step == THREE)
        def _():
            wait_all(cps.loads)
            for part in copies:
                wait_all(part)
            r.out[...] = mm(r.oa[...], r.dma[...]) + mm(r.ob[...], r.dmb[...])

        for p in range(THREE):
            @pl.when(step == p + FOUR)
            def _(p=p):
                r.out[...] = mm(r.dt_s[sw.core, p], r.ha[...]) + mm(third(r.dt_r, p)[...], r.hb[...])


def qkv_bwd_stage(layer, tables, w_qkv, x, gain, d_mid, d=None, link=None, grads=None, pairs=()):
    part = lambda s: jnp.minimum(s, TWO)
    ins = [('cos', tables[ZERO], TABLE), ('sin', tables[ONE], TABLE), ('w', w_qkv, spec((None, DM, DM), layer, ZERO, part)),
           ('x', x, TOK_SPEC), ('g', gain, GAINS), ('dmid', d_mid, TOK_SPEC)]
    outs = [('dx', TOKS, TOK_SPEC), ('gg', sds((ONE, DM), F32), spec((ONE, DM)))]
    feats = (THREE * PROJ, TOK)
    scratch = [('acc', pltpu.VMEM((DM, TOK), F32)), ('dt_s', pltpu.VMEM((TWO, THREE, PROJ, TOK), BF)), ('dt_all', pltpu.VMEM((DM, TOK), BF))]
    steps, alias = THREE, ()
    if grads is None:
        outs += [('dt_m', sds(feats, BF), ANY), ('dt_r', sds(feats, BF), ANY)]
    else:
        first = (ATT_ROWS + MLP_ROWS) // PROJ
        ins += [('d', d, spec((FOUR, ONE, THREE, HEAD, TOK), ZERO, part, ZERO, ZERO, ZERO)), ('grads', grads, ANY)]
        ins += [(n + '_in', arr, ANY) for n, arr in zip(NAMED, pairs)]
        outs += [('out', sds(grads.shape, F32), spec((PROJ, DM), lambda s: first + jnp.maximum(s - THREE, ZERO), ZERO))]
        scratch += [('dt_r', pltpu.VMEM(feats, BF))] + [(n, pltpu.VMEM(arr.shape, BF)) for n, arr in zip(NAMED, pairs)]
        steps, alias = steps + FOUR, (('grads', 'out'),)
    flag = grads is not None
    return Stage(functools.partial(qkv_bwd_body, layer=layer, grads=flag), steps, ins, outs, scratch + named_sems(TWELVE),
                 functools.partial(qkv_bwd_copies, grads=flag), {} if link is None else {'d': link}, alias)


NDOWN = DOWN // DM


def grad_call(body, grads, steps, in_specs, args, rows, first_row, total, scratch=()):
    shared = [] if grads is None else [grads]
    first = first_row // rows
    return call(
        body, (steps,), [ANY] * len(shared) + in_specs,
        spec((rows, DM), lambda s: first + s, ZERO), sds((total, DM), F32), scratch=scratch,
        flops=FOUR * steps * rows * TOK * DM, nbytes=20 * MIB, name=body.__name__,
        alias={ZERO: ZERO} if shared else None,
    )(*shared, *args)


GRAD_INS = 8


def grad_mlp_body(*refs):
    ma, mb, dya, dyb, ha, hb, dua, dub, out_ref, h_t = refs[-GRAD_INS - TWO:]
    step = pl.program_id(ZERO)

    @pl.when(step < NDOWN)
    def _():
        out_ref[...] = mm_tn(ma[...], dya[...]) + mm_tn(mb[...], dyb[...])

    @pl.when(step == NDOWN)
    def _():
        h_t[ZERO] = ha[...].T
        h_t[ONE] = hb[...].T

    @pl.when(step >= NDOWN)
    def _():
        out_ref[...] = mm(h_t[ZERO], dua[...]) + mm(h_t[ONE], dub[...])


def grad_mlp(grads, m, m_r, dy, dy_r, h, h_r, du, du_r, first_row, total):
    toks = spec(ALLTOK)
    m_col = spec(ALLTOK, ZERO, lambda s: jnp.minimum(s, NDOWN - ONE))
    du_col = spec(ALLTOK, ZERO, lambda s: jnp.maximum(s - NDOWN, ZERO))
    return grad_call(grad_mlp_body, grads, NDOWN + UP // DM, [m_col, m_col, toks, toks, toks, toks, du_col, du_col],
                     (m, m_r, dy, dy_r, h, h_r, du, du_r), DM, first_row, total, scratch=[pltpu.VMEM((TWO, DM, TOK), BF)])


def grad_att_body(*refs):
    oa, ob, dma, dmb, ta, tb, ha, hb, out_ref = refs[-GRAD_INS - ONE:]
    step = pl.program_id(ZERO)

    @pl.when(step == ZERO)
    def _():
        out_ref[...] = mm(oa[...], dma[...]) + mm(ob[...], dmb[...])

    @pl.when(step > ZERO)
    def _():
        out_ref[...] = mm(ta[...], ha[...]) + mm(tb[...], hb[...])


def grad_att(grads, of, of_r, dmid, dmid_r, dt, dt_r, h, h_r, first_row):
    toks = spec(ALLTOK)
    blk = (PROJ, TOK)
    dt_row = spec(blk, lambda s: jnp.maximum(s - ONE, ZERO), ZERO)
    return grad_call(grad_att_body, grads, ONE + QKV // PROJ, [spec(blk), spec(blk), toks, toks, dt_row, dt_row, toks, toks],
                     (of, of_r, dmid, dmid_r, dt, dt_r, h, h_r), PROJ, first_row, RING_ROWS)


NB, NS = 5, 6
CH = RING_ROWS // (NB * FOUR)
SB, LF = CH // FOUR, CH // 16
RS = 9
LAST = RS + RS
ADD_ROWS = 96


def ring_body(g_ref, *refs):
    gains, refs = refs[:FOUR], refs[FOUR:]
    (f_ref, lnout_ref, bufa, bufb, bufc, gath, stage, lnbuf, ssem, rsem, psem, qsem, csem, stsem, lns, lnr) = refs
    core, partner = core_and_partner()
    zy = lax.axis_index('zy')
    pos = (lax.axis_index('sp'), lax.rem(zy, FOUR), zy // FOUR)
    streams = [(c, sg) for c in range(THREE) for sg in (ONE, -ONE)]
    bufs, sizes = (bufa, bufb, bufc), (CH, SB, LF)
    peers = range(ONE, FOUR)

    def mod4(v):
        return lax.rem(v + 8, FOUR)

    def at(axis, val):
        if axis == ZERO:
            return {'sp': val}
        yz = (val, pos[TWO]) if axis == ONE else (pos[ONE], val)
        return {'zy': yz[ONE] * FOUR + yz[ZERO]}

    def shifted(axis, d):
        return at(axis, mod4(pos[axis] + d))

    def axis_of(s, ph):
        return (streams[s][ZERO] + ph) % THREE

    def idx(s, ph, t):
        return mod4(pos[axis_of(s, ph)] - streams[s][ONE] * t)

    def own(s, ph):
        return idx(s, ph, -ONE)

    def base(b):
        return b * (FOUR * CH)

    bar = pltpu.get_barrier_semaphore()
    for ax in range(THREE):
        for d in peers:
            pl.semaphore_signal(bar, inc=ONE, device_id=shifted(ax, d), device_id_type=MESH)
    pl.semaphore_signal(bar, inc=ONE, device_id=partner, device_id_type=MESH)
    pl.semaphore_wait(bar, 10)

    def rows(ref, start, n):
        return ref.at[pl.ds(pl.multiple_of(start, LF), n)]

    def grows(s, start, n):
        return g_ref.at[pl.ds(pl.multiple_of(start, LF), n), LANE * s:LANE * s + LANE]

    def frows(s, start, n):
        return f_ref.at[core, pl.ds(pl.multiple_of(start, LF), n), LANE * s:LANE * s + LANE]

    def same_bytes(b, k):
        if k < RS:
            return bufs[k // THREE].at[b, k % THREE]
        n = sizes[TWO - (k - RS) // THREE]
        return gath.at[b] if n == CH else gath.at[b, :, pl.ds(ZERO, n)]

    def wait_for(ref, sem):
        pltpu.make_async_copy(ref, ref, sem).wait()

    def send(b, s, k):
        ph = k // THREE if k < RS else TWO - (k - RS) // THREE
        t = k % THREE
        n = sizes[ph]
        if k < RS:
            dst = bufs[ph].at[b, t, s]
            if t:
                src = bufs[ph].at[b, t - ONE, s]
            elif ph:
                src = rows(bufs[ph - ONE].at[b, TWO, s], idx(s, ph, ZERO) * n, n)
            else:
                src = grows(s, base(b) + idx(s, ZERO, ZERO) * n, n)
        elif ph:
            off = own(s, ONE) * SB if ph == TWO else ZERO
            src = dst = rows(gath.at[b, s], off + idx(s, ph, t - ONE) * n, n)
        else:
            dst = frows(s, base(b) + idx(s, ZERO, t - ONE) * n, n)
            src = dst if t else gath.at[b, s]
        pltpu.make_async_remote_copy(src_ref=src, dst_ref=dst, send_sem=ssem.at[b, k], recv_sem=rsem.at[b, k],
                                     device_id=shifted(axis_of(s, ph), streams[s][ONE]), device_id_type=MESH).start()

    def stage_load(n):
        t, b, slot = n // NB, lax.rem(n, NB), lax.rem(n, TWO)
        for s in range(NS):
            pltpu.make_async_copy(grows(s, base(b) + idx(s, ZERO, t + ONE) * CH, CH), stage.at[slot, s],
                                  stsem.at[slot]).start()

    def ln_copy(ph, d):
        return pltpu.make_async_remote_copy(
            src_ref=lnbuf.at[ph, THREE], dst_ref=lnbuf.at[ph, d - ONE], send_sem=lns.at[ph, d - ONE],
            recv_sem=lnr.at[ph, d - ONE], device_id=shifted(ph, d) if ph < THREE else partner, device_id_type=MESH)

    def ln_sum(ph):
        vals = [lnbuf[ph, THREE]] + [lnbuf[ph, d - ONE] for d in peers]
        total = jnp.zeros_like(vals[ZERO])
        for p in range(FOUR):
            term = vals[ZERO]
            for d in peers:
                term = jnp.where(mod4(pos[ph] - d) == p, vals[d], term)
            total = total + term
        return total

    def batches(fn, start=ZERO):
        def body(b, c):
            fn(b)
            return c
        lax.fori_loop(start, NB, body, ZERO)

    def first(b):
        for s in range(NS):
            send(b, s, ZERO)

    lnbuf[ZERO, THREE] = jnp.zeros(lnout_ref.shape, F32)
    for n, gain in enumerate(gains):
        lnbuf[ZERO, THREE, n:n + ONE] = gain[...]
    first(ZERO)
    stage_load(jnp.int32(ZERO))
    for d in peers:
        ln_copy(ZERO, d).start()
    batches(first, ONE)

    for k in range(RS):
        ph, t = k // THREE, k % THREE
        buf, size = bufs[ph], sizes[ph]

        def step(b, k=k, ph=ph, t=t, buf=buf, size=size):
            n = k * NB + b
            slot = lax.rem(n, TWO)
            if not ph:
                @pl.when(n < THREE * NB - ONE)
                def _():
                    stage_load(n + ONE)
                wait_for(stage.at[slot], stsem.at[slot])
            wait_for(same_bytes(b, k), rsem.at[b, k])
            for s in range(NS):
                if ph:
                    off = pl.multiple_of(idx(s, ph, t + ONE) * size, LF)
                    buf[b, t, s] += bufs[ph - ONE][b, TWO, s, pl.ds(off, size)]
                else:
                    @pl.loop(ZERO, CH, step=ADD_ROWS)
                    def _(r):
                        at_r = pl.ds(pl.multiple_of(r, ADD_ROWS), ADD_ROWS)
                        buf[b, t, s, at_r] += stage[slot, s, at_r]
                if k == RS - ONE:
                    off = pl.multiple_of(own(s, ONE) * SB + own(s, TWO) * LF, LF)
                    gath[b, s, pl.ds(off, LF)] = bufc[b, TWO, s]
                send(b, s, k + ONE)

        batches(step)
        if k < SIX and k % TWO == ZERO:
            lp = k // TWO
            for d in peers:
                ln_copy(lp, d).wait()
            lnbuf[lp + ONE, THREE] = ln_sum(lp)
            for d in peers if lp < TWO else (ONE,):
                ln_copy(lp + ONE, d).start()

    def hand_over(b, s, j, src, start):
        pltpu.make_async_remote_copy(src_ref=src, dst_ref=frows(s, start, CH), send_sem=psem.at[b, j], recv_sem=qsem.at[b, j],
                                     device_id=partner, device_id_type=MESH).start()

    for k in range(RS, LAST):
        def step(b, k=k):
            wait_for(same_bytes(b, k), rsem.at[b, k])
            piece = k - (LAST - FOUR)
            for s in range(NS):
                if k < LAST - ONE:
                    send(b, s, k + ONE)
                if piece >= ZERO:
                    start = base(b) + idx(s, ZERO, piece - ONE) * CH
                    if piece:
                        hand_over(b, s, piece, frows(s, start, CH), start)
                    else:
                        pltpu.make_async_copy(gath.at[b, s], frows(s, start, CH), csem.at[b]).start()
                        hand_over(b, s, piece, gath.at[b, s], start)
        batches(step)

    ln_copy(THREE, ONE).wait()
    lnout_ref[...] = lnbuf[THREE, THREE] + lnbuf[THREE, ZERO]

    def finish(b):
        for k in range(LAST):
            wait_for(same_bytes(b, k), ssem.at[b, k])
        for j in range(FOUR):
            wait_for(gath.at[b], psem.at[b, j])
            wait_for(gath.at[b], qsem.at[b, j])
        wait_for(gath.at[b], csem.at[b])
    batches(finish)


def ring_all_reduce(g, gains, cid):
    vmem = pl.BlockSpec(memory_space=pltpu.VMEM)
    ln = sds((8, DM), F32)
    return pl.pallas_call(
        ring_body,
        in_specs=[ANY] + [vmem] * FOUR,
        out_specs=[ANY, vmem],
        out_shape=[sds((TWO, RING_ROWS, DM), F32), ln],
        scratch_shapes=[
            pltpu.VMEM((NB, THREE, NS, CH, LANE), F32), pltpu.VMEM((NB, THREE, NS, SB, LANE), F32),
            pltpu.VMEM((NB, THREE, NS, LF, LANE), F32), pltpu.VMEM((NB, NS, CH, LANE), F32),
            pltpu.VMEM((TWO, NS, CH, LANE), F32),
            pltpu.VMEM((FOUR, FOUR) + ln.shape, F32),
            DMA((NB, LAST)), DMA((NB, LAST)), DMA((NB, FOUR)), DMA((NB, FOUR)), DMA((NB,)), DMA((TWO,)),
            DMA((FOUR, THREE)), DMA((FOUR, THREE)),
        ],
        compiler_params=pltpu.CompilerParams(collective_id=cid, has_side_effects=True, vmem_limit_bytes=60 * MIB),
        cost_estimate=pl.CostEstimate(flops=MIB * MIB // FOUR, bytes_accessed=200 * MIB, transcendentals=ZERO),
        name="ring_all_reduce",
    )(g, *gains)


SLOTS, LAG = 8, 4
NTURN = TWO * THREE
OUT_SHAPE, IN_SHAPE = (TWO, FF, DM), (TWO, DM, TWO * FF)


def stream(pieces, buf, turned, isem, osem, between=None):
    def loads(i):
        slot, srcs = i % SLOTS, pieces[i][ZERO]
        n = srcs[ZERO].shape[ZERO]
        return [pltpu.make_async_copy(src, buf.at[slot, k * n:k * n + n], isem.at[slot, k]) for k, src in enumerate(srcs)]

    def store(i):
        _, dst, turn = pieces[i]
        src = buf.at[i % SLOTS, :dst.shape[ZERO]] if turn is None else turned.at[turn]
        return pltpu.make_async_copy(src, dst, osem.at[i % SLOTS])

    total = len(pieces)
    for i in range(total + LAG):
        if i == SLOTS and between:
            between()
        if i < total:
            if i >= SLOTS:
                store(i - SLOTS).wait()
            for cp in loads(i):
                cp.start()
        k = i - LAG
        if k >= ZERO:
            for cp in loads(k):
                cp.wait()
            turn = pieces[k][TWO]
            if turn is not None:
                for n in CHUNKS:
                    rows, col = LANE * n, RB * n
                    turned[turn, :, col:col + LANE] = buf[k % SLOTS, rows:rows + LANE].T
                    turned[turn, :, col + LANE:col + RB] = buf[k % SLOTS, PROJ + rows:PROJ + rows + LANE].T
            store(k).start()
    for i in range(max(total - SLOTS, ZERO), total):
        store(i).wait()


def unpack_ring_body(f, y_in, dx_in, gains, g_qkv, g_proj, g_in, g_out, y, dx, g_attn, g_mlp, y_s, dx_s, *scratch):
    small_in, small_out, *scratch = scratch
    loads = [pltpu.make_async_copy(src, dst, small_in.at[n]) for n, (src, dst) in enumerate(((y_in, y_s), (dx_in, dx_s)))]
    stores = [pltpu.make_async_copy(src, dst, small_out.at[n]) for n, (src, dst) in enumerate(((y_s, y), (dx_s, dx)))]
    start_all(loads)
    g_attn[...] = gains[:TWO]
    g_mlp[...] = gains[TWO:FOUR]

    def between():
        wait_all(loads)
        start_all(stores)

    def block(c, row, n=DM):
        return f.at[c, row:row + n]

    pieces = []
    for c in range(TWO):
        for n in range(NDOWN):
            pieces.append(([block(c, ATT_ROWS + DM * n)], g_out.at[ZERO, DOWN * c + DM * n:DOWN * c + DM * n + DM], None))
        for n in range(FOUR):
            col = UP * c + DM * n
            pieces.append(([block(c, ATT_ROWS + DOWN + DM * n)], g_in.at[ZERO, :, col:col + DM], None))
    for l in range(TWO):
        first = (ONE - l) * (ATT_ROWS + MLP_ROWS)
        for n in range(THREE):
            row = first + PROJ * (n + ONE)
            pieces.append(([block(c, row, PROJ) for c in range(TWO)], g_qkv.at[l, :, DM * n:DM * n + DM], THREE * l + n))
        for c in range(TWO):
            pieces.append(([block(c, first, PROJ)], g_proj.at[l, PROJ * c:PROJ * c + PROJ], None))
    stream(pieces, *scratch, between=between)
    wait_all(stores)


def unpack_mlp_body(own, other, in_0, out_0, g_in, g_out, *scratch):
    core = lax.axis_index('core')
    pieces = []
    for src, side in ((own, core), (other, ONE - core)):
        for n in range(NDOWN):
            row = pl.multiple_of(DOWN * side + DM * n, DM)
            pieces.append(([src.at[DM * n:DM * n + DM]], g_out.at[ONE, pl.ds(row, DM)], None))
        for n in range(FOUR):
            col = pl.multiple_of(UP * side + DM * n, DM)
            pieces.append(([src.at[DOWN + DM * n:DOWN + DM * n + DM]], g_in.at[ONE, :, pl.ds(col, DM)], None))
    stream(pieces, *scratch)


def unpack_call(body, args, outs, alias, name, in_specs=None, out_specs=None, small=()):
    return pl.pallas_call(
        body, in_specs=in_specs or [ANY] * len(args), out_specs=out_specs or [ANY] * len(outs), out_shape=outs,
        scratch_shapes=list(small) + [pltpu.VMEM((SLOTS, DM, DM), F32), pltpu.VMEM((NTURN, DM, DM), F32),
                                      DMA((SLOTS, TWO)), DMA((SLOTS,))],
        input_output_aliases=alias,
        compiler_params=pltpu.CompilerParams(vmem_limit_bytes=60 * MIB),
        cost_estimate=pl.CostEstimate(flops=MIB * MIB // RB, bytes_accessed=75 * MIB, transcendentals=ZERO), name=name,
    )(*args)


def rope_tables(pos, base):
    inv_freq = base ** (jnp.arange(HALF).astype(F32) * (-TWO / HEAD))
    angles = inv_freq[:, None] * pos.astype(F32)[None, :]
    return jnp.cos(angles), jnp.sin(angles)


def solution(mesh):
    n_sp = mesh.shape['sp']
    by_core = mesh.devices.reshape(n_sp, mesh.shape['dp'] // TWO, TWO)
    mesh = Mesh(by_core, ('sp', 'zy', 'core'))
    dp_axes = ('zy', 'core')
    row_axes = dp_axes + ('sp',)
    token_spec = P(row_axes, None)
    swap_cores = [(ZERO, ONE), (ONE, ZERO)]
    cids = list(range(RS))

    def exchange(arr):
        return lax.all_to_all(arr, 'sp', ZERO, ZERO, tiled=True)

    def device_step(x_loc, cu_loc, pos_loc, w_qkv, w_proj, w_in, w_out, ln_attn, ln_mlp, d_out):
        tab0, tab1 = [rope_tables(pos_loc, base) for base in BASES]
        mlp_args, w_mlp = (w_proj, ln_mlp), (w_in, w_out)

        q0, f0, q1 = run("layer0_qkv1", cids[ONE], row_peers, group_fwd_stage(cu_loc, ln_attn, w_qkv, tab0, x_loc),
                         mlp_stage(ZERO, True, False, *mlp_args, *w_mlp, links={'o': (ZERO, 'o_r')}, x=x_loc),
                         qkv_fwd_stage(ONE, ln_attn, w_qkv, tab1, (ONE, 'y')))
        kv_edges = (q1.left, q1.right)
        a1, f1, s1 = run("attn1_mlp1", cids[TWO], near_peers, attn1_fwd_stage(cu_loc, q1.out, *kv_edges),
                         mlp_stage(ONE, True, True, *mlp_args, *w_mlp, links={'o': (ZERO, 'o')}, x=f0.y, dy=d_out),
                         side_grad_stage(q1.out))
        g_side = lax.psum(s1.out, ('sp', 'zy'))
        far = [getattr(s1, n) for n in FAR]
        _, t1, b0 = run("attn1_qkv1_mlp0", cids[5], row_peers,
                        attn1_bwd_stage(cu_loc, q1.out, f1.d_o, a1.lse, f1.delta, kv_edges, far),
                        qkv_bwd_stage(ONE, tab1, w_qkv, f0.y, ln_attn, f1.dmid, link=(ZERO, 'out')),
                        mlp_stage(ZERO, False, True, *mlp_args, *w_mlp, links={'dy': (ONE, 'dx')}, x1=f0.x1_m, u=f0.u))
        dqkv0 = exchange(attn0_bwd(cu_loc, q0.out, q0.o_m, b0.d_o, q0.lse))
        grads = grad_att(None, f1.of_m, f1.of_r, f1.dmid, f1.dmid_r, t1.dt_m, t1.dt_r, q1.h_m, q1.h_r, ZERO)
        grads = grad_mlp(grads, f0.m_m, f0.m_r, t1.dx, b0.dy_r, f0.h_m, f0.h_r, b0.du_m, b0.du_r, ATT_ROWS, RING_ROWS)
        t0, = run("qkv0_grads", cids[SIX], partner_peer, qkv_bwd_stage(
            ZERO, tab0, w_qkv, x_loc, ln_attn, b0.dmid, d=dqkv0, grads=grads,
            pairs=(q0.h_m, q0.h_r, f0.of_m, f0.of_r, b0.dmid, b0.dmid_r)))

        gains = (t0.gg, t1.gg, b0.gg, f1.gg)
        summed, gains = ring_all_reduce(t0.out, gains, cids[ZERO])
        summed, g_side = lax.optimization_barrier((summed, g_side))
        from_partner = lax.ppermute(g_side, 'core', swap_cores)
        shapes = [sds(shape, F32) for shape in ((TWO, DM, THREE * DM), (TWO, DM, DM), IN_SHAPE, OUT_SHAPE)]
        vmem = pl.BlockSpec(memory_space=pltpu.VMEM)
        gain = sds((TWO, DM), F32)
        g_qkv, g_proj, g_in, g_out, y, dx, g_attn, g_mlp = unpack_call(
            unpack_ring_body, (summed, f1.y, t0.dx, gains), shapes + [TOKS, TOKS, gain, gain], {}, "unpack_ring",
            [ANY] * THREE + [vmem], [ANY] * SIX + [vmem] * TWO, [TOK_VMEM, TOK_VMEM, DMA((TWO,)), DMA((TWO,))])
        g_in, g_out = unpack_call(unpack_mlp_body, (g_side, from_partner, g_in, g_out), shapes[TWO:],
                                  {TWO: ZERO, THREE: ONE}, "unpack_mlp")
        return y, dx, g_qkv, g_proj, g_in, g_out, g_attn, g_mlp

    in_specs = (token_spec, P(dp_axes, None), P(row_axes)) + (P(),) * SIX + (token_spec,)
    out_specs = (token_spec, token_spec) + (P(),) * SIX
    return jax.shard_map(device_step, mesh=mesh, in_specs=in_specs, out_specs=out_specs, check_vma=False)
```

```python
import functools
import math
import jax
import jax.numpy as jnp
from jax import lax
from jax.experimental import pallas as pl
from jax.experimental.pallas import tpu as pltpu
from jax.sharding import Mesh, PartitionSpec as P

ZERO, ONE, TWO, THREE, FOUR = range(5)
SIX, TWELVE = 6, 12
HEAD = 64
HALF = 32
NHEAD = 12
DM = 768
FF = 3072
TOK = 512
GRP = 2048
WIN = 64
NDOC = 8
LANE = 128
EPS = 1e-5
NEG = -1e30
SCALE = 0.125
BASES = (160000.0, 10000.0)
F32 = jnp.float32
BF = jnp.bfloat16
QT = 256
FT = 768
NFT = FF // FT
QTILES = GRP // QT
MIB = 1024 * 1024
ALLTOK = (TOK, DM)
ALLDM = (DM, DM)
PROJ = DM // 2
DOWN = FF // 2
UP = FF
QKV = 3 * PROJ
MLP_ROWS = DOWN + UP
ATT_ROWS = PROJ + QKV
RING_ROWS = 2 * ATT_ROWS + MLP_ROWS
ANY = pl.BlockSpec(memory_space=pl.ANY)
DMA = pltpu.SemaphoreType.DMA
MESH = pl.DeviceIdType.MESH


def dot(a, b, ca, cb):
    return lax.dot_general(a, b, (((ca,), (cb,)), ((), ())), preferred_element_type=F32)


def mm(a, b):
    return dot(a, b, ONE, ZERO)


def mm_nt(a, b):
    return dot(a, b, ONE, ONE)


def mm_tn(a, b):
    return dot(a, b, ZERO, ZERO)


def call(body, grid, in_specs, out_specs, out_shape, scratch=(), prefetch=ZERO, flops=ZERO, nbytes=ZERO, name=None,
         cid=None, alias=None):
    extra = {} if cid is None else dict(collective_id=cid, has_side_effects=True)
    return pl.pallas_call(
        body,
        grid_spec=pltpu.PrefetchScalarGridSpec(
            num_scalar_prefetch=prefetch, grid=grid, in_specs=in_specs, out_specs=out_specs, scratch_shapes=scratch),
        out_shape=out_shape,
        input_output_aliases=alias or {},
        compiler_params=pltpu.CompilerParams(vmem_limit_bytes=60 * MIB, **extra),
        cost_estimate=pl.CostEstimate(flops=int(flops), bytes_accessed=int(nbytes), transcendentals=ZERO),
        name=name,
    )


def sds(shape, dtype):
    return jax.ShapeDtypeStruct(shape, dtype)


def spec(shape, *idx):
    idx = idx or (ZERO,) * len(shape)
    return pl.BlockSpec(shape, lambda *g: tuple(i(*g) if callable(i) else i for i in idx))


def step_of(s, *_):
    return s


def core_and_partner():
    core = lax.axis_index('core')
    return core, {'core': ONE - core}


def greet(devices):
    for dev in devices:
        pl.semaphore_signal(pltpu.get_barrier_semaphore(), inc=ONE, device_id=dev, device_id_type=MESH)


def all_here(devices):
    pl.semaphore_wait(pltpu.get_barrier_semaphore(), len(devices))


def sp_peer(d):
    return lax.rem(lax.axis_index('sp') + d, FOUR)


PEERS = range(ONE, FOUR)


class Swaps:
    def __init__(self, ssem, rsem, lsem):
        self.sems, self.waits, self.n = (ssem, rsem, lsem), [], ZERO
        self.core, self.partner = core_and_partner()
        self.other = ONE - self.core
        self.me = lax.axis_index('sp')

    def remote(self, src, dst, dev=None):
        ssem, rsem, _ = self.sems
        return self.later(pltpu.make_async_remote_copy(
            src_ref=src, dst_ref=dst, send_sem=ssem.at[self.n], recv_sem=rsem.at[self.n],
            device_id=self.partner if dev is None else dev, device_id_type=MESH))

    def local(self, src, dst):
        return self.later(pltpu.make_async_copy(src, dst, self.sems[TWO].at[self.n]))

    def later(self, cp):
        self.n += ONE
        self.waits.append(cp)
        return cp

    def to_all(self, src_of, dst_of):
        return [self.remote(src_of(sp_peer(d)), dst_of(self.me), {'sp': sp_peer(d)}) for d in PEERS] + [
            self.local(src_of(self.me), dst_of(self.me))]

    def to_sides(self, left_src, right_src, from_left, from_right):
        return [self.remote(right_src, from_left, {'sp': sp_peer(ONE)}), self.remote(left_src, from_right, {'sp': sp_peer(THREE)})]

    def early(self, some):
        gone = {id(cp) for cp in some}
        self.waits = [cp for cp in self.waits if id(cp) not in gone]
        return some

    def wait(self):
        for cp in self.waits:
            cp.wait()


def start_all(copies):
    for cp in copies:
        cp.start()


def wait_all(copies):
    for cp in copies:
        cp.wait()


def row_peers():
    return [core_and_partner()[ONE]] + [{'sp': sp_peer(d)} for d in PEERS]


def side_peers():
    return [{'sp': sp_peer(ONE)}, {'sp': sp_peer(THREE)}]


def partner_peer():
    return [core_and_partner()[ONE]]


def near_peers():
    return partner_peer() + side_peers()


def swap_sems(n):
    return [DMA((n,))] * THREE


def named_sems(n):
    return list(zip(('ssem', 'rsem', 'lsem'), swap_sems(n)))


class Refs:
    def __init__(self, named):
        self.__dict__.update(named)


class Stage:
    def __init__(self, body, steps, ins, outs, scratch, copies=None, links=None, alias=()):
        self.body, self.steps, self.ins, self.outs, self.scratch = body, steps, ins, outs, scratch
        self.copies, self.links, self.alias = copies, links or {}, alias


def shifted(block, first, steps):
    if block.index_map is None:
        return block
    return pl.BlockSpec(block.block_shape, lambda g: block.index_map(jnp.clip(g - first, ZERO, steps - ONE)))


def run(name, cid, peers, *stages):
    firsts = [sum(st.steps for st in stages[:k]) for k in range(len(stages))]

    def flat(kind):
        return [(k, entry) for k, st in enumerate(stages) for entry in getattr(st, kind)]

    ins, outs, scratch = flat('ins'), flat('outs'), flat('scratch')
    keys = [(k, entry[ZERO]) for k, entry in ins + outs + scratch]

    def body(*refs):
        pid = pl.program_id(ZERO)
        have = dict(zip(keys, refs))

        @pl.when(pid == ZERO)
        def _():
            greet(peers())

        talking = [k for k, st in enumerate(stages) if st.copies]
        views = []
        for k, st in enumerate(stages):
            r = Refs({n: ref for (at, n), ref in have.items() if at == k})
            for n, source in st.links.items():
                setattr(r, n, have[source])
            r.arrive = lambda k=k: all_here(peers()) if k == talking[ZERO] else None
            views.append(r)

            @pl.when((pid >= firsts[k]) & (pid < firsts[k] + st.steps))
            def _(st=st, r=r, k=k):
                st.body(r, pid - firsts[k])

        @pl.when(pid == firsts[-ONE] + stages[-ONE].steps - ONE)
        def _():
            for k in talking:
                stages[k].copies(views[k]).sw.wait()

    def placed(entries):
        return [shifted(entry[TWO], firsts[k], stages[k].steps) for k, entry in entries]

    alias = {[e[ZERO] for _, e in ins].index(a): [e[ZERO] for _, e in outs].index(b) for st in stages for a, b in st.alias}
    got = call(body, (sum(st.steps for st in stages),), placed(ins), placed(outs), [e[ONE] for _, e in outs],
               scratch=[e[ONE] for _, e in scratch], flops=16 * TOK * DM * FF, nbytes=30 * MIB, name=name, cid=cid,
               alias=alias)(*[e[ONE] for _, e in ins])
    out = [{} for _ in stages]
    for (k, e), arr in zip(outs, got):
        out[k][e[ZERO]] = arr
    return [Refs(named) for named in out]


def norm_parts(x_bf):
    rows = x_bf.astype(F32)
    cen = rows - jnp.mean(rows, axis=ONE, keepdims=True)
    var = jnp.mean(cen * cen, axis=ONE, keepdims=True)
    return cen, lax.rsqrt(var + EPS)


def norm_rows(x_bf, gain):
    cen, inv = norm_parts(x_bf)
    return (cen * inv * gain).astype(BF)


def norm_rows_grad(x_bf, gain, d_bf):
    cen, inv = norm_parts(x_bf)
    hat = cen * inv
    d_out = d_bf.astype(F32)
    g_gain = jnp.sum(d_out * hat, axis=ZERO, keepdims=True)
    d_hat = d_out * gain
    d_x = inv * (d_hat - jnp.mean(d_hat, axis=ONE, keepdims=True) - hat * jnp.mean(d_hat * hat, axis=ONE, keepdims=True))
    return d_x.astype(BF), g_gain


def add_bf(a, b):
    return (a.astype(F32) + b.astype(F32)).astype(BF)


RB = 256
ROPED = 6
CHUNKS = range(DM // RB)


def head_rows(ref, chunk, head):
    return ref.at[head, ZERO, chunk] if ref.shape[ZERO] == FOUR else ref.at[ZERO, chunk, head]


def weight_cols(layer, width, first=ZERO):
    return spec((None, DM, width), layer, ZERO, lambda s: first + s)


GAINS = spec((TWO, DM))


GROUP_QKV = (FOUR, THREE, THREE, HEAD, TOK)
OWN_QKV = (THREE * NHEAD, HEAD, TOK)
EDGE = (NHEAD, HEAD, LANE)
TOKS = jax.ShapeDtypeStruct(ALLTOK, BF)
TOK_SPEC = spec(ALLTOK)
TOK_VMEM = pltpu.VMEM(ALLTOK, BF)
TABLE = spec((HALF, TOK))
CU_SPEC = pl.BlockSpec(memory_space=pltpu.SMEM)


def rotated(a, b, r):
    cos, sin = r.cos[...], r.sin[...]
    return a * cos - b * sin, b * cos + a * sin


def qkv_chunk(r, w):
    return mm(r.h[...], w).astype(BF).astype(F32).T


def head_halves(t_rows, head):
    at = HEAD * head
    return t_rows[at:at + HALF], t_rows[at + HALF:at + HEAD]


def qkv_fwd_copies(r):
    sw = Swaps(r.ssem, r.rsem, r.lsem)
    return Refs(dict(sw=sw, start=[sw.remote(r.h, r.h_r), sw.local(r.h, r.h_m)],
                     edges=sw.to_sides(r.edge_s.at[ZERO], r.edge_s.at[ONE], r.left, r.right)))


def qkv_fwd_body(r, step, layer):
    cps = qkv_fwd_copies(r)

    @pl.when(step == ZERO)
    def _():
        r.h[...] = norm_rows(r.x[...], r.g[layer:layer + ONE])
        r.arrive()
        start_all(cps.start)

    for p in range(THREE):
        @pl.when(step == KVQ.index(p))
        def _(p=p):
            for chunk in CHUNKS:
                t_rows = qkv_chunk(r, r.w[:, RB * chunk:RB * chunk + RB])
                for head in range(FOUR):
                    a, b = head_halves(t_rows, head)
                    if p < TWO:
                        a, b = rotated(a, b, r)
                    n = FOUR * chunk + head
                    out = r.out.at[n]
                    out[:HALF] = a.astype(BF)
                    out[HALF:] = b.astype(BF)
                    if p:
                        lane = WIN * (p - ONE)
                        blk = out[...]
                        r.edge_s[ZERO, n, :, lane:lane + WIN] = blk[:, :WIN]
                        r.edge_s[ONE, n, :, lane:lane + WIN] = blk[:, TOK - WIN:]
            if p == TWO:
                start_all(cps.edges)


KVQ = (ONE, TWO, ZERO)


def kvq_part(s, *_):
    return (s + ONE) % THREE


def qkv_fwd_stage(layer, gain, w_qkv, tables, link):
    ins = [('g', gain, GAINS), ('w', w_qkv, spec((None, DM, DM), layer, ZERO, kvq_part)), ('cos', tables[ZERO], TABLE), ('sin', tables[ONE], TABLE)]
    outs = [('h_m', TOKS, ANY), ('h_r', TOKS, ANY), ('out', sds(OWN_QKV, BF), spec((NHEAD, HEAD, TOK), kvq_part, ZERO, ZERO)),
            ('left', sds(EDGE, BF), ANY), ('right', sds(EDGE, BF), ANY)]
    scratch = [('h', TOK_VMEM), ('edge_s', pltpu.VMEM((TWO,) + EDGE, BF))]
    return Stage(functools.partial(qkv_fwd_body, layer=layer), THREE, ins, outs, scratch + named_sems(FOUR),
                 qkv_fwd_copies, {'x': link})


def tile_src(i, *_):
    return i // TWO


def tile_side(i, *_):
    return i % TWO


Q_SPEC = spec((ONE, ONE, THREE, HEAD, QT), tile_src, ZERO, ZERO, ZERO, tile_side)
O_SPEC = spec((ONE, THREE, HEAD, QT), tile_src, ZERO, ZERO, tile_side)
STAT_SPEC = spec((8, QT), ZERO, step_of)


def kv_spec(part):
    return spec((FOUR, ONE, THREE, HEAD, TOK), ZERO, part, ZERO, ZERO, ZERO)


def key_tile(kt):
    return kt // TWO, pl.ds(pl.multiple_of((kt % TWO) * QT, QT), QT)


def key_rows(dst, k_ref):
    for src in range(FOUR):
        for h in range(THREE):
            dst[h, TOK * src:TOK * src + TOK] = k_ref[src, ZERO, h].T


def row_tile(kt):
    return pl.ds(pl.multiple_of(kt * QT, QT), QT)


def since(pos, start):
    return (pos - start).astype(jnp.uint32)


def doc_start(cu_ref, tok):
    start = jnp.zeros_like(tok)
    for d in range(ONE, NDOC):
        start = jnp.where(cu_ref[ZERO, d] <= tok, cu_ref[ZERO, d], start)
    return start


def doc_stop(cu_ref, tok):
    stop = jnp.full_like(tok, GRP)
    for d in range(NDOC - ONE, ZERO, -ONE):
        stop = jnp.where(cu_ref[ZERO, d] > tok, cu_ref[ZERO, d], stop)
    return stop


def tile_bounds(cu_ref, tile):
    first = tile * QT
    tok = lax.broadcasted_iota(jnp.int32, (ONE, QT), ONE) + first
    lo = doc_start(cu_ref, first) // QT
    hi = (doc_stop(cu_ref, first + QT - ONE) + QT - ONE) // QT
    return lo, hi, doc_start(cu_ref, tok), doc_stop(cu_ref, tok)


BY_OWNER = (FOUR, THREE, HEAD, TOK)


def group_copies(r):
    sw = Swaps(r.ssem, r.rsem, r.lsem)

    def head_parts(c):
        return [cp for p in range(THREE) for cp in sw.to_all(lambda dev: r.out_s.at[p, dev, c], lambda dev: r.got.at[dev, p, c])]

    start = [sw.remote(r.h, r.h_r), sw.local(r.h, r.h_m)]
    parts = [sw.early(head_parts(c)) for c in range(THREE)]
    heads = [sw.early(sw.to_all(lambda dev: r.o_s.at[dev, c], lambda dev: r.o_r.at[dev, c])) for c in range(THREE)]
    return Refs(dict(sw=sw, start=start, parts=parts, heads=heads, keep=[sw.local(r.got, r.out), sw.local(r.o_s, r.o_m)]))


def group_fwd_body(r, step):
    cps = group_copies(r)
    tiles = range(QTILES)

    @pl.when(step == ZERO)
    def _():
        r.h[...] = norm_rows(r.x[...], r.g[:ONE])
        r.arrive()
        start_all(cps.start)

    for c in range(THREE):
        @pl.when(step == c)
        def _(c=c):
            for p, w in enumerate((r.wq, r.wk, r.wv)):
                t_rows = qkv_chunk(r, w[...])
                for head in range(FOUR):
                    a, b = head_halves(t_rows, head)
                    if p < TWO:
                        a, b = rotated(a, b, r)
                    out = r.out_s.at[p, head, c]
                    out[:HALF] = a.astype(BF)
                    out[HALF:] = b.astype(BF)
                start_all(cps.parts[c][FOUR * p:FOUR * p + FOUR])

        @pl.when(step == c + THREE)
        def _(c=c):
            wait_all(cps.parts[c])
            for src in range(FOUR):
                r.kr_s[TOK * src:TOK * src + TOK] = r.got[src, ONE, c].T
            io = lax.broadcasted_iota(jnp.int32, (QT, QT), ZERO)

            def q_pair(n, carry):
                src = sp_peer(n + ONE)
                pair = range(TWO)
                cols = [slice(QT * a, QT * a + QT) for a in pair]
                toks = [lax.broadcasted_iota(jnp.int32, (ONE, QT), ONE) + src * TOK + QT * a for a in pair]
                st, en = [doc_start(r.cu, tok) for tok in toks], [doc_stop(r.cu, tok) for tok in toks]
                for a in pair:
                    q_t = r.got[src, ZERO, c, :, cols[a]] * SCALE
                    for k in tiles:
                        r.s_s[a, k] = mm(r.kr_s[QT * k:QT * k + QT], q_t)
                top, total = [], []
                size = [(en[a] - st[a]).astype(jnp.uint32) for a in pair]
                for a in pair:
                    m = jnp.full((ONE, QT), NEG, F32)
                    for k in tiles:
                        s = jnp.where(since(io, st[a] - QT * k) < size[a], r.s_s[a, k], NEG)
                        r.s_s[a, k] = s
                        m = jnp.maximum(m, jnp.max(s, axis=ZERO, keepdims=True))
                    top.append(m)
                for a in pair:
                    part = jnp.zeros((ONE, QT), F32)
                    for k in tiles:
                        p = jnp.exp(r.s_s[a, k] - top[a])
                        part += jnp.sum(p, axis=ZERO, keepdims=True)
                        r.p_s[a, QT * k:QT * k + QT] = p.astype(BF)
                    total.append(part)
                for a in pair:
                    acc = jnp.zeros((HEAD, QT), F32)
                    for k in range(FOUR):
                        acc += mm(r.got[k, TWO, c], r.p_s[a, TOK * k:TOK * k + TOK])
                    r.o_s[src, c, :, cols[a]] = (acc / total[a]).astype(BF)
                    r.lse[c:c + ONE, row_tile(TWO * src + a)] = top[a] + jnp.log(total[a])
                for k, cp in enumerate(cps.heads[c]):
                    @pl.when(n == k)
                    def _(cp=cp):
                        cp.start()
                return carry

            lax.fori_loop(ZERO, FOUR, q_pair, ZERO)

    @pl.when(step == ROPED - ONE)
    def _():
        start_all(cps.keep)
        for c in range(THREE):
            wait_all(cps.heads[c])


def group_fwd_stage(cu, gain, w_qkv, tables, x):
    part = lambda p: spec((None, DM, RB), ZERO, ZERO, lambda s: THREE * p + jnp.minimum(s, TWO))
    ins = [('cu', cu, CU_SPEC), ('g', gain, GAINS), ('wq', w_qkv, part(ZERO)), ('wk', w_qkv, part(ONE)), ('wv', w_qkv, part(TWO)),
           ('cos', tables[ZERO], TABLE), ('sin', tables[ONE], TABLE), ('x', x, TOK_SPEC)]
    outs = [('h_m', TOKS, ANY), ('h_r', TOKS, ANY), ('out', sds(GROUP_QKV, BF), ANY), ('o_m', sds(BY_OWNER, BF), ANY),
            ('lse', sds((8, GRP), F32), spec((8, GRP)))]
    owner = pltpu.VMEM(BY_OWNER, BF)
    scratch = [('h', TOK_VMEM), ('out_s', pltpu.VMEM((THREE, FOUR, THREE, HEAD, TOK), BF)), ('got', pltpu.VMEM(GROUP_QKV, BF)),
               ('kr_s', pltpu.VMEM((GRP, HEAD), BF)), ('s_s', pltpu.VMEM((TWO, QTILES, QT, QT), F32)), ('p_s', pltpu.VMEM((TWO, GRP, QT), BF)),
               ('o_s', owner), ('o_r', owner)]
    return Stage(group_fwd_body, ROPED, ins, outs, scratch + named_sems(FOUR * 16), group_copies)


def attn0_bwd_body(cu_ref, q_ref, k_ref, v_ref, o_ref, do_ref, lse_ref, out_ref,
                   dk_s, dv_s, dq_s, kr_s, vr_s, s_s, d_s, p_s, t_s):
    tile = pl.program_id(ZERO)
    first, last, st, en = tile_bounds(cu_ref, tile)
    heads = range(THREE)

    @pl.when(tile == ZERO)
    def _():
        dk_s[...] = jnp.zeros(dk_s.shape, F32)
        dv_s[...] = jnp.zeros(dv_s.shape, F32)
        key_rows(kr_s, k_ref)
        key_rows(vr_s, v_ref)

    dq_s[...] = jnp.zeros(dq_s.shape, F32)
    io = lax.broadcasted_iota(jnp.int32, (QT, QT), ZERO)
    q_t = [q_ref[ZERO, ZERO, h] * SCALE for h in heads]
    do_t = [do_ref[ZERO, h] for h in heads]
    q_rows, do_rows = [q_t[h].T for h in heads], [do_t[h].T for h in heads]
    delta = [jnp.sum(do_t[h].astype(F32) * o_ref[ZERO, h].astype(F32), axis=ZERO, keepdims=True) for h in heads]
    lse = [lse_ref[h:h + ONE] for h in heads]
    size = (en - st).astype(jnp.uint32)

    def body(kt, carry):
        base = kt * QT
        src, cols = key_tile(kt)
        rows = row_tile(kt)
        ok = since(io, st - base) < size
        for h in heads:
            s_s[h] = mm(kr_s[h, rows], q_t[h])
            d_s[h] = mm(vr_s[h, rows], do_t[h])
        for h in heads:
            p = jnp.exp(jnp.where(ok, s_s[h] - lse[h], NEG))
            p_s[h] = p.astype(BF)
            t_s[h] = (p * (d_s[h] - delta[h])).astype(BF)
        for h in heads:
            dv_s[h, rows] += mm(p_s[h], do_rows[h])
            dk_s[h, rows] += mm(t_s[h], q_rows[h])
            dq_s[h] += mm(k_ref[src, ZERO, h, :, cols], t_s[h])
        return carry

    lax.fori_loop(first, last, body, ZERO)
    src, cols = key_tile(tile)
    for h in heads:
        out_ref[src, ZERO, h, :, cols] = (dq_s[h] * SCALE).astype(BF)

    @pl.when(tile == QTILES - ONE)
    def _():
        for src in range(FOUR):
            for h in heads:
                out_ref[src, ONE, h] = dk_s[h, TOK * src:TOK * src + TOK].T.astype(BF)
                out_ref[src, TWO, h] = dv_s[h, TOK * src:TOK * src + TOK].T.astype(BF)


def attn0_bwd(cu, qkv, o_t, do_t, lse):
    acc, rows = pltpu.VMEM((THREE, GRP, HEAD), F32), pltpu.VMEM((THREE, GRP, HEAD), BF)
    sq32, sq16 = pltpu.VMEM((THREE, QT, QT), F32), pltpu.VMEM((THREE, QT, QT), BF)
    return call(
        attn0_bwd_body, (QTILES,),
        [Q_SPEC, kv_spec(ONE), kv_spec(TWO), O_SPEC, O_SPEC, STAT_SPEC],
        spec(GROUP_QKV), sds(GROUP_QKV, BF),
        scratch=[acc, acc, pltpu.VMEM((THREE, HEAD, QT), F32), rows, rows, sq32, sq32, sq16, sq16],
        prefetch=ONE, flops=30 * GRP * GRP * HEAD, nbytes=TWELVE * MIB, name="attn0_bwd",
    )(cu, qkv, qkv, qkv, o_t, do_t, lse)


NBLK = TOK // LANE
EXT = TOK + TWO * WIN
XBLK = EXT // LANE
REACH = LANE + TWO * WIN
AHEAD_FWD, AHEAD_BWD = 4, 2
HPS = 4
HSTEPS = NHEAD // HPS


def heads_of(width, part):
    return spec((HPS, HEAD, width), lambda n: HSTEPS * part + n, ZERO, ZERO)


def own_head(part):
    return heads_of(TOK, part)


def row_of(width):
    return spec((HPS, ONE, width), step_of, ZERO, ZERO)


LOW, HIGH = slice(None, WIN), slice(WIN, None)
STAT = jax.ShapeDtypeStruct((NHEAD, ONE, TOK), F32)
STAT_BLOCK = spec((NHEAD, ONE, TOK))


def joined(left, mid, right, h, left_lanes=HIGH, right_lanes=LOW):
    return jnp.concatenate([left[h][:, left_lanes], mid[h], right[h][:, right_lanes]], axis=ONE)


def blocks(first, last):
    return slice(LANE * first, LANE * last)


def near_bounds(cu_ref, before, width):
    shift = lax.axis_index('sp') * TOK
    tok = lax.broadcasted_iota(jnp.int32, (ONE, width), ONE) + (shift - before)
    inside = (tok >= ZERO) & (tok < GRP)
    lo = jnp.maximum(doc_start(cu_ref, tok), tok - WIN) - (shift - WIN)
    hi = jnp.minimum(doc_stop(cu_ref, tok), tok + WIN + ONE) - (shift - WIN)
    return lo, jnp.where(inside, hi - lo, ZERO).astype(jnp.uint32)


def in_bounds(bounds, cols, first, n):
    io = lax.broadcasted_iota(jnp.int32, (n, LANE), ZERO)
    return since(io, bounds[ZERO][:, cols] - first) < bounds[ONE][:, cols]


def every_head(fn, ahead):
    def body(g, c):
        fn([ahead * g + a for a in range(ahead)])
        return c
    lax.fori_loop(ZERO, HPS // ahead, body, ZERO)


def attn1_fwd_body(r, step):
    bounds = near_bounds(r.cu, ZERO, TOK)

    def some(heads):
        v_all = []
        for a, h in enumerate(heads):
            q_t = r.q[h] * SCALE
            k_rows = joined(r.left, r.k, r.right, h, LOW, LOW).T
            v_all.append(joined(r.left, r.v, r.right, h, HIGH, HIGH))
            for i in range(NBLK):
                r.s_s[a, i] = mm(k_rows[LANE * i:LANE * i + REACH], q_t[:, blocks(i, i + ONE)])
        for a, h in enumerate(heads):
            for i in range(NBLK):
                cols = blocks(i, i + ONE)
                s = jnp.where(in_bounds(bounds, cols, LANE * i, REACH), r.s_s[a, i], NEG)
                m = jnp.max(s, axis=ZERO, keepdims=True)
                e = jnp.exp(s - m)
                l = jnp.sum(e, axis=ZERO, keepdims=True)
                r.p_s[a, i] = (e * (ONE / l)).astype(BF)
                r.lse[HPS * step + h, :, cols] = m + jnp.log(l)
        for a, h in enumerate(heads):
            for i in range(NBLK):
                out = mm(v_all[a][:, LANE * i:LANE * i + REACH], r.p_s[a, i]).astype(BF)
                r.o[HPS * step + h, :, blocks(i, i + ONE)] = out
    every_head(some, AHEAD_FWD)


def attn1_fwd_stage(cu, qkv, left, right):
    tile, edge = (AHEAD_FWD, NBLK, REACH, LANE), heads_of(LANE, ZERO)
    return Stage(
        attn1_fwd_body, HSTEPS,
        [('cu', cu, CU_SPEC), ('q', qkv, own_head(ZERO)), ('k', qkv, own_head(ONE)), ('v', qkv, own_head(TWO)),
         ('left', left, edge), ('right', right, edge)],
        [('lse', STAT, STAT_BLOCK)],
        [('o', pltpu.VMEM((NHEAD, HEAD, TOK), BF)), ('s_s', pltpu.VMEM(tile, F32)), ('p_s', pltpu.VMEM(tile, BF))])


def attn1_bwd_body(r, step):
    bounds = near_bounds(r.cu, WIN, EXT)

    def window(e):
        first, last = max(LANE * e - WIN, ZERO), min(LANE * e + LANE + WIN, EXT)
        return first, last - first

    def parts(h):
        q_t = joined(r.ql, r.q, r.qr, h) * SCALE
        return q_t, joined(r.dl, r.d, r.dr, h), joined(r.left, r.k, r.right, h, LOW, LOW)

    def some(heads):
        for a, h in enumerate(heads):
            q_t, do_t, k_t = parts(h)
            for n, arr in enumerate((q_t, do_t, k_t)):
                r.x_s[a, n] = arr
            k_rows, v_rows = k_t.T, joined(r.left, r.v, r.right, h, HIGH, HIGH).T
            for e in range(XBLK):
                first, n = window(e)
                cols = blocks(e, e + ONE)
                r.s_s[a, e, :n] = mm(k_rows[first:first + n], q_t[:, cols])
                r.d_s[a, e, :n] = mm(v_rows[first:first + n], do_t[:, cols])
        for a, h in enumerate(heads):
            lse, delta = joined(r.ll, r.lse, r.lr, h), joined(r.el, r.delta, r.er, h)
            for e in range(XBLK):
                first, n = window(e)
                cols = blocks(e, e + ONE)
                ok = in_bounds(bounds, cols, first, n)
                p = jnp.exp(jnp.where(ok, r.s_s[a, e, :n] - lse[:, cols], NEG))
                r.p_s[a, first:first + n, cols] = p.astype(BF)
                r.t_s[a, first:first + n, cols] = (p * (r.d_s[a, e, :n] - delta[:, cols])).astype(BF)
        for a, h in enumerate(heads):
            got = [[], [], []]
            for b in range(XBLK):
                here, wide = blocks(b, b + ONE), blocks(max(b - ONE, ZERO), min(b + TWO, XBLK))
                got[ZERO].append(mm(r.x_s[a, TWO, :, wide], r.t_s[a, wide, here]) * SCALE)
                got[ONE].append(mm_nt(r.x_s[a, ZERO, :, wide], r.t_s[a, here, wide]))
                got[TWO].append(mm_nt(r.x_s[a, ONE, :, wide], r.p_s[a, here, wide]))
            for n in range(THREE):
                own = jnp.concatenate([g.astype(BF) for g in got[n]], axis=ONE)[:, WIN:WIN + TOK]
                r.out[n, HPS * step + h] = own

    @pl.when(step == ZERO)
    def _():
        r.p_s[...] = jnp.zeros(r.p_s.shape, BF)
        r.t_s[...] = jnp.zeros(r.t_s.shape, BF)

    every_head(some, AHEAD_BWD)


def attn1_bwd_stage(cu, qkv, do_t, lse, delta, edges, far):
    edge, row = heads_of(LANE, ZERO), row_of(LANE)
    blk = (AHEAD_BWD, XBLK, REACH, LANE)
    square = pltpu.VMEM((AHEAD_BWD, EXT, EXT), BF)
    names = ('left', 'right', 'ql', 'qr', 'dl', 'dr')
    return Stage(
        attn1_bwd_body, HSTEPS,
        [('cu', cu, CU_SPEC), ('q', qkv, own_head(ZERO)), ('k', qkv, own_head(ONE)), ('v', qkv, own_head(TWO)), ('d', do_t, own_head(ZERO)),
         ('lse', lse, row_of(TOK)), ('delta', delta, row_of(TOK))]
        + [(n, arr, edge) for n, arr in zip(names, list(edges) + far[:FOUR])]
        + [(n, arr, row) for n, arr in zip(('ll', 'lr', 'el', 'er'), far[FOUR:])],
        [], [('out', pltpu.VMEM((THREE, NHEAD, HEAD, TOK), BF)), ('s_s', pltpu.VMEM(blk, F32)), ('d_s', pltpu.VMEM(blk, F32)),
             ('p_s', square), ('t_s', square), ('x_s', pltpu.VMEM((AHEAD_BWD, THREE, HEAD, EXT), BF))])


ROWBLK = [slice(r, r + RB) for r in range(ZERO, TOK, RB)]
HALFT = NFT // TWO
SQRT_HALF = math.sqrt(SCALE * FOUR)
PDF_SCALE = SQRT_HALF / math.sqrt(math.pi)


def normal_cdf(a):
    return SQRT_HALF * SQRT_HALF * (ONE + lax.erf(a * SQRT_HALF))


def half_rows(ref, which):
    n = ref.shape[ZERO] // TWO
    return ref.at[pl.ds(pl.multiple_of(which * n, n), n)]


def col_tile(ref, n):
    return ref.at[:, pl.ds(pl.multiple_of(n * FT, FT), FT)]


def mlp_copies(r, fwd, bwd):
    sw = Swaps(r.ssem, r.rsem, r.lsem)
    both = fwd and bwd
    c = Refs(dict(sw=sw, start=[], first=[], second=[]))
    if fwd:
        c.start += [sw.remote(r.h, r.h_r), sw.remote(half_rows(r.of, sw.other), r.of_r), sw.local(half_rows(r.of, sw.core), r.of_m)]
        there = [sw.remote(r.m_s.at[HALFT * sw.other + n], r.m_r.at[n] if both else col_tile(r.m_r, n)) for n in range(HALFT)]
        here = [None] * HALFT
        if not both:
            c.start += [sw.local(r.h, r.h_m), sw.local(r.x1, r.x1_m)]
            here = [sw.local(r.m_s.at[HALFT * sw.core + n], col_tile(r.m_m, n)) for n in range(HALFT)]
        c.m_out = list(zip(there, here))
    if bwd:
        c.start.append(sw.remote(r.dy, r.dy_r))
        c.dmid_out = sw.remote(r.dmid, r.dmid_r)
        c.du_out = [[sw.remote(r.du_s.at[n, sw.other], r.du_r.at[n] if both else col_tile(r.du_r, n))] for n in range(NFT)]
        if not both:
            for n in range(NFT):
                c.du_out[n].append(sw.local(r.du_s.at[n, sw.core], col_tile(r.du_m, n)))
            c.do_out = sw.to_all(lambda dev: r.do_s.at[dev], lambda dev: r.d_o.at[dev])
    if both:
        c.first = sw.early([c.start[ZERO], c.start[-ONE]] + there)
        c.second = sw.early([cp for part in c.du_out for cp in part])
    return c


def mlp_body(r, step, layer, fwd, bwd):
    cps = mlp_copies(r, fwd, bwd)
    sw, start, whole_group = cps.sw, cps.start, not (fwd and bwd)
    if fwd:
        m_out = cps.m_out
    if bwd:
        dmid_out, du_out = cps.dmid_out, cps.du_out

    @pl.when(step == ZERO)
    def _():
        if fwd:
            for n in range(NHEAD):
                r.of[HEAD * n:HEAD * n + HEAD, :] = (r.o[n % FOUR, n // FOUR] if whole_group else r.o[n])
            x1 = (r.x[...].astype(F32) + mm_tn(r.of[...], r.wp[...])).astype(BF)
            r.x1[...] = x1
            r.h[...] = norm_rows(x1, r.g[layer:layer + ONE])
            r.acc[...] = x1.astype(F32)
        if bwd:
            r.dacc[...] = jnp.zeros(r.dacc.shape, F32)
        r.arrive()
        start_all(start)

    for rows in ROWBLK:
        if fwd:
            ua = mm(r.h[rows], r.wa[...]).astype(BF)
            ub = mm(r.h[rows], r.wb[...]).astype(BF)
            if not bwd:
                r.u[ZERO, rows] = ua
                r.u[ONE, rows] = ub
        else:
            ua, ub = r.u[ZERO, rows], r.u[ONE, rows]
        a, b = ua.astype(F32), ub.astype(F32)
        cdf = normal_cdf(a)
        gate = a * cdf
        if fwd:
            m = (gate * b).astype(BF)
            r.m_s[step, rows] = m
            r.acc[rows] += mm(m, r.wo[...])
        if bwd:
            dm = mm_nt(r.dy[rows], r.wo[...]).astype(BF).astype(F32)
            pdf = jnp.exp(a * a * (SCALE * FOUR - ONE)) * PDF_SCALE
            db = (dm * gate).astype(BF)
            da = (dm * b * (cdf + a * pdf)).astype(BF)
            r.du_s[step, ZERO, rows] = da
            r.du_s[step, ONE, rows] = db
            r.dacc[rows] += mm_nt(da, r.wa[...]) + mm_nt(db, r.wb[...])

    for n in range(NFT):
        @pl.when(step == n)
        def _(n=n):
            if fwd:
                there, here = m_out[n % HALFT]

                if here:
                    @pl.when(sw.core == n // HALFT)
                    def _():
                        here.start()

                @pl.when(sw.other == n // HALFT)
                def _():
                    there.start()
            if bwd:
                for cp in du_out[n]:
                    cp.start()

    @pl.when(step == NFT - ONE)
    def _():
        if fwd:
            r.y[...] = r.acc[...].astype(BF)
        if bwd:
            d_ln, gg = norm_rows_grad(r.x1[...], r.g[layer:layer + ONE], r.dacc[...].astype(BF))
            r.gg[...] = gg
            d_mid = add_bf(r.dy[...], d_ln)
            r.dmid[...] = d_mid
            dmid_out.start()
            d_att = mm_nt(r.wp[...], d_mid).astype(BF)
            for n in range(NHEAD):
                rows = slice(HEAD * n, HEAD * n + HEAD)
                blk = d_att[rows]
                if whole_group:
                    r.do_s[n % FOUR, n // FOUR] = blk
                else:
                    r.d_o[n] = blk
                    r.delta[n] = jnp.sum(blk.astype(F32) * r.of[rows].astype(F32), axis=ZERO, keepdims=True)
            if whole_group:
                start_all(cps.do_out)


def mlp_stage(layer, fwd, bwd, w_proj, gain, w_in, w_out, links=None, **arrays):
    u_spec = spec((TWO, TOK, FT), ZERO, ZERO, step_of)
    half_o = sds((DM // TWO, TOK), BF)
    half_m, half_u = sds((TOK, FF // TWO), BF), sds((TOK, FF), BF)
    heads = (NHEAD, HEAD, TOK)
    sums = pltpu.VMEM(ALLTOK, F32)
    links = links or {}
    ins = [('wp', w_proj, spec((None, DM, DM), layer, ZERO, ZERO)), ('g', gain, GAINS),
           ('wa', w_in, weight_cols(layer, FT)), ('wb', w_in, weight_cols(layer, FT, NFT)),
           ('wo', w_out, spec((None, FT, DM), layer, step_of, ZERO))]
    kinds = dict(x=TOK_SPEC, dy=TOK_SPEC, x1=TOK_SPEC, u=u_spec)
    ins += [(n, arr, kinds[n]) for n, arr in arrays.items()]
    outs, scratch, both = [], [], fwd and bwd
    own_tiles, far_tiles = pltpu.VMEM((HALFT, TOK, FT), BF), pltpu.VMEM((NFT, TOK, FT), BF)
    if fwd:
        outs += [('y', TOKS, TOK_SPEC), ('of_m', half_o, ANY), ('of_r', half_o, ANY)]
        scratch += [('acc', sums), ('of', pltpu.VMEM((DM, TOK), BF)), ('m_s', pltpu.VMEM((NFT, TOK, FT), BF)), ('h', TOK_VMEM),
                    ('x1', TOK_VMEM)]
    if fwd and not bwd:
        outs += [('h_m', TOKS, ANY), ('h_r', TOKS, ANY), ('m_m', half_m, ANY), ('m_r', half_m, ANY)]
        outs += [('x1_m', TOKS, ANY), ('u', sds((TWO, TOK, FF), BF), u_spec)]
    if bwd:
        shape = heads if fwd else BY_OWNER
        outs += [('dmid', TOKS, TOK_SPEC), ('gg', sds((ONE, DM), F32), spec((ONE, DM))), ('d_o', sds(shape, BF), spec(shape) if fwd else ANY),
                 ('dmid_r', TOKS, ANY)]
        scratch += [('dacc', sums), ('du_s', pltpu.VMEM((NFT, TWO, TOK, FT), BF))]
    if bwd and not fwd:
        outs += [('dy_r', TOKS, ANY), ('du_m', half_u, ANY), ('du_r', half_u, ANY)]
    if both:
        outs += [('delta', STAT, STAT_BLOCK)]
        scratch += [('h_r', TOK_VMEM), ('dy_r', TOK_VMEM), ('m_r', own_tiles), ('du_r', far_tiles)]
    if not fwd:
        scratch += [('do_s', pltpu.VMEM(BY_OWNER, BF))]
    return Stage(functools.partial(mlp_body, layer=layer, fwd=fwd, bwd=bwd), NFT, ins, outs, scratch + named_sems(FOUR * NFT),
                 functools.partial(mlp_copies, fwd=fwd, bwd=bwd), links)


def side_grad_copies(r):
    sw = Swaps(r.ssem, r.rsem, r.lsem)
    for n, src in enumerate((r.q_all.at[:NHEAD], r.d_o, r.lse, r.delta)):
        sw.to_sides(src.at[:, :, :LANE], src.at[:, :, TOK - LANE:], getattr(r, FAR[TWO * n]), getattr(r, FAR[TWO * n + ONE]))
    return Refs(dict(sw=sw))


def side_grad_body(r, step):
    sw = side_grad_copies(r).sw
    mlp = mlp_copies(Refs(dict(r.__dict__, ssem=r.mlp_ssem, rsem=r.mlp_rsem, lsem=r.mlp_lsem)), True, True)

    @pl.when(step == ZERO)
    def _():
        start_all(sw.waits)
        wait_all(mlp.first)

    @pl.when(step < HALFT)
    def _():
        r.out[...] = mm_tn(r.m_s[HALFT * sw.core + step], r.dy[...]) + mm_tn(r.m_r[step], r.dy_r[...])

    @pl.when(step == HALFT)
    def _():
        wait_all(mlp.second)
        r.h_t[ZERO] = r.h[...].T
        r.h_t[ONE] = r.h_r[...].T

    @pl.when(step >= HALFT)
    def _():
        n = step - HALFT
        r.out[...] = mm(r.h_t[ZERO], r.du_s[n, sw.core]) + mm(r.h_t[ONE], r.du_r[n])


FAR = ('ql', 'qr', 'dl', 'dr', 'll', 'lr', 'el', 'er')


def side_grad_stage(qkv):
    kinds = [(NHEAD, HEAD, LANE, BF)] * FOUR + [(NHEAD, ONE, LANE, F32)] * FOUR
    far = [(n, sds(shape, dtype), ANY) for n, (*shape, dtype) in zip(FAR, kinds)]
    names = ('m_s', 'du_s', 'h', 'h_r', 'dy', 'dy_r', 'm_r', 'du_r', 'd_o', 'delta', 'of', 'of_r', 'of_m', 'dmid', 'dmid_r')
    links = {n: (ONE, n) for n in names}
    links.update({'mlp_' + n: (ONE, n) for n in ('ssem', 'rsem', 'lsem')}, lse=(ZERO, 'lse'))
    return Stage(side_grad_body, HALFT + NFT, [('q_all', qkv, ANY)],
                 [('out', sds((MLP_ROWS, DM), F32), spec(ALLDM, step_of, ZERO))] + far,
                 [('h_t', pltpu.VMEM((TWO, DM, TOK), BF))] + named_sems(8), side_grad_copies, links)


NAMED = ('ha', 'hb', 'oa', 'ob', 'dma', 'dmb')


def third(ref, n):
    return ref.at[PROJ * n:PROJ * n + PROJ]


def qkv_bwd_copies(r, grads):
    sw = Swaps(r.ssem, r.rsem, r.lsem)
    c = Refs(dict(sw=sw, parts=[[sw.remote(r.dt_s.at[sw.other, n], third(r.dt_r, n))] for n in range(THREE)]))
    if grads:
        c.loads = sw.early([sw.local(getattr(r, n + '_in'), getattr(r, n)) for n in NAMED])
        for part in c.parts:
            sw.early(part)
    else:
        for n in range(THREE):
            c.parts[n].append(sw.local(r.dt_s.at[sw.core, n], third(r.dt_m, n)))
    return c


def qkv_bwd_body(r, step, layer, grads):
    cps = qkv_bwd_copies(r, grads)
    sw, copies = cps.sw, cps.parts

    @pl.when(step == ZERO)
    def _():
        r.acc[...] = jnp.zeros(r.acc.shape, F32)
        if grads:
            start_all(cps.loads)

    for p in range(THREE):
        @pl.when(step == p)
        def _(p=p):
            cos, sin = r.cos[...], r.sin[...]
            for chunk in CHUNKS:
                for head in range(FOUR):
                    blk = r.d[head, ZERO, chunk] if grads else r.d[p, FOUR * chunk + head]
                    a, b = blk[:HALF], blk[HALF:]
                    if p < TWO:
                        a, b = a.astype(F32), b.astype(F32)
                        a, b = (a * cos + b * sin).astype(BF), (b * cos - a * sin).astype(BF)
                    at, full = LANE * chunk + HEAD * (head % TWO), RB * chunk + HEAD * head
                    for n, val in ((ZERO, a), (HALF, b)):
                        r.dt_s[head // TWO, p, at + n:at + n + HALF] = val
                        r.dt_all[full + n:full + n + HALF] = val
            if p == ZERO:
                r.arrive()
            start_all(copies[p])
            r.acc[...] += mm(r.w[...], r.dt_all[...])

    @pl.when(step == TWO)
    def _():
        d_ln, gg = norm_rows_grad(r.x[...], r.g[layer:layer + ONE], r.acc[...].T.astype(BF))
        r.gg[...] = gg
        r.dx[...] = add_bf(r.dmid[...], d_ln)

    if grads:
        @pl.when(step == THREE)
        def _():
            wait_all(cps.loads)
            for part in copies:
                wait_all(part)
            r.out[...] = mm(r.oa[...], r.dma[...]) + mm(r.ob[...], r.dmb[...])

        for p in range(THREE):
            @pl.when(step == p + FOUR)
            def _(p=p):
                r.out[...] = mm(r.dt_s[sw.core, p], r.ha[...]) + mm(third(r.dt_r, p)[...], r.hb[...])


def qkv_bwd_stage(layer, tables, w_qkv, x, gain, d_mid, d=None, link=None, grads=None, pairs=()):
    part = lambda s: jnp.minimum(s, TWO)
    ins = [('cos', tables[ZERO], TABLE), ('sin', tables[ONE], TABLE), ('w', w_qkv, spec((None, DM, DM), layer, ZERO, part)),
           ('x', x, TOK_SPEC), ('g', gain, GAINS), ('dmid', d_mid, TOK_SPEC)]
    outs = [('dx', TOKS, TOK_SPEC), ('gg', sds((ONE, DM), F32), spec((ONE, DM)))]
    feats = (THREE * PROJ, TOK)
    scratch = [('acc', pltpu.VMEM((DM, TOK), F32)), ('dt_s', pltpu.VMEM((TWO, THREE, PROJ, TOK), BF)), ('dt_all', pltpu.VMEM((DM, TOK), BF))]
    steps, alias = THREE, ()
    if grads is None:
        outs += [('dt_m', sds(feats, BF), ANY), ('dt_r', sds(feats, BF), ANY)]
    else:
        first = (ATT_ROWS + MLP_ROWS) // PROJ
        ins += [('d', d, spec((FOUR, ONE, THREE, HEAD, TOK), ZERO, part, ZERO, ZERO, ZERO)), ('grads', grads, ANY)]
        ins += [(n + '_in', arr, ANY) for n, arr in zip(NAMED, pairs)]
        outs += [('out', sds(grads.shape, F32), spec((PROJ, DM), lambda s: first + jnp.maximum(s - THREE, ZERO), ZERO))]
        scratch += [('dt_r', pltpu.VMEM(feats, BF))] + [(n, pltpu.VMEM(arr.shape, BF)) for n, arr in zip(NAMED, pairs)]
        steps, alias = steps + FOUR, (('grads', 'out'),)
    flag = grads is not None
    return Stage(functools.partial(qkv_bwd_body, layer=layer, grads=flag), steps, ins, outs, scratch + named_sems(TWELVE),
                 functools.partial(qkv_bwd_copies, grads=flag), {} if link is None else {'d': link}, alias)


NDOWN = DOWN // DM


def grad_call(body, grads, steps, in_specs, args, rows, first_row, total, scratch=()):
    shared = [] if grads is None else [grads]
    first = first_row // rows
    return call(
        body, (steps,), [ANY] * len(shared) + in_specs,
        spec((rows, DM), lambda s: first + s, ZERO), sds((total, DM), F32), scratch=scratch,
        flops=FOUR * steps * rows * TOK * DM, nbytes=20 * MIB, name=body.__name__,
        alias={ZERO: ZERO} if shared else None,
    )(*shared, *args)


GRAD_INS = 8


def grad_mlp_body(*refs):
    ma, mb, dya, dyb, ha, hb, dua, dub, out_ref, h_t = refs[-GRAD_INS - TWO:]
    step = pl.program_id(ZERO)

    @pl.when(step < NDOWN)
    def _():
        out_ref[...] = mm_tn(ma[...], dya[...]) + mm_tn(mb[...], dyb[...])

    @pl.when(step == NDOWN)
    def _():
        h_t[ZERO] = ha[...].T
        h_t[ONE] = hb[...].T

    @pl.when(step >= NDOWN)
    def _():
        out_ref[...] = mm(h_t[ZERO], dua[...]) + mm(h_t[ONE], dub[...])


def grad_mlp(grads, m, m_r, dy, dy_r, h, h_r, du, du_r, first_row, total):
    toks = spec(ALLTOK)
    m_col = spec(ALLTOK, ZERO, lambda s: jnp.minimum(s, NDOWN - ONE))
    du_col = spec(ALLTOK, ZERO, lambda s: jnp.maximum(s - NDOWN, ZERO))
    return grad_call(grad_mlp_body, grads, NDOWN + UP // DM, [m_col, m_col, toks, toks, toks, toks, du_col, du_col],
                     (m, m_r, dy, dy_r, h, h_r, du, du_r), DM, first_row, total, scratch=[pltpu.VMEM((TWO, DM, TOK), BF)])


def grad_att_body(*refs):
    oa, ob, dma, dmb, ta, tb, ha, hb, out_ref = refs[-GRAD_INS - ONE:]
    step = pl.program_id(ZERO)

    @pl.when(step == ZERO)
    def _():
        out_ref[...] = mm(oa[...], dma[...]) + mm(ob[...], dmb[...])

    @pl.when(step > ZERO)
    def _():
        out_ref[...] = mm(ta[...], ha[...]) + mm(tb[...], hb[...])


def grad_att(grads, of, of_r, dmid, dmid_r, dt, dt_r, h, h_r, first_row):
    toks = spec(ALLTOK)
    blk = (PROJ, TOK)
    dt_row = spec(blk, lambda s: jnp.maximum(s - ONE, ZERO), ZERO)
    return grad_call(grad_att_body, grads, ONE + QKV // PROJ, [spec(blk), spec(blk), toks, toks, dt_row, dt_row, toks, toks],
                     (of, of_r, dmid, dmid_r, dt, dt_r, h, h_r), PROJ, first_row, RING_ROWS)


NB, NS = 5, 6
CH = RING_ROWS // (NB * FOUR)
SB, LF = CH // FOUR, CH // 16
RS = 9
LAST = RS + RS
ADD_ROWS = 96


def ring_body(g_ref, *refs):
    gains, refs = refs[:FOUR], refs[FOUR:]
    (f_ref, lnout_ref, bufa, bufb, bufc, gath, stage, lnbuf, ssem, rsem, psem, qsem, csem, stsem, lns, lnr) = refs
    core, partner = core_and_partner()
    zy = lax.axis_index('zy')
    pos = (lax.axis_index('sp'), lax.rem(zy, FOUR), zy // FOUR)
    streams = [(c, sg) for c in range(THREE) for sg in (ONE, -ONE)]
    bufs, sizes = (bufa, bufb, bufc), (CH, SB, LF)
    peers = range(ONE, FOUR)

    def mod4(v):
        return lax.rem(v + 8, FOUR)

    def at(axis, val):
        if axis == ZERO:
            return {'sp': val}
        yz = (val, pos[TWO]) if axis == ONE else (pos[ONE], val)
        return {'zy': yz[ONE] * FOUR + yz[ZERO]}

    def shifted(axis, d):
        return at(axis, mod4(pos[axis] + d))

    def axis_of(s, ph):
        return (streams[s][ZERO] + ph) % THREE

    def idx(s, ph, t):
        return mod4(pos[axis_of(s, ph)] - streams[s][ONE] * t)

    def own(s, ph):
        return idx(s, ph, -ONE)

    def base(b):
        return b * (FOUR * CH)

    bar = pltpu.get_barrier_semaphore()
    for ax in range(THREE):
        for d in peers:
            pl.semaphore_signal(bar, inc=ONE, device_id=shifted(ax, d), device_id_type=MESH)
    pl.semaphore_signal(bar, inc=ONE, device_id=partner, device_id_type=MESH)
    pl.semaphore_wait(bar, 10)

    def rows(ref, start, n):
        return ref.at[pl.ds(pl.multiple_of(start, LF), n)]

    def grows(s, start, n):
        return g_ref.at[pl.ds(pl.multiple_of(start, LF), n), LANE * s:LANE * s + LANE]

    def frows(s, start, n):
        return f_ref.at[core, pl.ds(pl.multiple_of(start, LF), n), LANE * s:LANE * s + LANE]

    def same_bytes(b, k):
        if k < RS:
            return bufs[k // THREE].at[b, k % THREE]
        n = sizes[TWO - (k - RS) // THREE]
        return gath.at[b] if n == CH else gath.at[b, :, pl.ds(ZERO, n)]

    def wait_for(ref, sem):
        pltpu.make_async_copy(ref, ref, sem).wait()

    def send(b, s, k):
        ph = k // THREE if k < RS else TWO - (k - RS) // THREE
        t = k % THREE
        n = sizes[ph]
        if k < RS:
            dst = bufs[ph].at[b, t, s]
            if t:
                src = bufs[ph].at[b, t - ONE, s]
            elif ph:
                src = rows(bufs[ph - ONE].at[b, TWO, s], idx(s, ph, ZERO) * n, n)
            else:
                src = grows(s, base(b) + idx(s, ZERO, ZERO) * n, n)
        elif ph:
            off = own(s, ONE) * SB if ph == TWO else ZERO
            src = dst = rows(gath.at[b, s], off + idx(s, ph, t - ONE) * n, n)
        else:
            dst = frows(s, base(b) + idx(s, ZERO, t - ONE) * n, n)
            src = dst if t else gath.at[b, s]
        pltpu.make_async_remote_copy(src_ref=src, dst_ref=dst, send_sem=ssem.at[b, k], recv_sem=rsem.at[b, k],
                                     device_id=shifted(axis_of(s, ph), streams[s][ONE]), device_id_type=MESH).start()

    def stage_load(n):
        t, b, slot = n // NB, lax.rem(n, NB), lax.rem(n, TWO)
        for s in range(NS):
            pltpu.make_async_copy(grows(s, base(b) + idx(s, ZERO, t + ONE) * CH, CH), stage.at[slot, s],
                                  stsem.at[slot]).start()

    def ln_copy(ph, d):
        return pltpu.make_async_remote_copy(
            src_ref=lnbuf.at[ph, THREE], dst_ref=lnbuf.at[ph, d - ONE], send_sem=lns.at[ph, d - ONE],
            recv_sem=lnr.at[ph, d - ONE], device_id=shifted(ph, d) if ph < THREE else partner, device_id_type=MESH)

    def ln_sum(ph):
        vals = [lnbuf[ph, THREE]] + [lnbuf[ph, d - ONE] for d in peers]
        total = jnp.zeros_like(vals[ZERO])
        for p in range(FOUR):
            term = vals[ZERO]
            for d in peers:
                term = jnp.where(mod4(pos[ph] - d) == p, vals[d], term)
            total = total + term
        return total

    def batches(fn, start=ZERO):
        def body(b, c):
            fn(b)
            return c
        lax.fori_loop(start, NB, body, ZERO)

    def first(b):
        for s in range(NS):
            send(b, s, ZERO)

    lnbuf[ZERO, THREE] = jnp.zeros(lnout_ref.shape, F32)
    for n, gain in enumerate(gains):
        lnbuf[ZERO, THREE, n:n + ONE] = gain[...]
    first(ZERO)
    stage_load(jnp.int32(ZERO))
    for d in peers:
        ln_copy(ZERO, d).start()
    batches(first, ONE)

    for k in range(RS):
        ph, t = k // THREE, k % THREE
        buf, size = bufs[ph], sizes[ph]

        def step(b, k=k, ph=ph, t=t, buf=buf, size=size):
            n = k * NB + b
            slot = lax.rem(n, TWO)
            if not ph:
                @pl.when(n < THREE * NB - ONE)
                def _():
                    stage_load(n + ONE)
                wait_for(stage.at[slot], stsem.at[slot])
            wait_for(same_bytes(b, k), rsem.at[b, k])
            for s in range(NS):
                if ph:
                    off = pl.multiple_of(idx(s, ph, t + ONE) * size, LF)
                    buf[b, t, s] += bufs[ph - ONE][b, TWO, s, pl.ds(off, size)]
                else:
                    @pl.loop(ZERO, CH, step=ADD_ROWS)
                    def _(r):
                        at_r = pl.ds(pl.multiple_of(r, ADD_ROWS), ADD_ROWS)
                        buf[b, t, s, at_r] += stage[slot, s, at_r]
                if k == RS - ONE:
                    off = pl.multiple_of(own(s, ONE) * SB + own(s, TWO) * LF, LF)
                    gath[b, s, pl.ds(off, LF)] = bufc[b, TWO, s]
                send(b, s, k + ONE)

        batches(step)
        if k < SIX and k % TWO == ZERO:
            lp = k // TWO
            for d in peers:
                ln_copy(lp, d).wait()
            lnbuf[lp + ONE, THREE] = ln_sum(lp)
            for d in peers if lp < TWO else (ONE,):
                ln_copy(lp + ONE, d).start()

    def hand_over(b, s, j, src, start):
        pltpu.make_async_remote_copy(src_ref=src, dst_ref=frows(s, start, CH), send_sem=psem.at[b, j], recv_sem=qsem.at[b, j],
                                     device_id=partner, device_id_type=MESH).start()

    for k in range(RS, LAST):
        def step(b, k=k):
            wait_for(same_bytes(b, k), rsem.at[b, k])
            piece = k - (LAST - FOUR)
            for s in range(NS):
                if k < LAST - ONE:
                    send(b, s, k + ONE)
                if piece >= ZERO:
                    start = base(b) + idx(s, ZERO, piece - ONE) * CH
                    if piece:
                        hand_over(b, s, piece, frows(s, start, CH), start)
                    else:
                        pltpu.make_async_copy(gath.at[b, s], frows(s, start, CH), csem.at[b]).start()
                        hand_over(b, s, piece, gath.at[b, s], start)
        batches(step)

    ln_copy(THREE, ONE).wait()
    lnout_ref[...] = lnbuf[THREE, THREE] + lnbuf[THREE, ZERO]

    def finish(b):
        for k in range(LAST):
            wait_for(same_bytes(b, k), ssem.at[b, k])
        for j in range(FOUR):
            wait_for(gath.at[b], psem.at[b, j])
            wait_for(gath.at[b], qsem.at[b, j])
        wait_for(gath.at[b], csem.at[b])
    batches(finish)


def ring_all_reduce(g, gains, cid):
    vmem = pl.BlockSpec(memory_space=pltpu.VMEM)
    ln = sds((8, DM), F32)
    return pl.pallas_call(
        ring_body,
        in_specs=[ANY] + [vmem] * FOUR,
        out_specs=[ANY, vmem],
        out_shape=[sds((TWO, RING_ROWS, DM), F32), ln],
        scratch_shapes=[
            pltpu.VMEM((NB, THREE, NS, CH, LANE), F32), pltpu.VMEM((NB, THREE, NS, SB, LANE), F32),
            pltpu.VMEM((NB, THREE, NS, LF, LANE), F32), pltpu.VMEM((NB, NS, CH, LANE), F32),
            pltpu.VMEM((TWO, NS, CH, LANE), F32),
            pltpu.VMEM((FOUR, FOUR) + ln.shape, F32),
            DMA((NB, LAST)), DMA((NB, LAST)), DMA((NB, FOUR)), DMA((NB, FOUR)), DMA((NB,)), DMA((TWO,)),
            DMA((FOUR, THREE)), DMA((FOUR, THREE)),
        ],
        compiler_params=pltpu.CompilerParams(collective_id=cid, has_side_effects=True, vmem_limit_bytes=60 * MIB),
        cost_estimate=pl.CostEstimate(flops=MIB * MIB // FOUR, bytes_accessed=200 * MIB, transcendentals=ZERO),
        name="ring_all_reduce",
    )(g, *gains)


SLOTS, LAG = 12, 6
NTURN = TWO * THREE
OUT_SHAPE, IN_SHAPE = (TWO, FF, DM), (TWO, DM, TWO * FF)


def stream(pieces, buf, turned, isem, osem, between=None):
    def loads(i):
        slot, srcs = i % SLOTS, pieces[i][ZERO]
        n = srcs[ZERO].shape[ZERO]
        return [pltpu.make_async_copy(src, buf.at[slot, k * n:k * n + n], isem.at[slot, k]) for k, src in enumerate(srcs)]

    def store(i):
        _, dst, turn = pieces[i]
        src = buf.at[i % SLOTS, :dst.shape[ZERO]] if turn is None else turned.at[turn]
        return pltpu.make_async_copy(src, dst, osem.at[i % SLOTS])

    total = len(pieces)
    for i in range(total + LAG):
        if i == SLOTS and between:
            between()
        if i < total:
            if i >= SLOTS:
                store(i - SLOTS).wait()
            for cp in loads(i):
                cp.start()
        k = i - LAG
        if k >= ZERO:
            for cp in loads(k):
                cp.wait()
            turn = pieces[k][TWO]
            if turn is not None:
                for n in CHUNKS:
                    rows, col = LANE * n, RB * n
                    turned[turn, :, col:col + LANE] = buf[k % SLOTS, rows:rows + LANE].T
                    turned[turn, :, col + LANE:col + RB] = buf[k % SLOTS, PROJ + rows:PROJ + rows + LANE].T
            store(k).start()
    for i in range(max(total - SLOTS, ZERO), total):
        store(i).wait()


def unpack_ring_body(f, y_in, dx_in, gains, g_qkv, g_proj, g_in, g_out, y, dx, g_attn, g_mlp, y_s, dx_s, *scratch):
    small_in, small_out, *scratch = scratch
    loads = [pltpu.make_async_copy(src, dst, small_in.at[n]) for n, (src, dst) in enumerate(((y_in, y_s), (dx_in, dx_s)))]
    stores = [pltpu.make_async_copy(src, dst, small_out.at[n]) for n, (src, dst) in enumerate(((y_s, y), (dx_s, dx)))]
    start_all(loads)
    g_attn[...] = gains[:TWO]
    g_mlp[...] = gains[TWO:FOUR]

    def between():
        wait_all(loads)
        start_all(stores)

    def block(c, row, n=DM):
        return f.at[c, row:row + n]

    pieces = []
    for c in range(TWO):
        for n in range(NDOWN):
            pieces.append(([block(c, ATT_ROWS + DM * n)], g_out.at[ZERO, DOWN * c + DM * n:DOWN * c + DM * n + DM], None))
        for n in range(FOUR):
            col = UP * c + DM * n
            pieces.append(([block(c, ATT_ROWS + DOWN + DM * n)], g_in.at[ZERO, :, col:col + DM], None))
    for l in range(TWO):
        first = (ONE - l) * (ATT_ROWS + MLP_ROWS)
        for n in range(THREE):
            row = first + PROJ * (n + ONE)
            pieces.append(([block(c, row, PROJ) for c in range(TWO)], g_qkv.at[l, :, DM * n:DM * n + DM], THREE * l + n))
        for c in range(TWO):
            pieces.append(([block(c, first, PROJ)], g_proj.at[l, PROJ * c:PROJ * c + PROJ], None))
    stream(pieces, *scratch, between=between)
    wait_all(stores)


def unpack_mlp_body(own, other, in_0, out_0, g_in, g_out, *scratch):
    core = lax.axis_index('core')
    pieces = []
    for src, side in ((own, core), (other, ONE - core)):
        for n in range(NDOWN):
            row = pl.multiple_of(DOWN * side + DM * n, DM)
            pieces.append(([src.at[DM * n:DM * n + DM]], g_out.at[ONE, pl.ds(row, DM)], None))
        for n in range(FOUR):
            col = pl.multiple_of(UP * side + DM * n, DM)
            pieces.append(([src.at[DOWN + DM * n:DOWN + DM * n + DM]], g_in.at[ONE, :, pl.ds(col, DM)], None))
    stream(pieces, *scratch)


def unpack_call(body, args, outs, alias, name, in_specs=None, out_specs=None, small=()):
    return pl.pallas_call(
        body, in_specs=in_specs or [ANY] * len(args), out_specs=out_specs or [ANY] * len(outs), out_shape=outs,
        scratch_shapes=list(small) + [pltpu.VMEM((SLOTS, DM, DM), F32), pltpu.VMEM((NTURN, DM, DM), F32),
                                      DMA((SLOTS, TWO)), DMA((SLOTS,))],
        input_output_aliases=alias,
        compiler_params=pltpu.CompilerParams(vmem_limit_bytes=60 * MIB),
        cost_estimate=pl.CostEstimate(flops=MIB * MIB // RB, bytes_accessed=75 * MIB, transcendentals=ZERO), name=name,
    )(*args)


def rope_tables(pos, base):
    inv_freq = base ** (jnp.arange(HALF).astype(F32) * (-TWO / HEAD))
    angles = inv_freq[:, None] * pos.astype(F32)[None, :]
    return jnp.cos(angles), jnp.sin(angles)


def solution(mesh):
    n_sp = mesh.shape['sp']
    by_core = mesh.devices.reshape(n_sp, mesh.shape['dp'] // TWO, TWO)
    mesh = Mesh(by_core, ('sp', 'zy', 'core'))
    dp_axes = ('zy', 'core')
    row_axes = dp_axes + ('sp',)
    token_spec = P(row_axes, None)
    swap_cores = [(ZERO, ONE), (ONE, ZERO)]
    cids = list(range(RS))

    def exchange(arr):
        return lax.all_to_all(arr, 'sp', ZERO, ZERO, tiled=True)

    def device_step(x_loc, cu_loc, pos_loc, w_qkv, w_proj, w_in, w_out, ln_attn, ln_mlp, d_out):
        tab0, tab1 = [rope_tables(pos_loc, base) for base in BASES]
        mlp_args, w_mlp = (w_proj, ln_mlp), (w_in, w_out)

        q0, f0, q1 = run("layer0_qkv1", cids[ONE], row_peers, group_fwd_stage(cu_loc, ln_attn, w_qkv, tab0, x_loc),
                         mlp_stage(ZERO, True, False, *mlp_args, *w_mlp, links={'o': (ZERO, 'o_r'), 'x': (ZERO, 'x')}),
                         qkv_fwd_stage(ONE, ln_attn, w_qkv, tab1, (ONE, 'y')))
        kv_edges = (q1.left, q1.right)
        a1, f1, s1 = run("attn1_mlp1", cids[TWO], near_peers, attn1_fwd_stage(cu_loc, q1.out, *kv_edges),
                         mlp_stage(ONE, True, True, *mlp_args, *w_mlp, links={'o': (ZERO, 'o')}, x=f0.y, dy=d_out),
                         side_grad_stage(q1.out))
        g_side = lax.psum(s1.out, ('sp', 'zy'))
        far = [getattr(s1, n) for n in FAR]
        _, t1, b0 = run("attn1_qkv1_mlp0", cids[5], row_peers,
                        attn1_bwd_stage(cu_loc, q1.out, f1.d_o, a1.lse, f1.delta, kv_edges, far),
                        qkv_bwd_stage(ONE, tab1, w_qkv, f0.y, ln_attn, f1.dmid, link=(ZERO, 'out')),
                        mlp_stage(ZERO, False, True, *mlp_args, *w_mlp, links={'dy': (ONE, 'dx')}, x1=f0.x1_m, u=f0.u))
        dqkv0 = exchange(attn0_bwd(cu_loc, q0.out, q0.o_m, b0.d_o, q0.lse))
        grads = grad_att(None, f1.of_m, f1.of_r, f1.dmid, f1.dmid_r, t1.dt_m, t1.dt_r, q1.h_m, q1.h_r, ZERO)
        grads = grad_mlp(grads, f0.m_m, f0.m_r, t1.dx, b0.dy_r, f0.h_m, f0.h_r, b0.du_m, b0.du_r, ATT_ROWS, RING_ROWS)
        t0, = run("qkv0_grads", cids[SIX], partner_peer, qkv_bwd_stage(
            ZERO, tab0, w_qkv, x_loc, ln_attn, b0.dmid, d=dqkv0, grads=grads,
            pairs=(q0.h_m, q0.h_r, f0.of_m, f0.of_r, b0.dmid, b0.dmid_r)))

        gains = (t0.gg, t1.gg, b0.gg, f1.gg)
        summed, gains = ring_all_reduce(t0.out, gains, cids[ZERO])
        summed, g_side = lax.optimization_barrier((summed, g_side))
        from_partner = lax.ppermute(g_side, 'core', swap_cores)
        shapes = [sds(shape, F32) for shape in ((TWO, DM, THREE * DM), (TWO, DM, DM), IN_SHAPE, OUT_SHAPE)]
        vmem = pl.BlockSpec(memory_space=pltpu.VMEM)
        gain = sds((TWO, DM), F32)
        g_qkv, g_proj, g_in, g_out, y, dx, g_attn, g_mlp = unpack_call(
            unpack_ring_body, (summed, f1.y, t0.dx, gains), shapes + [TOKS, TOKS, gain, gain], {}, "unpack_ring",
            [ANY] * THREE + [vmem], [ANY] * SIX + [vmem] * TWO, [TOK_VMEM, TOK_VMEM, DMA((TWO,)), DMA((TWO,))])
        g_in, g_out = unpack_call(unpack_mlp_body, (g_side, from_partner, g_in, g_out), shapes[TWO:],
                                  {TWO: ZERO, THREE: ONE}, "unpack_mlp")
        return y, dx, g_qkv, g_proj, g_in, g_out, g_attn, g_mlp

    in_specs = (token_spec, P(dp_axes, None), P(row_axes)) + (P(),) * SIX + (token_spec,)
    out_specs = (token_spec, token_spec) + (P(),) * SIX
    return jax.shard_map(device_step, mesh=mesh, in_specs=in_specs, out_specs=out_specs, check_vma=False)
```
